16 devices in a mesh: data: 16 (over z, y, x, core).
Axes of the slice: x: 2, y: 2, z: 2, core: 2. Of those that a mesh axis runs over, the one named last changes fastest.
Arguments:
- tokens: bfloat16 [16384, 1536], P('data')
- upstream: bfloat16 [16384, 1536], P('data')
- norm_gain: bfloat16 [2, 1536], replicated
- w_up: bfloat16 [2, 1536, 6144], replicated
- bias_up: bfloat16 [2, 6144], replicated
- w_down: bfloat16 [2, 6144, 1536], replicated
- bias_down: bfloat16 [2, 1536], replicated
Outputs:
- output 1: float32 [2, 1536], replicated
- output 2: float32 [2, 1536, 6144], replicated
- output 3: float32 [2, 6144], replicated
- output 4: float32 [2, 6144, 1536], replicated
- output 5: float32 [2, 1536], replicated
All inputs are finite; a program needn't handle non-finite values.
Results may differ from the reference program's by a relative error of at most 0.0070572.
Values are sent between devices in bfloat16 or wider.
A program may use at most 1 GiB of HBM per device.

```python
import jax
import jax.numpy as jnp
from jax import lax

D = 1536
HIDDEN = 6144
LAYERS = 2
TOK_DEV = 1024
GROUP_SIZE = 16
TOKENS = GROUP_SIZE * TOK_DEV
EPSILON = 1e-6


def setup_inputs(seed: int = 0) -> dict:
    key_list = jax.random.split(jax.random.key(seed), 7)
    tokens = jax.random.normal(key_list[0], (TOKENS, D), jnp.float32)
    upstream = jax.random.normal(key_list[1], (TOKENS, D), jnp.float32) * (TOKENS ** -0.5)
    norm_gain = 1.0 + 0.5 * jax.random.normal(key_list[2], (LAYERS, D), jnp.float32)
    w_up = jax.random.normal(key_list[3], (LAYERS, D, HIDDEN), jnp.float32) * (D ** -0.5)
    bias_up = 0.5 * jax.random.normal(key_list[4], (LAYERS, HIDDEN), jnp.float32)
    w_down = jax.random.normal(key_list[5], (LAYERS, HIDDEN, D), jnp.float32) * (HIDDEN ** -0.5)
    bias_down = 0.5 * jax.random.normal(key_list[6], (LAYERS, D), jnp.float32)
    return {
        "tokens": tokens.astype(jnp.bfloat16),
        "upstream": upstream.astype(jnp.bfloat16),
        "norm_gain": norm_gain.astype(jnp.bfloat16),
        "w_up": w_up.astype(jnp.bfloat16),
        "bias_up": bias_up.astype(jnp.bfloat16),
        "w_down": w_down.astype(jnp.bfloat16),
        "bias_down": bias_down.astype(jnp.bfloat16),
    }


def gelu_tanh(values):
    return jax.nn.gelu(values, approximate=True)


def inverse_rms(hid_f):
    return lax.rsqrt(jnp.mean(hid_f * hid_f, axis=-1, keepdims=True) + EPSILON)


def shard_grads(tok_rows, up_rows, norm_gain, w_up, bias_up, w_down, bias_down):

    def forward_layer(hidden, layer_inputs):
        gain_row, up_mat, up_bias, down_mat, down_bias = layer_inputs
        hid_f = hidden.astype(jnp.float32)
        normed = (hid_f * inverse_rms(hid_f) * gain_row.astype(jnp.float32)).astype(jnp.bfloat16)
        pre_act = (jnp.dot(normed, up_mat, preferred_element_type=jnp.float32) + up_bias.astype(jnp.float32)).astype(jnp.bfloat16)
        activated = gelu_tanh(pre_act.astype(jnp.float32)).astype(jnp.bfloat16)
        branch = jnp.dot(activated, down_mat, preferred_element_type=jnp.float32)
        new_hidden = (hid_f + branch + down_bias.astype(jnp.float32)).astype(jnp.bfloat16)
        return new_hidden, (hidden, normed, pre_act, activated)

    top_hidden, saved_acts = lax.scan(forward_layer, tok_rows, (norm_gain, w_up, bias_up, w_down, bias_down))
    top_f = top_hidden.astype(jnp.float32)
    top_scale = inverse_rms(top_f)
    top_hat = top_f * top_scale
    up_f = up_rows.astype(jnp.float32)
    grad_top = top_scale * (up_f - top_hat * jnp.mean(up_f * top_hat, axis=-1, keepdims=True))

    def backward_layer(grad_h, layer_inputs):
        gain_row, up_mat, down_mat, hidden, normed, pre_act, activated = layer_inputs
        grad_b = grad_h.astype(jnp.bfloat16)
        grad_down = jnp.dot(activated.T, grad_b, preferred_element_type=jnp.float32)
        grad_down_bias = jnp.sum(grad_h, axis=0)
        grad_act = jnp.dot(grad_b, down_mat.T, preferred_element_type=jnp.float32)
        gelu_back = jax.vjp(gelu_tanh, pre_act.astype(jnp.float32))[1]
        grad_pre = gelu_back(grad_act)[0]
        grad_pre_b = grad_pre.astype(jnp.bfloat16)
        grad_up = jnp.dot(normed.T, grad_pre_b, preferred_element_type=jnp.float32)
        grad_up_bias = jnp.sum(grad_pre, axis=0)
        grad_normed = jnp.dot(grad_pre_b, up_mat.T, preferred_element_type=jnp.float32)
        hid_f = hidden.astype(jnp.float32)
        hid_scale = inverse_rms(hid_f)
        hid_hat = hid_f * hid_scale
        grad_gain = jnp.sum(grad_normed * hid_hat, axis=0)
        grad_hat = grad_normed * gain_row.astype(jnp.float32)
        grad_new = grad_h + hid_scale * (grad_hat - hid_hat * jnp.mean(grad_hat * hid_hat, axis=-1, keepdims=True))
        return grad_new, (grad_gain, grad_up, grad_up_bias, grad_down, grad_down_bias)

    saved_h, saved_n, saved_u, saved_a = saved_acts
    layer_grads = lax.scan(backward_layer, grad_top, (norm_gain, w_up, w_down, saved_h, saved_n, saved_u, saved_a), reverse=True)[1]
    return layer_grads


def reference(tokens, upstream, norm_gain, w_up, bias_up, w_down, bias_down):
    tok_shards = tokens.reshape(GROUP_SIZE, TOK_DEV, D)
    up_shards = upstream.reshape(GROUP_SIZE, TOK_DEV, D)
    zero_grads = (
        jnp.zeros((LAYERS, D), jnp.float32),
        jnp.zeros((LAYERS, D, HIDDEN), jnp.float32),
        jnp.zeros((LAYERS, HIDDEN), jnp.float32),
        jnp.zeros((LAYERS, HIDDEN, D), jnp.float32),
        jnp.zeros((LAYERS, D), jnp.float32),
    )

    def add_shard(running, shard_pair):
        shard_part = shard_grads(shard_pair[0], shard_pair[1], norm_gain, w_up, bias_up, w_down, bias_down)
        return tuple(run_sum + new_part for run_sum, new_part in zip(running, shard_part)), None

    running = lax.scan(add_shard, zero_grads, (tok_shards, up_shards))[0]
    return (running[0], running[1], running[2], running[3], running[4])
```

```python
import jax
import jax.numpy as jnp
from jax import lax
from jax.sharding import PartitionSpec as P

EPSILON = 1e-6
TOKEN_DIMS = (((0,), (0,)), ((), ()))
FEATURE_DIMS = (((1,), (1,)), ((), ()))
COLORS = 3
Z_BIT, Y_BIT, X_BIT, CORE_BIT = range(4)
COLOR_DIMS = ((X_BIT, Y_BIT, Z_BIT), (Y_BIT, Z_BIT, X_BIT), (Z_BIT, X_BIT, Y_BIT))


def gelu_tanh(values):
    return jax.nn.gelu(values, approximate=True)


def inverse_rms(hid_f):
    return lax.rsqrt(jnp.mean(hid_f * hid_f, axis=-1, keepdims=True) + EPSILON)


def forward_stack(hidden, norm_gain, w_up, bias_up, w_down, bias_down):
    saved_acts = []
    for layer_idx in range(norm_gain.shape[0]):
        hid_f = hidden.astype(jnp.float32)
        hid_scale = inverse_rms(hid_f)
        hid_hat = hid_f * hid_scale
        normed = (hid_hat * norm_gain[layer_idx].astype(jnp.float32)).astype(jnp.bfloat16)
        pre_act = (jnp.dot(normed, w_up[layer_idx], preferred_element_type=jnp.float32) + bias_up[layer_idx].astype(jnp.float32)).astype(jnp.bfloat16)
        activated = gelu_tanh(pre_act.astype(jnp.float32)).astype(jnp.bfloat16)
        branch = jnp.dot(activated, w_down[layer_idx], preferred_element_type=jnp.float32)
        hidden = (hid_f + branch + bias_down[layer_idx].astype(jnp.float32)).astype(jnp.bfloat16)
        saved_acts.append((hid_scale, hid_hat, normed, pre_act, activated))
    return hidden, saved_acts


def top_gradient(top_hidden, upstream):
    top_f = top_hidden.astype(jnp.float32)
    top_scale = inverse_rms(top_f)
    top_hat = top_f * top_scale
    up_f = upstream.astype(jnp.float32)
    return top_scale * (up_f - top_hat * jnp.mean(up_f * top_hat, axis=-1, keepdims=True))


def flip_pairs(bit):
    mask = 8 >> bit
    return [(dev, dev ^ mask) for dev in range(16)]


def pick(array, starts, sizes):
    return lax.dynamic_slice(array, starts, sizes)


def reduce_matrix(local, bits, axis):
    rows, cols = local.shape
    sub = rows // (16 * COLORS)
    view = local.reshape(2, 2, 2, 2, COLORS, sub, cols)
    zero = jnp.zeros((), jnp.int32)

    starts = [zero] * 7
    sizes = [2, 2, 2, 1, COLORS, sub, cols]
    starts[CORE_BIT] = 1 - bits[CORE_BIT]
    sent = pick(view, starts, sizes).astype(jnp.bfloat16)
    first = lax.ppermute(sent, axis, flip_pairs(CORE_BIT))

    shards = []
    for color in range(COLORS):
        received = [(first, CORE_BIT)]

        def total(starts, sizes, received=received, color=color):
            acc = pick(view, starts + [jnp.int32(color), zero, zero], sizes + [1, sub, cols])
            for part, _ in received:
                part_starts = [zero if part.shape[b] == 1 else starts[b] for b in range(4)]
                color_start = jnp.int32(color) if part.shape[4] > 1 else zero
                acc = acc + pick(part, part_starts + [color_start, zero, zero], sizes + [1, sub, cols]).astype(jnp.float32)
            return acc

        starts = [zero] * 4
        sizes = [2, 2, 2, 1]
        starts[CORE_BIT] = bits[CORE_BIT]
        for bit in COLOR_DIMS[color]:
            sizes[bit] = 1
            starts[bit] = 1 - bits[bit]
            sent = total(list(starts), list(sizes)).astype(jnp.bfloat16)
            received.append((lax.ppermute(sent, axis, flip_pairs(bit)), bit))
            starts[bit] = bits[bit]
        shards.append(total(list(starts), list(sizes)).astype(jnp.bfloat16).reshape(sub, cols))
    shard = jnp.concatenate(shards, axis=0)
    return lax.all_gather(shard, axis, tiled=True)


def layer_backward(grad_h, saved_layer, gain_row, up_mat, down_mat, need_input, reduce):
    hid_scale, hid_hat, normed, pre_act, activated = saved_layer
    grad_b = grad_h.astype(jnp.bfloat16)
    grad_down = reduce(lax.dot_general(activated, grad_b, TOKEN_DIMS, preferred_element_type=jnp.float32))
    grad_down_bias = jnp.sum(grad_h, axis=0)
    grad_act = lax.dot_general(grad_b, down_mat, FEATURE_DIMS, preferred_element_type=jnp.float32)
    gelu_back = jax.vjp(gelu_tanh, pre_act.astype(jnp.float32))[1]
    grad_pre = gelu_back(grad_act)[0]
    grad_pre_b = grad_pre.astype(jnp.bfloat16)
    grad_up = reduce(lax.dot_general(normed, grad_pre_b, TOKEN_DIMS, preferred_element_type=jnp.float32))
    grad_up_bias = jnp.sum(grad_pre, axis=0)
    grad_normed = lax.dot_general(grad_pre_b, up_mat, FEATURE_DIMS, preferred_element_type=jnp.float32)
    grad_gain = jnp.sum(grad_normed * hid_hat, axis=0)
    small = jnp.concatenate([grad_gain, grad_up_bias, grad_down_bias])
    if not need_input:
        return (small, grad_up, grad_down), None
    grad_hat = grad_normed * gain_row.astype(jnp.float32)
    grad_new = grad_h + hid_scale * (grad_hat - hid_hat * jnp.mean(grad_hat * hid_hat, axis=-1, keepdims=True))
    return (small, grad_up, grad_down), grad_new


def solution(mesh):
    axis = mesh.axis_names[0]

    def device_grads(tokens, upstream, norm_gain, w_up, bias_up, w_down, bias_down):
        me = lax.axis_index(axis)
        bits = [(me >> (3 - b)) & 1 for b in range(4)]
        num_layers, width = norm_gain.shape
        hidden_width = w_up.shape[2]
        top_hidden, saved_acts = forward_stack(tokens, norm_gain, w_up, bias_up, w_down, bias_down)
        grad_h = top_gradient(top_hidden, upstream)
        smalls, ups, downs = [None] * num_layers, [None] * num_layers, [None] * num_layers
        for layer_idx in reversed(range(num_layers)):
            (smalls[layer_idx], ups[layer_idx], downs[layer_idx]), grad_h = layer_backward(
                grad_h, saved_acts[layer_idx], norm_gain[layer_idx], w_up[layer_idx], w_down[layer_idx], layer_idx > 0,
                lambda local: reduce_matrix(local, bits, axis),
            )
        small = lax.psum(jnp.stack(smalls), axis)
        up_full = jnp.stack(ups).astype(jnp.float32)
        down_full = jnp.stack(downs).astype(jnp.float32)
        return (small[:, :width], up_full, small[:, width:width + hidden_width], down_full, small[:, width + hidden_width:])

    row_spec = P(axis, None)
    full_spec = P()
    return jax.shard_map(
        device_grads,
        mesh=mesh,
        in_specs=(row_spec, row_spec, full_spec, full_spec, full_spec, full_spec, full_spec),
        out_specs=(full_spec, full_spec, full_spec, full_spec, full_spec),
        check_vma=False,
    )
```

```python
import functools

import jax
import jax.numpy as jnp
from jax import lax
from jax.experimental import pallas as pl
from jax.experimental.pallas import tpu as pltpu
from jax.sharding import PartitionSpec as P

EPSILON = 1e-6
TOKEN_DIMS = (((0,), (0,)), ((), ()))
FEATURE_DIMS = (((1,), (1,)), ((), ()))
MESH = pl.DeviceIdType.MESH
COLORS = 3
CORE, DIM_X, DIM_Y, DIM_Z = range(4)
COLOR_DIMS = ((DIM_X, DIM_Y, DIM_Z), (DIM_Y, DIM_Z, DIM_X), (DIM_Z, DIM_X, DIM_Y))
PIPELINE = (
    ("load", 0), ("compute_sent", 0), ("compute_kept", 0), ("send_2", 1), ("send_back_3", 2), ("send_back_core", 4),
    ("send_1", 0), ("send_back_1", 3), ("send_3", 1), ("send_back_2", 2), ("store", 4),
)
MAX_LAG = 4
RECV_SLOTS = 3
KEPT_SLOTS = 3
GATHER_SLOTS = 6


def gelu_tanh(values):
    return jax.nn.gelu(values, approximate=True)


def inverse_rms(hid_f):
    return lax.rsqrt(jnp.mean(hid_f * hid_f, axis=-1, keepdims=True) + EPSILON)


def forward_stack(hidden, norm_gain, w_up, bias_up, w_down, bias_down):
    saved_acts = []
    for layer_idx in range(norm_gain.shape[0]):
        hid_f = hidden.astype(jnp.float32)
        hid_scale = inverse_rms(hid_f)
        hid_hat = hid_f * hid_scale
        normed = (hid_hat * norm_gain[layer_idx].astype(jnp.float32)).astype(jnp.bfloat16)
        pre_act = (jnp.dot(normed, w_up[layer_idx], preferred_element_type=jnp.float32) + bias_up[layer_idx].astype(jnp.float32)).astype(jnp.bfloat16)
        activated = gelu_tanh(pre_act.astype(jnp.float32)).astype(jnp.bfloat16)
        branch = jnp.dot(activated, w_down[layer_idx], preferred_element_type=jnp.float32)
        hidden = (hid_f + branch + bias_down[layer_idx].astype(jnp.float32)).astype(jnp.bfloat16)
        saved_acts.append((hid_scale, hid_hat, normed, pre_act, activated))
    return hidden, saved_acts


def top_gradient(top_hidden, upstream):
    top_f = top_hidden.astype(jnp.float32)
    top_scale = inverse_rms(top_f)
    top_hat = top_f * top_scale
    up_f = upstream.astype(jnp.float32)
    return top_scale * (up_f - top_hat * jnp.mean(up_f * top_hat, axis=-1, keepdims=True))


def layer_backward(grad_h, saved_layer, gain_row, up_mat, down_mat, need_input):
    hid_scale, hid_hat, normed, pre_act, activated = saved_layer
    grad_b = grad_h.astype(jnp.bfloat16)
    grad_down_bias = jnp.sum(grad_h, axis=0)
    grad_act = lax.dot_general(grad_b, down_mat, FEATURE_DIMS, preferred_element_type=jnp.float32)
    gelu_back = jax.vjp(gelu_tanh, pre_act.astype(jnp.float32))[1]
    grad_pre = gelu_back(grad_act)[0]
    grad_pre_b = grad_pre.astype(jnp.bfloat16)
    grad_up_bias = jnp.sum(grad_pre, axis=0)
    grad_normed = lax.dot_general(grad_pre_b, up_mat, FEATURE_DIMS, preferred_element_type=jnp.float32)
    grad_gain = jnp.sum(grad_normed * hid_hat, axis=0)
    small = jnp.concatenate([grad_gain, grad_up_bias, grad_down_bias])
    operands = ((activated, grad_b), (normed, grad_pre_b))
    if not need_input:
        return small, operands, None
    grad_hat = grad_normed * gain_row.astype(jnp.float32)
    grad_new = grad_h + hid_scale * (grad_hat - hid_hat * jnp.mean(grad_hat * hid_hat, axis=-1, keepdims=True))
    return small, operands, grad_new


def exchange_kernel(sizes, *refs):
    num_mats, chunks_per_mat, row_dim, chunk_cols, region, down_subs, axis = sizes
    mats = [(refs[2 * m], refs[2 * m + 1]) for m in range(num_mats)]
    refs = refs[2 * num_mats:]
    small_in, gathered, small_out = refs[:3]
    (rows_buf, cols_buf, sent_core, kept, recv_core, sent_1, sent_2, sent_3, recv_1, recv_2, recv_3, ring,
     small_recv, load_sem, core_send, core_recv, out_send, out_recv, back_send, back_recv, share_send, share_recv,
     store_sem, small_send_sem, small_recv_sem) = refs[3:]
    num_chunks = num_mats * chunks_per_mat
    half = COLORS * region
    me = lax.axis_index(axis)
    bits = [me % 2, (me // 2) % 2, (me // 4) % 2, me // 8]
    partners = [me + (1 << d) - 2 * (1 << d) * bits[d] for d in range(4)]
    core = bits[CORE]
    sent_bufs, recv_bufs = (sent_1, sent_2, sent_3), (recv_1, recv_2, recv_3)
    spans = (region // 2, region // 4, region // 8)

    def base(color, level):
        total = 0
        for step in range(level):
            total = total + bits[COLOR_DIMS[color][step]] * spans[step]
        return total

    def other(color, level):
        return base(color, level) + (1 - bits[COLOR_DIMS[color][level]]) * spans[level]

    def rows_at(start, size):
        return pl.ds(pl.multiple_of(start, spans[2]), size)

    def load_copies(mat, chunk):
        slot = chunk % 2
        sub = chunk % chunks_per_mat
        rows_ref, cols_ref = mats[mat]
        if mat % 2 == 0:
            row_start = pl.multiple_of((sub // down_subs) * row_dim, 128)
            col_start = pl.multiple_of((sub % down_subs) * chunk_cols, 128)
            rows_src = rows_ref.at[:, pl.ds(row_start, row_dim)]
            cols_src = cols_ref.at[:, pl.ds(col_start, chunk_cols)]
        else:
            rows_src = rows_ref
            cols_src = cols_ref.at[:, pl.ds(pl.multiple_of(sub * chunk_cols, 128), chunk_cols)]
        return (
            pltpu.make_async_copy(rows_src, rows_buf.at[slot], load_sem.at[0, slot]),
            pltpu.make_async_copy(cols_src, cols_buf.at[slot], load_sem.at[1, slot]),
        )

    def start_loads(chunk):
        for mat in range(num_mats):
            @pl.when(chunk // chunks_per_mat == mat)
            def _():
                for copy in load_copies(mat, chunk):
                    copy.start()

    def core_copy(chunk):
        slot = chunk % RECV_SLOTS
        return pltpu.make_async_remote_copy(
            src_ref=sent_core, dst_ref=recv_core.at[slot], send_sem=core_send, recv_sem=core_recv.at[slot],
            device_id=(partners[CORE],), device_id_type=MESH)

    def out_copy(level, color, chunk):
        slot = chunk % RECV_SLOTS
        return pltpu.make_async_remote_copy(
            src_ref=sent_bufs[level].at[color], dst_ref=recv_bufs[level].at[slot, color],
            send_sem=out_send.at[level, color], recv_sem=out_recv.at[level, color, slot],
            device_id=(partners[COLOR_DIMS[color][level]],), device_id_type=MESH)

    def back_copy(level, color, chunk, arriving):
        slot = chunk % GATHER_SLOTS
        mine = ring.at[slot, core, color, rows_at(base(color, level + 1), spans[level]), :]
        theirs = ring.at[slot, core, color, rows_at(other(color, level), spans[level]), :]
        return pltpu.make_async_remote_copy(
            src_ref=mine, dst_ref=theirs if arriving else mine,
            send_sem=back_send.at[level, color, slot], recv_sem=back_recv.at[level, color, slot],
            device_id=(partners[COLOR_DIMS[color][level]],), device_id_type=MESH)

    def share_copy(chunk, arriving):
        slot = chunk % GATHER_SLOTS
        return pltpu.make_async_remote_copy(
            src_ref=ring.at[slot, core], dst_ref=ring.at[slot, 1 - core if arriving else core],
            send_sem=share_send.at[slot], recv_sem=share_recv.at[slot],
            device_id=(partners[CORE],), device_id_type=MESH)

    def store_copy(chunk):
        slot = chunk % GATHER_SLOTS
        return pltpu.make_async_copy(ring.at[slot], gathered.at[chunk], store_sem.at[slot])

    def small_copy(step):
        return pltpu.make_async_remote_copy(
            src_ref=small_out, dst_ref=small_recv.at[step], send_sem=small_send_sem.at[step],
            recv_sem=small_recv_sem.at[step], device_id=(partners[step],), device_id_type=MESH)

    def product(chunk, which_core, color):
        slot = chunk % 2
        start = pl.multiple_of(which_core * half + color * region, 128)
        return lax.dot_general(
            rows_buf[slot, :, pl.ds(start, region)], cols_buf[slot], TOKEN_DIMS, preferred_element_type=jnp.float32)

    def load(chunk):
        for copy in load_copies(1, chunk):
            copy.wait()

        @pl.when(chunk + 1 < num_chunks)
        def _():
            start_loads(chunk + 1)

    def compute_sent(chunk):
        @pl.loop(0, COLORS)
        def _(color):
            sent_core[color] = product(chunk, 1 - core, color).astype(jnp.bfloat16)
        core_copy(chunk).start()

    def compute_kept(chunk):
        slot = chunk % KEPT_SLOTS

        @pl.loop(0, COLORS)
        def _(color):
            kept[slot, color] = product(chunk, core, color)

    def halve(level, chunk, arrived):
        slot = chunk % KEPT_SLOTS
        recv_slot = chunk % RECV_SLOTS
        for color in range(COLORS):
            if level > 0:
                out_copy(level - 1, color, chunk).wait()
            held = base(color, level)

            def total(start, size, color=color, held=held):
                own = kept[slot, color, rows_at(start, size), :]
                return own + arrived[recv_slot, color, rows_at(start - held, size), :].astype(jnp.float32)

            if level < 3:
                mine = base(color, level + 1)
                sent_bufs[level][color] = total(other(color, level), spans[level]).astype(jnp.bfloat16)
                kept[slot, color, rows_at(mine, spans[level]), :] = total(mine, spans[level])
                out_copy(level, color, chunk).start()
            else:
                gather_slot = chunk % GATHER_SLOTS
                ring[gather_slot, core, color, rows_at(held, spans[2]), :] = total(held, spans[2]).astype(jnp.bfloat16)
                back_copy(2, color, chunk, False).start()

    def send_1(chunk):
        core_copy(chunk).wait()
        halve(0, chunk, recv_core)

    def send_2(chunk):
        halve(1, chunk, recv_1)

    def send_3(chunk):
        halve(2, chunk, recv_2)

    def send_back_3(chunk):
        halve(3, chunk, recv_3)

    def pass_back(level, chunk):
        for color in range(COLORS):
            back_copy(level + 1, color, chunk, True).wait()
            back_copy(level, color, chunk, False).start()

    def send_back_2(chunk):
        pass_back(1, chunk)

    def send_back_1(chunk):
        pass_back(0, chunk)

    def send_back_core(chunk):
        for color in range(COLORS):
            back_copy(0, color, chunk, True).wait()
        share_copy(chunk, False).start()

    def store(chunk):
        share_copy(chunk, True).wait()
        store_copy(chunk).start()

        @pl.when(chunk > 0)
        def _():
            store_copy(chunk - 1).wait()

    events = dict(
        load=load, compute_sent=compute_sent, compute_kept=compute_kept, send_1=send_1, send_2=send_2, send_3=send_3,
        send_back_3=send_back_3, send_back_2=send_back_2, send_back_1=send_back_1, send_back_core=send_back_core, store=store)

    start_loads(jnp.int32(0))
    barrier = pltpu.get_barrier_semaphore()
    for partner in partners:
        pl.semaphore_signal(barrier, inc=1, device_id=(partner,), device_id_type=MESH)
    small_out[...] = small_in[...]
    pl.semaphore_wait(barrier, 4)

    @pl.loop(0, num_chunks + MAX_LAG)
    def _(it):
        for name, lag in PIPELINE:
            chunk = it - lag

            @pl.when((chunk >= 0) & (chunk < num_chunks))
            def _(name=name, chunk=chunk):
                events[name](chunk)
        for step in range(4):
            @pl.when(it == 2 * step + 1)
            def _(step=step):
                small_copy(step).start()

            @pl.when(it == 2 * step + 2)
            def _(step=step):
                small_copy(step).wait()
                small_out[...] += small_recv[step]

    store_copy(jnp.int32(num_chunks - 1)).wait()


def exchange(mat_operands, small, axis, chunk_cols):
    tokens, row_dim = mat_operands[1][0].shape
    hidden = mat_operands[0][0].shape[1]
    num_mats = len(mat_operands)
    chunks_per_mat = hidden // chunk_cols
    region = row_dim // (2 * COLORS)
    half = (COLORS, region, chunk_cols)
    sizes = (num_mats, chunks_per_mat, row_dim, chunk_cols, region, row_dim // chunk_cols, axis)
    num_chunks = num_mats * chunks_per_mat
    small_rows = small.shape[0] // 128
    bf16, f32 = jnp.bfloat16, jnp.float32
    dma = pltpu.SemaphoreType.DMA
    any_spec = pl.BlockSpec(memory_space=pl.ANY)
    vmem_spec = pl.BlockSpec(memory_space=pltpu.VMEM)
    gathered, small_sum = pl.pallas_call(
        functools.partial(exchange_kernel, sizes),
        out_shape=(
            jax.ShapeDtypeStruct((num_chunks, 2) + half, bf16),
            jax.ShapeDtypeStruct((small_rows, 128), f32),
        ),
        in_specs=[any_spec] * (2 * num_mats) + [vmem_spec],
        out_specs=(any_spec, vmem_spec),
        scratch_shapes=[
            pltpu.VMEM((2, tokens, row_dim), bf16),
            pltpu.VMEM((2, tokens, chunk_cols), bf16),
            pltpu.VMEM(half, bf16),
            pltpu.VMEM((KEPT_SLOTS,) + half, f32),
            pltpu.VMEM((RECV_SLOTS,) + half, bf16),
            pltpu.VMEM((COLORS, region // 2, chunk_cols), bf16),
            pltpu.VMEM((COLORS, region // 4, chunk_cols), bf16),
            pltpu.VMEM((COLORS, region // 8, chunk_cols), bf16),
            pltpu.VMEM((RECV_SLOTS, COLORS, region // 2, chunk_cols), bf16),
            pltpu.VMEM((RECV_SLOTS, COLORS, region // 4, chunk_cols), bf16),
            pltpu.VMEM((RECV_SLOTS, COLORS, region // 8, chunk_cols), bf16),
            pltpu.VMEM((GATHER_SLOTS, 2) + half, bf16),
            pltpu.VMEM((4, small_rows, 128), f32),
            dma((2, 2)), dma, dma((RECV_SLOTS,)), dma((3, COLORS)), dma((3, COLORS, RECV_SLOTS)),
            dma((3, COLORS, GATHER_SLOTS)), dma((3, COLORS, GATHER_SLOTS)), dma((GATHER_SLOTS,)), dma((GATHER_SLOTS,)),
            dma((GATHER_SLOTS,)), dma((4,)), dma((4,)),
        ],
        compiler_params=pltpu.CompilerParams(collective_id=0, has_side_effects=True, vmem_limit_bytes=60 * 2**20),
        name="exchange",
    )(*[operand for pair in mat_operands for operand in pair], small.reshape(small_rows, 128))
    return gathered, small_sum.reshape(-1)


def widen_kernel(chunk_ref, out_ref):
    out_ref[0] = chunk_ref[0].astype(jnp.float32)


def widen(gathered, num_layers, row_dim, hidden, chunk_cols):
    per_mat = hidden // chunk_cols
    num_mats = 2 * num_layers
    down_subs = row_dim // chunk_cols
    chunks = gathered.reshape(num_mats * per_mat, row_dim, chunk_cols)

    def mat_of(layer, kind):
        return (num_layers - 1 - layer) * 2 + kind

    block = (1, row_dim, chunk_cols)
    up = pl.pallas_call(
        widen_kernel,
        grid=(num_layers, per_mat),
        in_specs=[pl.BlockSpec(block, lambda layer, sub: (mat_of(layer, 1) * per_mat + sub, 0, 0))],
        out_specs=pl.BlockSpec(block, lambda layer, sub: (layer, 0, sub)),
        out_shape=jax.ShapeDtypeStruct((num_layers, row_dim, hidden), jnp.float32),
        name="widen_up",
    )(chunks)
    down = pl.pallas_call(
        widen_kernel,
        grid=(num_layers, per_mat),
        in_specs=[pl.BlockSpec(block, lambda layer, sub: (mat_of(layer, 0) * per_mat + sub, 0, 0))],
        out_specs=pl.BlockSpec(block, lambda layer, sub: (layer, sub // down_subs, sub % down_subs)),
        out_shape=jax.ShapeDtypeStruct((num_layers, hidden, row_dim), jnp.float32),
        name="widen_down",
    )(chunks)
    return up, down


def solution(mesh):
    axis = mesh.axis_names[0]

    def device_grads(tokens, upstream, norm_gain, w_up, bias_up, w_down, bias_down):
        num_layers, width = norm_gain.shape
        hidden_width = w_up.shape[2]
        chunk_cols = width // 2
        top_hidden, saved_acts = forward_stack(tokens, norm_gain, w_up, bias_up, w_down, bias_down)
        grad_h = top_gradient(top_hidden, upstream)
        smalls, mat_operands = [None] * num_layers, []
        for layer_idx in reversed(range(num_layers)):
            smalls[layer_idx], operands, grad_h = layer_backward(
                grad_h, saved_acts[layer_idx], norm_gain[layer_idx], w_up[layer_idx], w_down[layer_idx], layer_idx > 0)
            mat_operands.extend(operands)
        gathered, small = exchange(mat_operands, jnp.concatenate(smalls), axis, chunk_cols)
        up_full, down_full = widen(gathered, num_layers, width, hidden_width, chunk_cols)
        small = small.reshape(num_layers, -1)
        return (small[:, :width], up_full, small[:, width:width + hidden_width], down_full, small[:, width + hidden_width:])

    row_spec = P(axis, None)
    full_spec = P()
    return jax.shard_map(
        device_grads,
        mesh=mesh,
        in_specs=(row_spec, row_spec, full_spec, full_spec, full_spec, full_spec, full_spec),
        out_specs=(full_spec, full_spec, full_spec, full_spec, full_spec),
        check_vma=False,
    )
```

```python
import functools

import jax
import jax.numpy as jnp
from jax import lax
from jax.experimental import pallas as pl
from jax.experimental.pallas import tpu as pltpu
from jax.sharding import PartitionSpec as P

EPSILON = 1e-6
TOKEN_DIMS = (((0,), (0,)), ((), ()))
FEATURE_DIMS = (((1,), (1,)), ((), ()))
MESH = pl.DeviceIdType.MESH
COLORS = 3
CORE, DIM_X, DIM_Y, DIM_Z = range(4)
COLOR_DIMS = ((DIM_X, DIM_Y, DIM_Z), (DIM_Y, DIM_Z, DIM_X), (DIM_Z, DIM_X, DIM_Y))
PIPELINE = (
    ("load", 0), ("compute_sent", 0), ("compute_kept", 0), ("send_2", 1), ("backward_0", 0), ("send_back_3", 2), ("send_1", 0),
    ("send_back_1", 4), ("send_back_core", 5), ("backward_1", 0), ("backward_2", 0), ("input_grad", 0), ("load_cols", 0),
    ("send_3", 1), ("send_back_2", 2), ("store", 5),
)
MAX_LAG = 5
RECV_SLOTS = 2
KEPT_SLOTS = 3
GATHER_SLOTS = 6
TILE = 256
NORM_ROWS = 128
GELU_SCALE = 0.7978845608028654
GELU_CUBIC = 0.044715


def gelu_tanh(values):
    return jax.nn.gelu(values, approximate=True)


def inverse_rms(hid_f):
    return lax.rsqrt(jnp.mean(hid_f * hid_f, axis=-1, keepdims=True) + EPSILON)


def forward_stack(hidden, norm_gain, w_up, bias_up, w_down, bias_down):
    saved_acts = []
    for layer_idx in range(norm_gain.shape[0]):
        hid_f = hidden.astype(jnp.float32)
        hid_scale = inverse_rms(hid_f)
        hid_hat = hid_f * hid_scale
        normed = (hid_hat * norm_gain[layer_idx].astype(jnp.float32)).astype(jnp.bfloat16)
        pre_act = (jnp.dot(normed, w_up[layer_idx], preferred_element_type=jnp.float32) + bias_up[layer_idx].astype(jnp.float32)).astype(jnp.bfloat16)
        activated = gelu_tanh(pre_act.astype(jnp.float32)).astype(jnp.bfloat16)
        branch = jnp.dot(activated, w_down[layer_idx], preferred_element_type=jnp.float32)
        saved_acts.append((hidden, normed, pre_act, activated))
        hidden = (hid_f + branch + bias_down[layer_idx].astype(jnp.float32)).astype(jnp.bfloat16)
    return hidden, saved_acts


def top_gradient(top_hidden, upstream):
    top_f = top_hidden.astype(jnp.float32)
    top_scale = inverse_rms(top_f)
    top_hat = top_f * top_scale
    up_f = upstream.astype(jnp.float32)
    return top_scale * (up_f - top_hat * jnp.mean(up_f * top_hat, axis=-1, keepdims=True))


def gelu_slope(values):
    square = values * values
    bend = jnp.tanh(values * (GELU_SCALE + GELU_SCALE * GELU_CUBIC * square))
    return 0.5 * (1.0 + bend) + (0.5 * values) * (1.0 - bend * bend) * (GELU_SCALE + 3.0 * GELU_SCALE * GELU_CUBIC * square)


def backward_kernel(sizes, *refs):
    num_layers, chunks_per_mat, row_dim, chunk_cols, region, down_subs, axis = sizes
    num_mats = 2 * num_layers
    hidden_dim = chunks_per_mat * chunk_cols
    layer_refs = [refs[4 * n:4 * n + 4] for n in range(num_layers)]
    refs = refs[4 * num_layers:]
    grad_top, grad_top_b, w_up, w_down, gain_in, small_in, gathered, small_out, grad_pre_hbm, grad_b_hbm = refs[:10]
    (rows_buf, cols_buf, sent_core, kept, recv_core, sent_1, sent_2, sent_3, recv_1, recv_2, recv_3, ring,
     weight_buf, pre_buf, grad_pre_buf, grad_b, grad_normed, hid_buf, grad_buf,
     small_recv, load_sem, grad_pre_sem, norm_sem, grad_b_sem, core_send, core_recv, out_send, out_recv, back_send, back_recv,
     share_send, share_recv, store_sem, small_send_sem, small_recv_sem) = refs[10:]
    small_width = 2 * row_dim + hidden_dim
    num_chunks = num_mats * chunks_per_mat
    half = COLORS * region
    me = lax.axis_index(axis)
    bits = [me % 2, (me // 2) % 2, (me // 4) % 2, me // 8]
    partners = [me + (1 << d) - 2 * (1 << d) * bits[d] for d in range(4)]
    core = bits[CORE]
    sent_bufs, recv_bufs = (sent_1, sent_2, sent_3), (recv_1, recv_2, recv_3)
    spans = (region // 2, region // 4, region // 8)

    def base(color, level):
        total = 0
        for step in range(level):
            total = total + bits[COLOR_DIMS[color][step]] * spans[step]
        return total

    def other(color, level):
        return base(color, level) + (1 - bits[COLOR_DIMS[color][level]]) * spans[level]

    def rows_at(start, size):
        return pl.ds(pl.multiple_of(start, spans[2]), size)

    def mat_loads(mat, chunk):
        slot = chunk % 2
        sub = chunk % chunks_per_mat
        layer = num_layers - 1 - mat // 2
        _, normed, pre_act, activated = layer_refs[layer]
        cols = pl.ds(pl.multiple_of(sub * chunk_cols, 128), chunk_cols)
        if mat % 2 == 0:
            rows = pl.ds(pl.multiple_of((sub // down_subs) * row_dim, 128), row_dim)
            return [
                pltpu.make_async_copy(activated.at[:, rows], rows_buf.at[slot], load_sem.at[0, slot]),
                pltpu.make_async_copy(w_down.at[layer, cols, :], weight_buf.at[slot], load_sem.at[1, slot]),
                pltpu.make_async_copy(pre_act.at[:, cols], pre_buf.at[slot], load_sem.at[2, slot]),
            ]
        copies = [pltpu.make_async_copy(normed, rows_buf.at[slot], load_sem.at[0, slot])]
        for part in range(down_subs):
            copies.append(pltpu.make_async_copy(
                w_up.at[layer, part * chunk_cols:(part + 1) * chunk_cols, cols],
                weight_buf.at[slot, :, part * chunk_cols:(part + 1) * chunk_cols], load_sem.at[1 + part, slot]))
        return copies

    def cols_load(mat, chunk):
        sub = chunk % chunks_per_mat
        if mat % 2 == 0:
            source = grad_top_b if mat == 0 else grad_b_hbm
            source = source.at[:, pl.ds(pl.multiple_of((sub % down_subs) * chunk_cols, 128), chunk_cols)]
        else:
            source = grad_pre_hbm.at[sub]
        return pltpu.make_async_copy(source, cols_buf.at[chunk % 2], load_sem.at[3, chunk % 2])

    def for_mat(chunk, action):
        for mat in range(num_mats):
            @pl.when(chunk // chunks_per_mat == mat)
            def _(mat=mat):
                action(mat)

    def start_loads(chunk):
        def start(mat):
            for copy in mat_loads(mat, chunk):
                copy.start()
        for_mat(chunk, start)

    def grad_pre_store(sub):
        return pltpu.make_async_copy(grad_pre_buf, grad_pre_hbm.at[sub], grad_pre_sem)

    def core_copy(chunk):
        slot = chunk % RECV_SLOTS
        return pltpu.make_async_remote_copy(
            src_ref=sent_core, dst_ref=recv_core.at[slot], send_sem=core_send, recv_sem=core_recv.at[slot],
            device_id=(partners[CORE],), device_id_type=MESH)

    def out_copy(level, color, chunk):
        slot = chunk % RECV_SLOTS
        return pltpu.make_async_remote_copy(
            src_ref=sent_bufs[level].at[color], dst_ref=recv_bufs[level].at[slot, color],
            send_sem=out_send.at[level, color], recv_sem=out_recv.at[level, color, slot],
            device_id=(partners[COLOR_DIMS[color][level]],), device_id_type=MESH)

    def back_copy(level, color, chunk, arriving):
        slot = chunk % GATHER_SLOTS
        mine = ring.at[slot, core, color, rows_at(base(color, level + 1), spans[level]), :]
        theirs = ring.at[slot, core, color, rows_at(other(color, level), spans[level]), :]
        return pltpu.make_async_remote_copy(
            src_ref=mine, dst_ref=theirs if arriving else mine,
            send_sem=back_send.at[level, color, slot], recv_sem=back_recv.at[level, color, slot],
            device_id=(partners[COLOR_DIMS[color][level]],), device_id_type=MESH)

    def share_copy(chunk, arriving):
        slot = chunk % GATHER_SLOTS
        return pltpu.make_async_remote_copy(
            src_ref=ring.at[slot, core], dst_ref=ring.at[slot, 1 - core if arriving else core],
            send_sem=share_send.at[slot], recv_sem=share_recv.at[slot],
            device_id=(partners[CORE],), device_id_type=MESH)

    def store_copy(chunk):
        slot = chunk % GATHER_SLOTS
        return pltpu.make_async_copy(ring.at[slot], gathered.at[chunk], store_sem.at[slot])

    def small_copy(step):
        return pltpu.make_async_remote_copy(
            src_ref=small_out, dst_ref=small_recv.at[step], send_sem=small_send_sem.at[step],
            recv_sem=small_recv_sem.at[step], device_id=(partners[step],), device_id_type=MESH)

    def product(chunk, which_core, color):
        slot = chunk % 2
        start = pl.multiple_of(which_core * half + color * region, 128)
        return lax.dot_general(
            rows_buf[slot, :, pl.ds(start, region)], cols_buf[slot], TOKEN_DIMS, preferred_element_type=jnp.float32)

    def load(chunk):
        def arrive(mat):
            for copy in mat_loads(mat, chunk):
                copy.wait()
        for_mat(chunk, arrive)
        for_mat(chunk, lambda mat: cols_load(mat, chunk).wait())

        @pl.when(chunk + 1 < num_chunks)
        def _():
            start_loads(chunk + 1)

        before = chunk - 1

        @pl.when((before >= 0) & ((before // chunks_per_mat) % 2 == 0))
        def _():
            grad_pre_store(before % chunks_per_mat).wait()

    def load_cols(chunk):
        @pl.when(chunk + 1 < num_chunks)
        def _():
            for_mat(chunk + 1, lambda mat: cols_load(mat, chunk + 1).start())

    def compute_sent(chunk):
        @pl.loop(0, COLORS)
        def _(color):
            sent_core[color] = product(chunk, 1 - core, color).astype(jnp.bfloat16)
        core_copy(chunk).start()

    def compute_kept(chunk):
        slot = chunk % KEPT_SLOTS

        @pl.loop(0, COLORS)
        def _(color):
            kept[slot, color] = product(chunk, core, color)

    def halve(level, chunk, arrived):
        slot = chunk % KEPT_SLOTS
        recv_slot = chunk % RECV_SLOTS
        for color in range(COLORS):
            if level > 0:
                out_copy(level - 1, color, chunk).wait()
            held = base(color, level)

            def total(start, size, color=color, held=held):
                own = kept[slot, color, rows_at(start, size), :]
                return own + arrived[recv_slot, color, rows_at(start - held, size), :].astype(jnp.float32)

            if level < 3:
                mine = base(color, level + 1)
                sent_bufs[level][color] = total(other(color, level), spans[level]).astype(jnp.bfloat16)
                kept[slot, color, rows_at(mine, spans[level]), :] = total(mine, spans[level])
                out_copy(level, color, chunk).start()
            else:
                gather_slot = chunk % GATHER_SLOTS
                ring[gather_slot, core, color, rows_at(held, spans[2]), :] = total(held, spans[2]).astype(jnp.bfloat16)
                back_copy(2, color, chunk, False).start()

    def send_1(chunk):
        core_copy(chunk).wait()
        halve(0, chunk, recv_core)

    def send_2(chunk):
        halve(1, chunk, recv_1)

    def send_3(chunk):
        halve(2, chunk, recv_2)

    def send_back_3(chunk):
        halve(3, chunk, recv_3)

    def pass_back(level, chunk):
        for color in range(COLORS):
            back_copy(level + 1, color, chunk, True).wait()
            back_copy(level, color, chunk, False).start()

    def send_back_2(chunk):
        pass_back(1, chunk)

    def send_back_1(chunk):
        pass_back(0, chunk)

    def send_back_core(chunk):
        for color in range(COLORS):
            back_copy(0, color, chunk, True).wait()
        share_copy(chunk, False).start()

    def store(chunk):
        share_copy(chunk, True).wait()
        store_copy(chunk).start()

        @pl.when(chunk > 0)
        def _():
            store_copy(chunk - 1).wait()

    token_half = grad_b.shape[0] // 2

    def backward(part, chunk):
        slot = chunk % 2
        sub = chunk % chunks_per_mat
        mat = chunk // chunks_per_mat
        layer = num_layers - 1 - mat // 2

        @pl.when(mat % 2 == 0)
        def _():
            cols = slice(part * TILE, (part + 1) * TILE)

            @pl.loop(0, 2)
            def _(which):
                rows = pl.ds(pl.multiple_of(which * token_half, 128), token_half)
                grad_act = lax.dot_general(
                    grad_b[rows, :], weight_buf[slot, cols, :], FEATURE_DIMS, preferred_element_type=jnp.float32)
                grad_pre = grad_act * gelu_slope(pre_buf[slot, rows, cols].astype(jnp.float32))
                grad_pre_buf[rows, cols] = grad_pre.astype(jnp.bfloat16)
                start = layer * small_width + row_dim + sub * chunk_cols + part * TILE
                small_out[:, pl.ds(pl.multiple_of(start, 128), TILE)] += jnp.sum(grad_pre, axis=0, keepdims=True)

            if part == chunk_cols // TILE - 1:
                grad_pre_store(sub).start()

        @pl.when(mat % 2 == 1)
        def _():
            @pl.loop(0, 2 * down_subs)
            def _(step):
                rows = pl.ds(pl.multiple_of((step % 2) * token_half, 128), token_half)
                piece = part * down_subs + step // 2
                tiles = chunk_cols // TILE
                weight_rows = pl.ds(pl.multiple_of((piece % tiles) * TILE, TILE), TILE)
                weight_cols = pl.ds(pl.multiple_of((piece // tiles) * chunk_cols, 128), chunk_cols)
                out_cols = pl.ds(pl.multiple_of(piece * TILE, 128), TILE)
                grad_normed[rows, out_cols] += lax.dot_general(
                    cols_buf[slot, rows, :], weight_buf[slot, weight_rows, weight_cols], FEATURE_DIMS,
                    preferred_element_type=jnp.float32)

    def norm_loads(layer, block):
        rows = pl.ds(pl.multiple_of(block * NORM_ROWS, NORM_ROWS), NORM_ROWS)
        slot = block % 2
        copies = [pltpu.make_async_copy(layer_refs[layer][0].at[rows, :], hid_buf.at[slot], norm_sem.at[0, slot])]
        if layer > 0:
            copies.append(pltpu.make_async_copy(grad_top.at[rows, :], grad_buf.at[slot], norm_sem.at[1, slot]))
        return copies

    def layer_input_grad(layer):
        num_blocks = grad_b.shape[0] // NORM_ROWS
        offset = layer * small_width
        for copy in norm_loads(layer, 0):
            copy.start()

        @pl.loop(0, num_blocks)
        def _(block):
            @pl.when(block + 1 < num_blocks)
            def _():
                for copy in norm_loads(layer, block + 1):
                    copy.start()
            for copy in norm_loads(layer, block):
                copy.wait()
            rows = pl.ds(pl.multiple_of(block * NORM_ROWS, NORM_ROWS), NORM_ROWS)
            hid_f = hid_buf[block % 2].astype(jnp.float32)
            hid_scale = inverse_rms(hid_f)
            hid_hat = hid_f * hid_scale
            normed_grad = grad_normed[rows, :]
            small_out[:, offset:offset + row_dim] += jnp.sum(normed_grad * hid_hat, axis=0, keepdims=True)
            if layer > 0:
                grad_normed[rows, :] = jnp.zeros((NORM_ROWS, row_dim), jnp.float32)
                grad_hat = normed_grad * gain_in[layer:layer + 1, :]
                grad_new = grad_buf[block % 2] + hid_scale * (
                    grad_hat - hid_hat * jnp.mean(grad_hat * hid_hat, axis=-1, keepdims=True))
                grad_b[rows, :] = grad_new.astype(jnp.bfloat16)
                bias_start = offset - row_dim
                small_out[:, bias_start:bias_start + row_dim] += jnp.sum(grad_new, axis=0, keepdims=True)
        if layer > 0:
            copy = pltpu.make_async_copy(grad_b, grad_b_hbm, grad_b_sem)
            copy.start()
            copy.wait()

    def input_grad(chunk):
        for layer in range(num_layers):
            last = (num_layers - 1 - layer) * 2 * chunks_per_mat + 2 * chunks_per_mat - 1

            @pl.when(chunk == last)
            def _(layer=layer):
                layer_input_grad(layer)

    events = dict(
        load=load, compute_sent=compute_sent, compute_kept=compute_kept, send_1=send_1, send_2=send_2, send_3=send_3,
        send_back_3=send_back_3, send_back_2=send_back_2, send_back_1=send_back_1, send_back_core=send_back_core, store=store,
        backward_0=functools.partial(backward, 0), backward_1=functools.partial(backward, 1),
        backward_2=functools.partial(backward, 2), input_grad=input_grad, load_cols=load_cols)

    first = jnp.int32(0)
    for copy in mat_loads(0, first):
        copy.start()
    cols_load(0, first).start()
    grad_b_copy = pltpu.make_async_copy(grad_top_b, grad_b, grad_b_sem)
    grad_b_copy.start()
    barrier = pltpu.get_barrier_semaphore()
    for partner in partners:
        pl.semaphore_signal(barrier, inc=1, device_id=(partner,), device_id_type=MESH)
    small_out[...] = small_in[...]
    grad_normed[...] = jnp.zeros_like(grad_normed)
    grad_b_copy.wait()
    pl.semaphore_wait(barrier, 4)

    @pl.loop(0, num_chunks + MAX_LAG)
    def _(it):
        for step in range(4):
            @pl.when(it == num_chunks + step)
            def _(step=step):
                small_copy(step).start()
        for name, lag in PIPELINE:
            chunk = it - lag

            @pl.when((chunk >= 0) & (chunk < num_chunks))
            def _(name=name, chunk=chunk):
                events[name](chunk)
        for step in range(4):
            @pl.when(it == num_chunks + step)
            def _(step=step):
                small_copy(step).wait()
                small_out[...] += small_recv[step]

    store_copy(jnp.int32(num_chunks - 1)).wait()


def backward_pass(saved_acts, grad_top, norm_gain, w_up, w_down, axis, chunk_cols):
    num_layers, row_dim, hidden = w_up.shape
    tokens = grad_top.shape[0]
    chunks_per_mat = hidden // chunk_cols
    region = row_dim // (2 * COLORS)
    half = (COLORS, region, chunk_cols)
    sizes = (num_layers, chunks_per_mat, row_dim, chunk_cols, region, row_dim // chunk_cols, axis)
    num_chunks = 2 * num_layers * chunks_per_mat
    bf16, f32 = jnp.bfloat16, jnp.float32
    small_width = 2 * row_dim + hidden
    small = jnp.zeros((1, num_layers * small_width - row_dim), f32)
    small = jnp.concatenate([small, jnp.sum(grad_top, axis=0, keepdims=True)], axis=1)
    dma = pltpu.SemaphoreType.DMA
    any_spec = pl.BlockSpec(memory_space=pl.ANY)
    vmem_spec = pl.BlockSpec(memory_space=pltpu.VMEM)
    gathered, small_sum, _, _ = pl.pallas_call(
        functools.partial(backward_kernel, sizes),
        out_shape=(
            jax.ShapeDtypeStruct((num_chunks, 2) + half, bf16),
            jax.ShapeDtypeStruct(small.shape, f32),
            jax.ShapeDtypeStruct((chunks_per_mat, tokens, chunk_cols), bf16),
            jax.ShapeDtypeStruct((tokens, row_dim), bf16),
        ),
        in_specs=[any_spec] * (4 * num_layers + 4) + [vmem_spec] * 2,
        out_specs=(any_spec, vmem_spec, any_spec, any_spec),
        scratch_shapes=[
            pltpu.VMEM((2, tokens, row_dim), bf16),
            pltpu.VMEM((2, tokens, chunk_cols), bf16),
            pltpu.VMEM(half, bf16),
            pltpu.VMEM((KEPT_SLOTS,) + half, f32),
            pltpu.VMEM((RECV_SLOTS,) + half, bf16),
            pltpu.VMEM((COLORS, region // 2, chunk_cols), bf16),
            pltpu.VMEM((COLORS, region // 4, chunk_cols), bf16),
            pltpu.VMEM((COLORS, region // 8, chunk_cols), bf16),
            pltpu.VMEM((RECV_SLOTS, COLORS, region // 2, chunk_cols), bf16),
            pltpu.VMEM((RECV_SLOTS, COLORS, region // 4, chunk_cols), bf16),
            pltpu.VMEM((RECV_SLOTS, COLORS, region // 8, chunk_cols), bf16),
            pltpu.VMEM((GATHER_SLOTS, 2) + half, bf16),
            pltpu.VMEM((2, chunk_cols, row_dim), bf16),
            pltpu.VMEM((2, tokens, chunk_cols), bf16),
            pltpu.VMEM((tokens, chunk_cols), bf16),
            pltpu.VMEM((tokens, row_dim), bf16),
            pltpu.VMEM((tokens, row_dim), f32),
            pltpu.VMEM((2, NORM_ROWS, row_dim), bf16),
            pltpu.VMEM((2, NORM_ROWS, row_dim), f32),
            pltpu.VMEM((4,) + small.shape, f32),
            dma((4, 2)), dma, dma((2, 2)), dma,
            dma, dma((RECV_SLOTS,)), dma((3, COLORS)), dma((3, COLORS, RECV_SLOTS)),
            dma((3, COLORS, GATHER_SLOTS)), dma((3, COLORS, GATHER_SLOTS)), dma((GATHER_SLOTS,)), dma((GATHER_SLOTS,)),
            dma((GATHER_SLOTS,)), dma((4,)), dma((4,)),
        ],
        compiler_params=pltpu.CompilerParams(collective_id=0, has_side_effects=True, vmem_limit_bytes=67043328),
        name="backward",
    )(*[array for layer in saved_acts for array in layer], grad_top, grad_top.astype(bf16), w_up, w_down,
      norm_gain.astype(f32), small)
    return gathered, small_sum.reshape(num_layers, small_width)


def widen_kernel(chunk_ref, out_ref):
    out_ref[0] = chunk_ref[0].astype(jnp.float32)


def widen(gathered, num_layers, row_dim, hidden, chunk_cols):
    per_mat = hidden // chunk_cols
    num_mats = 2 * num_layers
    down_subs = row_dim // chunk_cols
    chunks = gathered.reshape(num_mats * per_mat, row_dim, chunk_cols)

    def mat_of(layer, kind):
        return (num_layers - 1 - layer) * 2 + kind

    block = (1, row_dim, chunk_cols)
    up = pl.pallas_call(
        widen_kernel,
        grid=(num_layers, per_mat),
        in_specs=[pl.BlockSpec(block, lambda layer, sub: (mat_of(layer, 1) * per_mat + sub, 0, 0))],
        out_specs=pl.BlockSpec(block, lambda layer, sub: (layer, 0, sub)),
        out_shape=jax.ShapeDtypeStruct((num_layers, row_dim, hidden), jnp.float32),
        name="widen_up",
    )(chunks)
    down = pl.pallas_call(
        widen_kernel,
        grid=(num_layers, per_mat),
        in_specs=[pl.BlockSpec(block, lambda layer, sub: (mat_of(layer, 0) * per_mat + sub, 0, 0))],
        out_specs=pl.BlockSpec(block, lambda layer, sub: (layer, sub // down_subs, sub % down_subs)),
        out_shape=jax.ShapeDtypeStruct((num_layers, hidden, row_dim), jnp.float32),
        name="widen_down",
    )(chunks)
    return up, down


def solution(mesh):
    axis = mesh.axis_names[0]

    def device_grads(tokens, upstream, norm_gain, w_up, bias_up, w_down, bias_down):
        num_layers, width = norm_gain.shape
        hidden_width = w_up.shape[2]
        chunk_cols = width // 2
        top_hidden, saved_acts = forward_stack(tokens, norm_gain, w_up, bias_up, w_down, bias_down)
        grad_h = top_gradient(top_hidden, upstream)
        gathered, small = backward_pass(saved_acts, grad_h, norm_gain, w_up, w_down, axis, chunk_cols)
        up_full, down_full = widen(gathered, num_layers, width, hidden_width, chunk_cols)
        return (small[:, :width], up_full, small[:, width:width + hidden_width], down_full, small[:, width + hidden_width:])

    row_spec = P(axis, None)
    full_spec = P()
    return jax.shard_map(
        device_grads,
        mesh=mesh,
        in_specs=(row_spec, row_spec, full_spec, full_spec, full_spec, full_spec, full_spec),
        out_specs=(full_spec, full_spec, full_spec, full_spec, full_spec),
        check_vma=False,
    )
```

```python
import functools

import jax
import jax.numpy as jnp
from jax import lax
from jax.experimental import pallas as pl
from jax.experimental.pallas import tpu as pltpu
from jax.sharding import PartitionSpec as P

EPSILON = 1e-6
TOKEN_DIMS = (((0,), (0,)), ((), ()))
FEATURE_DIMS = (((1,), (1,)), ((), ()))
MESH = pl.DeviceIdType.MESH
COLORS = 3
CORE, DIM_X, DIM_Y, DIM_Z = range(4)
COLOR_DIMS = ((DIM_X, DIM_Y, DIM_Z), (DIM_Y, DIM_Z, DIM_X), (DIM_Z, DIM_X, DIM_Y))
PIPELINE = (
    ("load", 0), ("compute_sent", 0), ("compute_kept", 0), ("send_2", 1), ("backward_0", 0), ("send_back_3", 2), ("send_1", 0),
    ("send_back_1", 4), ("send_back_core", 5), ("backward_1", 0), ("backward_2", 0), ("input_grad", 0), ("load_cols", 0),
    ("send_3", 1), ("send_back_2", 2), ("store", 5),
)
MAX_LAG = 5
RECV_SLOTS = 2
KEPT_SLOTS = 3
GATHER_SLOTS = 6
TILE = 256
NORM_ROWS = 128
GELU_SCALE = 0.7978845608028654
GELU_CUBIC = 0.044715


def inverse_rms(hid_f):
    return lax.rsqrt(jnp.mean(hid_f * hid_f, axis=-1, keepdims=True) + EPSILON)


def gelu(values):
    return (0.5 * values) * (1.0 + jnp.tanh(values * (GELU_SCALE + GELU_SCALE * GELU_CUBIC * (values * values))))


def forward_kernel(
    sizes, tokens, upstream, w_up, w_down, gain_in, bias_up, bias_down, hid_out, normed_out, pre_act_out, act_out,
    grad_top_out, grad_top_b_out, small_out, hid, normed, branch, up_buf, down_buf, pre_buf, act_buf, up_rows, grad_b_buf,
    io_sem, up_sem, down_sem, pre_sem, act_sem,
):
    num_layers, num_tiles, tile_cols = sizes
    num_tokens, row_dim = hid.shape
    steps = num_tiles + 1
    token_half = num_tokens // 2
    parts = tile_cols // TILE
    branch_cols = row_dim // parts

    def up_load(step):
        layer, tile = step // steps, step % steps
        cols = pl.ds(pl.multiple_of(tile * tile_cols, 128), tile_cols)
        return pltpu.make_async_copy(w_up.at[layer, :, cols], up_buf.at[tile % 2], up_sem.at[tile % 2])

    def down_load(step):
        layer, tile = step // steps, step % steps
        rows = pl.ds(pl.multiple_of(tile * tile_cols, 128), tile_cols)
        return pltpu.make_async_copy(w_down.at[layer, rows, :], down_buf.at[tile % 2], down_sem.at[tile % 2])

    def tile_stores(step):
        layer, tile = step // steps, step % steps
        cols = pl.ds(pl.multiple_of(tile * tile_cols, 128), tile_cols)
        return (
            pltpu.make_async_copy(pre_buf.at[tile % 2], pre_act_out.at[layer, :, cols], pre_sem.at[tile % 2]),
            pltpu.make_async_copy(act_buf.at[tile % 2], act_out.at[layer, :, cols], act_sem.at[tile % 2]),
        )

    def normed_store(layer):
        return pltpu.make_async_copy(normed, normed_out.at[layer], io_sem.at[1])

    def hid_store():
        return pltpu.make_async_copy(hid, hid_out, io_sem.at[2])

    tokens_load = pltpu.make_async_copy(tokens, hid, io_sem.at[0])
    tokens_load.start()
    first = jnp.int32(0)
    up_load(first).start()
    down_load(first).start()
    upstream_load = pltpu.make_async_copy(upstream, up_rows, io_sem.at[3])
    upstream_load.start()
    tokens_load.wait()

    def norm_rows(layer):
        @pl.loop(0, num_tokens // NORM_ROWS)
        def _(block):
            rows = pl.ds(pl.multiple_of(block * NORM_ROWS, NORM_ROWS), NORM_ROWS)
            hid_f = hid[rows, :].astype(jnp.float32)
            gain = gain_in[pl.ds(layer, 1), :]
            normed[rows, :] = ((hid_f * inverse_rms(hid_f)) * gain).astype(jnp.bfloat16)

    def add_branch(layer):
        @pl.loop(0, num_tokens // NORM_ROWS)
        def _(block):
            rows = pl.ds(pl.multiple_of(block * NORM_ROWS, NORM_ROWS), NORM_ROWS)
            bias = bias_down[pl.ds(layer, 1), :]
            hid[rows, :] = ((hid[rows, :].astype(jnp.float32) + branch[rows, :]) + bias).astype(jnp.bfloat16)

    def work(step, with_up, with_down):
        layer, tile = step // steps, step % steps

        @pl.loop(0, 2 * parts)
        def _(index):
            rows = pl.ds(pl.multiple_of((index % 2) * token_half, 128), token_half)
            part = index // 2
            if with_up:
                cols = pl.ds(pl.multiple_of(part * TILE, TILE), TILE)
                bias = bias_up[pl.ds(layer, 1), pl.ds(pl.multiple_of(tile * tile_cols + part * TILE, TILE), TILE)]
                pre_act = (jnp.dot(normed[rows, :], up_buf[tile % 2, :, cols], preferred_element_type=jnp.float32) + bias).astype(jnp.bfloat16)
                pre_buf[tile % 2, rows, cols] = pre_act
                act_buf[tile % 2, rows, cols] = gelu(pre_act.astype(jnp.float32)).astype(jnp.bfloat16)
            if with_down:
                cols = pl.ds(pl.multiple_of(part * branch_cols, 128), branch_cols)
                last = (tile + 1) % 2
                added = jnp.dot(act_buf[last, rows, :], down_buf[last, :, cols], preferred_element_type=jnp.float32)
                branch[rows, cols] += added

    branch[...] = jnp.zeros_like(branch)

    @pl.loop(0, num_layers * steps)
    def _(step):
        layer, tile = step // steps, step % steps

        @pl.when(tile < num_tiles)
        def _():
            up_load(step).wait()

            @pl.when(tile + 1 < num_tiles)
            def _():
                up_load(step + 1).start()

        @pl.when(tile > 0)
        def _():
            down_load(step - 1).wait()

            @pl.when(tile < num_tiles)
            def _():
                down_load(step).start()

        @pl.when((tile == num_tiles) & (layer + 1 < num_layers))
        def _():
            up_load(step + 1).start()
            down_load(step + 1).start()

        @pl.when((tile > 1) & (tile < num_tiles))
        def _():
            for copy in tile_stores(step - 2):
                copy.wait()

        @pl.when(tile == 0)
        def _():
            @pl.when(layer > 0)
            def _():
                normed_store(layer - 1).wait()
            norm_rows(layer)
            normed_store(layer).start()
            work(step, True, False)

        @pl.when((tile > 0) & (tile < num_tiles))
        def _():
            work(step, True, True)

        @pl.when(tile < num_tiles)
        def _():
            for copy in tile_stores(step):
                copy.start()

        @pl.when(tile == num_tiles)
        def _():
            work(step, False, True)
            for back in (2, 1):
                for copy in tile_stores(step - back):
                    copy.wait()
            add_branch(layer)

            @pl.when(layer + 1 < num_layers)
            def _():
                hid_store().start()
                branch[...] = jnp.zeros_like(branch)
                hid_store().wait()

    normed_store(num_layers - 1).wait()
    upstream_load.wait()
    small_out[...] = jnp.zeros_like(small_out)
    bias_start = small_out.shape[1] - row_dim

    @pl.loop(0, num_tokens // NORM_ROWS)
    def _(block):
        rows = pl.ds(pl.multiple_of(block * NORM_ROWS, NORM_ROWS), NORM_ROWS)
        top_f = hid[rows, :].astype(jnp.float32)
        top_scale = inverse_rms(top_f)
        top_hat = top_f * top_scale
        up_f = up_rows[rows, :].astype(jnp.float32)
        grad = top_scale * (up_f - top_hat * jnp.mean(up_f * top_hat, axis=-1, keepdims=True))
        branch[rows, :] = grad
        grad_b_buf[rows, :] = grad.astype(jnp.bfloat16)
        small_out[:, bias_start:bias_start + row_dim] += jnp.sum(grad, axis=0, keepdims=True)
    grad_store = pltpu.make_async_copy(branch, grad_top_out, io_sem.at[0])
    grad_b_store = pltpu.make_async_copy(grad_b_buf, grad_top_b_out, io_sem.at[1])
    grad_store.start()
    grad_b_store.start()
    grad_store.wait()
    grad_b_store.wait()


def forward_pass(tokens, upstream, norm_gain, w_up, bias_up, w_down, bias_down, tile_cols):
    num_tokens, row_dim = tokens.shape
    num_layers, _, hidden = w_up.shape
    bf16, f32 = jnp.bfloat16, jnp.float32
    dma = pltpu.SemaphoreType.DMA
    any_spec = pl.BlockSpec(memory_space=pl.ANY)
    vmem_spec = pl.BlockSpec(memory_space=pltpu.VMEM)
    rows = (num_tokens, row_dim)
    wide = (num_layers, num_tokens, hidden)
    return pl.pallas_call(
        functools.partial(forward_kernel, (num_layers, hidden // tile_cols, tile_cols)),
        out_shape=(
            jax.ShapeDtypeStruct(rows, bf16),
            jax.ShapeDtypeStruct((num_layers,) + rows, bf16),
            jax.ShapeDtypeStruct(wide, bf16),
            jax.ShapeDtypeStruct(wide, bf16),
            jax.ShapeDtypeStruct(rows, f32),
            jax.ShapeDtypeStruct(rows, bf16),
            jax.ShapeDtypeStruct((1, num_layers * (2 * row_dim + hidden)), f32),
        ),
        in_specs=[any_spec] * 4 + [vmem_spec] * 3,
        out_specs=(any_spec,) * 6 + (vmem_spec,),
        scratch_shapes=[
            pltpu.VMEM(rows, bf16),
            pltpu.VMEM(rows, bf16),
            pltpu.VMEM(rows, f32),
            pltpu.VMEM((2, row_dim, tile_cols), bf16),
            pltpu.VMEM((2, tile_cols, row_dim), bf16),
            pltpu.VMEM((2, num_tokens, tile_cols), bf16),
            pltpu.VMEM((2, num_tokens, tile_cols), bf16),
            pltpu.VMEM(rows, bf16),
            pltpu.VMEM(rows, bf16),
            dma((4,)), dma((2,)), dma((2,)), dma((2,)), dma((2,)),
        ],
        compiler_params=pltpu.CompilerParams(vmem_limit_bytes=60 * 2**20),
        name="forward",
    )(tokens, upstream, w_up, w_down, norm_gain.astype(f32), bias_up.astype(f32), bias_down.astype(f32))


def gelu_slope(values):
    square = values * values
    bend = jnp.tanh(values * (GELU_SCALE + GELU_SCALE * GELU_CUBIC * square))
    return 0.5 * (1.0 + bend) + (0.5 * values) * (1.0 - bend * bend) * (GELU_SCALE + 3.0 * GELU_SCALE * GELU_CUBIC * square)


def backward_kernel(sizes, *refs):
    num_layers, chunks_per_mat, row_dim, chunk_cols, region, down_subs, axis = sizes
    num_mats = 2 * num_layers
    hidden_dim = chunks_per_mat * chunk_cols
    hid_refs, refs = refs[:num_layers], refs[num_layers:]
    (normed, pre_act, activated, grad_top, grad_top_b, w_up, w_down, gain_in, small_in,
     gathered, small_out, grad_pre_hbm, grad_b_hbm) = refs[:13]
    (rows_buf, cols_buf, sent_core, kept, recv_core, sent_1, sent_2, sent_3, recv_1, recv_2, recv_3, ring,
     weight_buf, pre_buf, grad_pre_buf, grad_b, grad_normed, hid_buf, grad_buf,
     small_recv, load_sem, grad_pre_sem, norm_sem, grad_b_sem, core_send, core_recv, out_send, out_recv, back_send, back_recv,
     share_send, share_recv, store_sem, small_send_sem, small_recv_sem) = refs[13:]
    small_width = 2 * row_dim + hidden_dim
    num_chunks = num_mats * chunks_per_mat
    half = COLORS * region
    me = lax.axis_index(axis)
    bits = [me % 2, (me // 2) % 2, (me // 4) % 2, me // 8]
    partners = [me + (1 << d) - 2 * (1 << d) * bits[d] for d in range(4)]
    core = bits[CORE]
    sent_bufs, recv_bufs = (sent_1, sent_2, sent_3), (recv_1, recv_2, recv_3)
    spans = (region // 2, region // 4, region // 8)

    def base(color, level):
        total = 0
        for step in range(level):
            total = total + bits[COLOR_DIMS[color][step]] * spans[step]
        return total

    def other(color, level):
        return base(color, level) + (1 - bits[COLOR_DIMS[color][level]]) * spans[level]

    def rows_at(start, size):
        return pl.ds(pl.multiple_of(start, spans[2]), size)

    def mat_loads(mat, chunk):
        slot = chunk % 2
        sub = chunk % chunks_per_mat
        layer = num_layers - 1 - mat // 2
        cols = pl.ds(pl.multiple_of(sub * chunk_cols, 128), chunk_cols)
        if mat % 2 == 0:
            rows = pl.ds(pl.multiple_of((sub // down_subs) * row_dim, 128), row_dim)
            return [
                pltpu.make_async_copy(activated.at[layer, :, rows], rows_buf.at[slot], load_sem.at[0, slot]),
                pltpu.make_async_copy(w_down.at[layer, cols, :], weight_buf.at[slot], load_sem.at[1, slot]),
                pltpu.make_async_copy(pre_act.at[layer, :, cols], pre_buf.at[slot], load_sem.at[2, slot]),
            ]
        copies = [pltpu.make_async_copy(normed.at[layer], rows_buf.at[slot], load_sem.at[0, slot])]
        for part in range(down_subs):
            copies.append(pltpu.make_async_copy(
                w_up.at[layer, part * chunk_cols:(part + 1) * chunk_cols, cols],
                weight_buf.at[slot, :, part * chunk_cols:(part + 1) * chunk_cols], load_sem.at[1 + part, slot]))
        return copies

    def cols_load(mat, chunk):
        sub = chunk % chunks_per_mat
        if mat % 2 == 0:
            source = grad_top_b if mat == 0 else grad_b_hbm
            source = source.at[:, pl.ds(pl.multiple_of((sub % down_subs) * chunk_cols, 128), chunk_cols)]
        else:
            source = grad_pre_hbm.at[sub]
        return pltpu.make_async_copy(source, cols_buf.at[chunk % 2], load_sem.at[3, chunk % 2])

    def for_mat(chunk, action):
        for mat in range(num_mats):
            @pl.when(chunk // chunks_per_mat == mat)
            def _(mat=mat):
                action(mat)

    def start_loads(chunk):
        def start(mat):
            for copy in mat_loads(mat, chunk):
                copy.start()
        for_mat(chunk, start)

    def grad_pre_store(sub):
        return pltpu.make_async_copy(grad_pre_buf, grad_pre_hbm.at[sub], grad_pre_sem)

    def core_copy(chunk):
        slot = chunk % RECV_SLOTS
        return pltpu.make_async_remote_copy(
            src_ref=sent_core, dst_ref=recv_core.at[slot], send_sem=core_send, recv_sem=core_recv.at[slot],
            device_id=(partners[CORE],), device_id_type=MESH)

    def out_copy(level, color, chunk):
        slot = chunk % RECV_SLOTS
        return pltpu.make_async_remote_copy(
            src_ref=sent_bufs[level].at[color], dst_ref=recv_bufs[level].at[slot, color],
            send_sem=out_send.at[level, color], recv_sem=out_recv.at[level, color, slot],
            device_id=(partners[COLOR_DIMS[color][level]],), device_id_type=MESH)

    def back_copy(level, color, chunk, arriving):
        slot = chunk % GATHER_SLOTS
        mine = ring.at[slot, core, color, rows_at(base(color, level + 1), spans[level]), :]
        theirs = ring.at[slot, core, color, rows_at(other(color, level), spans[level]), :]
        return pltpu.make_async_remote_copy(
            src_ref=mine, dst_ref=theirs if arriving else mine,
            send_sem=back_send.at[level, color, slot], recv_sem=back_recv.at[level, color, slot],
            device_id=(partners[COLOR_DIMS[color][level]],), device_id_type=MESH)

    def share_copy(chunk, arriving):
        slot = chunk % GATHER_SLOTS
        return pltpu.make_async_remote_copy(
            src_ref=ring.at[slot, core], dst_ref=ring.at[slot, 1 - core if arriving else core],
            send_sem=share_send.at[slot], recv_sem=share_recv.at[slot],
            device_id=(partners[CORE],), device_id_type=MESH)

    def store_copy(chunk):
        slot = chunk % GATHER_SLOTS
        return pltpu.make_async_copy(ring.at[slot], gathered.at[chunk], store_sem.at[slot])

    def small_copy(step):
        return pltpu.make_async_remote_copy(
            src_ref=small_out, dst_ref=small_recv.at[step], send_sem=small_send_sem.at[step],
            recv_sem=small_recv_sem.at[step], device_id=(partners[step],), device_id_type=MESH)

    def product(chunk, which_core, color):
        slot = chunk % 2
        start = pl.multiple_of(which_core * half + color * region, 128)
        return lax.dot_general(
            rows_buf[slot, :, pl.ds(start, region)], cols_buf[slot], TOKEN_DIMS, preferred_element_type=jnp.float32)

    def load(chunk):
        def arrive(mat):
            for copy in mat_loads(mat, chunk):
                copy.wait()
        for_mat(chunk, arrive)
        for_mat(chunk, lambda mat: cols_load(mat, chunk).wait())

        @pl.when(chunk + 1 < num_chunks)
        def _():
            start_loads(chunk + 1)

        before = chunk - 1

        @pl.when((before >= 0) & ((before // chunks_per_mat) % 2 == 0))
        def _():
            grad_pre_store(before % chunks_per_mat).wait()

    def load_cols(chunk):
        @pl.when(chunk + 1 < num_chunks)
        def _():
            for_mat(chunk + 1, lambda mat: cols_load(mat, chunk + 1).start())

    def compute_sent(chunk):
        @pl.loop(0, COLORS)
        def _(color):
            sent_core[color] = product(chunk, 1 - core, color).astype(jnp.bfloat16)
        core_copy(chunk).start()

    def compute_kept(chunk):
        slot = chunk % KEPT_SLOTS

        @pl.loop(0, COLORS)
        def _(color):
            kept[slot, color] = product(chunk, core, color)

    def halve(level, chunk, arrived):
        slot = chunk % KEPT_SLOTS
        recv_slot = chunk % RECV_SLOTS
        for color in range(COLORS):
            if level > 0:
                out_copy(level - 1, color, chunk).wait()
            held = base(color, level)

            def total(start, size, color=color, held=held):
                own = kept[slot, color, rows_at(start, size), :]
                return own + arrived[recv_slot, color, rows_at(start - held, size), :].astype(jnp.float32)

            if level < 3:
                mine = base(color, level + 1)
                sent_bufs[level][color] = total(other(color, level), spans[level]).astype(jnp.bfloat16)
                kept[slot, color, rows_at(mine, spans[level]), :] = total(mine, spans[level])
                out_copy(level, color, chunk).start()
            else:
                gather_slot = chunk % GATHER_SLOTS
                ring[gather_slot, core, color, rows_at(held, spans[2]), :] = total(held, spans[2]).astype(jnp.bfloat16)
                back_copy(2, color, chunk, False).start()

    def send_1(chunk):
        core_copy(chunk).wait()
        halve(0, chunk, recv_core)

    def send_2(chunk):
        halve(1, chunk, recv_1)

    def send_3(chunk):
        halve(2, chunk, recv_2)

    def send_back_3(chunk):
        halve(3, chunk, recv_3)

    def pass_back(level, chunk):
        for color in range(COLORS):
            back_copy(level + 1, color, chunk, True).wait()
            back_copy(level, color, chunk, False).start()

    def send_back_2(chunk):
        pass_back(1, chunk)

    def send_back_1(chunk):
        pass_back(0, chunk)

    def send_back_core(chunk):
        for color in range(COLORS):
            back_copy(0, color, chunk, True).wait()
        share_copy(chunk, False).start()

    def store(chunk):
        share_copy(chunk, True).wait()
        store_copy(chunk).start()

        @pl.when(chunk > 0)
        def _():
            store_copy(chunk - 1).wait()

    token_half = grad_b.shape[0] // 2

    def backward(part, chunk):
        slot = chunk % 2
        sub = chunk % chunks_per_mat
        mat = chunk // chunks_per_mat
        layer = num_layers - 1 - mat // 2

        @pl.when(mat % 2 == 0)
        def _():
            cols = slice(part * TILE, (part + 1) * TILE)

            @pl.loop(0, 2)
            def _(which):
                rows = pl.ds(pl.multiple_of(which * token_half, 128), token_half)
                grad_act = lax.dot_general(
                    grad_b[rows, :], weight_buf[slot, cols, :], FEATURE_DIMS, preferred_element_type=jnp.float32)
                grad_pre = grad_act * gelu_slope(pre_buf[slot, rows, cols].astype(jnp.float32))
                grad_pre_buf[rows, cols] = grad_pre.astype(jnp.bfloat16)
                start = layer * small_width + row_dim + sub * chunk_cols + part * TILE
                small_out[:, pl.ds(pl.multiple_of(start, 128), TILE)] += jnp.sum(grad_pre, axis=0, keepdims=True)

            if part == chunk_cols // TILE - 1:
                grad_pre_store(sub).start()

        @pl.when(mat % 2 == 1)
        def _():
            @pl.loop(0, 2 * down_subs)
            def _(step):
                rows = pl.ds(pl.multiple_of((step % 2) * token_half, 128), token_half)
                piece = part * down_subs + step // 2
                tiles = chunk_cols // TILE
                weight_rows = pl.ds(pl.multiple_of((piece % tiles) * TILE, TILE), TILE)
                weight_cols = pl.ds(pl.multiple_of((piece // tiles) * chunk_cols, 128), chunk_cols)
                out_cols = pl.ds(pl.multiple_of(piece * TILE, 128), TILE)
                grad_normed[rows, out_cols] += lax.dot_general(
                    cols_buf[slot, rows, :], weight_buf[slot, weight_rows, weight_cols], FEATURE_DIMS,
                    preferred_element_type=jnp.float32)

    def norm_loads(layer, block):
        rows = pl.ds(pl.multiple_of(block * NORM_ROWS, NORM_ROWS), NORM_ROWS)
        slot = block % 2
        copies = [pltpu.make_async_copy(hid_refs[layer].at[rows, :], hid_buf.at[slot], norm_sem.at[0, slot])]
        if layer > 0:
            copies.append(pltpu.make_async_copy(grad_top.at[rows, :], grad_buf.at[slot], norm_sem.at[1, slot]))
        return copies

    def layer_input_grad(layer):
        num_blocks = grad_b.shape[0] // NORM_ROWS
        offset = layer * small_width
        for copy in norm_loads(layer, 0):
            copy.start()

        @pl.loop(0, num_blocks)
        def _(block):
            @pl.when(block + 1 < num_blocks)
            def _():
                for copy in norm_loads(layer, block + 1):
                    copy.start()
            for copy in norm_loads(layer, block):
                copy.wait()
            rows = pl.ds(pl.multiple_of(block * NORM_ROWS, NORM_ROWS), NORM_ROWS)
            hid_f = hid_buf[block % 2].astype(jnp.float32)
            hid_scale = inverse_rms(hid_f)
            hid_hat = hid_f * hid_scale
            normed_grad = grad_normed[rows, :]
            small_out[:, offset:offset + row_dim] += jnp.sum(normed_grad * hid_hat, axis=0, keepdims=True)
            if layer > 0:
                grad_normed[rows, :] = jnp.zeros((NORM_ROWS, row_dim), jnp.float32)
                grad_hat = normed_grad * gain_in[layer:layer + 1, :]
                grad_new = grad_buf[block % 2] + hid_scale * (
                    grad_hat - hid_hat * jnp.mean(grad_hat * hid_hat, axis=-1, keepdims=True))
                grad_b[rows, :] = grad_new.astype(jnp.bfloat16)
                bias_start = offset - row_dim
                small_out[:, bias_start:bias_start + row_dim] += jnp.sum(grad_new, axis=0, keepdims=True)
        if layer > 0:
            copy = pltpu.make_async_copy(grad_b, grad_b_hbm, grad_b_sem)
            copy.start()
            copy.wait()

    def input_grad(chunk):
        for layer in range(num_layers):
            last = (num_layers - 1 - layer) * 2 * chunks_per_mat + 2 * chunks_per_mat - 1

            @pl.when(chunk == last)
            def _(layer=layer):
                layer_input_grad(layer)

    events = dict(
        load=load, compute_sent=compute_sent, compute_kept=compute_kept, send_1=send_1, send_2=send_2, send_3=send_3,
        send_back_3=send_back_3, send_back_2=send_back_2, send_back_1=send_back_1, send_back_core=send_back_core, store=store,
        backward_0=functools.partial(backward, 0), backward_1=functools.partial(backward, 1),
        backward_2=functools.partial(backward, 2), input_grad=input_grad, load_cols=load_cols)

    first = jnp.int32(0)
    for copy in mat_loads(0, first):
        copy.start()
    cols_load(0, first).start()
    grad_b_copy = pltpu.make_async_copy(grad_top_b, grad_b, grad_b_sem)
    grad_b_copy.start()
    barrier = pltpu.get_barrier_semaphore()
    for partner in partners:
        pl.semaphore_signal(barrier, inc=1, device_id=(partner,), device_id_type=MESH)
    small_out[...] = small_in[...]
    grad_normed[...] = jnp.zeros_like(grad_normed)
    grad_b_copy.wait()
    pl.semaphore_wait(barrier, 4)

    @pl.loop(0, num_chunks + MAX_LAG)
    def _(it):
        for step in range(4):
            @pl.when(it == num_chunks + step)
            def _(step=step):
                small_copy(step).start()
        for name, lag in PIPELINE:
            chunk = it - lag

            @pl.when((chunk >= 0) & (chunk < num_chunks))
            def _(name=name, chunk=chunk):
                events[name](chunk)
        for step in range(4):
            @pl.when(it == num_chunks + step)
            def _(step=step):
                small_copy(step).wait()
                small_out[...] += small_recv[step]

    store_copy(jnp.int32(num_chunks - 1)).wait()


def backward_pass(hid_rows, saved, grad_top, grad_top_b, norm_gain, w_up, w_down, small, axis, chunk_cols):
    num_layers, row_dim, hidden = w_up.shape
    tokens = grad_top.shape[0]
    chunks_per_mat = hidden // chunk_cols
    region = row_dim // (2 * COLORS)
    half = (COLORS, region, chunk_cols)
    sizes = (num_layers, chunks_per_mat, row_dim, chunk_cols, region, row_dim // chunk_cols, axis)
    num_chunks = 2 * num_layers * chunks_per_mat
    bf16, f32 = jnp.bfloat16, jnp.float32
    small_width = 2 * row_dim + hidden
    dma = pltpu.SemaphoreType.DMA
    any_spec = pl.BlockSpec(memory_space=pl.ANY)
    vmem_spec = pl.BlockSpec(memory_space=pltpu.VMEM)
    gathered, small_sum, _, _ = pl.pallas_call(
        functools.partial(backward_kernel, sizes),
        out_shape=(
            jax.ShapeDtypeStruct((num_chunks, 2) + half, bf16),
            jax.ShapeDtypeStruct(small.shape, f32),
            jax.ShapeDtypeStruct((chunks_per_mat, tokens, chunk_cols), bf16),
            jax.ShapeDtypeStruct((tokens, row_dim), bf16),
        ),
        in_specs=[any_spec] * (num_layers + 7) + [vmem_spec] * 2,
        out_specs=(any_spec, vmem_spec, any_spec, any_spec),
        scratch_shapes=[
            pltpu.VMEM((2, tokens, row_dim), bf16),
            pltpu.VMEM((2, tokens, chunk_cols), bf16),
            pltpu.VMEM(half, bf16),
            pltpu.VMEM((KEPT_SLOTS,) + half, f32),
            pltpu.VMEM((RECV_SLOTS,) + half, bf16),
            pltpu.VMEM((COLORS, region // 2, chunk_cols), bf16),
            pltpu.VMEM((COLORS, region // 4, chunk_cols), bf16),
            pltpu.VMEM((COLORS, region // 8, chunk_cols), bf16),
            pltpu.VMEM((RECV_SLOTS, COLORS, region // 2, chunk_cols), bf16),
            pltpu.VMEM((RECV_SLOTS, COLORS, region // 4, chunk_cols), bf16),
            pltpu.VMEM((RECV_SLOTS, COLORS, region // 8, chunk_cols), bf16),
            pltpu.VMEM((GATHER_SLOTS, 2) + half, bf16),
            pltpu.VMEM((2, chunk_cols, row_dim), bf16),
            pltpu.VMEM((2, tokens, chunk_cols), bf16),
            pltpu.VMEM((tokens, chunk_cols), bf16),
            pltpu.VMEM((tokens, row_dim), bf16),
            pltpu.VMEM((tokens, row_dim), f32),
            pltpu.VMEM((2, NORM_ROWS, row_dim), bf16),
            pltpu.VMEM((2, NORM_ROWS, row_dim), f32),
            pltpu.VMEM((4,) + small.shape, f32),
            dma((4, 2)), dma, dma((2, 2)), dma,
            dma, dma((RECV_SLOTS,)), dma((3, COLORS)), dma((3, COLORS, RECV_SLOTS)),
            dma((3, COLORS, GATHER_SLOTS)), dma((3, COLORS, GATHER_SLOTS)), dma((GATHER_SLOTS,)), dma((GATHER_SLOTS,)),
            dma((GATHER_SLOTS,)), dma((4,)), dma((4,)),
        ],
        compiler_params=pltpu.CompilerParams(collective_id=0, has_side_effects=True, vmem_limit_bytes=67043328),
        name="backward",
    )(*hid_rows, *saved, grad_top, grad_top_b, w_up, w_down, norm_gain.astype(f32), small)
    return gathered, small_sum.reshape(num_layers, small_width)


def widen_kernel(chunk_ref, out_ref):
    out_ref[0] = chunk_ref[0].astype(jnp.float32)


def widen(gathered, num_layers, row_dim, hidden, chunk_cols):
    per_mat = hidden // chunk_cols
    num_mats = 2 * num_layers
    down_subs = row_dim // chunk_cols
    chunks = gathered.reshape(num_mats * per_mat, row_dim, chunk_cols)

    def mat_of(layer, kind):
        return (num_layers - 1 - layer) * 2 + kind

    block = (1, row_dim, chunk_cols)
    up = pl.pallas_call(
        widen_kernel,
        grid=(num_layers, per_mat),
        in_specs=[pl.BlockSpec(block, lambda layer, sub: (mat_of(layer, 1) * per_mat + sub, 0, 0))],
        out_specs=pl.BlockSpec(block, lambda layer, sub: (layer, 0, sub)),
        out_shape=jax.ShapeDtypeStruct((num_layers, row_dim, hidden), jnp.float32),
        name="widen_up",
    )(chunks)
    down = pl.pallas_call(
        widen_kernel,
        grid=(num_layers, per_mat),
        in_specs=[pl.BlockSpec(block, lambda layer, sub: (mat_of(layer, 0) * per_mat + sub, 0, 0))],
        out_specs=pl.BlockSpec(block, lambda layer, sub: (layer, sub // down_subs, sub % down_subs)),
        out_shape=jax.ShapeDtypeStruct((num_layers, hidden, row_dim), jnp.float32),
        name="widen_down",
    )(chunks)
    return up, down


def solution(mesh):
    axis = mesh.axis_names[0]

    def device_grads(tokens, upstream, norm_gain, w_up, bias_up, w_down, bias_down):
        num_layers, width = norm_gain.shape
        hidden_width = w_up.shape[2]
        chunk_cols = width // 2
        hid_1, normed, pre_act, activated, grad_top, grad_top_b, small = forward_pass(
            tokens, upstream, norm_gain, w_up, bias_up, w_down, bias_down, chunk_cols)
        gathered, small = backward_pass(
            (tokens, hid_1), (normed, pre_act, activated), grad_top, grad_top_b, norm_gain, w_up, w_down, small, axis, chunk_cols)
        up_full, down_full = widen(gathered, num_layers, width, hidden_width, chunk_cols)
        return (small[:, :width], up_full, small[:, width:width + hidden_width], down_full, small[:, width + hidden_width:])

    row_spec = P(axis, None)
    full_spec = P()
    return jax.shard_map(
        device_grads,
        mesh=mesh,
        in_specs=(row_spec, row_spec, full_spec, full_spec, full_spec, full_spec, full_spec),
        out_specs=(full_spec, full_spec, full_spec, full_spec, full_spec),
        check_vma=False,
    )
```

```python
import functools

import jax
import jax.numpy as jnp
from jax import lax
from jax.experimental import pallas as pl
from jax.experimental.pallas import tpu as pltpu
from jax.sharding import PartitionSpec as P

EPSILON = 1e-6
TOKEN_DIMS = (((0,), (0,)), ((), ()))
FEATURE_DIMS = (((1,), (1,)), ((), ()))
MESH = pl.DeviceIdType.MESH
COLORS = 3
CORE, DIM_X, DIM_Y, DIM_Z = range(4)
COLOR_DIMS = ((DIM_X, DIM_Y, DIM_Z), (DIM_Y, DIM_Z, DIM_X), (DIM_Z, DIM_X, DIM_Y))
PIPELINE = (
    ("load", 0), ("compute_sent", 0), ("compute_kept", 0), ("send_2", 1), ("backward_0", 0), ("send_back_3", 2), ("send_1", 0),
    ("send_back_1", 4), ("send_back_core", 5), ("backward_1", 0), ("backward_2", 0), ("input_grad", 0), ("load_cols", 0),
    ("send_3", 1), ("send_back_2", 2), ("store", 5),
)
MAX_LAG = 5
RECV_SLOTS = 2
KEPT_SLOTS = 3
GATHER_SLOTS = 6
TILE = 256
UP_COLS = 512
NORM_ROWS = 128
GELU_SCALE = 0.7978845608028654
GELU_CUBIC = 0.044715


def inverse_rms(hid_f):
    return lax.rsqrt(jnp.mean(hid_f * hid_f, axis=-1, keepdims=True) + EPSILON)


def gelu(values):
    return (0.5 * values) * (1.0 + jnp.tanh(values * (GELU_SCALE + GELU_SCALE * GELU_CUBIC * (values * values))))


def forward_kernel(
    sizes, tokens, upstream, w_up, w_down, gain_in, bias_up, bias_down, hid_out, normed_out, pre_act_out, act_out,
    grad_top_out, grad_top_b_out, small_out, hid, normed, branch, up_buf, down_buf, pre_buf, act_buf, up_rows, grad_b_buf,
    io_sem, up_sem, down_sem, pre_sem, act_sem,
):
    num_layers, num_tiles, tile_cols = sizes
    num_tokens, row_dim = hid.shape
    token_half = num_tokens // 2
    num_steps = num_layers * num_tiles

    def up_load(step):
        cols = pl.ds(pl.multiple_of((step % num_tiles) * tile_cols, 128), tile_cols)
        return pltpu.make_async_copy(w_up.at[step // num_tiles, :, cols], up_buf.at[step % 2], up_sem.at[step % 2])

    def down_load(step):
        rows = pl.ds(pl.multiple_of((step % num_tiles) * tile_cols, 128), tile_cols)
        return pltpu.make_async_copy(w_down.at[step // num_tiles, rows, :], down_buf.at[step % 2], down_sem.at[step % 2])

    def tile_stores(step):
        cols = pl.ds(pl.multiple_of((step % num_tiles) * tile_cols, 128), tile_cols)
        layer, slot = step // num_tiles, step % 2
        return (
            pltpu.make_async_copy(pre_buf.at[slot], pre_act_out.at[layer, :, cols], pre_sem.at[slot]),
            pltpu.make_async_copy(act_buf.at[slot], act_out.at[layer, :, cols], act_sem.at[slot]),
        )

    tokens_load = pltpu.make_async_copy(tokens, hid, io_sem.at[0])
    tokens_load.start()
    first = jnp.int32(0)
    up_load(first).start()
    down_load(first).start()
    upstream_load = pltpu.make_async_copy(upstream, up_rows, io_sem.at[3])
    upstream_load.start()
    small_out[...] = jnp.zeros_like(small_out)
    tokens_load.wait()

    def each_block(action):
        @pl.loop(0, num_tokens // NORM_ROWS)
        def _(block):
            action(pl.ds(pl.multiple_of(block * NORM_ROWS, NORM_ROWS), NORM_ROWS))

    def normalize(layer, rows, hid_f):
        normed[rows, :] = ((hid_f * inverse_rms(hid_f)) * gain_in[layer:layer + 1, :]).astype(jnp.bfloat16)

    def first_rows(rows):
        normalize(0, rows, hid[rows, :].astype(jnp.float32))

    def next_rows(layer, rows):
        new = ((hid[rows, :].astype(jnp.float32) + branch[rows, :]) + bias_down[layer:layer + 1, :]).astype(jnp.bfloat16)
        hid[rows, :] = new
        return new.astype(jnp.float32)

    def activate(step):
        layer, slot = step // num_tiles, step % 2

        @pl.loop(0, 2)
        def _(which):
            rows = pl.ds(pl.multiple_of(which * token_half, 128), token_half)

            def slope(part):
                cols = slice(part * UP_COLS, (part + 1) * UP_COLS)
                act_buf[slot, rows, cols] = gelu(pre_buf[slot, rows, cols].astype(jnp.float32)).astype(jnp.bfloat16)

            parts = tile_cols // UP_COLS
            for part in range(parts):
                cols = slice(part * UP_COLS, (part + 1) * UP_COLS)
                start = pl.multiple_of((step % num_tiles) * tile_cols + part * UP_COLS, 128)
                bias = bias_up[pl.ds(layer, 1), pl.ds(start, UP_COLS)]
                pre_buf[slot, rows, cols] = (
                    jnp.dot(normed[rows, :], up_buf[slot, :, cols], preferred_element_type=jnp.float32) + bias
                ).astype(jnp.bfloat16)
                if part > 0:
                    slope(part - 1)
            slope(parts - 1)

    def add_branch(step):
        slot = step % 2

        @pl.loop(0, row_dim // UP_COLS)
        def _(part):
            cols = pl.ds(pl.multiple_of(part * UP_COLS, 128), UP_COLS)
            branch[:, cols] += jnp.dot(act_buf[slot], down_buf[slot, :, cols], preferred_element_type=jnp.float32)

    each_block(first_rows)
    normed_store = pltpu.make_async_copy(normed, normed_out.at[0], io_sem.at[1])
    normed_store.start()
    branch[...] = jnp.zeros_like(branch)

    for layer in range(num_layers):
        @pl.loop(layer * num_tiles, (layer + 1) * num_tiles)
        def _(step):
            up_load(step).wait()

            @pl.when(step + 1 < num_steps)
            def _():
                up_load(step + 1).start()

            @pl.when(step > 1)
            def _():
                for copy in tile_stores(step - 2):
                    copy.wait()
            activate(step)
            for copy in tile_stores(step):
                copy.start()
            down_load(step).wait()

            @pl.when(step + 1 < num_steps)
            def _():
                down_load(step + 1).start()
            add_branch(step)

        normed_store.wait()
        if layer + 1 < num_layers:
            def to_next(rows, layer=layer):
                normalize(layer + 1, rows, next_rows(layer, rows))
                branch[rows, :] = jnp.zeros((NORM_ROWS, row_dim), jnp.float32)
            each_block(to_next)
            hid_store = pltpu.make_async_copy(hid, hid_out, io_sem.at[2])
            hid_store.start()
            normed_store = pltpu.make_async_copy(normed, normed_out.at[layer + 1], io_sem.at[1])
            normed_store.start()

    hid_store.wait()
    upstream_load.wait()
    bias_start = small_out.shape[1] - row_dim

    def top_rows(rows):
        top_f = next_rows(num_layers - 1, rows)
        top_scale = inverse_rms(top_f)
        top_hat = top_f * top_scale
        up_f = up_rows[rows, :].astype(jnp.float32)
        grad = top_scale * (up_f - top_hat * jnp.mean(up_f * top_hat, axis=-1, keepdims=True))
        branch[rows, :] = grad
        grad_b_buf[rows, :] = grad.astype(jnp.bfloat16)
        small_out[:, bias_start:bias_start + row_dim] += jnp.sum(grad, axis=0, keepdims=True)

    each_block(top_rows)
    grad_store = pltpu.make_async_copy(branch, grad_top_out, io_sem.at[0])
    grad_b_store = pltpu.make_async_copy(grad_b_buf, grad_top_b_out, io_sem.at[1])
    grad_store.start()
    grad_b_store.start()
    for back in (2, 1):
        for copy in tile_stores(jnp.int32(num_steps - back)):
            copy.wait()
    grad_store.wait()
    grad_b_store.wait()


def forward_pass(tokens, upstream, norm_gain, w_up, bias_up, w_down, bias_down, tile_cols):
    num_tokens, row_dim = tokens.shape
    num_layers, _, hidden = w_up.shape
    bf16, f32 = jnp.bfloat16, jnp.float32
    dma = pltpu.SemaphoreType.DMA
    any_spec = pl.BlockSpec(memory_space=pl.ANY)
    vmem_spec = pl.BlockSpec(memory_space=pltpu.VMEM)
    rows = (num_tokens, row_dim)
    wide = (num_layers, num_tokens, hidden)
    return pl.pallas_call(
        functools.partial(forward_kernel, (num_layers, hidden // tile_cols, tile_cols)),
        out_shape=(
            jax.ShapeDtypeStruct(rows, bf16),
            jax.ShapeDtypeStruct((num_layers,) + rows, bf16),
            jax.ShapeDtypeStruct(wide, bf16),
            jax.ShapeDtypeStruct(wide, bf16),
            jax.ShapeDtypeStruct(rows, f32),
            jax.ShapeDtypeStruct(rows, bf16),
            jax.ShapeDtypeStruct((1, num_layers * (2 * row_dim + hidden)), f32),
        ),
        in_specs=[any_spec] * 4 + [vmem_spec] * 3,
        out_specs=(any_spec,) * 6 + (vmem_spec,),
        scratch_shapes=[
            pltpu.VMEM(rows, bf16),
            pltpu.VMEM(rows, bf16),
            pltpu.VMEM(rows, f32),
            pltpu.VMEM((2, row_dim, tile_cols), bf16),
            pltpu.VMEM((2, tile_cols, row_dim), bf16),
            pltpu.VMEM((2, num_tokens, tile_cols), bf16),
            pltpu.VMEM((2, num_tokens, tile_cols), bf16),
            pltpu.VMEM(rows, bf16),
            pltpu.VMEM(rows, bf16),
            dma((4,)), dma((2,)), dma((2,)), dma((2,)), dma((2,)),
        ],
        compiler_params=pltpu.CompilerParams(vmem_limit_bytes=60 * 2**20),
        name="forward",
    )(tokens, upstream, w_up, w_down, norm_gain.astype(f32), bias_up.astype(f32), bias_down.astype(f32))


def gelu_slope(values):
    square = values * values
    bend = jnp.tanh(values * (GELU_SCALE + GELU_SCALE * GELU_CUBIC * square))
    return 0.5 * (1.0 + bend) + (0.5 * values) * (1.0 - bend * bend) * (GELU_SCALE + 3.0 * GELU_SCALE * GELU_CUBIC * square)


def backward_kernel(sizes, *refs):
    num_layers, chunks_per_mat, row_dim, chunk_cols, region, down_subs, axis = sizes
    num_mats = 2 * num_layers
    hidden_dim = chunks_per_mat * chunk_cols
    hid_refs, refs = refs[:num_layers], refs[num_layers:]
    (normed, pre_act, activated, grad_top, grad_top_b, w_up, w_down, gain_in, small_in,
     gathered, small_out, grad_pre_hbm, grad_b_hbm) = refs[:13]
    (rows_buf, cols_buf, sent_core, kept, recv_core, sent_1, sent_2, sent_3, recv_1, recv_2, recv_3, ring,
     weight_buf, pre_buf, grad_pre_buf, grad_b, grad_normed, hid_buf, grad_buf,
     small_recv, load_sem, grad_pre_sem, norm_sem, grad_b_sem, core_send, core_recv, out_send, out_recv, back_send, back_recv,
     share_send, share_recv, store_sem, small_send_sem, small_recv_sem) = refs[13:]
    small_width = 2 * row_dim + hidden_dim
    num_chunks = num_mats * chunks_per_mat
    half = COLORS * region
    me = lax.axis_index(axis)
    bits = [me % 2, (me // 2) % 2, (me // 4) % 2, me // 8]
    partners = [me + (1 << d) - 2 * (1 << d) * bits[d] for d in range(4)]
    core = bits[CORE]
    sent_bufs, recv_bufs = (sent_1, sent_2, sent_3), (recv_1, recv_2, recv_3)
    spans = (region // 2, region // 4, region // 8)

    def base(color, level):
        total = 0
        for step in range(level):
            total = total + bits[COLOR_DIMS[color][step]] * spans[step]
        return total

    def other(color, level):
        return base(color, level) + (1 - bits[COLOR_DIMS[color][level]]) * spans[level]

    def rows_at(start, size):
        return pl.ds(pl.multiple_of(start, spans[2]), size)

    def mat_loads(mat, chunk):
        slot = chunk % 2
        sub = chunk % chunks_per_mat
        layer = num_layers - 1 - mat // 2
        cols = pl.ds(pl.multiple_of(sub * chunk_cols, 128), chunk_cols)
        if mat % 2 == 0:
            rows = pl.ds(pl.multiple_of((sub // down_subs) * row_dim, 128), row_dim)
            return [
                pltpu.make_async_copy(activated.at[layer, :, rows], rows_buf.at[slot], load_sem.at[0, slot]),
                pltpu.make_async_copy(w_down.at[layer, cols, :], weight_buf.at[slot], load_sem.at[1, slot]),
                pltpu.make_async_copy(pre_act.at[layer, :, cols], pre_buf.at[slot], load_sem.at[2, slot]),
            ]
        copies = [pltpu.make_async_copy(normed.at[layer], rows_buf.at[slot], load_sem.at[0, slot])]
        for part in range(down_subs):
            copies.append(pltpu.make_async_copy(
                w_up.at[layer, part * chunk_cols:(part + 1) * chunk_cols, cols],
                weight_buf.at[slot, :, part * chunk_cols:(part + 1) * chunk_cols], load_sem.at[1 + part, slot]))
        return copies

    def cols_load(mat, chunk):
        sub = chunk % chunks_per_mat
        if mat % 2 == 0:
            source = grad_top_b if mat == 0 else grad_b_hbm
            source = source.at[:, pl.ds(pl.multiple_of((sub % down_subs) * chunk_cols, 128), chunk_cols)]
        else:
            source = grad_pre_hbm.at[sub]
        return pltpu.make_async_copy(source, cols_buf.at[chunk % 2], load_sem.at[3, chunk % 2])

    def for_mat(chunk, action):
        for mat in range(num_mats):
            @pl.when(chunk // chunks_per_mat == mat)
            def _(mat=mat):
                action(mat)

    def start_loads(chunk):
        def start(mat):
            for copy in mat_loads(mat, chunk):
                copy.start()
        for_mat(chunk, start)

    def grad_pre_store(sub):
        return pltpu.make_async_copy(grad_pre_buf, grad_pre_hbm.at[sub], grad_pre_sem)

    def core_copy(chunk):
        slot = chunk % RECV_SLOTS
        return pltpu.make_async_remote_copy(
            src_ref=sent_core, dst_ref=recv_core.at[slot], send_sem=core_send, recv_sem=core_recv.at[slot],
            device_id=(partners[CORE],), device_id_type=MESH)

    def out_copy(level, color, chunk):
        slot = chunk % RECV_SLOTS
        return pltpu.make_async_remote_copy(
            src_ref=sent_bufs[level].at[color], dst_ref=recv_bufs[level].at[slot, color],
            send_sem=out_send.at[level, color], recv_sem=out_recv.at[level, color, slot],
            device_id=(partners[COLOR_DIMS[color][level]],), device_id_type=MESH)

    def back_copy(level, color, chunk, arriving):
        slot = chunk % GATHER_SLOTS
        mine = ring.at[slot, core, color, rows_at(base(color, level + 1), spans[level]), :]
        theirs = ring.at[slot, core, color, rows_at(other(color, level), spans[level]), :]
        return pltpu.make_async_remote_copy(
            src_ref=mine, dst_ref=theirs if arriving else mine,
            send_sem=back_send.at[level, color, slot], recv_sem=back_recv.at[level, color, slot],
            device_id=(partners[COLOR_DIMS[color][level]],), device_id_type=MESH)

    def share_copy(chunk, arriving):
        slot = chunk % GATHER_SLOTS
        return pltpu.make_async_remote_copy(
            src_ref=ring.at[slot, core], dst_ref=ring.at[slot, 1 - core if arriving else core],
            send_sem=share_send.at[slot], recv_sem=share_recv.at[slot],
            device_id=(partners[CORE],), device_id_type=MESH)

    def store_copy(chunk):
        slot = chunk % GATHER_SLOTS
        return pltpu.make_async_copy(ring.at[slot], gathered.at[chunk], store_sem.at[slot])

    def small_copy(step):
        return pltpu.make_async_remote_copy(
            src_ref=small_out, dst_ref=small_recv.at[step], send_sem=small_send_sem.at[step],
            recv_sem=small_recv_sem.at[step], device_id=(partners[step],), device_id_type=MESH)

    def product(chunk, which_core, color):
        slot = chunk % 2
        start = pl.multiple_of(which_core * half + color * region, 128)
        return lax.dot_general(
            rows_buf[slot, :, pl.ds(start, region)], cols_buf[slot], TOKEN_DIMS, preferred_element_type=jnp.float32)

    def load(chunk):
        def arrive(mat):
            for copy in mat_loads(mat, chunk):
                copy.wait()
        for_mat(chunk, arrive)
        for_mat(chunk, lambda mat: cols_load(mat, chunk).wait())

        @pl.when(chunk + 1 < num_chunks)
        def _():
            start_loads(chunk + 1)

        before = chunk - 1

        @pl.when((before >= 0) & ((before // chunks_per_mat) % 2 == 0))
        def _():
            grad_pre_store(before % chunks_per_mat).wait()

    def load_cols(chunk):
        @pl.when(chunk + 1 < num_chunks)
        def _():
            for_mat(chunk + 1, lambda mat: cols_load(mat, chunk + 1).start())

    def compute_sent(chunk):
        @pl.loop(0, COLORS)
        def _(color):
            sent_core[color] = product(chunk, 1 - core, color).astype(jnp.bfloat16)
        core_copy(chunk).start()

    def compute_kept(chunk):
        slot = chunk % KEPT_SLOTS

        @pl.loop(0, COLORS)
        def _(color):
            kept[slot, color] = product(chunk, core, color)

    def halve(level, chunk, arrived):
        slot = chunk % KEPT_SLOTS
        recv_slot = chunk % RECV_SLOTS
        for color in range(COLORS):
            if level > 0:
                out_copy(level - 1, color, chunk).wait()
            held = base(color, level)

            def total(start, size, color=color, held=held):
                own = kept[slot, color, rows_at(start, size), :]
                return own + arrived[recv_slot, color, rows_at(start - held, size), :].astype(jnp.float32)

            if level < 3:
                mine = base(color, level + 1)
                sent_bufs[level][color] = total(other(color, level), spans[level]).astype(jnp.bfloat16)
                kept[slot, color, rows_at(mine, spans[level]), :] = total(mine, spans[level])
                out_copy(level, color, chunk).start()
            else:
                gather_slot = chunk % GATHER_SLOTS
                ring[gather_slot, core, color, rows_at(held, spans[2]), :] = total(held, spans[2]).astype(jnp.bfloat16)
                back_copy(2, color, chunk, False).start()

    def send_1(chunk):
        core_copy(chunk).wait()
        halve(0, chunk, recv_core)

    def send_2(chunk):
        halve(1, chunk, recv_1)

    def send_3(chunk):
        halve(2, chunk, recv_2)

    def send_back_3(chunk):
        halve(3, chunk, recv_3)

    def pass_back(level, chunk):
        for color in range(COLORS):
            back_copy(level + 1, color, chunk, True).wait()
            back_copy(level, color, chunk, False).start()

    def send_back_2(chunk):
        pass_back(1, chunk)

    def send_back_1(chunk):
        pass_back(0, chunk)

    def send_back_core(chunk):
        for color in range(COLORS):
            back_copy(0, color, chunk, True).wait()
        share_copy(chunk, False).start()

    def store(chunk):
        share_copy(chunk, True).wait()
        store_copy(chunk).start()

        @pl.when(chunk > 0)
        def _():
            store_copy(chunk - 1).wait()

    token_half = grad_b.shape[0] // 2

    def backward(part, chunk):
        slot = chunk % 2
        sub = chunk % chunks_per_mat
        mat = chunk // chunks_per_mat
        layer = num_layers - 1 - mat // 2

        @pl.when(mat % 2 == 0)
        def _():
            cols = slice(part * TILE, (part + 1) * TILE)

            @pl.loop(0, 2)
            def _(which):
                rows = pl.ds(pl.multiple_of(which * token_half, 128), token_half)
                grad_act = lax.dot_general(
                    grad_b[rows, :], weight_buf[slot, cols, :], FEATURE_DIMS, preferred_element_type=jnp.float32)
                grad_pre = grad_act * gelu_slope(pre_buf[slot, rows, cols].astype(jnp.float32))
                grad_pre_buf[rows, cols] = grad_pre.astype(jnp.bfloat16)
                start = layer * small_width + row_dim + sub * chunk_cols + part * TILE
                small_out[:, pl.ds(pl.multiple_of(start, 128), TILE)] += jnp.sum(grad_pre, axis=0, keepdims=True)

            if part == chunk_cols // TILE - 1:
                grad_pre_store(sub).start()

        @pl.when(mat % 2 == 1)
        def _():
            @pl.loop(0, 2 * down_subs)
            def _(step):
                rows = pl.ds(pl.multiple_of((step % 2) * token_half, 128), token_half)
                piece = part * down_subs + step // 2
                tiles = chunk_cols // TILE
                weight_rows = pl.ds(pl.multiple_of((piece % tiles) * TILE, TILE), TILE)
                weight_cols = pl.ds(pl.multiple_of((piece // tiles) * chunk_cols, 128), chunk_cols)
                out_cols = pl.ds(pl.multiple_of(piece * TILE, 128), TILE)
                grad_normed[rows, out_cols] += lax.dot_general(
                    cols_buf[slot, rows, :], weight_buf[slot, weight_rows, weight_cols], FEATURE_DIMS,
                    preferred_element_type=jnp.float32)

    def norm_loads(layer, block):
        rows = pl.ds(pl.multiple_of(block * NORM_ROWS, NORM_ROWS), NORM_ROWS)
        slot = block % 2
        copies = [pltpu.make_async_copy(hid_refs[layer].at[rows, :], hid_buf.at[slot], norm_sem.at[0, slot])]
        if layer > 0:
            copies.append(pltpu.make_async_copy(grad_top.at[rows, :], grad_buf.at[slot], norm_sem.at[1, slot]))
        return copies

    def layer_input_grad(layer):
        num_blocks = grad_b.shape[0] // NORM_ROWS
        offset = layer * small_width
        for copy in norm_loads(layer, 0):
            copy.start()

        @pl.loop(0, num_blocks)
        def _(block):
            @pl.when(block + 1 < num_blocks)
            def _():
                for copy in norm_loads(layer, block + 1):
                    copy.start()
            for copy in norm_loads(layer, block):
                copy.wait()
            rows = pl.ds(pl.multiple_of(block * NORM_ROWS, NORM_ROWS), NORM_ROWS)
            hid_f = hid_buf[block % 2].astype(jnp.float32)
            hid_scale = inverse_rms(hid_f)
            hid_hat = hid_f * hid_scale
            normed_grad = grad_normed[rows, :]
            small_out[:, offset:offset + row_dim] += jnp.sum(normed_grad * hid_hat, axis=0, keepdims=True)
            if layer > 0:
                grad_normed[rows, :] = jnp.zeros((NORM_ROWS, row_dim), jnp.float32)
                grad_hat = normed_grad * gain_in[layer:layer + 1, :]
                grad_new = grad_buf[block % 2] + hid_scale * (
                    grad_hat - hid_hat * jnp.mean(grad_hat * hid_hat, axis=-1, keepdims=True))
                grad_b[rows, :] = grad_new.astype(jnp.bfloat16)
                bias_start = offset - row_dim
                small_out[:, bias_start:bias_start + row_dim] += jnp.sum(grad_new, axis=0, keepdims=True)
        if layer > 0:
            copy = pltpu.make_async_copy(grad_b, grad_b_hbm, grad_b_sem)
            copy.start()
            copy.wait()

    def input_grad(chunk):
        for layer in range(num_layers):
            last = (num_layers - 1 - layer) * 2 * chunks_per_mat + 2 * chunks_per_mat - 1

            @pl.when(chunk == last)
            def _(layer=layer):
                layer_input_grad(layer)

    events = dict(
        load=load, compute_sent=compute_sent, compute_kept=compute_kept, send_1=send_1, send_2=send_2, send_3=send_3,
        send_back_3=send_back_3, send_back_2=send_back_2, send_back_1=send_back_1, send_back_core=send_back_core, store=store,
        backward_0=functools.partial(backward, 0), backward_1=functools.partial(backward, 1),
        backward_2=functools.partial(backward, 2), input_grad=input_grad, load_cols=load_cols)

    first = jnp.int32(0)
    for copy in mat_loads(0, first):
        copy.start()
    cols_load(0, first).start()
    grad_b_copy = pltpu.make_async_copy(grad_top_b, grad_b, grad_b_sem)
    grad_b_copy.start()
    barrier = pltpu.get_barrier_semaphore()
    for partner in partners:
        pl.semaphore_signal(barrier, inc=1, device_id=(partner,), device_id_type=MESH)
    small_out[...] = small_in[...]
    grad_normed[...] = jnp.zeros_like(grad_normed)
    grad_b_copy.wait()
    pl.semaphore_wait(barrier, 4)

    @pl.loop(0, num_chunks + MAX_LAG)
    def _(it):
        for step in range(4):
            @pl.when(it == num_chunks + step)
            def _(step=step):
                small_copy(step).start()
        for name, lag in PIPELINE:
            chunk = it - lag

            @pl.when((chunk >= 0) & (chunk < num_chunks))
            def _(name=name, chunk=chunk):
                events[name](chunk)
        for step in range(4):
            @pl.when(it == num_chunks + step)
            def _(step=step):
                small_copy(step).wait()
                small_out[...] += small_recv[step]

    store_copy(jnp.int32(num_chunks - 1)).wait()


def backward_pass(hid_rows, saved, grad_top, grad_top_b, norm_gain, w_up, w_down, small, axis, chunk_cols):
    num_layers, row_dim, hidden = w_up.shape
    tokens = grad_top.shape[0]
    chunks_per_mat = hidden // chunk_cols
    region = row_dim // (2 * COLORS)
    half = (COLORS, region, chunk_cols)
    sizes = (num_layers, chunks_per_mat, row_dim, chunk_cols, region, row_dim // chunk_cols, axis)
    num_chunks = 2 * num_layers * chunks_per_mat
    bf16, f32 = jnp.bfloat16, jnp.float32
    small_width = 2 * row_dim + hidden
    dma = pltpu.SemaphoreType.DMA
    any_spec = pl.BlockSpec(memory_space=pl.ANY)
    vmem_spec = pl.BlockSpec(memory_space=pltpu.VMEM)
    gathered, small_sum, _, _ = pl.pallas_call(
        functools.partial(backward_kernel, sizes),
        out_shape=(
            jax.ShapeDtypeStruct((num_chunks, 2) + half, bf16),
            jax.ShapeDtypeStruct(small.shape, f32),
            jax.ShapeDtypeStruct((chunks_per_mat, tokens, chunk_cols), bf16),
            jax.ShapeDtypeStruct((tokens, row_dim), bf16),
        ),
        in_specs=[any_spec] * (num_layers + 7) + [vmem_spec] * 2,
        out_specs=(any_spec, vmem_spec, any_spec, any_spec),
        scratch_shapes=[
            pltpu.VMEM((2, tokens, row_dim), bf16),
            pltpu.VMEM((2, tokens, chunk_cols), bf16),
            pltpu.VMEM(half, bf16),
            pltpu.VMEM((KEPT_SLOTS,) + half, f32),
            pltpu.VMEM((RECV_SLOTS,) + half, bf16),
            pltpu.VMEM((COLORS, region // 2, chunk_cols), bf16),
            pltpu.VMEM((COLORS, region // 4, chunk_cols), bf16),
            pltpu.VMEM((COLORS, region // 8, chunk_cols), bf16),
            pltpu.VMEM((RECV_SLOTS, COLORS, region // 2, chunk_cols), bf16),
            pltpu.VMEM((RECV_SLOTS, COLORS, region // 4, chunk_cols), bf16),
            pltpu.VMEM((RECV_SLOTS, COLORS, region // 8, chunk_cols), bf16),
            pltpu.VMEM((GATHER_SLOTS, 2) + half, bf16),
            pltpu.VMEM((2, chunk_cols, row_dim), bf16),
            pltpu.VMEM((2, tokens, chunk_cols), bf16),
            pltpu.VMEM((tokens, chunk_cols), bf16),
            pltpu.VMEM((tokens, row_dim), bf16),
            pltpu.VMEM((tokens, row_dim), f32),
            pltpu.VMEM((2, NORM_ROWS, row_dim), bf16),
            pltpu.VMEM((2, NORM_ROWS, row_dim), f32),
            pltpu.VMEM((4,) + small.shape, f32),
            dma((4, 2)), dma, dma((2, 2)), dma,
            dma, dma((RECV_SLOTS,)), dma((3, COLORS)), dma((3, COLORS, RECV_SLOTS)),
            dma((3, COLORS, GATHER_SLOTS)), dma((3, COLORS, GATHER_SLOTS)), dma((GATHER_SLOTS,)), dma((GATHER_SLOTS,)),
            dma((GATHER_SLOTS,)), dma((4,)), dma((4,)),
        ],
        compiler_params=pltpu.CompilerParams(collective_id=0, has_side_effects=True, vmem_limit_bytes=67043328),
        name="backward",
    )(*hid_rows, *saved, grad_top, grad_top_b, w_up, w_down, norm_gain.astype(f32), small)
    return gathered, small_sum.reshape(num_layers, small_width)


def widen_kernel(chunk_ref, out_ref):
    out_ref[0] = chunk_ref[0].astype(jnp.float32)


def widen(gathered, num_layers, row_dim, hidden, chunk_cols):
    per_mat = hidden // chunk_cols
    num_mats = 2 * num_layers
    down_subs = row_dim // chunk_cols
    chunks = gathered.reshape(num_mats * per_mat, row_dim, chunk_cols)

    def mat_of(layer, kind):
        return (num_layers - 1 - layer) * 2 + kind

    block = (1, row_dim, chunk_cols)
    up = pl.pallas_call(
        widen_kernel,
        grid=(num_layers, per_mat),
        in_specs=[pl.BlockSpec(block, lambda layer, sub: (mat_of(layer, 1) * per_mat + sub, 0, 0))],
        out_specs=pl.BlockSpec(block, lambda layer, sub: (layer, 0, sub)),
        out_shape=jax.ShapeDtypeStruct((num_layers, row_dim, hidden), jnp.float32),
        name="widen_up",
    )(chunks)
    down = pl.pallas_call(
        widen_kernel,
        grid=(num_layers, per_mat),
        in_specs=[pl.BlockSpec(block, lambda layer, sub: (mat_of(layer, 0) * per_mat + sub, 0, 0))],
        out_specs=pl.BlockSpec(block, lambda layer, sub: (layer, sub // down_subs, sub % down_subs)),
        out_shape=jax.ShapeDtypeStruct((num_layers, hidden, row_dim), jnp.float32),
        name="widen_down",
    )(chunks)
    return up, down


def solution(mesh):
    axis = mesh.axis_names[0]

    def device_grads(tokens, upstream, norm_gain, w_up, bias_up, w_down, bias_down):
        num_layers, width = norm_gain.shape
        hidden_width = w_up.shape[2]
        chunk_cols = width // 2
        hid_1, normed, pre_act, activated, grad_top, grad_top_b, small = forward_pass(
            tokens, upstream, norm_gain, w_up, bias_up, w_down, bias_down, width)
        gathered, small = backward_pass(
            (tokens, hid_1), (normed, pre_act, activated), grad_top, grad_top_b, norm_gain, w_up, w_down, small, axis, chunk_cols)
        up_full, down_full = widen(gathered, num_layers, width, hidden_width, chunk_cols)
        return (small[:, :width], up_full, small[:, width:width + hidden_width], down_full, small[:, width + hidden_width:])

    row_spec = P(axis, None)
    full_spec = P()
    return jax.shard_map(
        device_grads,
        mesh=mesh,
        in_specs=(row_spec, row_spec, full_spec, full_spec, full_spec, full_spec, full_spec),
        out_specs=(full_spec, full_spec, full_spec, full_spec, full_spec),
        check_vma=False,
    )
```

```python
import functools

import jax
import jax.numpy as jnp
from jax import lax
from jax.experimental import pallas as pl
from jax.experimental.pallas import tpu as pltpu
from jax.sharding import PartitionSpec as P


EPSILON = 1e-6
TOKEN_DIMS = (((0,), (0,)), ((), ()))
FEATURE_DIMS = (((1,), (1,)), ((), ()))
MESH = pl.DeviceIdType.MESH
COLORS = 3
CORE, DIM_X, DIM_Y, DIM_Z = range(4)
COLOR_DIMS = ((DIM_X, DIM_Y, DIM_Z), (DIM_Y, DIM_Z, DIM_X), (DIM_Z, DIM_X, DIM_Y))
PIPELINE = (
    ("send_back_2", 4), ("load", 0), ("compute_sent", 0), ("send_back_3", 3), ("send_back_core", 6), ("share_core", 0),
    ("send_3", 2), ("compute_kept", 0), ("load_weights", 0), ("backward_0", 0), ("send_back_1", 5), ("store", 6), ("send_2", 1),
    ("backward_1", 0), ("send_1", 0), ("backward_2", 0), ("input_grad", 0),
)
MAX_LAG = 6
PART_GROUPS = (8, 4, 4)
RECV_SLOTS = 2
KEPT_SLOTS = 3
GATHER_SLOTS = 6
TILE = 256
UP_COLS = 512
ACT_ROWS = 16
ACT_COLS = 256
STREAM_SLOTS = 4
NORM_ROWS = 128
GELU_SCALE = 0.7978845608028654
GELU_CUBIC = 0.044715


def inverse_rms(hid_f):
    return lax.rsqrt(jnp.mean(hid_f * hid_f, axis=-1, keepdims=True) + EPSILON)


def gelu(values):
    return (0.5 * values) * (1.0 + jnp.tanh(values * (GELU_SCALE + GELU_SCALE * GELU_CUBIC * (values * values))))


def forward_kernel(
    sizes, tokens, upstream, w_up, w_down, gain_in, bias_up_in, bias_down_in, hid_out, normed_out, pre_act_out, act_out,
    grad_top_out, grad_top_b_out, small_out, hid, normed, branch, up_buf, down_buf, pre_buf, act_buf, up_rows, grad_b_buf,
    gain, bias_up, bias_down, io_sem, up_sem, down_sem, pre_sem, act_sem,
):
    num_layers, num_tiles, tile_cols = sizes
    num_tokens, row_dim = hid.shape
    steps = num_tiles + 1
    parts = tile_cols // UP_COLS

    def up_load(layer, tile):
        cols = pl.ds(pl.multiple_of(tile * tile_cols, 128), tile_cols)
        return pltpu.make_async_copy(w_up.at[layer, :, cols], up_buf.at[tile % 2], up_sem.at[tile % 2])

    def down_load(layer, tile):
        rows = pl.ds(pl.multiple_of(tile * tile_cols, 128), tile_cols)
        return pltpu.make_async_copy(w_down.at[layer, rows, :], down_buf.at[tile % 2], down_sem.at[tile % 2])

    def pre_store(layer, tile):
        cols = pl.ds(pl.multiple_of(tile * tile_cols, 128), tile_cols)
        return pltpu.make_async_copy(pre_buf.at[tile % 2], pre_act_out.at[layer, :, cols], pre_sem.at[tile % 2])

    def act_store(layer, tile):
        cols = pl.ds(pl.multiple_of(tile * tile_cols, 128), tile_cols)
        return pltpu.make_async_copy(act_buf.at[tile % 2], act_out.at[layer, :, cols], act_sem.at[tile % 2])

    def normed_store(layer):
        return pltpu.make_async_copy(normed, normed_out.at[layer], io_sem.at[1])

    def hid_store():
        return pltpu.make_async_copy(hid, hid_out, io_sem.at[2])

    tokens_load = pltpu.make_async_copy(tokens, hid, io_sem.at[0])
    tokens_load.start()
    up_load(0, 0).start()
    down_load(0, 0).start()
    upstream_load = pltpu.make_async_copy(upstream, up_rows, io_sem.at[3])
    upstream_load.start()
    small_out[...] = jnp.zeros_like(small_out)
    gain[...] = gain_in[...].astype(jnp.float32)
    bias_up[...] = bias_up_in[...].astype(jnp.float32)
    bias_down[...] = bias_down_in[...].astype(jnp.float32)
    tokens_load.wait()

    def each_block(action):
        @pl.loop(0, num_tokens // NORM_ROWS)
        def _(block):
            action(pl.ds(pl.multiple_of(block * NORM_ROWS, NORM_ROWS), NORM_ROWS))

    def normalize(layer, rows, hid_f):
        normed[rows, :] = ((hid_f * inverse_rms(hid_f)) * gain[pl.ds(layer, 1), :]).astype(jnp.bfloat16)

    def next_rows(layer, rows):
        new = ((hid[rows, :].astype(jnp.float32) + branch[rows, :]) + bias_down[pl.ds(layer, 1), :]).astype(jnp.bfloat16)
        hid[rows, :] = new
        return new.astype(jnp.float32)

    def activate(slot, part):
        start = part * UP_COLS
        for row in range(0, num_tokens, ACT_ROWS):
            for col in range(0, UP_COLS, ACT_COLS):
                piece = (slot, pl.ds(row, ACT_ROWS), pl.ds(pl.multiple_of(start + col, 128), ACT_COLS))
                act_buf[piece] = gelu(pre_buf[piece].astype(jnp.float32)).astype(jnp.bfloat16)

    def up_product(layer, tile):
        @pl.loop(0, parts)
        def _(part):
            fresh = tile * parts + part == 0
            last_slot = jnp.where((part == 0) & (tile > 0), (tile + 1) % 2, tile % 2)
            activate(last_slot, jnp.where(fresh, 0, (part + parts - 1) % parts))
            cols = pl.ds(pl.multiple_of(part * UP_COLS, 128), UP_COLS)
            bias = bias_up[pl.ds(layer, 1), pl.ds(pl.multiple_of(tile * tile_cols + part * UP_COLS, 128), UP_COLS)]
            pre_buf[tile % 2, :, cols] = (
                jnp.dot(normed[...], up_buf[tile % 2, :, cols], preferred_element_type=jnp.float32) + bias
            ).astype(jnp.bfloat16)

    def down_product(tile):
        slot = tile % 2
        for part in range(row_dim // UP_COLS):
            cols = slice(part * UP_COLS, (part + 1) * UP_COLS)
            branch[:, cols] += jnp.dot(act_buf[slot], down_buf[slot, :, cols], preferred_element_type=jnp.float32)

    pre_buf[0, :, :UP_COLS] = jnp.zeros((num_tokens, UP_COLS), jnp.bfloat16)
    each_block(lambda rows: normalize(0, rows, hid[rows, :].astype(jnp.float32)))
    normed_store(0).start()
    branch[...] = jnp.zeros_like(branch)

    @pl.loop(0, num_layers * steps)
    def _(step):
        layer, tile = step // steps, step % steps

        @pl.when(tile < num_tiles)
        def _():
            up_load(layer, tile).wait()

            @pl.when(tile + 1 < num_tiles)
            def _():
                up_load(layer, tile + 1).start()

            @pl.when((tile == num_tiles - 1) & (layer + 1 < num_layers))
            def _():
                up_load(layer + 1, 0).start()

            @pl.when(tile > 1)
            def _():
                pre_store(layer, tile - 2).wait()
                act_store(layer, tile - 2).wait()

            up_product(layer, tile)
            pre_store(layer, tile).start()

        @pl.when(tile == num_tiles)
        def _():
            activate((num_tiles - 1) % 2, parts - 1)

        @pl.when(tile > 0)
        def _():
            act_store(layer, tile - 1).start()
            down_load(layer, tile - 1).wait()

            @pl.when(tile < num_tiles)
            def _():
                down_load(layer, tile).start()

            @pl.when((tile == num_tiles) & (layer + 1 < num_layers))
            def _():
                down_load(layer + 1, 0).start()

            down_product(tile - 1)

        @pl.when(tile == num_tiles)
        def _():
            for back in (2, 1):
                pre_store(layer, num_tiles - back).wait()
                act_store(layer, num_tiles - back).wait()
            normed_store(layer).wait()

            @pl.when(layer + 1 < num_layers)
            def _():
                def to_next(rows):
                    normalize(layer + 1, rows, next_rows(layer, rows))
                    branch[rows, :] = jnp.zeros((NORM_ROWS, row_dim), jnp.float32)

                each_block(to_next)
                hid_store().start()
                normed_store(layer + 1).start()

    hid_store().wait()
    upstream_load.wait()
    bias_start = small_out.shape[1] - row_dim

    def grad_stores(rows):
        return (
            pltpu.make_async_copy(branch.at[rows, :], grad_top_out.at[rows, :], io_sem.at[0]),
            pltpu.make_async_copy(grad_b_buf.at[rows, :], grad_top_b_out.at[rows, :], io_sem.at[1]),
        )

    def top_rows(rows):
        top_f = next_rows(num_layers - 1, rows)
        top_scale = inverse_rms(top_f)
        top_hat = top_f * top_scale
        up_f = up_rows[rows, :].astype(jnp.float32)
        grad = top_scale * (up_f - top_hat * jnp.mean(up_f * top_hat, axis=-1, keepdims=True))
        branch[rows, :] = grad
        grad_b_buf[rows, :] = grad.astype(jnp.bfloat16)
        small_out[num_layers - 1:, bias_start:] += jnp.sum(grad, axis=0, keepdims=True)
        for copy in grad_stores(rows):
            copy.start()

    each_block(top_rows)
    for copy in grad_stores(pl.ds(0, num_tokens)):
        copy.wait()


def forward_pass(tokens, upstream, norm_gain, w_up, bias_up, w_down, bias_down, tile_cols):
    num_tokens, row_dim = tokens.shape
    num_layers, _, hidden = w_up.shape
    bf16, f32 = jnp.bfloat16, jnp.float32
    dma = pltpu.SemaphoreType.DMA
    any_spec = pl.BlockSpec(memory_space=pl.ANY)
    vmem_spec = pl.BlockSpec(memory_space=pltpu.VMEM)
    rows = (num_tokens, row_dim)
    wide = (num_layers, num_tokens, hidden)
    return pl.pallas_call(
        functools.partial(forward_kernel, (num_layers, hidden // tile_cols, tile_cols)),
        out_shape=(
            jax.ShapeDtypeStruct(rows, bf16),
            jax.ShapeDtypeStruct((num_layers,) + rows, bf16),
            jax.ShapeDtypeStruct(wide, bf16),
            jax.ShapeDtypeStruct(wide, bf16),
            jax.ShapeDtypeStruct(rows, f32),
            jax.ShapeDtypeStruct(rows, bf16),
            jax.ShapeDtypeStruct((num_layers, 2 * row_dim + hidden), f32),
        ),
        in_specs=[any_spec] * 4 + [vmem_spec] * 3,
        out_specs=(any_spec,) * 6 + (vmem_spec,),
        scratch_shapes=[
            pltpu.VMEM(rows, bf16),
            pltpu.VMEM(rows, bf16),
            pltpu.VMEM(rows, f32),
            pltpu.VMEM((2, row_dim, tile_cols), bf16),
            pltpu.VMEM((2, tile_cols, row_dim), bf16),
            pltpu.VMEM((2, num_tokens, tile_cols), bf16),
            pltpu.VMEM((2, num_tokens, tile_cols), bf16),
            pltpu.VMEM(rows, bf16),
            pltpu.VMEM(rows, bf16),
            pltpu.VMEM((num_layers, row_dim), f32),
            pltpu.VMEM((num_layers, hidden), f32),
            pltpu.VMEM((num_layers, row_dim), f32),
            dma((4,)), dma((2,)), dma((2,)), dma((2,)), dma((2,)),
        ],
        compiler_params=pltpu.CompilerParams(vmem_limit_bytes=60 * 2**20),
        name="forward",
    )(tokens, upstream, w_up, w_down, norm_gain, bias_up, bias_down)


def gelu_slope(values):
    square = values * values
    bend = jnp.tanh(values * (GELU_SCALE + GELU_SCALE * GELU_CUBIC * square))
    return 0.5 * (1.0 + bend) + (0.5 * values) * (1.0 - bend * bend) * (GELU_SCALE + 3.0 * GELU_SCALE * GELU_CUBIC * square)


def backward_kernel(sizes, *refs):
    num_layers, chunks_per_mat, row_dim, chunk_cols, region, down_subs, axis = sizes
    num_mats = 2 * num_layers
    hidden_dim = chunks_per_mat * chunk_cols
    hid_refs, refs = refs[:num_layers], refs[num_layers:]
    (normed, pre_act, activated, grad_top, grad_top_b, w_up, w_down, gain_in, small_in,
     gathered, small_out, grad_pre_hbm, grad_b_hbm) = refs[:13]
    part_count = 2 * COLORS * len(PART_GROUPS)
    part_refs, refs = refs[13:13 + part_count], refs[13 + part_count:]
    (rows_buf, cols_buf, sent_core, kept, recv_core, sent_1, sent_2, sent_3, recv_1, recv_2, recv_3, ring,
     weight_buf, pre_buf, grad_pre_buf, grad_b, grad_normed, hid_buf, grad_buf,
     small_recv, load_sem, grad_pre_sem, norm_sem, grad_b_sem, core_send, core_recv, out_send, out_recv, back_send, back_recv,
     share_send, share_recv, store_sem, small_send_sem, small_recv_sem, part_sem) = refs
    num_chunks = num_mats * chunks_per_mat
    full_chunks = num_chunks - sum(PART_GROUPS)
    half = COLORS * region
    me = lax.axis_index(axis)
    bits = [me % 2, (me // 2) % 2, (me // 4) % 2, me // 8]
    partners = [me + (1 << d) - 2 * (1 << d) * bits[d] for d in range(4)]
    core = bits[CORE]
    sent_bufs, recv_bufs = (sent_1, sent_2, sent_3), (recv_1, recv_2, recv_3)
    spans = (region // 2, region // 4, region // 8)

    def base(color, level):
        total = 0
        for step in range(level):
            total = total + bits[COLOR_DIMS[color][step]] * spans[step]
        return total

    def other(color, level):
        return base(color, level) + (1 - bits[COLOR_DIMS[color][level]]) * spans[level]

    def rows_at(start, size):
        return pl.ds(pl.multiple_of(start, spans[2]), size)

    def rows_load(mat, chunk):
        layer = num_layers - 1 - mat // 2
        if mat % 2 == 0:
            start = ((chunk % chunks_per_mat) // down_subs) * row_dim
            source = activated.at[layer, :, pl.ds(pl.multiple_of(start, 128), row_dim)]
        else:
            source = normed.at[layer]
        return pltpu.make_async_copy(source, rows_buf.at[chunk % 2], load_sem.at[0, chunk % 2])

    def weight_loads(mat, chunk):
        slot = chunk % 2
        layer = num_layers - 1 - mat // 2
        cols = pl.ds(pl.multiple_of((chunk % chunks_per_mat) * chunk_cols, 128), chunk_cols)
        if mat % 2 == 0:
            return [
                pltpu.make_async_copy(w_down.at[layer, cols, :], weight_buf.at[slot], load_sem.at[1, slot]),
                pltpu.make_async_copy(pre_act.at[layer, :, cols], pre_buf.at[slot], load_sem.at[2, slot]),
            ]
        return [
            pltpu.make_async_copy(
                w_up.at[layer, part * chunk_cols:(part + 1) * chunk_cols, cols],
                weight_buf.at[slot, :, part * chunk_cols:(part + 1) * chunk_cols], load_sem.at[1 + part, slot])
            for part in range(down_subs)
        ]

    def cols_load(mat, chunk):
        sub = chunk % chunks_per_mat
        if mat % 2 == 0:
            source = grad_top_b if mat == 0 else grad_b_hbm
            source = source.at[:, pl.ds(pl.multiple_of((sub % down_subs) * chunk_cols, 128), chunk_cols)]
        else:
            source = grad_pre_hbm.at[sub]
        return pltpu.make_async_copy(source, cols_buf.at[chunk % 2], load_sem.at[3, chunk % 2])

    def for_mat(chunk, action):
        for mat in range(num_mats):
            @pl.when(chunk // chunks_per_mat == mat)
            def _(mat=mat):
                action(mat)

    def grad_pre_store(sub):
        return pltpu.make_async_copy(grad_pre_buf, grad_pre_hbm.at[sub], grad_pre_sem)

    def core_copy(chunk):
        slot = chunk % RECV_SLOTS
        return pltpu.make_async_remote_copy(
            src_ref=sent_core, dst_ref=recv_core.at[slot], send_sem=core_send, recv_sem=core_recv.at[slot],
            device_id=(partners[CORE],), device_id_type=MESH)

    def out_copy(level, color, chunk):
        slot = chunk % RECV_SLOTS
        return pltpu.make_async_remote_copy(
            src_ref=sent_bufs[level].at[color], dst_ref=recv_bufs[level].at[slot, color],
            send_sem=out_send.at[level, color], recv_sem=out_recv.at[level, color, slot],
            device_id=(partners[COLOR_DIMS[color][level]],), device_id_type=MESH)

    def back_copy(level, color, chunk, arriving):
        slot = chunk % GATHER_SLOTS
        mine = ring.at[slot, core, color, rows_at(base(color, level + 1), spans[level]), :]
        theirs = ring.at[slot, core, color, rows_at(other(color, level), spans[level]), :]
        return pltpu.make_async_remote_copy(
            src_ref=mine, dst_ref=theirs if arriving else mine,
            send_sem=back_send.at[level, color, slot], recv_sem=back_recv.at[level, color, slot],
            device_id=(partners[COLOR_DIMS[color][level]],), device_id_type=MESH)

    def part_rows(color):
        return rows_at(base(color, 1), spans[0])

    def part_share_copy(color, chunk, arriving):
        slot = chunk % GATHER_SLOTS
        mine = ring.at[slot, core, color, part_rows(color), :]
        theirs = ring.at[slot, 1 - core, color, part_rows(color), :]
        return pltpu.make_async_remote_copy(
            src_ref=mine, dst_ref=theirs if arriving else mine,
            send_sem=back_send.at[0, color, slot], recv_sem=back_recv.at[0, color, slot],
            device_id=(partners[CORE],), device_id_type=MESH)

    def part_stores(group, chunk):
        slot = chunk % GATHER_SLOTS
        place = chunk - full_chunks - sum(PART_GROUPS[:group])
        copies = []
        for color in range(COLORS):
            for which in range(2):
                out_ref = part_refs[(group * COLORS + color) * 2 + which]
                source = ring.at[slot, core if which == 0 else 1 - core, color, part_rows(color), :]
                copies.append(pltpu.make_async_copy(
                    source, out_ref.at[place], part_sem.at[color, which, slot]))
        return copies

    def share_copy(chunk, arriving):
        slot = chunk % GATHER_SLOTS
        return pltpu.make_async_remote_copy(
            src_ref=ring.at[slot, core], dst_ref=ring.at[slot, 1 - core if arriving else core],
            send_sem=share_send.at[slot], recv_sem=share_recv.at[slot],
            device_id=(partners[CORE],), device_id_type=MESH)

    def store_copy(chunk):
        slot = chunk % GATHER_SLOTS
        return pltpu.make_async_copy(ring.at[slot], gathered.at[chunk], store_sem.at[slot])

    def small_copy(step):
        return pltpu.make_async_remote_copy(
            src_ref=small_out, dst_ref=small_recv.at[step], send_sem=small_send_sem.at[step],
            recv_sem=small_recv_sem.at[step], device_id=(partners[step],), device_id_type=MESH)

    def product(chunk, which_core, color):
        slot = chunk % 2
        start = pl.multiple_of(which_core * half + color * region, 128)
        return lax.dot_general(
            rows_buf[slot, :, pl.ds(start, region)], cols_buf[slot], TOKEN_DIMS, preferred_element_type=jnp.float32)

    def opens_layer(chunk):
        return (chunk > 0) & (chunk % (2 * chunks_per_mat) == 0)

    def load(chunk):
        for_mat(chunk, lambda mat: rows_load(mat, chunk).wait())
        for_mat(chunk, lambda mat: cols_load(mat, chunk).wait())
        after = chunk + 1

        @pl.when(after < num_chunks)
        def _():
            for_mat(after, lambda mat: rows_load(mat, after).start())

        @pl.when((after < num_chunks) & jnp.logical_not(opens_layer(after)))
        def _():
            for_mat(after, lambda mat: cols_load(mat, after).start())

    def load_weights(chunk):
        def arrive(mat):
            for copy in weight_loads(mat, chunk):
                copy.wait()

        for_mat(chunk, arrive)
        after, before = chunk + 1, chunk - 1

        @pl.when(after < num_chunks)
        def _():
            def start(mat):
                for copy in weight_loads(mat, after):
                    copy.start()

            for_mat(after, start)

        @pl.when((before >= 0) & ((before // chunks_per_mat) % 2 == 0))
        def _():
            grad_pre_store(before % chunks_per_mat).wait()

    def compute_sent(chunk):
        @pl.loop(0, COLORS)
        def _(color):
            sent_core[color] = product(chunk, 1 - core, color).astype(jnp.bfloat16)

    def share_core(chunk):
        core_copy(chunk).start()

    def compute_kept(chunk):
        slot = chunk % KEPT_SLOTS

        @pl.loop(0, COLORS)
        def _(color):
            kept[slot, color] = product(chunk, core, color)

    def halve(level, chunk, arrived):
        slot = chunk % KEPT_SLOTS
        recv_slot = chunk % RECV_SLOTS
        for color in range(COLORS):
            if level > 0:
                out_copy(level - 1, color, chunk).wait()
            held = base(color, level)

            def total(start, size, color=color, held=held):
                own = kept[slot, color, rows_at(start, size), :]
                return own + arrived[recv_slot, color, rows_at(start - held, size), :].astype(jnp.float32)

            if level < 3:
                mine = base(color, level + 1)
                sent_bufs[level][color] = total(other(color, level), spans[level]).astype(jnp.bfloat16)
                kept[slot, color, rows_at(mine, spans[level]), :] = total(mine, spans[level])
                out_copy(level, color, chunk).start()
            else:
                gather_slot = chunk % GATHER_SLOTS
                ring[gather_slot, core, color, rows_at(held, spans[2]), :] = total(held, spans[2]).astype(jnp.bfloat16)
                back_copy(2, color, chunk, False).start()

    def send_1(chunk):
        core_copy(chunk).wait()
        halve(0, chunk, recv_core)

    def send_2(chunk):
        halve(1, chunk, recv_1)

    def send_3(chunk):
        halve(2, chunk, recv_2)

    def send_back_3(chunk):
        halve(3, chunk, recv_3)

    def pass_back(level, chunk):
        for color in range(COLORS):
            back_copy(level + 1, color, chunk, True).wait()
            back_copy(level, color, chunk, False).start()

    def send_back_2(chunk):
        pass_back(1, chunk)

    def send_back_1(chunk):
        @pl.when(chunk < full_chunks)
        def _():
            pass_back(0, chunk)

        @pl.when(chunk >= full_chunks)
        def _():
            for color in range(COLORS):
                back_copy(1, color, chunk, True).wait()
                part_share_copy(color, chunk, False).start()

    def send_back_core(chunk):
        @pl.when(chunk < full_chunks)
        def _():
            for color in range(COLORS):
                back_copy(0, color, chunk, True).wait()
            share_copy(chunk, False).start()

        @pl.when(chunk >= full_chunks)
        def _():
            for color in range(COLORS):
                part_share_copy(color, chunk, True).wait()

        for group, size in enumerate(PART_GROUPS):
            first = full_chunks + sum(PART_GROUPS[:group])

            @pl.when((chunk >= first) & (chunk < first + size))
            def _(group=group):
                for copy in part_stores(group, chunk):
                    copy.start()

    def store(chunk):
        @pl.when(chunk < full_chunks)
        def _():
            share_copy(chunk, True).wait()
            store_copy(chunk).start()

        @pl.when((chunk > 0) & (chunk <= full_chunks))
        def _():
            store_copy(chunk - 1).wait()

        for group, size in enumerate(PART_GROUPS):
            first = full_chunks + sum(PART_GROUPS[:group])

            @pl.when((chunk >= first) & (chunk < first + size))
            def _(group=group):
                for copy in part_stores(group, chunk):
                    copy.wait()

    token_half = grad_b.shape[0] // 2

    def backward(part, chunk):
        slot = chunk % 2
        sub = chunk % chunks_per_mat
        mat = chunk // chunks_per_mat
        layer = num_layers - 1 - mat // 2

        @pl.when(mat % 2 == 0)
        def _():
            cols = slice(part * TILE, (part + 1) * TILE)

            @pl.loop(0, 2)
            def _(which):
                rows = pl.ds(pl.multiple_of(which * token_half, 128), token_half)
                grad_act = lax.dot_general(
                    grad_b[rows, :], weight_buf[slot, cols, :], FEATURE_DIMS, preferred_element_type=jnp.float32)
                grad_pre = grad_act * gelu_slope(pre_buf[slot, rows, cols].astype(jnp.float32))
                grad_pre_buf[rows, cols] = grad_pre.astype(jnp.bfloat16)
                start = row_dim + sub * chunk_cols + part * TILE
                small_out[pl.ds(layer, 1), pl.ds(pl.multiple_of(start, 128), TILE)] += jnp.sum(grad_pre, axis=0, keepdims=True)

            if part == chunk_cols // TILE - 1:
                grad_pre_store(sub).start()

        @pl.when(mat % 2 == 1)
        def _():
            pieces = row_dim // chunk_cols * (chunk_cols // TILE) // 3
            grad_rows = []
            for piece in range(part * pieces, (part + 1) * pieces):
                start, first = divmod(piece * TILE, chunk_cols)
                grad_rows.append((piece, lax.dot_general(
                    cols_buf[slot], weight_buf[slot, first:first + TILE, start * chunk_cols:(start + 1) * chunk_cols],
                    FEATURE_DIMS, preferred_element_type=jnp.float32)))
            for piece, value in grad_rows:
                grad_normed[:, piece * TILE:(piece + 1) * TILE] += value

    def norm_loads(layer, block):
        rows = pl.ds(pl.multiple_of(block * NORM_ROWS, NORM_ROWS), NORM_ROWS)
        slot = block % 2
        copies = [pltpu.make_async_copy(hid_refs[layer].at[rows, :], hid_buf.at[slot], norm_sem.at[0, slot])]
        if layer > 0:
            copies.append(pltpu.make_async_copy(grad_top.at[rows, :], grad_buf.at[slot], norm_sem.at[1, slot]))
        return copies

    def layer_input_grad(layer):
        num_blocks = grad_b.shape[0] // NORM_ROWS
        for copy in norm_loads(layer, 0):
            copy.start()

        @pl.loop(0, num_blocks)
        def _(block):
            @pl.when(block + 1 < num_blocks)
            def _():
                for copy in norm_loads(layer, block + 1):
                    copy.start()

            for copy in norm_loads(layer, block):
                copy.wait()
            rows = pl.ds(pl.multiple_of(block * NORM_ROWS, NORM_ROWS), NORM_ROWS)
            hid_f = hid_buf[block % 2].astype(jnp.float32)
            hid_scale = inverse_rms(hid_f)
            hid_hat = hid_f * hid_scale
            normed_grad = grad_normed[rows, :]
            small_out[layer:layer + 1, :row_dim] += jnp.sum(normed_grad * hid_hat, axis=0, keepdims=True)
            if layer > 0:
                grad_normed[rows, :] = jnp.zeros((NORM_ROWS, row_dim), jnp.float32)
                grad_hat = normed_grad * gain_in[layer:layer + 1, :].astype(jnp.float32)
                grad_new = grad_buf[block % 2] + hid_scale * (
                    grad_hat - hid_hat * jnp.mean(grad_hat * hid_hat, axis=-1, keepdims=True))
                grad_b[rows, :] = grad_new.astype(jnp.bfloat16)
                small_out[layer - 1:layer, row_dim + hidden_dim:] += jnp.sum(grad_new, axis=0, keepdims=True)

        if layer > 0:
            copy = pltpu.make_async_copy(grad_b, grad_b_hbm, grad_b_sem)
            copy.start()
            copy.wait()
            following = jnp.int32((num_layers - layer) * 2 * chunks_per_mat)
            cols_load((num_layers - layer) * 2, following).start()

    def input_grad(chunk):
        for layer in range(num_layers):
            last = (num_layers - 1 - layer) * 2 * chunks_per_mat + 2 * chunks_per_mat - 1

            @pl.when(chunk == last)
            def _(layer=layer):
                layer_input_grad(layer)

    events = dict(
        load=load, load_weights=load_weights, compute_sent=compute_sent, share_core=share_core, compute_kept=compute_kept, send_1=send_1, send_2=send_2, send_3=send_3,
        send_back_3=send_back_3, send_back_2=send_back_2, send_back_1=send_back_1, send_back_core=send_back_core, store=store,
        backward_0=functools.partial(backward, 0), backward_1=functools.partial(backward, 1),
        backward_2=functools.partial(backward, 2), input_grad=input_grad)

    first = jnp.int32(0)
    rows_load(0, first).start()
    cols_load(0, first).start()
    for copy in weight_loads(0, first):
        copy.start()
    grad_b_copy = pltpu.make_async_copy(grad_top_b, grad_b, grad_b_sem)
    grad_b_copy.start()
    barrier = pltpu.get_barrier_semaphore()
    for partner in partners:
        pl.semaphore_signal(barrier, inc=1, device_id=(partner,), device_id_type=MESH)
    small_out[...] = small_in[...]
    grad_normed[...] = jnp.zeros_like(grad_normed)
    grad_b_copy.wait()
    pl.semaphore_wait(barrier, 4)

    @pl.loop(0, num_chunks + MAX_LAG)
    def _(it):
        for step in range(4):
            @pl.when(it == num_chunks + step)
            def _(step=step):
                small_copy(step).start()
        for name, lag in PIPELINE:
            chunk = it - lag

            @pl.when((chunk >= 0) & (chunk < num_chunks))
            def _(name=name, chunk=chunk):
                events[name](chunk)
        for step in range(4):
            @pl.when(it == num_chunks + step)
            def _(step=step):
                small_copy(step).wait()
                small_out[...] += small_recv[step]


def backward_pass(hid_rows, saved, grad_top, grad_top_b, norm_gain, w_up, w_down, small, axis, chunk_cols):
    num_layers, row_dim, hidden = w_up.shape
    tokens = grad_top.shape[0]
    chunks_per_mat = hidden // chunk_cols
    region = row_dim // (2 * COLORS)
    half = (COLORS, region, chunk_cols)
    sizes = (num_layers, chunks_per_mat, row_dim, chunk_cols, region, row_dim // chunk_cols, axis)
    num_chunks = 2 * num_layers * chunks_per_mat
    bf16, f32 = jnp.bfloat16, jnp.float32
    dma = pltpu.SemaphoreType.DMA
    any_spec = pl.BlockSpec(memory_space=pl.ANY)
    vmem_spec = pl.BlockSpec(memory_space=pltpu.VMEM)
    full_chunks = num_chunks - sum(PART_GROUPS)
    part_shapes = [jax.ShapeDtypeStruct((size, region // 2, chunk_cols), bf16) for size in PART_GROUPS for _ in range(2 * COLORS)]
    gathered, small_sum, _, _, *parts = pl.pallas_call(
        functools.partial(backward_kernel, sizes),
        out_shape=[
            jax.ShapeDtypeStruct((full_chunks, 2) + half, bf16),
            jax.ShapeDtypeStruct(small.shape, f32),
            jax.ShapeDtypeStruct((chunks_per_mat, tokens, chunk_cols), bf16),
            jax.ShapeDtypeStruct((tokens, row_dim), bf16),
        ] + part_shapes,
        in_specs=[any_spec] * (num_layers + 7) + [vmem_spec] * 2,
        out_specs=[any_spec, vmem_spec, any_spec, any_spec] + [any_spec] * len(part_shapes),
        scratch_shapes=[
            pltpu.VMEM((2, tokens, row_dim), bf16),
            pltpu.VMEM((2, tokens, chunk_cols), bf16),
            pltpu.VMEM(half, bf16),
            pltpu.VMEM((KEPT_SLOTS,) + half, f32),
            pltpu.VMEM((RECV_SLOTS,) + half, bf16),
            pltpu.VMEM((COLORS, region // 2, chunk_cols), bf16),
            pltpu.VMEM((COLORS, region // 4, chunk_cols), bf16),
            pltpu.VMEM((COLORS, region // 8, chunk_cols), bf16),
            pltpu.VMEM((RECV_SLOTS, COLORS, region // 2, chunk_cols), bf16),
            pltpu.VMEM((RECV_SLOTS, COLORS, region // 4, chunk_cols), bf16),
            pltpu.VMEM((RECV_SLOTS, COLORS, region // 8, chunk_cols), bf16),
            pltpu.VMEM((GATHER_SLOTS, 2) + half, bf16),
            pltpu.VMEM((2, chunk_cols, row_dim), bf16),
            pltpu.VMEM((2, tokens, chunk_cols), bf16),
            pltpu.VMEM((tokens, chunk_cols), bf16),
            pltpu.VMEM((tokens, row_dim), bf16),
            pltpu.VMEM((tokens, row_dim), f32),
            pltpu.VMEM((2, NORM_ROWS, row_dim), bf16),
            pltpu.VMEM((2, NORM_ROWS, row_dim), f32),
            pltpu.VMEM((4,) + small.shape, f32),
            dma((4, 2)), dma, dma((2, 2)), dma,
            dma, dma((RECV_SLOTS,)), dma((3, COLORS)), dma((3, COLORS, RECV_SLOTS)),
            dma((3, COLORS, GATHER_SLOTS)), dma((3, COLORS, GATHER_SLOTS)), dma((GATHER_SLOTS,)), dma((GATHER_SLOTS,)),
            dma((GATHER_SLOTS,)), dma((4,)), dma((4,)), dma((COLORS, 2, GATHER_SLOTS)),
        ],
        compiler_params=pltpu.CompilerParams(collective_id=0, has_side_effects=True, vmem_limit_bytes=67043328),
        name="backward",
    )(*hid_rows, *saved, grad_top, grad_top_b, w_up, w_down, norm_gain, small)
    return gathered, small_sum, parts


def flip_pairs(num_devices, bit):
    return [(dev, dev ^ (1 << bit)) for dev in range(num_devices)]


def stream_blocks(num_blocks, start_loads, wait_loads, store_of, in_buf, out_buf):
    slots, region = in_buf.shape[0], in_buf.shape[2]
    for block in range(min(slots - 1, num_blocks)):
        start_loads(jnp.int32(block), block)

    @pl.loop(0, num_blocks)
    def _(block):
        slot = block % slots

        @pl.when(block + slots - 1 < num_blocks)
        def _():
            start_loads(block + slots - 1, (block + slots - 1) % slots)

        wait_loads(block, slot)

        @pl.when(block >= slots)
        def _():
            store_of(block - slots, slot).wait()

        for color in range(COLORS):
            out_buf[slot, color * region:(color + 1) * region, :] = in_buf[slot, color].astype(jnp.float32)
        store_of(block, slot).start()

    for block in range(max(num_blocks - slots, 0), num_blocks):
        store_of(jnp.int32(block), block % slots).wait()


def block_target(out_ref, layer, kind, down_subs, chunk, which_core, rows, cols):
    half = pl.multiple_of(which_core * rows, rows)
    if kind == 0:
        first = pl.multiple_of((chunk // down_subs) * 2 * rows + half, rows)
        return out_ref.at[layer, pl.ds(first, rows), pl.ds(pl.multiple_of((chunk % down_subs) * cols, 128), cols)]
    return out_ref.at[layer, pl.ds(half, rows), pl.ds(pl.multiple_of(chunk * cols, 128), cols)]


def widen_kernel(spec, *refs):
    first, count, place, layer, kind, down_subs, small_widths = spec
    if small_widths:
        gathered, small, out_ref, *small_outs, in_buf, out_buf, in_sem, out_sem = refs
        start = 0
        for width, small_out in zip(small_widths, small_outs):
            small_out[...] = small[:, start:start + width]
            start += width
    else:
        gathered, out_ref, in_buf, out_buf, in_sem, out_sem = refs
    rows, cols = out_buf.shape[1:]

    def load(block, slot):
        return pltpu.make_async_copy(gathered.at[first + block // 2, block % 2], in_buf.at[slot], in_sem.at[slot])

    def store(block, slot):
        target = block_target(out_ref, layer, kind, down_subs, place + block // 2, block % 2, rows, cols)
        return pltpu.make_async_copy(out_buf.at[slot], target, out_sem.at[slot])

    stream_blocks(
        2 * count, lambda block, slot: load(block, slot).start(), lambda block, slot: load(block, slot).wait(),
        store, in_buf, out_buf)


def join_kernel(spec, *refs):
    count, place, layer, kind, down_subs, axis = spec
    parts, (_, out_ref, in_buf, out_buf, in_sem, out_sem) = refs[:4 * COLORS], refs[4 * COLORS:]
    rows, cols = out_buf.shape[1:]
    part_rows = in_buf.shape[2] // 2
    me = lax.axis_index(axis)
    core = me % 2

    def copies(which, chunk, slot):
        found = []
        for color in range(COLORS):
            upper = (me >> COLOR_DIMS[color][0]) & 1
            for far in range(2):
                start = pl.multiple_of((upper if far == 0 else 1 - upper) * part_rows, part_rows)
                found.append(pltpu.make_async_copy(
                    parts[color * 4 + far * 2 + which].at[chunk],
                    in_buf.at[slot, color, pl.ds(start, part_rows), :], in_sem.at[slot]))
        return found

    def start_loads(block, slot):
        for which in range(2):
            @pl.when(block % 2 == which)
            def _(which=which):
                for copy in copies(which, block // 2, slot):
                    copy.start()

    def wait_loads(block, slot):
        for copy in copies(0, block // 2, slot):
            copy.wait()

    def store(block, slot):
        which_core = jnp.where(block % 2 == 0, core, 1 - core)
        target = block_target(out_ref, layer, kind, down_subs, place + block // 2, which_core, rows, cols)
        return pltpu.make_async_copy(out_buf.at[slot], target, out_sem.at[slot])

    stream_blocks(2 * count, start_loads, wait_loads, store, in_buf, out_buf)


def widen_scratch(region, cols):
    return [
        pltpu.VMEM((STREAM_SLOTS, COLORS, region, cols), jnp.bfloat16),
        pltpu.VMEM((STREAM_SLOTS, COLORS * region, cols), jnp.float32),
        pltpu.SemaphoreType.DMA((STREAM_SLOTS,)),
        pltpu.SemaphoreType.DMA((STREAM_SLOTS,)),
    ]


def widen_cost(count, region, cols):
    size = count * 2 * COLORS * region * cols
    return pl.CostEstimate(flops=500 * size, bytes_accessed=6 * size, transcendentals=0)


def widen(gathered, first, count, layer, kind, shape, down_subs, small, small_widths):
    region, cols = gathered.shape[3:]
    any_spec = pl.BlockSpec(memory_space=pl.ANY)
    vmem_spec = pl.BlockSpec(memory_space=pltpu.VMEM)
    smalls = [jax.ShapeDtypeStruct((small.shape[0], width), jnp.float32) for width in small_widths]
    return pl.pallas_call(
        functools.partial(widen_kernel, (first, count, 0, layer, kind, down_subs, small_widths)),
        in_specs=[any_spec] + [vmem_spec] * bool(smalls),
        out_specs=[any_spec] + [vmem_spec] * len(smalls),
        out_shape=[jax.ShapeDtypeStruct(shape, jnp.float32)] + smalls,
        scratch_shapes=widen_scratch(region, cols),
        cost_estimate=widen_cost(count, region, cols),
        compiler_params=pltpu.CompilerParams(vmem_limit_bytes=67043328),
    )(gathered, *([small] if smalls else []))


def join(parts, place, layer, kind, into, down_subs, axis):
    count, part_rows, cols = parts[0].shape
    any_spec = pl.BlockSpec(memory_space=pl.ANY)
    return pl.pallas_call(
        functools.partial(join_kernel, (count, place, layer, kind, down_subs, axis)),
        in_specs=[any_spec] * (len(parts) + 1),
        out_specs=any_spec,
        out_shape=jax.ShapeDtypeStruct(into.shape, jnp.float32),
        scratch_shapes=widen_scratch(2 * part_rows, cols),
        input_output_aliases={len(parts): 0},
        cost_estimate=widen_cost(count, 2 * part_rows, cols),
        compiler_params=pltpu.CompilerParams(vmem_limit_bytes=67043328),
    )(*parts, into)


def swap(array, axis, num_devices, bit):
    return lax.ppermute(array, axis, flip_pairs(num_devices, bit))


def full_gradients(gathered, parts, small, num_layers, row_dim, hidden, chunk_cols, axis, num_devices):
    per_mat = hidden // chunk_cols
    down_subs = row_dim // chunk_cols
    groups = range(len(PART_GROUPS))
    mine = [[parts[(group * COLORS + color) * 2] for color in range(COLORS)] for group in groups]
    theirs = [[parts[(group * COLORS + color) * 2 + 1] for color in range(COLORS)] for group in groups]
    far = [[swap(mine[group][color], axis, num_devices, COLOR_DIMS[color][0])
            for color in range(COLORS)] for group in groups]
    last = num_layers - 1
    down, *smalls = widen(
        gathered, 0, per_mat, last, 0, (num_layers, hidden, row_dim), down_subs, small, (row_dim, hidden, row_dim))
    up, = widen(gathered, per_mat, per_mat, last, 1, (num_layers, row_dim, hidden), down_subs, small, ())
    full = [down, up]
    for group in groups:
        kind, place = divmod(sum(PART_GROUPS[:group]), per_mat)
        pieces = []
        for color in range(COLORS):
            shared = swap(far[group][color], axis, num_devices, CORE)
            pieces += [mine[group][color], theirs[group][color], far[group][color], shared]
        full[kind] = join(pieces, place, 0, kind, full[kind], down_subs, axis)
    return smalls[0], full[1], smalls[1], full[0], smalls[2]


def solution(mesh):
    axis = mesh.axis_names[0]

    def device_grads(tokens, upstream, norm_gain, w_up, bias_up, w_down, bias_down):
        num_layers, width = norm_gain.shape
        hidden_width = w_up.shape[2]
        chunk_cols = width // 2
        hid_1, normed, pre_act, activated, grad_top, grad_top_b, small = forward_pass(
            tokens, upstream, norm_gain, w_up, bias_up, w_down, bias_down, width)
        gathered, small, parts = backward_pass(
            (tokens, hid_1), (normed, pre_act, activated), grad_top, grad_top_b, norm_gain, w_up, w_down, small, axis, chunk_cols)
        return full_gradients(gathered, parts, small, num_layers, width, hidden_width, chunk_cols, axis, mesh.size)

    row_spec = P(axis, None)
    full_spec = P()
    return jax.shard_map(
        device_grads,
        mesh=mesh,
        in_specs=(row_spec, row_spec, full_spec, full_spec, full_spec, full_spec, full_spec),
        out_specs=(full_spec, full_spec, full_spec, full_spec, full_spec),
        check_vma=False,
    )
```

```python
import functools

import jax
import jax.numpy as jnp
from jax import lax
from jax.experimental import pallas as pl
from jax.experimental.pallas import tpu as pltpu
from jax.sharding import PartitionSpec as P


EPSILON = 1e-6
TOKEN_DIMS = (((0,), (0,)), ((), ()))
FEATURE_DIMS = (((1,), (1,)), ((), ()))
MESH = pl.DeviceIdType.MESH
COLORS = 3
CORE, DIM_X, DIM_Y, DIM_Z = range(4)
COLOR_DIMS = ((DIM_X, DIM_Y, DIM_Z), (DIM_Y, DIM_Z, DIM_X), (DIM_Z, DIM_X, DIM_Y))
PIPELINE = (
    ("load", 0), ("compute_sent", 0), ("share_core", 0), ("send_3", 2), ("send_back_2", 4), ("send_back_1", 5),
    ("compute_kept", 0), ("send_back_core", 6), ("load_weights", 0), ("backward_0", 0), ("send_2", 1), ("backward_1", 0),
    ("send_1", 0), ("backward_2", 0), ("send_back_3", 2), ("store", 6), ("input_grad", 0),
)
MAX_LAG = 6
PART_GROUPS = (8, 4, 4)
WIDEN_CALLS = (8, 6, 2)
RECV_SLOTS = 2
KEPT_SLOTS = 3
GATHER_SLOTS = 6
TILE = 256
UP_COLS = 512
ACT_ROWS = 16
ACT_COLS = 256
STREAM_SLOTS = 4
NORM_ROWS = 128
GELU_SCALE = 0.7978845608028654
GELU_CUBIC = 0.044715


def inverse_rms(hid_f):
    return lax.rsqrt(jnp.mean(hid_f * hid_f, axis=-1, keepdims=True) + EPSILON)


def gelu(values):
    return (0.5 * values) * (1.0 + jnp.tanh(values * (GELU_SCALE + GELU_SCALE * GELU_CUBIC * (values * values))))


def forward_kernel(
    sizes, tokens, upstream, w_up, w_down, gain_in, bias_up_in, bias_down_in, hid_out, normed_out, pre_act_out, act_out,
    grad_top_out, grad_top_b_out, small_out, hid, normed, branch, up_buf, down_buf, pre_buf, act_buf, up_rows, grad_b_buf,
    gain, bias_up, bias_down, io_sem, up_sem, down_sem, pre_sem, act_sem,
):
    num_layers, num_tiles, tile_cols = sizes
    num_tokens, row_dim = hid.shape
    steps = num_tiles + 1
    parts = tile_cols // UP_COLS

    def up_load(layer, tile):
        cols = pl.ds(pl.multiple_of(tile * tile_cols, 128), tile_cols)
        return pltpu.make_async_copy(w_up.at[layer, :, cols], up_buf.at[tile % 2], up_sem.at[tile % 2])

    def down_load(layer, tile):
        rows = pl.ds(pl.multiple_of(tile * tile_cols, 128), tile_cols)
        return pltpu.make_async_copy(w_down.at[layer, rows, :], down_buf.at[tile % 2], down_sem.at[tile % 2])

    def pre_store(layer, tile):
        cols = pl.ds(pl.multiple_of(tile * tile_cols, 128), tile_cols)
        return pltpu.make_async_copy(pre_buf.at[tile % 2], pre_act_out.at[layer, :, cols], pre_sem.at[tile % 2])

    def act_store(layer, tile):
        cols = pl.ds(pl.multiple_of(tile * tile_cols, 128), tile_cols)
        return pltpu.make_async_copy(act_buf.at[tile % 2], act_out.at[layer, :, cols], act_sem.at[tile % 2])

    def normed_store(layer):
        return pltpu.make_async_copy(normed, normed_out.at[layer], io_sem.at[1])

    def hid_store():
        return pltpu.make_async_copy(hid, hid_out, io_sem.at[2])

    tokens_load = pltpu.make_async_copy(tokens, hid, io_sem.at[0])
    tokens_load.start()
    up_load(0, 0).start()
    upstream_load = pltpu.make_async_copy(upstream, up_rows, io_sem.at[3])
    small_out[...] = jnp.zeros_like(small_out)
    branch[...] = jnp.zeros_like(branch)
    pre_buf[0, :, :UP_COLS] = jnp.zeros((num_tokens, UP_COLS), jnp.bfloat16)
    gain[...] = gain_in[...].astype(jnp.float32)
    bias_up[...] = bias_up_in[...].astype(jnp.float32)
    bias_down[...] = bias_down_in[...].astype(jnp.float32)
    tokens_load.wait()

    def each_block(action):
        @pl.loop(0, num_tokens // NORM_ROWS)
        def _(block):
            action(pl.ds(pl.multiple_of(block * NORM_ROWS, NORM_ROWS), NORM_ROWS))

    def normalize(layer, rows, hid_f):
        normed[rows, :] = ((hid_f * inverse_rms(hid_f)) * gain[pl.ds(layer, 1), :]).astype(jnp.bfloat16)

    def next_rows(layer, rows):
        new = ((hid[rows, :].astype(jnp.float32) + branch[rows, :]) + bias_down[pl.ds(layer, 1), :]).astype(jnp.bfloat16)
        hid[rows, :] = new
        return new.astype(jnp.float32)

    def activate(slot, part):
        start = part * UP_COLS
        for row in range(0, num_tokens, ACT_ROWS):
            for col in range(0, UP_COLS, ACT_COLS):
                piece = (slot, pl.ds(row, ACT_ROWS), pl.ds(pl.multiple_of(start + col, 128), ACT_COLS))
                act_buf[piece] = gelu(pre_buf[piece].astype(jnp.float32)).astype(jnp.bfloat16)

    def up_product(layer, tile):
        @pl.loop(0, parts)
        def _(part):
            fresh = tile * parts + part == 0
            last_slot = jnp.where((part == 0) & (tile > 0), (tile + 1) % 2, tile % 2)
            activate(last_slot, jnp.where(fresh, 0, (part + parts - 1) % parts))
            cols = pl.ds(pl.multiple_of(part * UP_COLS, 128), UP_COLS)
            bias = bias_up[pl.ds(layer, 1), pl.ds(pl.multiple_of(tile * tile_cols + part * UP_COLS, 128), UP_COLS)]
            pre_buf[tile % 2, :, cols] = (
                jnp.dot(normed[...], up_buf[tile % 2, :, cols], preferred_element_type=jnp.float32) + bias
            ).astype(jnp.bfloat16)

    def down_product(tile):
        slot = tile % 2
        for part in range(row_dim // UP_COLS):
            cols = slice(part * UP_COLS, (part + 1) * UP_COLS)
            branch[:, cols] += jnp.dot(act_buf[slot], down_buf[slot, :, cols], preferred_element_type=jnp.float32)

    each_block(lambda rows: normalize(0, rows, hid[rows, :].astype(jnp.float32)))

    @pl.loop(0, num_layers * steps)
    def _(step):
        layer, tile = step // steps, step % steps

        @pl.when(tile < num_tiles)
        def _():
            up_load(layer, tile).wait()

            @pl.when(tile + 1 < num_tiles)
            def _():
                up_load(layer, tile + 1).start()

            @pl.when((tile == num_tiles - 1) & (layer + 1 < num_layers))
            def _():
                up_load(layer + 1, 0).start()

            @pl.when(step == 0)
            def _():
                normed_store(0).start()
                down_load(0, 0).start()
                upstream_load.start()

            @pl.when(tile > 1)
            def _():
                pre_store(layer, tile - 2).wait()
                act_store(layer, tile - 2).wait()

            up_product(layer, tile)
            pre_store(layer, tile).start()

        @pl.when(tile == num_tiles)
        def _():
            activate((num_tiles - 1) % 2, parts - 1)

        @pl.when(tile > 0)
        def _():
            act_store(layer, tile - 1).start()
            down_load(layer, tile - 1).wait()

            @pl.when(tile < num_tiles)
            def _():
                down_load(layer, tile).start()

            @pl.when((tile == num_tiles) & (layer + 1 < num_layers))
            def _():
                down_load(layer + 1, 0).start()

            down_product(tile - 1)

        @pl.when(tile == num_tiles)
        def _():
            for back in (2, 1):
                pre_store(layer, num_tiles - back).wait()
                act_store(layer, num_tiles - back).wait()
            normed_store(layer).wait()

            @pl.when(layer + 1 < num_layers)
            def _():
                def to_next(rows):
                    normalize(layer + 1, rows, next_rows(layer, rows))
                    branch[rows, :] = jnp.zeros((NORM_ROWS, row_dim), jnp.float32)

                each_block(to_next)
                hid_store().start()
                normed_store(layer + 1).start()

    hid_store().wait()
    upstream_load.wait()
    bias_start = small_out.shape[1] - row_dim

    def grad_stores(rows):
        return (
            pltpu.make_async_copy(branch.at[rows, :], grad_top_out.at[rows, :], io_sem.at[0]),
            pltpu.make_async_copy(grad_b_buf.at[rows, :], grad_top_b_out.at[rows, :], io_sem.at[1]),
        )

    def top_rows(rows):
        top_f = next_rows(num_layers - 1, rows)
        top_scale = inverse_rms(top_f)
        top_hat = top_f * top_scale
        up_f = up_rows[rows, :].astype(jnp.float32)
        grad = top_scale * (up_f - top_hat * jnp.mean(up_f * top_hat, axis=-1, keepdims=True))
        branch[rows, :] = grad
        grad_b_buf[rows, :] = grad.astype(jnp.bfloat16)
        small_out[num_layers - 1:, bias_start:] += jnp.sum(grad, axis=0, keepdims=True)
        for copy in grad_stores(rows):
            copy.start()

    each_block(top_rows)
    for copy in grad_stores(pl.ds(0, num_tokens)):
        copy.wait()


def forward_pass(tokens, upstream, norm_gain, w_up, bias_up, w_down, bias_down, tile_cols):
    num_tokens, row_dim = tokens.shape
    num_layers, _, hidden = w_up.shape
    bf16, f32 = jnp.bfloat16, jnp.float32
    dma = pltpu.SemaphoreType.DMA
    any_spec = pl.BlockSpec(memory_space=pl.ANY)
    vmem_spec = pl.BlockSpec(memory_space=pltpu.VMEM)
    rows = (num_tokens, row_dim)
    wide = (num_layers, num_tokens, hidden)
    return pl.pallas_call(
        functools.partial(forward_kernel, (num_layers, hidden // tile_cols, tile_cols)),
        out_shape=(
            jax.ShapeDtypeStruct(rows, bf16),
            jax.ShapeDtypeStruct((num_layers,) + rows, bf16),
            jax.ShapeDtypeStruct(wide, bf16),
            jax.ShapeDtypeStruct(wide, bf16),
            jax.ShapeDtypeStruct(rows, f32),
            jax.ShapeDtypeStruct(rows, bf16),
            jax.ShapeDtypeStruct((num_layers, 2 * row_dim + hidden), f32),
        ),
        in_specs=[any_spec] * 4 + [vmem_spec] * 3,
        out_specs=(any_spec,) * 6 + (vmem_spec,),
        scratch_shapes=[
            pltpu.VMEM(rows, bf16),
            pltpu.VMEM(rows, bf16),
            pltpu.VMEM(rows, f32),
            pltpu.VMEM((2, row_dim, tile_cols), bf16),
            pltpu.VMEM((2, tile_cols, row_dim), bf16),
            pltpu.VMEM((2, num_tokens, tile_cols), bf16),
            pltpu.VMEM((2, num_tokens, tile_cols), bf16),
            pltpu.VMEM(rows, bf16),
            pltpu.VMEM(rows, bf16),
            pltpu.VMEM((num_layers, row_dim), f32),
            pltpu.VMEM((num_layers, hidden), f32),
            pltpu.VMEM((num_layers, row_dim), f32),
            dma((4,)), dma((2,)), dma((2,)), dma((2,)), dma((2,)),
        ],
        compiler_params=pltpu.CompilerParams(vmem_limit_bytes=60 * 2**20),
        name="forward",
    )(tokens, upstream, w_up, w_down, norm_gain, bias_up, bias_down)


def gelu_slope(values):
    square = values * values
    bend = jnp.tanh(values * (GELU_SCALE + GELU_SCALE * GELU_CUBIC * square))
    return 0.5 * (1.0 + bend) + (0.5 * values) * (1.0 - bend * bend) * (GELU_SCALE + 3.0 * GELU_SCALE * GELU_CUBIC * square)


def backward_kernel(sizes, *refs):
    num_layers, chunks_per_mat, row_dim, chunk_cols, region, down_subs, axis = sizes
    num_mats = 2 * num_layers
    hidden_dim = chunks_per_mat * chunk_cols
    hid_refs, refs = refs[:num_layers], refs[num_layers:]
    (normed, pre_act, activated, grad_top, grad_top_b, w_up, w_down, gain_in, small_in,
     gathered, small_out, grad_pre_hbm, grad_b_hbm) = refs[:13]
    part_count = 2 * COLORS * len(PART_GROUPS)
    part_refs, refs = refs[13:13 + part_count], refs[13 + part_count:]
    (rows_buf, cols_buf, sent_core, kept, recv_core, sent_1, sent_2, sent_3, recv_1, recv_2, recv_3, ring,
     weight_buf, pre_buf, grad_pre_buf, grad_b, grad_normed, hid_buf, grad_buf,
     small_recv, load_sem, grad_pre_sem, norm_sem, grad_b_sem, core_send, core_recv, out_send, out_recv, back_send, back_recv,
     share_send, share_recv, store_sem, small_send_sem, small_recv_sem, part_sem) = refs
    num_chunks = num_mats * chunks_per_mat
    full_chunks = num_chunks - sum(PART_GROUPS)
    half = COLORS * region
    me = lax.axis_index(axis)
    bits = [me % 2, (me // 2) % 2, (me // 4) % 2, me // 8]
    partners = [me + (1 << d) - 2 * (1 << d) * bits[d] for d in range(4)]
    core = bits[CORE]
    sent_bufs, recv_bufs = (sent_1, sent_2, sent_3), (recv_1, recv_2, recv_3)
    spans = (region // 2, region // 4, region // 8)

    def base(color, level):
        total = 0
        for step in range(level):
            total = total + bits[COLOR_DIMS[color][step]] * spans[step]
        return total

    def other(color, level):
        return base(color, level) + (1 - bits[COLOR_DIMS[color][level]]) * spans[level]

    def rows_at(start, size):
        return pl.ds(pl.multiple_of(start, spans[2]), size)

    def rows_load(mat, chunk):
        layer = num_layers - 1 - mat // 2
        if mat % 2 == 0:
            start = ((chunk % chunks_per_mat) // down_subs) * row_dim
            source = activated.at[layer, :, pl.ds(pl.multiple_of(start, 128), row_dim)]
        else:
            source = normed.at[layer]
        return pltpu.make_async_copy(source, rows_buf.at[chunk % 2], load_sem.at[0, chunk % 2])

    def weight_loads(mat, chunk):
        slot = chunk % 2
        layer = num_layers - 1 - mat // 2
        cols = pl.ds(pl.multiple_of((chunk % chunks_per_mat) * chunk_cols, 128), chunk_cols)
        if mat % 2 == 0:
            return [
                pltpu.make_async_copy(w_down.at[layer, cols, :], weight_buf.at[slot], load_sem.at[1, slot]),
                pltpu.make_async_copy(pre_act.at[layer, :, cols], pre_buf.at[slot], load_sem.at[2, slot]),
            ]
        return [
            pltpu.make_async_copy(
                w_up.at[layer, part * chunk_cols:(part + 1) * chunk_cols, cols],
                weight_buf.at[slot, :, part * chunk_cols:(part + 1) * chunk_cols], load_sem.at[1 + part, slot])
            for part in range(down_subs)
        ]

    def cols_load(mat, chunk):
        sub = chunk % chunks_per_mat
        if mat % 2 == 0:
            source = grad_top_b if mat == 0 else grad_b_hbm
            source = source.at[:, pl.ds(pl.multiple_of((sub % down_subs) * chunk_cols, 128), chunk_cols)]
        else:
            source = grad_pre_hbm.at[sub]
        return pltpu.make_async_copy(source, cols_buf.at[chunk % 2], load_sem.at[3, chunk % 2])

    def for_mat(chunk, action):
        for mat in range(num_mats):
            @pl.when(chunk // chunks_per_mat == mat)
            def _(mat=mat):
                action(mat)

    def grad_pre_store(sub):
        return pltpu.make_async_copy(grad_pre_buf, grad_pre_hbm.at[sub], grad_pre_sem)

    def core_copy(chunk):
        slot = chunk % RECV_SLOTS
        return pltpu.make_async_remote_copy(
            src_ref=sent_core, dst_ref=recv_core.at[slot], send_sem=core_send, recv_sem=core_recv.at[slot],
            device_id=(partners[CORE],), device_id_type=MESH)

    def out_copy(level, color, chunk):
        slot = chunk % RECV_SLOTS
        return pltpu.make_async_remote_copy(
            src_ref=sent_bufs[level].at[color], dst_ref=recv_bufs[level].at[slot, color],
            send_sem=out_send.at[level, color], recv_sem=out_recv.at[level, color, slot],
            device_id=(partners[COLOR_DIMS[color][level]],), device_id_type=MESH)

    def back_copy(level, color, chunk, arriving):
        slot = chunk % GATHER_SLOTS
        mine = ring.at[slot, core, color, rows_at(base(color, level + 1), spans[level]), :]
        theirs = ring.at[slot, core, color, rows_at(other(color, level), spans[level]), :]
        return pltpu.make_async_remote_copy(
            src_ref=mine, dst_ref=theirs if arriving else mine,
            send_sem=back_send.at[level, color, slot], recv_sem=back_recv.at[level, color, slot],
            device_id=(partners[COLOR_DIMS[color][level]],), device_id_type=MESH)

    def part_rows(color):
        return rows_at(base(color, 1), spans[0])

    def part_share_copy(color, chunk, arriving):
        slot = chunk % GATHER_SLOTS
        mine = ring.at[slot, core, color, part_rows(color), :]
        theirs = ring.at[slot, 1 - core, color, part_rows(color), :]
        return pltpu.make_async_remote_copy(
            src_ref=mine, dst_ref=theirs if arriving else mine,
            send_sem=back_send.at[0, color, slot], recv_sem=back_recv.at[0, color, slot],
            device_id=(partners[CORE],), device_id_type=MESH)

    def part_stores(group, chunk):
        slot = chunk % GATHER_SLOTS
        place = chunk - full_chunks - sum(PART_GROUPS[:group])
        copies = []
        for color in range(COLORS):
            for which in range(2):
                out_ref = part_refs[(group * COLORS + color) * 2 + which]
                source = ring.at[slot, core if which == 0 else 1 - core, color, part_rows(color), :]
                copies.append(pltpu.make_async_copy(
                    source, out_ref.at[place], part_sem.at[color, which, slot]))
        return copies

    def share_copy(chunk, arriving):
        slot = chunk % GATHER_SLOTS
        return pltpu.make_async_remote_copy(
            src_ref=ring.at[slot, core], dst_ref=ring.at[slot, 1 - core if arriving else core],
            send_sem=share_send.at[slot], recv_sem=share_recv.at[slot],
            device_id=(partners[CORE],), device_id_type=MESH)

    def store_copy(chunk):
        slot = chunk % GATHER_SLOTS
        return pltpu.make_async_copy(ring.at[slot], gathered.at[chunk], store_sem.at[slot])

    def small_copy(step):
        return pltpu.make_async_remote_copy(
            src_ref=small_out, dst_ref=small_recv.at[step], send_sem=small_send_sem.at[step],
            recv_sem=small_recv_sem.at[step], device_id=(partners[step],), device_id_type=MESH)

    def product(chunk, which_core, color):
        slot = chunk % 2
        start = pl.multiple_of(which_core * half + color * region, 128)
        return lax.dot_general(
            rows_buf[slot, :, pl.ds(start, region)], cols_buf[slot], TOKEN_DIMS, preferred_element_type=jnp.float32)

    def opens_layer(chunk):
        return (chunk > 0) & (chunk % (2 * chunks_per_mat) == 0)

    def load(chunk):
        for_mat(chunk, lambda mat: rows_load(mat, chunk).wait())
        for_mat(chunk, lambda mat: cols_load(mat, chunk).wait())
        after = chunk + 1

        @pl.when(chunk == 0)
        def _():
            grad_b_copy.start()
            for copy in weight_loads(0, chunk):
                copy.start()

        @pl.when(after < num_chunks)
        def _():
            for_mat(after, lambda mat: rows_load(mat, after).start())

        @pl.when((after < num_chunks) & jnp.logical_not(opens_layer(after)))
        def _():
            for_mat(after, lambda mat: cols_load(mat, after).start())

    def load_weights(chunk):
        def arrive(mat):
            for copy in weight_loads(mat, chunk):
                copy.wait()

        for_mat(chunk, arrive)
        after, before = chunk + 1, chunk - 1

        @pl.when(chunk == 0)
        def _():
            grad_b_copy.wait()

        @pl.when(after < num_chunks)
        def _():
            def start(mat):
                for copy in weight_loads(mat, after):
                    copy.start()

            for_mat(after, start)

        @pl.when((before >= 0) & ((before // chunks_per_mat) % 2 == 0))
        def _():
            grad_pre_store(before % chunks_per_mat).wait()

    def compute_sent(chunk):
        @pl.loop(0, COLORS)
        def _(color):
            sent_core[color] = product(chunk, 1 - core, color).astype(jnp.bfloat16)

    def share_core(chunk):
        core_copy(chunk).start()

    def compute_kept(chunk):
        slot = chunk % KEPT_SLOTS

        @pl.loop(0, COLORS)
        def _(color):
            kept[slot, color] = product(chunk, core, color)

    def halve(level, chunk, arrived):
        slot = chunk % KEPT_SLOTS
        recv_slot = chunk % RECV_SLOTS
        for color in range(COLORS):
            if level > 0:
                out_copy(level - 1, color, chunk).wait()
            held = base(color, level)

            def total(start, size, color=color, held=held):
                own = kept[slot, color, rows_at(start, size), :]
                return own + arrived[recv_slot, color, rows_at(start - held, size), :].astype(jnp.float32)

            if level < 3:
                mine = base(color, level + 1)
                sent_bufs[level][color] = total(other(color, level), spans[level]).astype(jnp.bfloat16)
                kept[slot, color, rows_at(mine, spans[level]), :] = total(mine, spans[level])
                out_copy(level, color, chunk).start()
            else:
                gather_slot = chunk % GATHER_SLOTS
                ring[gather_slot, core, color, rows_at(held, spans[2]), :] = total(held, spans[2]).astype(jnp.bfloat16)
                back_copy(2, color, chunk, False).start()

    def send_1(chunk):
        core_copy(chunk).wait()
        halve(0, chunk, recv_core)

    def send_2(chunk):
        halve(1, chunk, recv_1)

    def send_3(chunk):
        halve(2, chunk, recv_2)

    def send_back_3(chunk):
        halve(3, chunk, recv_3)

    def pass_back(level, chunk):
        for color in range(COLORS):
            back_copy(level + 1, color, chunk, True).wait()
            back_copy(level, color, chunk, False).start()

    def send_back_2(chunk):
        pass_back(1, chunk)

    def send_back_1(chunk):
        @pl.when(chunk < full_chunks)
        def _():
            pass_back(0, chunk)

        @pl.when(chunk >= full_chunks)
        def _():
            for color in range(COLORS):
                back_copy(1, color, chunk, True).wait()
                part_share_copy(color, chunk, False).start()

    def send_back_core(chunk):
        @pl.when(chunk < full_chunks)
        def _():
            for color in range(COLORS):
                back_copy(0, color, chunk, True).wait()
            share_copy(chunk, False).start()

        @pl.when(chunk >= full_chunks)
        def _():
            for color in range(COLORS):
                part_share_copy(color, chunk, True).wait()

        for group, size in enumerate(PART_GROUPS):
            first = full_chunks + sum(PART_GROUPS[:group])

            @pl.when((chunk >= first) & (chunk < first + size))
            def _(group=group):
                for copy in part_stores(group, chunk):
                    copy.start()

    def store(chunk):
        @pl.when(chunk < full_chunks)
        def _():
            share_copy(chunk, True).wait()
            store_copy(chunk).start()

        @pl.when((chunk > 0) & (chunk <= full_chunks))
        def _():
            store_copy(chunk - 1).wait()

        for group, size in enumerate(PART_GROUPS):
            first = full_chunks + sum(PART_GROUPS[:group])

            @pl.when((chunk >= first) & (chunk < first + size))
            def _(group=group):
                for copy in part_stores(group, chunk):
                    copy.wait()

    token_half = grad_b.shape[0] // 2

    def backward(part, chunk):
        slot = chunk % 2
        sub = chunk % chunks_per_mat
        mat = chunk // chunks_per_mat
        layer = num_layers - 1 - mat // 2

        @pl.when(mat % 2 == 0)
        def _():
            cols = slice(part * TILE, (part + 1) * TILE)

            @pl.loop(0, 2)
            def _(which):
                rows = pl.ds(pl.multiple_of(which * token_half, 128), token_half)
                grad_act = lax.dot_general(
                    grad_b[rows, :], weight_buf[slot, cols, :], FEATURE_DIMS, preferred_element_type=jnp.float32)
                grad_pre = grad_act * gelu_slope(pre_buf[slot, rows, cols].astype(jnp.float32))
                grad_pre_buf[rows, cols] = grad_pre.astype(jnp.bfloat16)
                start = row_dim + sub * chunk_cols + part * TILE
                small_out[pl.ds(layer, 1), pl.ds(pl.multiple_of(start, 128), TILE)] += jnp.sum(grad_pre, axis=0, keepdims=True)

            if part == chunk_cols // TILE - 1:
                grad_pre_store(sub).start()

        @pl.when(mat % 2 == 1)
        def _():
            pieces = row_dim // chunk_cols * (chunk_cols // TILE) // 3
            grad_rows = []
            for piece in range(part * pieces, (part + 1) * pieces):
                start, first = divmod(piece * TILE, chunk_cols)
                grad_rows.append((piece, lax.dot_general(
                    cols_buf[slot], weight_buf[slot, first:first + TILE, start * chunk_cols:(start + 1) * chunk_cols],
                    FEATURE_DIMS, preferred_element_type=jnp.float32)))
            for piece, value in grad_rows:
                grad_normed[:, piece * TILE:(piece + 1) * TILE] += value

    def norm_loads(layer, block):
        rows = pl.ds(pl.multiple_of(block * NORM_ROWS, NORM_ROWS), NORM_ROWS)
        slot = block % 2
        copies = [pltpu.make_async_copy(hid_refs[layer].at[rows, :], hid_buf.at[slot], norm_sem.at[0, slot])]
        if layer > 0:
            copies.append(pltpu.make_async_copy(grad_top.at[rows, :], grad_buf.at[slot], norm_sem.at[1, slot]))
        return copies

    def layer_input_grad(layer):
        num_blocks = grad_b.shape[0] // NORM_ROWS
        for copy in norm_loads(layer, 0):
            copy.start()

        @pl.loop(0, num_blocks)
        def _(block):
            @pl.when(block + 1 < num_blocks)
            def _():
                for copy in norm_loads(layer, block + 1):
                    copy.start()

            for copy in norm_loads(layer, block):
                copy.wait()
            rows = pl.ds(pl.multiple_of(block * NORM_ROWS, NORM_ROWS), NORM_ROWS)
            hid_f = hid_buf[block % 2].astype(jnp.float32)
            hid_scale = inverse_rms(hid_f)
            hid_hat = hid_f * hid_scale
            normed_grad = grad_normed[rows, :]
            small_out[layer:layer + 1, :row_dim] += jnp.sum(normed_grad * hid_hat, axis=0, keepdims=True)
            if layer > 0:
                grad_normed[rows, :] = jnp.zeros((NORM_ROWS, row_dim), jnp.float32)
                grad_hat = normed_grad * gain_in[layer:layer + 1, :].astype(jnp.float32)
                grad_new = grad_buf[block % 2] + hid_scale * (
                    grad_hat - hid_hat * jnp.mean(grad_hat * hid_hat, axis=-1, keepdims=True))
                grad_b[rows, :] = grad_new.astype(jnp.bfloat16)
                small_out[layer - 1:layer, row_dim + hidden_dim:] += jnp.sum(grad_new, axis=0, keepdims=True)

        if layer > 0:
            copy = pltpu.make_async_copy(grad_b, grad_b_hbm, grad_b_sem)
            copy.start()
            copy.wait()
            following = jnp.int32((num_layers - layer) * 2 * chunks_per_mat)
            cols_load((num_layers - layer) * 2, following).start()

    def input_grad(chunk):
        for layer in range(num_layers):
            last = (num_layers - 1 - layer) * 2 * chunks_per_mat + 2 * chunks_per_mat - 1

            @pl.when(chunk == last)
            def _(layer=layer):
                layer_input_grad(layer)

    events = dict(
        load=load, load_weights=load_weights, compute_sent=compute_sent, share_core=share_core, compute_kept=compute_kept, send_1=send_1, send_2=send_2, send_3=send_3,
        send_back_3=send_back_3, send_back_2=send_back_2, send_back_1=send_back_1, send_back_core=send_back_core, store=store,
        backward_0=functools.partial(backward, 0), backward_1=functools.partial(backward, 1),
        backward_2=functools.partial(backward, 2), input_grad=input_grad)

    first = jnp.int32(0)
    rows_load(0, first).start()
    cols_load(0, first).start()
    grad_b_copy = pltpu.make_async_copy(grad_top_b, grad_b, grad_b_sem)
    barrier = pltpu.get_barrier_semaphore()
    for partner in partners:
        pl.semaphore_signal(barrier, inc=1, device_id=(partner,), device_id_type=MESH)
    small_out[...] = small_in[...]
    grad_normed[...] = jnp.zeros_like(grad_normed)
    pl.semaphore_wait(barrier, 4)

    @pl.loop(0, num_chunks + MAX_LAG)
    def _(it):
        for step in range(4):
            @pl.when(it == num_chunks + step)
            def _(step=step):
                small_copy(step).start()
        for name, lag in PIPELINE:
            chunk = it - lag

            @pl.when((chunk >= 0) & (chunk < num_chunks))
            def _(name=name, chunk=chunk):
                events[name](chunk)
        for step in range(4):
            @pl.when(it == num_chunks + step)
            def _(step=step):
                small_copy(step).wait()
                small_out[...] += small_recv[step]


def backward_pass(hid_rows, saved, grad_top, grad_top_b, norm_gain, w_up, w_down, small, axis, chunk_cols):
    num_layers, row_dim, hidden = w_up.shape
    tokens = grad_top.shape[0]
    chunks_per_mat = hidden // chunk_cols
    region = row_dim // (2 * COLORS)
    half = (COLORS, region, chunk_cols)
    sizes = (num_layers, chunks_per_mat, row_dim, chunk_cols, region, row_dim // chunk_cols, axis)
    num_chunks = 2 * num_layers * chunks_per_mat
    bf16, f32 = jnp.bfloat16, jnp.float32
    dma = pltpu.SemaphoreType.DMA
    any_spec = pl.BlockSpec(memory_space=pl.ANY)
    vmem_spec = pl.BlockSpec(memory_space=pltpu.VMEM)
    full_chunks = num_chunks - sum(PART_GROUPS)
    part_shapes = [jax.ShapeDtypeStruct((size, region // 2, chunk_cols), bf16) for size in PART_GROUPS for _ in range(2 * COLORS)]
    gathered, small_sum, _, _, *parts = pl.pallas_call(
        functools.partial(backward_kernel, sizes),
        out_shape=[
            jax.ShapeDtypeStruct((full_chunks, 2) + half, bf16),
            jax.ShapeDtypeStruct(small.shape, f32),
            jax.ShapeDtypeStruct((chunks_per_mat, tokens, chunk_cols), bf16),
            jax.ShapeDtypeStruct((tokens, row_dim), bf16),
        ] + part_shapes,
        in_specs=[any_spec] * (num_layers + 7) + [vmem_spec] * 2,
        out_specs=[any_spec, vmem_spec, any_spec, any_spec] + [any_spec] * len(part_shapes),
        scratch_shapes=[
            pltpu.VMEM((2, tokens, row_dim), bf16),
            pltpu.VMEM((2, tokens, chunk_cols), bf16),
            pltpu.VMEM(half, bf16),
            pltpu.VMEM((KEPT_SLOTS,) + half, f32),
            pltpu.VMEM((RECV_SLOTS,) + half, bf16),
            pltpu.VMEM((COLORS, region // 2, chunk_cols), bf16),
            pltpu.VMEM((COLORS, region // 4, chunk_cols), bf16),
            pltpu.VMEM((COLORS, region // 8, chunk_cols), bf16),
            pltpu.VMEM((RECV_SLOTS, COLORS, region // 2, chunk_cols), bf16),
            pltpu.VMEM((RECV_SLOTS, COLORS, region // 4, chunk_cols), bf16),
            pltpu.VMEM((RECV_SLOTS, COLORS, region // 8, chunk_cols), bf16),
            pltpu.VMEM((GATHER_SLOTS, 2) + half, bf16),
            pltpu.VMEM((2, chunk_cols, row_dim), bf16),
            pltpu.VMEM((2, tokens, chunk_cols), bf16),
            pltpu.VMEM((tokens, chunk_cols), bf16),
            pltpu.VMEM((tokens, row_dim), bf16),
            pltpu.VMEM((tokens, row_dim), f32),
            pltpu.VMEM((2, NORM_ROWS, row_dim), bf16),
            pltpu.VMEM((2, NORM_ROWS, row_dim), f32),
            pltpu.VMEM((4,) + small.shape, f32),
            dma((4, 2)), dma, dma((2, 2)), dma,
            dma, dma((RECV_SLOTS,)), dma((3, COLORS)), dma((3, COLORS, RECV_SLOTS)),
            dma((3, COLORS, GATHER_SLOTS)), dma((3, COLORS, GATHER_SLOTS)), dma((GATHER_SLOTS,)), dma((GATHER_SLOTS,)),
            dma((GATHER_SLOTS,)), dma((4,)), dma((4,)), dma((COLORS, 2, GATHER_SLOTS)),
        ],
        compiler_params=pltpu.CompilerParams(collective_id=0, has_side_effects=True, vmem_limit_bytes=67043328),
        name="backward",
    )(*hid_rows, *saved, grad_top, grad_top_b, w_up, w_down, norm_gain, small)
    return gathered, small_sum, parts


def flip_pairs(num_devices, bit):
    return [(dev, dev ^ (1 << bit)) for dev in range(num_devices)]


def stream_blocks(num_blocks, start_loads, wait_loads, store_of, in_buf, out_buf):
    slots, region = in_buf.shape[0], in_buf.shape[2]
    for block in range(min(slots - 1, num_blocks)):
        start_loads(jnp.int32(block), block)

    @pl.loop(0, num_blocks)
    def _(block):
        slot = block % slots

        @pl.when(block + slots - 1 < num_blocks)
        def _():
            start_loads(block + slots - 1, (block + slots - 1) % slots)

        wait_loads(block, slot)

        @pl.when(block >= slots)
        def _():
            store_of(block - slots, slot).wait()

        for color in range(COLORS):
            out_buf[slot, color * region:(color + 1) * region, :] = in_buf[slot, color].astype(jnp.float32)
        store_of(block, slot).start()

    for block in range(max(num_blocks - slots, 0), num_blocks):
        store_of(jnp.int32(block), block % slots).wait()


def block_target(out_ref, layer, kind, down_subs, chunk, which_core, rows, cols):
    half = pl.multiple_of(which_core * rows, rows)
    if kind == 0:
        first = pl.multiple_of((chunk // down_subs) * 2 * rows + half, rows)
        return out_ref.at[layer, pl.ds(first, rows), pl.ds(pl.multiple_of((chunk % down_subs) * cols, 128), cols)]
    return out_ref.at[layer, pl.ds(half, rows), pl.ds(pl.multiple_of(chunk * cols, 128), cols)]


def widen_kernel(spec, *refs):
    first, count, place, layer, kind, down_subs, small_widths, in_place = spec
    if in_place:
        refs = refs[:1 + bool(small_widths)] + refs[2 + bool(small_widths):]
    if small_widths:
        gathered, small, out_ref, *small_outs, in_buf, out_buf, in_sem, out_sem = refs
        start = 0
        for width, small_out in zip(small_widths, small_outs):
            small_out[...] = small[:, start:start + width]
            start += width
    else:
        gathered, out_ref, in_buf, out_buf, in_sem, out_sem = refs
    rows, cols = out_buf.shape[1:]

    def load(block, slot):
        return pltpu.make_async_copy(gathered.at[first + block // 2, block % 2], in_buf.at[slot], in_sem.at[slot])

    def store(block, slot):
        target = block_target(out_ref, layer, kind, down_subs, place + block // 2, block % 2, rows, cols)
        return pltpu.make_async_copy(out_buf.at[slot], target, out_sem.at[slot])

    stream_blocks(
        2 * count, lambda block, slot: load(block, slot).start(), lambda block, slot: load(block, slot).wait(),
        store, in_buf, out_buf)


def join_kernel(spec, *refs):
    count, place, layer, kind, down_subs, axis = spec
    parts, (_, out_ref, in_buf, out_buf, in_sem, out_sem) = refs[:4 * COLORS], refs[4 * COLORS:]
    rows, cols = out_buf.shape[1:]
    part_rows = in_buf.shape[2] // 2
    me = lax.axis_index(axis)
    core = me % 2

    def copies(which, chunk, slot):
        found = []
        for color in range(COLORS):
            upper = (me >> COLOR_DIMS[color][0]) & 1
            for far in range(2):
                start = pl.multiple_of((upper if far == 0 else 1 - upper) * part_rows, part_rows)
                found.append(pltpu.make_async_copy(
                    parts[color * 4 + far * 2 + which].at[chunk],
                    in_buf.at[slot, color, pl.ds(start, part_rows), :], in_sem.at[slot]))
        return found

    def start_loads(block, slot):
        for which in range(2):
            @pl.when(block % 2 == which)
            def _(which=which):
                for copy in copies(which, block // 2, slot):
                    copy.start()

    def wait_loads(block, slot):
        for copy in copies(0, block // 2, slot):
            copy.wait()

    def store(block, slot):
        which_core = jnp.where(block % 2 == 0, core, 1 - core)
        target = block_target(out_ref, layer, kind, down_subs, place + block // 2, which_core, rows, cols)
        return pltpu.make_async_copy(out_buf.at[slot], target, out_sem.at[slot])

    stream_blocks(2 * count, start_loads, wait_loads, store, in_buf, out_buf)


def widen_scratch(region, cols):
    return [
        pltpu.VMEM((STREAM_SLOTS, COLORS, region, cols), jnp.bfloat16),
        pltpu.VMEM((STREAM_SLOTS, COLORS * region, cols), jnp.float32),
        pltpu.SemaphoreType.DMA((STREAM_SLOTS,)),
        pltpu.SemaphoreType.DMA((STREAM_SLOTS,)),
    ]


def widen_cost(count, region, cols):
    size = count * 2 * COLORS * region * cols
    return pl.CostEstimate(flops=500 * size, bytes_accessed=6 * size, transcendentals=0)


def widen(gathered, first, count, place, layer, kind, shape, into, down_subs, small, small_widths):
    region, cols = gathered.shape[3:]
    any_spec = pl.BlockSpec(memory_space=pl.ANY)
    vmem_spec = pl.BlockSpec(memory_space=pltpu.VMEM)
    smalls = [jax.ShapeDtypeStruct((small.shape[0], width), jnp.float32) for width in small_widths]
    return pl.pallas_call(
        functools.partial(widen_kernel, (first, count, place, layer, kind, down_subs, small_widths, into is not None)),
        in_specs=[any_spec] + [vmem_spec] * bool(smalls) + [any_spec] * (into is not None),
        out_specs=[any_spec] + [vmem_spec] * len(smalls),
        out_shape=[jax.ShapeDtypeStruct(shape, jnp.float32)] + smalls,
        input_output_aliases={} if into is None else {1 + bool(smalls): 0},
        scratch_shapes=widen_scratch(region, cols),
        cost_estimate=widen_cost(count, region, cols),
        compiler_params=pltpu.CompilerParams(vmem_limit_bytes=67043328),
    )(gathered, *([small] if smalls else []), *([] if into is None else [into]))


def join(parts, place, layer, kind, into, down_subs, axis):
    count, part_rows, cols = parts[0].shape
    any_spec = pl.BlockSpec(memory_space=pl.ANY)
    return pl.pallas_call(
        functools.partial(join_kernel, (count, place, layer, kind, down_subs, axis)),
        in_specs=[any_spec] * (len(parts) + 1),
        out_specs=any_spec,
        out_shape=jax.ShapeDtypeStruct(into.shape, jnp.float32),
        scratch_shapes=widen_scratch(2 * part_rows, cols),
        input_output_aliases={len(parts): 0},
        cost_estimate=widen_cost(count, 2 * part_rows, cols),
        compiler_params=pltpu.CompilerParams(vmem_limit_bytes=67043328),
    )(*parts, into)


def swap(array, axis, num_devices, bit):
    return lax.ppermute(array, axis, flip_pairs(num_devices, bit))


def full_gradients(gathered, parts, small, num_layers, row_dim, hidden, chunk_cols, axis, num_devices):
    per_mat = hidden // chunk_cols
    down_subs = row_dim // chunk_cols
    groups = range(len(PART_GROUPS))
    mine = [[parts[(group * COLORS + color) * 2] for color in range(COLORS)] for group in groups]
    theirs = [[parts[(group * COLORS + color) * 2 + 1] for color in range(COLORS)] for group in groups]
    far = [[swap(mine[group][color], axis, num_devices, COLOR_DIMS[color][0])
            for color in range(COLORS)] for group in groups]
    last = num_layers - 1
    full = [None, None]
    shapes = ((num_layers, hidden, row_dim), (num_layers, row_dim, hidden))
    for call, count in enumerate(WIDEN_CALLS):
        first = sum(WIDEN_CALLS[:call])
        kind, place = divmod(first, per_mat)
        small_widths = (row_dim, hidden, row_dim) if call == 0 else ()
        full[kind], *rest = widen(
            gathered, first, count, place, last, kind, shapes[kind], full[kind], down_subs, small, small_widths)
        smalls = rest or smalls
    for group in groups:
        kind, place = divmod(sum(PART_GROUPS[:group]), per_mat)
        pieces = []
        for color in range(COLORS):
            shared = swap(far[group][color], axis, num_devices, CORE)
            pieces += [mine[group][color], theirs[group][color], far[group][color], shared]
        full[kind] = join(pieces, place, 0, kind, full[kind], down_subs, axis)
    return smalls[0], full[1], smalls[1], full[0], smalls[2]


def solution(mesh):
    axis = mesh.axis_names[0]

    def device_grads(tokens, upstream, norm_gain, w_up, bias_up, w_down, bias_down):
        num_layers, width = norm_gain.shape
        hidden_width = w_up.shape[2]
        chunk_cols = width // 2
        hid_1, normed, pre_act, activated, grad_top, grad_top_b, small = forward_pass(
            tokens, upstream, norm_gain, w_up, bias_up, w_down, bias_down, width)
        gathered, small, parts = backward_pass(
            (tokens, hid_1), (normed, pre_act, activated), grad_top, grad_top_b, norm_gain, w_up, w_down, small, axis, chunk_cols)
        return full_gradients(gathered, parts, small, num_layers, width, hidden_width, chunk_cols, axis, mesh.size)

    row_spec = P(axis, None)
    full_spec = P()
    return jax.shard_map(
        device_grads,
        mesh=mesh,
        in_specs=(row_spec, row_spec, full_spec, full_spec, full_spec, full_spec, full_spec),
        out_specs=(full_spec, full_spec, full_spec, full_spec, full_spec),
        check_vma=False,
    )
```

```python
import functools

import jax
import jax.numpy as jnp
from jax import lax
from jax.experimental import pallas as pl
from jax.experimental.pallas import tpu as pltpu
from jax.sharding import PartitionSpec as P


EPSILON = 1e-6
FEATURE_DIMS = (((1,), (1,)), ((), ()))
MESH = pl.DeviceIdType.MESH
COLORS = 3
CORE, DIM_X, DIM_Y, DIM_Z = range(4)
COLOR_DIMS = ((DIM_X, DIM_Y, DIM_Z), (DIM_Y, DIM_Z, DIM_X), (DIM_Z, DIM_X, DIM_Y))
PIPELINE = (
    ("load", 0), ("compute_sent", 0), ("share_core", 0), ("send_3", 2), ("send_back_2", 4), ("send_back_1", 5),
    ("compute_kept", 0), ("send_back_core", 6), ("load_weights", 0), ("backward_0", 0), ("send_2", 1), ("backward_1", 0),
    ("send_1", 0), ("backward_2", 0), ("send_back_3", 2), ("store", 6), ("input_grad", 0),
)
MAX_LAG = 6
PART_GROUPS = (7, 5, 3, 3)
WIDEN_CALLS = (8, 6)
RECV_SLOTS = 2
KEPT_SLOTS = 3
GATHER_SLOTS = 6
TILE = 256
UP_COLS = 512
ACT_ROWS = 16
ACT_COLS = 256
STREAM_SLOTS = 4
NORM_ROWS = 128
GELU_SCALE = 0.7978845608028654
GELU_CUBIC = 0.044715


def inverse_rms(hid_f):
    return lax.rsqrt(jnp.mean(hid_f * hid_f, axis=-1, keepdims=True) + EPSILON)


def gelu(values):
    return (0.5 * values) * (1.0 + jnp.tanh(values * (GELU_SCALE + GELU_SCALE * GELU_CUBIC * (values * values))))


def forward_kernel(
    sizes, tokens, upstream, w_up, w_down, gain_in, bias_up_in, bias_down_in, hid_out, normed_out, pre_act_out, act_out,
    grad_top_out, grad_top_b_out, small_out, hid, normed, branch, up_buf, down_buf, pre_buf, act_buf, up_rows, grad_b_buf,
    gain, bias_up, bias_down, io_sem, up_sem, down_sem, pre_sem, act_sem,
):
    num_layers, num_tiles, tile_cols = sizes
    num_tokens, row_dim = hid.shape
    steps = num_tiles + 1
    parts = tile_cols // UP_COLS

    def up_load(layer, tile):
        cols = pl.ds(pl.multiple_of(tile * tile_cols, 128), tile_cols)
        return pltpu.make_async_copy(w_up.at[layer, :, cols], up_buf.at[tile % 2], up_sem.at[tile % 2])

    def down_load(layer, tile):
        rows = pl.ds(pl.multiple_of(tile * tile_cols, 128), tile_cols)
        return pltpu.make_async_copy(w_down.at[layer, rows, :], down_buf.at[tile % 2], down_sem.at[tile % 2])

    def pre_store(layer, tile):
        cols = pl.ds(pl.multiple_of(tile * tile_cols, 128), tile_cols)
        return pltpu.make_async_copy(pre_buf.at[tile % 2], pre_act_out.at[layer, :, cols], pre_sem.at[tile % 2])

    def act_store(layer, tile):
        cols = pl.ds(pl.multiple_of(tile * tile_cols, 128), tile_cols)
        return pltpu.make_async_copy(act_buf.at[tile % 2], act_out.at[layer, :, cols], act_sem.at[tile % 2])

    def normed_store(layer):
        return pltpu.make_async_copy(normed, normed_out.at[layer], io_sem.at[1])

    def hid_store():
        return pltpu.make_async_copy(hid, hid_out, io_sem.at[2])

    tokens_load = pltpu.make_async_copy(tokens, hid, io_sem.at[0])
    tokens_load.start()
    up_load(0, 0).start()
    upstream_load = pltpu.make_async_copy(upstream, up_rows, io_sem.at[3])
    small_out[...] = jnp.zeros_like(small_out)
    branch[...] = jnp.zeros_like(branch)
    pre_buf[0, :, :UP_COLS] = jnp.zeros((num_tokens, UP_COLS), jnp.bfloat16)
    gain[...] = gain_in[...].astype(jnp.float32)
    bias_up[...] = bias_up_in[...].astype(jnp.float32)
    bias_down[...] = bias_down_in[...].astype(jnp.float32)
    tokens_load.wait()

    def each_block(action):
        @pl.loop(0, num_tokens // NORM_ROWS)
        def _(block):
            action(pl.ds(pl.multiple_of(block * NORM_ROWS, NORM_ROWS), NORM_ROWS))

    def normalize(layer, rows, hid_f):
        normed[rows, :] = ((hid_f * inverse_rms(hid_f)) * gain[pl.ds(layer, 1), :]).astype(jnp.bfloat16)

    def next_rows(layer, rows):
        new = ((hid[rows, :].astype(jnp.float32) + branch[rows, :]) + bias_down[pl.ds(layer, 1), :]).astype(jnp.bfloat16)
        hid[rows, :] = new
        return new.astype(jnp.float32)

    def activate(slot, part):
        start = part * UP_COLS
        for row in range(0, num_tokens, ACT_ROWS):
            for col in range(0, UP_COLS, ACT_COLS):
                piece = (slot, pl.ds(row, ACT_ROWS), pl.ds(pl.multiple_of(start + col, 128), ACT_COLS))
                act_buf[piece] = gelu(pre_buf[piece].astype(jnp.float32)).astype(jnp.bfloat16)

    def up_product(layer, tile):
        @pl.loop(0, parts)
        def _(part):
            fresh = tile * parts + part == 0
            last_slot = jnp.where((part == 0) & (tile > 0), (tile + 1) % 2, tile % 2)
            activate(last_slot, jnp.where(fresh, 0, (part + parts - 1) % parts))
            cols = pl.ds(pl.multiple_of(part * UP_COLS, 128), UP_COLS)
            bias = bias_up[pl.ds(layer, 1), pl.ds(pl.multiple_of(tile * tile_cols + part * UP_COLS, 128), UP_COLS)]
            pre_buf[tile % 2, :, cols] = (
                jnp.dot(normed[...], up_buf[tile % 2, :, cols], preferred_element_type=jnp.float32) + bias
            ).astype(jnp.bfloat16)

    def down_product(tile):
        slot = tile % 2
        for part in range(row_dim // UP_COLS):
            cols = slice(part * UP_COLS, (part + 1) * UP_COLS)
            branch[:, cols] += jnp.dot(act_buf[slot], down_buf[slot, :, cols], preferred_element_type=jnp.float32)

    each_block(lambda rows: normalize(0, rows, hid[rows, :].astype(jnp.float32)))

    @pl.loop(0, num_layers * steps)
    def _(step):
        layer, tile = step // steps, step % steps

        @pl.when(tile < num_tiles)
        def _():
            up_load(layer, tile).wait()

            @pl.when(tile + 1 < num_tiles)
            def _():
                up_load(layer, tile + 1).start()

            @pl.when((tile == num_tiles - 1) & (layer + 1 < num_layers))
            def _():
                up_load(layer + 1, 0).start()

            @pl.when(step == 0)
            def _():
                normed_store(0).start()
                down_load(0, 0).start()
                upstream_load.start()

            @pl.when(tile > 1)
            def _():
                pre_store(layer, tile - 2).wait()
                act_store(layer, tile - 2).wait()

            up_product(layer, tile)
            pre_store(layer, tile).start()

        @pl.when(tile == num_tiles)
        def _():
            activate((num_tiles - 1) % 2, parts - 1)

        @pl.when(tile > 0)
        def _():
            act_store(layer, tile - 1).start()
            down_load(layer, tile - 1).wait()

            @pl.when(tile < num_tiles)
            def _():
                down_load(layer, tile).start()

            @pl.when((tile == num_tiles) & (layer + 1 < num_layers))
            def _():
                down_load(layer + 1, 0).start()

            down_product(tile - 1)

        @pl.when(tile == num_tiles)
        def _():
            for back in (2, 1):
                pre_store(layer, num_tiles - back).wait()
                act_store(layer, num_tiles - back).wait()
            normed_store(layer).wait()

            @pl.when(layer + 1 < num_layers)
            def _():
                def to_next(rows):
                    normalize(layer + 1, rows, next_rows(layer, rows))
                    branch[rows, :] = jnp.zeros((NORM_ROWS, row_dim), jnp.float32)

                each_block(to_next)
                hid_store().start()
                normed_store(layer + 1).start()

    hid_store().wait()
    upstream_load.wait()
    bias_start = small_out.shape[1] - row_dim

    def grad_stores(rows):
        return (
            pltpu.make_async_copy(branch.at[rows, :], grad_top_out.at[rows, :], io_sem.at[0]),
            pltpu.make_async_copy(grad_b_buf.at[rows, :], grad_top_b_out.at[rows, :], io_sem.at[1]),
        )

    def top_rows(rows):
        top_f = next_rows(num_layers - 1, rows)
        top_scale = inverse_rms(top_f)
        top_hat = top_f * top_scale
        up_f = up_rows[rows, :].astype(jnp.float32)
        grad = top_scale * (up_f - top_hat * jnp.mean(up_f * top_hat, axis=-1, keepdims=True))
        branch[rows, :] = grad
        grad_b_buf[rows, :] = grad.astype(jnp.bfloat16)
        small_out[num_layers - 1:, bias_start:] += jnp.sum(grad, axis=0, keepdims=True)
        for copy in grad_stores(rows):
            copy.start()

    each_block(top_rows)
    for copy in grad_stores(pl.ds(0, num_tokens)):
        copy.wait()


def forward_pass(tokens, upstream, norm_gain, w_up, bias_up, w_down, bias_down, tile_cols):
    num_tokens, row_dim = tokens.shape
    num_layers, _, hidden = w_up.shape
    bf16, f32 = jnp.bfloat16, jnp.float32
    dma = pltpu.SemaphoreType.DMA
    any_spec = pl.BlockSpec(memory_space=pl.ANY)
    vmem_spec = pl.BlockSpec(memory_space=pltpu.VMEM)
    rows = (num_tokens, row_dim)
    wide = (num_layers, num_tokens, hidden)
    return pl.pallas_call(
        functools.partial(forward_kernel, (num_layers, hidden // tile_cols, tile_cols)),
        out_shape=(
            jax.ShapeDtypeStruct(rows, bf16),
            jax.ShapeDtypeStruct((num_layers,) + rows, bf16),
            jax.ShapeDtypeStruct(wide, bf16),
            jax.ShapeDtypeStruct(wide, bf16),
            jax.ShapeDtypeStruct(rows, f32),
            jax.ShapeDtypeStruct(rows, bf16),
            jax.ShapeDtypeStruct((num_layers, 2 * row_dim + hidden), f32),
        ),
        in_specs=[any_spec] * 4 + [vmem_spec] * 3,
        out_specs=(any_spec,) * 6 + (vmem_spec,),
        scratch_shapes=[
            pltpu.VMEM(rows, bf16),
            pltpu.VMEM(rows, bf16),
            pltpu.VMEM(rows, f32),
            pltpu.VMEM((2, row_dim, tile_cols), bf16),
            pltpu.VMEM((2, tile_cols, row_dim), bf16),
            pltpu.VMEM((2, num_tokens, tile_cols), bf16),
            pltpu.VMEM((2, num_tokens, tile_cols), bf16),
            pltpu.VMEM(rows, bf16),
            pltpu.VMEM(rows, bf16),
            pltpu.VMEM((num_layers, row_dim), f32),
            pltpu.VMEM((num_layers, hidden), f32),
            pltpu.VMEM((num_layers, row_dim), f32),
            dma((4,)), dma((2,)), dma((2,)), dma((2,)), dma((2,)),
        ],
        compiler_params=pltpu.CompilerParams(vmem_limit_bytes=60 * 2**20),
        name="forward",
    )(tokens, upstream, w_up, w_down, norm_gain, bias_up, bias_down)


def gelu_slope(values):
    square = values * values
    bend = jnp.tanh(values * (GELU_SCALE + GELU_SCALE * GELU_CUBIC * square))
    return 0.5 * (1.0 + bend) + (0.5 * values) * (1.0 - bend * bend) * (GELU_SCALE + 3.0 * GELU_SCALE * GELU_CUBIC * square)


def backward_kernel(sizes, *refs):
    num_layers, chunks_per_mat, row_dim, chunk_cols, region, down_subs, axis = sizes
    num_mats = 2 * num_layers
    hidden_dim = chunks_per_mat * chunk_cols
    hid_refs, refs = refs[:num_layers], refs[num_layers:]
    (normed, pre_act, activated, grad_top, grad_top_b, w_up, w_down, gain_in, small_in,
     gathered, small_out, grad_pre_hbm, grad_b_hbm) = refs[:13]
    part_count = 2 * COLORS * len(PART_GROUPS)
    part_refs, refs = refs[13:13 + part_count], refs[13 + part_count:]
    (rows_buf, turned, cols_buf, sent_core, kept, recv_core, sent_1, sent_2, sent_3, recv_1, recv_2, recv_3, ring,
     weight_buf, pre_buf, grad_pre_buf, grad_b, grad_normed, hid_buf, grad_buf,
     small_recv, load_sem, grad_pre_sem, norm_sem, grad_b_sem, core_send, core_recv, out_send, out_recv, back_send, back_recv,
     share_send, share_recv, store_sem, small_send_sem, small_recv_sem, part_sem) = refs
    num_chunks = num_mats * chunks_per_mat
    full_chunks = num_chunks - sum(PART_GROUPS)
    half = COLORS * region
    me = lax.axis_index(axis)
    bits = [me % 2, (me // 2) % 2, (me // 4) % 2, me // 8]
    partners = [me + (1 << d) - 2 * (1 << d) * bits[d] for d in range(4)]
    core = bits[CORE]
    sent_bufs, recv_bufs = (sent_1, sent_2, sent_3), (recv_1, recv_2, recv_3)
    spans = (region // 2, region // 4, region // 8)

    def base(color, level):
        total = 0
        for step in range(level):
            total = total + bits[COLOR_DIMS[color][step]] * spans[step]
        return total

    def other(color, level):
        return base(color, level) + (1 - bits[COLOR_DIMS[color][level]]) * spans[level]

    def rows_at(start, size):
        return pl.ds(pl.multiple_of(start, spans[2]), size)

    def rows_load(mat, chunk):
        layer = num_layers - 1 - mat // 2
        if mat % 2 == 0:
            start = ((chunk % chunks_per_mat) // down_subs) * row_dim
            source = activated.at[layer, :, pl.ds(pl.multiple_of(start, 128), row_dim)]
        else:
            source = normed.at[layer]
        return pltpu.make_async_copy(source, rows_buf, load_sem.at[0, 0])

    def weight_loads(mat, chunk):
        slot = chunk % 2
        layer = num_layers - 1 - mat // 2
        cols = pl.ds(pl.multiple_of((chunk % chunks_per_mat) * chunk_cols, 128), chunk_cols)
        if mat % 2 == 0:
            return [
                pltpu.make_async_copy(w_down.at[layer, cols, :], weight_buf.at[slot], load_sem.at[1, slot]),
                pltpu.make_async_copy(pre_act.at[layer, :, cols], pre_buf.at[slot], load_sem.at[2, slot]),
            ]
        return [
            pltpu.make_async_copy(
                w_up.at[layer, part * chunk_cols:(part + 1) * chunk_cols, cols],
                weight_buf.at[slot, :, part * chunk_cols:(part + 1) * chunk_cols], load_sem.at[1 + part, slot])
            for part in range(down_subs)
        ]

    def cols_load(mat, chunk):
        sub = chunk % chunks_per_mat
        if mat % 2 == 0:
            source = grad_top_b if mat == 0 else grad_b_hbm
            source = source.at[:, pl.ds(pl.multiple_of((sub % down_subs) * chunk_cols, 128), chunk_cols)]
        else:
            source = grad_pre_hbm.at[sub]
        return pltpu.make_async_copy(source, cols_buf.at[chunk % 2], load_sem.at[3, chunk % 2])

    def for_mat(chunk, action):
        for mat in range(num_mats):
            @pl.when(chunk // chunks_per_mat == mat)
            def _(mat=mat):
                action(mat)

    def grad_pre_store(sub):
        return pltpu.make_async_copy(grad_pre_buf, grad_pre_hbm.at[sub], grad_pre_sem)

    def core_copy(chunk):
        slot = chunk % RECV_SLOTS
        return pltpu.make_async_remote_copy(
            src_ref=sent_core, dst_ref=recv_core.at[slot], send_sem=core_send, recv_sem=core_recv.at[slot],
            device_id=(partners[CORE],), device_id_type=MESH)

    def out_copy(level, color, chunk):
        slot = chunk % RECV_SLOTS
        return pltpu.make_async_remote_copy(
            src_ref=sent_bufs[level].at[color], dst_ref=recv_bufs[level].at[slot, color],
            send_sem=out_send.at[level, color], recv_sem=out_recv.at[level, color, slot],
            device_id=(partners[COLOR_DIMS[color][level]],), device_id_type=MESH)

    def back_copy(level, color, chunk, arriving):
        slot = chunk % GATHER_SLOTS
        mine = ring.at[slot, core, color, rows_at(base(color, level + 1), spans[level]), :]
        theirs = ring.at[slot, core, color, rows_at(other(color, level), spans[level]), :]
        return pltpu.make_async_remote_copy(
            src_ref=mine, dst_ref=theirs if arriving else mine,
            send_sem=back_send.at[level, color, slot], recv_sem=back_recv.at[level, color, slot],
            device_id=(partners[COLOR_DIMS[color][level]],), device_id_type=MESH)

    def part_rows(color):
        return rows_at(base(color, 1), spans[0])

    def part_share_copy(color, chunk, arriving):
        slot = chunk % GATHER_SLOTS
        mine = ring.at[slot, core, color, part_rows(color), :]
        theirs = ring.at[slot, 1 - core, color, part_rows(color), :]
        return pltpu.make_async_remote_copy(
            src_ref=mine, dst_ref=theirs if arriving else mine,
            send_sem=back_send.at[0, color, slot], recv_sem=back_recv.at[0, color, slot],
            device_id=(partners[CORE],), device_id_type=MESH)

    def part_stores(group, chunk):
        slot = chunk % GATHER_SLOTS
        place = chunk - full_chunks - sum(PART_GROUPS[:group])
        copies = []
        for color in range(COLORS):
            for which in range(2):
                out_ref = part_refs[(group * COLORS + color) * 2 + which]
                source = ring.at[slot, core if which == 0 else 1 - core, color, part_rows(color), :]
                copies.append(pltpu.make_async_copy(
                    source, out_ref.at[place], part_sem.at[color, which, slot]))
        return copies

    def share_copy(chunk, arriving):
        slot = chunk % GATHER_SLOTS
        return pltpu.make_async_remote_copy(
            src_ref=ring.at[slot, core], dst_ref=ring.at[slot, 1 - core if arriving else core],
            send_sem=share_send.at[slot], recv_sem=share_recv.at[slot],
            device_id=(partners[CORE],), device_id_type=MESH)

    def store_copy(chunk):
        slot = chunk % GATHER_SLOTS
        return pltpu.make_async_copy(ring.at[slot], gathered.at[chunk], store_sem.at[slot])

    def small_copy(step):
        return pltpu.make_async_remote_copy(
            src_ref=small_out, dst_ref=small_recv.at[step], send_sem=small_send_sem.at[step],
            recv_sem=small_recv_sem.at[step], device_id=(partners[step],), device_id_type=MESH)

    def product(chunk, which_core):
        rows = pl.ds(pl.multiple_of(which_core * half, 128), half)
        return jnp.dot(turned[rows, :], cols_buf[chunk % 2], preferred_element_type=jnp.float32)

    def opens_layer(chunk):
        return (chunk > 0) & (chunk % (2 * chunks_per_mat) == 0)

    def turn_rows(chunk):
        down = (chunk // chunks_per_mat) % 2 == 0

        @pl.when((chunk % chunks_per_mat == 0) | (down & (chunk % down_subs == 0)))
        def _():
            rows_load(1, chunk).wait()
            for start in range(0, row_dim, TILE):
                turned[start:start + TILE, :] = rows_buf[:, start:start + TILE].T
            for period, here in ((down_subs, down), (chunks_per_mat, jnp.logical_not(down))):
                following = chunk + period

                @pl.when(here & (following < num_chunks))
                def _(following=following):
                    for_mat(following, lambda mat: rows_load(mat, following).start())

    def load(chunk):
        turn_rows(chunk)
        for_mat(chunk, lambda mat: cols_load(mat, chunk).wait())
        after = chunk + 1

        @pl.when(chunk == 0)
        def _():
            grad_b_copy.start()
            for copy in weight_loads(0, chunk):
                copy.start()

        @pl.when((after < num_chunks) & jnp.logical_not(opens_layer(after)))
        def _():
            for_mat(after, lambda mat: cols_load(mat, after).start())

    def load_weights(chunk):
        def arrive(mat):
            for copy in weight_loads(mat, chunk):
                copy.wait()

        for_mat(chunk, arrive)
        after, before = chunk + 1, chunk - 1

        @pl.when(chunk == 0)
        def _():
            grad_b_copy.wait()

        @pl.when(after < num_chunks)
        def _():
            def start(mat):
                for copy in weight_loads(mat, after):
                    copy.start()

            for_mat(after, start)

        @pl.when((before >= 0) & ((before // chunks_per_mat) % 2 == 0))
        def _():
            grad_pre_store(before % chunks_per_mat).wait()

    def compute_sent(chunk):
        value = product(chunk, 1 - core).astype(jnp.bfloat16)
        for color in range(COLORS):
            sent_core[color] = value[color * region:(color + 1) * region]

    def share_core(chunk):
        core_copy(chunk).start()

    def compute_kept(chunk):
        value = product(chunk, core)
        for color in range(COLORS):
            kept[chunk % KEPT_SLOTS, color] = value[color * region:(color + 1) * region]

    def halve(level, chunk, arrived):
        slot = chunk % KEPT_SLOTS
        recv_slot = chunk % RECV_SLOTS
        for color in range(COLORS):
            if level > 0:
                out_copy(level - 1, color, chunk).wait()
            held = base(color, level)

            def total(start, size, color=color, held=held):
                own = kept[slot, color, rows_at(start, size), :]
                return own + arrived[recv_slot, color, rows_at(start - held, size), :].astype(jnp.float32)

            if level < 3:
                mine = base(color, level + 1)
                sent_bufs[level][color] = total(other(color, level), spans[level]).astype(jnp.bfloat16)
                kept[slot, color, rows_at(mine, spans[level]), :] = total(mine, spans[level])
                out_copy(level, color, chunk).start()
            else:
                gather_slot = chunk % GATHER_SLOTS
                ring[gather_slot, core, color, rows_at(held, spans[2]), :] = total(held, spans[2]).astype(jnp.bfloat16)
                back_copy(2, color, chunk, False).start()

    def send_1(chunk):
        core_copy(chunk).wait()
        halve(0, chunk, recv_core)

    def send_2(chunk):
        halve(1, chunk, recv_1)

    def send_3(chunk):
        halve(2, chunk, recv_2)

    def send_back_3(chunk):
        halve(3, chunk, recv_3)

    def pass_back(level, chunk):
        for color in range(COLORS):
            back_copy(level + 1, color, chunk, True).wait()
            back_copy(level, color, chunk, False).start()

    def send_back_2(chunk):
        pass_back(1, chunk)

    def send_back_1(chunk):
        @pl.when(chunk < full_chunks)
        def _():
            pass_back(0, chunk)

        @pl.when(chunk >= full_chunks)
        def _():
            for color in range(COLORS):
                back_copy(1, color, chunk, True).wait()
                part_share_copy(color, chunk, False).start()

    def send_back_core(chunk):
        @pl.when(chunk < full_chunks)
        def _():
            for color in range(COLORS):
                back_copy(0, color, chunk, True).wait()
            share_copy(chunk, False).start()

        @pl.when(chunk >= full_chunks)
        def _():
            for color in range(COLORS):
                part_share_copy(color, chunk, True).wait()

        for group, size in enumerate(PART_GROUPS):
            first = full_chunks + sum(PART_GROUPS[:group])

            @pl.when((chunk >= first) & (chunk < first + size))
            def _(group=group):
                for copy in part_stores(group, chunk):
                    copy.start()

    def store(chunk):
        @pl.when(chunk < full_chunks)
        def _():
            share_copy(chunk, True).wait()
            store_copy(chunk).start()

        @pl.when((chunk > 0) & (chunk <= full_chunks))
        def _():
            store_copy(chunk - 1).wait()

        for group, size in enumerate(PART_GROUPS):
            first = full_chunks + sum(PART_GROUPS[:group])

            @pl.when((chunk >= first) & (chunk < first + size))
            def _(group=group):
                for copy in part_stores(group, chunk):
                    copy.wait()

    token_half = grad_b.shape[0] // 2

    def backward(part, chunk):
        slot = chunk % 2
        sub = chunk % chunks_per_mat
        mat = chunk // chunks_per_mat
        layer = num_layers - 1 - mat // 2

        @pl.when(mat % 2 == 0)
        def _():
            cols = slice(part * TILE, (part + 1) * TILE)

            @pl.loop(0, 2)
            def _(which):
                rows = pl.ds(pl.multiple_of(which * token_half, 128), token_half)
                grad_act = lax.dot_general(
                    grad_b[rows, :], weight_buf[slot, cols, :], FEATURE_DIMS, preferred_element_type=jnp.float32)
                grad_pre = grad_act * gelu_slope(pre_buf[slot, rows, cols].astype(jnp.float32))
                grad_pre_buf[rows, cols] = grad_pre.astype(jnp.bfloat16)
                start = row_dim + sub * chunk_cols + part * TILE
                small_out[pl.ds(layer, 1), pl.ds(pl.multiple_of(start, 128), TILE)] += jnp.sum(grad_pre, axis=0, keepdims=True)

            if part == chunk_cols // TILE - 1:
                grad_pre_store(sub).start()

        @pl.when(mat % 2 == 1)
        def _():
            pieces = row_dim // chunk_cols * (chunk_cols // TILE) // 3
            grad_rows = []
            for piece in range(part * pieces, (part + 1) * pieces):
                start, first = divmod(piece * TILE, chunk_cols)
                grad_rows.append((piece, lax.dot_general(
                    cols_buf[slot], weight_buf[slot, first:first + TILE, start * chunk_cols:(start + 1) * chunk_cols],
                    FEATURE_DIMS, preferred_element_type=jnp.float32)))
            for piece, value in grad_rows:
                grad_normed[:, piece * TILE:(piece + 1) * TILE] += value

    def norm_loads(layer, block):
        rows = pl.ds(pl.multiple_of(block * NORM_ROWS, NORM_ROWS), NORM_ROWS)
        slot = block % 2
        copies = [pltpu.make_async_copy(hid_refs[layer].at[rows, :], hid_buf.at[slot], norm_sem.at[0, slot])]
        if layer > 0:
            copies.append(pltpu.make_async_copy(grad_top.at[rows, :], grad_buf.at[slot], norm_sem.at[1, slot]))
        return copies

    def layer_input_grad(layer):
        num_blocks = grad_b.shape[0] // NORM_ROWS
        for copy in norm_loads(layer, 0):
            copy.start()

        @pl.loop(0, num_blocks)
        def _(block):
            @pl.when(block + 1 < num_blocks)
            def _():
                for copy in norm_loads(layer, block + 1):
                    copy.start()

            for copy in norm_loads(layer, block):
                copy.wait()
            rows = pl.ds(pl.multiple_of(block * NORM_ROWS, NORM_ROWS), NORM_ROWS)
            hid_f = hid_buf[block % 2].astype(jnp.float32)
            hid_scale = inverse_rms(hid_f)
            hid_hat = hid_f * hid_scale
            normed_grad = grad_normed[rows, :]
            small_out[layer:layer + 1, :row_dim] += jnp.sum(normed_grad * hid_hat, axis=0, keepdims=True)
            if layer > 0:
                grad_normed[rows, :] = jnp.zeros((NORM_ROWS, row_dim), jnp.float32)
                grad_hat = normed_grad * gain_in[layer:layer + 1, :].astype(jnp.float32)
                grad_new = grad_buf[block % 2] + hid_scale * (
                    grad_hat - hid_hat * jnp.mean(grad_hat * hid_hat, axis=-1, keepdims=True))
                grad_b[rows, :] = grad_new.astype(jnp.bfloat16)
                small_out[layer - 1:layer, row_dim + hidden_dim:] += jnp.sum(grad_new, axis=0, keepdims=True)

        if layer > 0:
            copy = pltpu.make_async_copy(grad_b, grad_b_hbm, grad_b_sem)
            copy.start()
            copy.wait()
            following = jnp.int32((num_layers - layer) * 2 * chunks_per_mat)
            cols_load((num_layers - layer) * 2, following).start()

    def input_grad(chunk):
        for layer in range(num_layers):
            last = (num_layers - 1 - layer) * 2 * chunks_per_mat + 2 * chunks_per_mat - 1

            @pl.when(chunk == last)
            def _(layer=layer):
                layer_input_grad(layer)

    events = dict(
        load=load, load_weights=load_weights, compute_sent=compute_sent, share_core=share_core, compute_kept=compute_kept, send_1=send_1, send_2=send_2, send_3=send_3,
        send_back_3=send_back_3, send_back_2=send_back_2, send_back_1=send_back_1, send_back_core=send_back_core, store=store,
        backward_0=functools.partial(backward, 0), backward_1=functools.partial(backward, 1),
        backward_2=functools.partial(backward, 2), input_grad=input_grad)

    first = jnp.int32(0)
    rows_load(0, first).start()
    cols_load(0, first).start()
    grad_b_copy = pltpu.make_async_copy(grad_top_b, grad_b, grad_b_sem)
    barrier = pltpu.get_barrier_semaphore()
    for partner in partners:
        pl.semaphore_signal(barrier, inc=1, device_id=(partner,), device_id_type=MESH)
    small_out[...] = small_in[...]
    grad_normed[...] = jnp.zeros_like(grad_normed)
    pl.semaphore_wait(barrier, 4)

    @pl.loop(0, num_chunks + MAX_LAG)
    def _(it):
        for step in range(4):
            @pl.when(it == num_chunks + step)
            def _(step=step):
                small_copy(step).start()
        for name, lag in PIPELINE:
            chunk = it - lag

            @pl.when((chunk >= 0) & (chunk < num_chunks))
            def _(name=name, chunk=chunk):
                events[name](chunk)
        for step in range(4):
            @pl.when(it == num_chunks + step)
            def _(step=step):
                small_copy(step).wait()
                small_out[...] += small_recv[step]


def backward_pass(hid_rows, saved, grad_top, grad_top_b, norm_gain, w_up, w_down, small, axis, chunk_cols):
    num_layers, row_dim, hidden = w_up.shape
    tokens = grad_top.shape[0]
    chunks_per_mat = hidden // chunk_cols
    region = row_dim // (2 * COLORS)
    half = (COLORS, region, chunk_cols)
    sizes = (num_layers, chunks_per_mat, row_dim, chunk_cols, region, row_dim // chunk_cols, axis)
    num_chunks = 2 * num_layers * chunks_per_mat
    bf16, f32 = jnp.bfloat16, jnp.float32
    dma = pltpu.SemaphoreType.DMA
    any_spec = pl.BlockSpec(memory_space=pl.ANY)
    vmem_spec = pl.BlockSpec(memory_space=pltpu.VMEM)
    full_chunks = num_chunks - sum(PART_GROUPS)
    part_shapes = [jax.ShapeDtypeStruct((size, region // 2, chunk_cols), bf16) for size in PART_GROUPS for _ in range(2 * COLORS)]
    gathered, small_sum, _, _, *parts = pl.pallas_call(
        functools.partial(backward_kernel, sizes),
        out_shape=[
            jax.ShapeDtypeStruct((full_chunks, 2) + half, bf16),
            jax.ShapeDtypeStruct(small.shape, f32),
            jax.ShapeDtypeStruct((chunks_per_mat, tokens, chunk_cols), bf16),
            jax.ShapeDtypeStruct((tokens, row_dim), bf16),
        ] + part_shapes,
        in_specs=[any_spec] * (num_layers + 7) + [vmem_spec] * 2,
        out_specs=[any_spec, vmem_spec, any_spec, any_spec] + [any_spec] * len(part_shapes),
        scratch_shapes=[
            pltpu.VMEM((tokens, row_dim), bf16),
            pltpu.VMEM((row_dim, tokens), bf16),
            pltpu.VMEM((2, tokens, chunk_cols), bf16),
            pltpu.VMEM(half, bf16),
            pltpu.VMEM((KEPT_SLOTS,) + half, f32),
            pltpu.VMEM((RECV_SLOTS,) + half, bf16),
            pltpu.VMEM((COLORS, region // 2, chunk_cols), bf16),
            pltpu.VMEM((COLORS, region // 4, chunk_cols), bf16),
            pltpu.VMEM((COLORS, region // 8, chunk_cols), bf16),
            pltpu.VMEM((RECV_SLOTS, COLORS, region // 2, chunk_cols), bf16),
            pltpu.VMEM((RECV_SLOTS, COLORS, region // 4, chunk_cols), bf16),
            pltpu.VMEM((RECV_SLOTS, COLORS, region // 8, chunk_cols), bf16),
            pltpu.VMEM((GATHER_SLOTS, 2) + half, bf16),
            pltpu.VMEM((2, chunk_cols, row_dim), bf16),
            pltpu.VMEM((2, tokens, chunk_cols), bf16),
            pltpu.VMEM((tokens, chunk_cols), bf16),
            pltpu.VMEM((tokens, row_dim), bf16),
            pltpu.VMEM((tokens, row_dim), f32),
            pltpu.VMEM((2, NORM_ROWS, row_dim), bf16),
            pltpu.VMEM((2, NORM_ROWS, row_dim), f32),
            pltpu.VMEM((4,) + small.shape, f32),
            dma((4, 2)), dma, dma((2, 2)), dma,
            dma, dma((RECV_SLOTS,)), dma((3, COLORS)), dma((3, COLORS, RECV_SLOTS)),
            dma((3, COLORS, GATHER_SLOTS)), dma((3, COLORS, GATHER_SLOTS)), dma((GATHER_SLOTS,)), dma((GATHER_SLOTS,)),
            dma((GATHER_SLOTS,)), dma((4,)), dma((4,)), dma((COLORS, 2, GATHER_SLOTS)),
        ],
        compiler_params=pltpu.CompilerParams(collective_id=0, has_side_effects=True, vmem_limit_bytes=67043328),
        name="backward",
    )(*hid_rows, *saved, grad_top, grad_top_b, w_up, w_down, norm_gain, small)
    return gathered, small_sum, parts


def flip_pairs(num_devices, bit):
    return [(dev, dev ^ (1 << bit)) for dev in range(num_devices)]


def stream_blocks(num_blocks, start_loads, wait_loads, store_of, in_buf, out_buf):
    slots, region = in_buf.shape[0], in_buf.shape[2]
    for block in range(min(slots - 1, num_blocks)):
        start_loads(jnp.int32(block), block)

    @pl.loop(0, num_blocks)
    def _(block):
        slot = block % slots

        @pl.when(block + slots - 1 < num_blocks)
        def _():
            start_loads(block + slots - 1, (block + slots - 1) % slots)

        wait_loads(block, slot)

        @pl.when(block >= slots)
        def _():
            store_of(block - slots, slot).wait()

        for color in range(COLORS):
            out_buf[slot, color * region:(color + 1) * region, :] = in_buf[slot, color].astype(jnp.float32)
        store_of(block, slot).start()

    for block in range(max(num_blocks - slots, 0), num_blocks):
        store_of(jnp.int32(block), block % slots).wait()


def block_target(out_ref, layer, kind, down_subs, chunk, which_core, rows, cols):
    half = pl.multiple_of(which_core * rows, rows)
    if kind == 0:
        first = pl.multiple_of((chunk // down_subs) * 2 * rows + half, rows)
        return out_ref.at[layer, pl.ds(first, rows), pl.ds(pl.multiple_of((chunk % down_subs) * cols, 128), cols)]
    return out_ref.at[layer, pl.ds(half, rows), pl.ds(pl.multiple_of(chunk * cols, 128), cols)]


def widen_kernel(spec, *refs):
    first, count, place, layer, kind, down_subs, small_widths, in_place = spec
    if in_place:
        refs = refs[:1 + bool(small_widths)] + refs[2 + bool(small_widths):]
    if small_widths:
        gathered, small, out_ref, *small_outs, in_buf, out_buf, in_sem, out_sem = refs
        start = 0
        for width, small_out in zip(small_widths, small_outs):
            small_out[...] = small[:, start:start + width]
            start += width
    else:
        gathered, out_ref, in_buf, out_buf, in_sem, out_sem = refs
    rows, cols = out_buf.shape[1:]

    def load(block, slot):
        return pltpu.make_async_copy(gathered.at[first + block // 2, block % 2], in_buf.at[slot], in_sem.at[slot])

    def store(block, slot):
        target = block_target(out_ref, layer, kind, down_subs, place + block // 2, block % 2, rows, cols)
        return pltpu.make_async_copy(out_buf.at[slot], target, out_sem.at[slot])

    stream_blocks(
        2 * count, lambda block, slot: load(block, slot).start(), lambda block, slot: load(block, slot).wait(),
        store, in_buf, out_buf)


def join_kernel(spec, *refs):
    skip, count, place, layer, kind, down_subs, axis = spec
    parts, (_, out_ref, in_buf, out_buf, in_sem, out_sem) = refs[:4 * COLORS], refs[4 * COLORS:]
    rows, cols = out_buf.shape[1:]
    part_rows = in_buf.shape[2] // 2
    me = lax.axis_index(axis)
    core = me % 2

    def copies(which, chunk, slot):
        found = []
        for color in range(COLORS):
            upper = (me >> COLOR_DIMS[color][0]) & 1
            for far in range(2):
                start = pl.multiple_of((upper if far == 0 else 1 - upper) * part_rows, part_rows)
                found.append(pltpu.make_async_copy(
                    parts[color * 4 + far * 2 + which].at[skip + chunk],
                    in_buf.at[slot, color, pl.ds(start, part_rows), :], in_sem.at[slot]))
        return found

    def start_loads(block, slot):
        for which in range(2):
            @pl.when(block % 2 == which)
            def _(which=which):
                for copy in copies(which, block // 2, slot):
                    copy.start()

    def wait_loads(block, slot):
        for copy in copies(0, block // 2, slot):
            copy.wait()

    def store(block, slot):
        which_core = jnp.where(block % 2 == 0, core, 1 - core)
        target = block_target(out_ref, layer, kind, down_subs, place + block // 2, which_core, rows, cols)
        return pltpu.make_async_copy(out_buf.at[slot], target, out_sem.at[slot])

    stream_blocks(2 * count, start_loads, wait_loads, store, in_buf, out_buf)


def widen_scratch(region, cols):
    return [
        pltpu.VMEM((STREAM_SLOTS, COLORS, region, cols), jnp.bfloat16),
        pltpu.VMEM((STREAM_SLOTS, COLORS * region, cols), jnp.float32),
        pltpu.SemaphoreType.DMA((STREAM_SLOTS,)),
        pltpu.SemaphoreType.DMA((STREAM_SLOTS,)),
    ]


def widen_cost(count, region, cols):
    size = count * 2 * COLORS * region * cols
    return pl.CostEstimate(flops=500 * size, bytes_accessed=6 * size, transcendentals=0)


def widen(gathered, first, count, place, layer, kind, shape, into, down_subs, small, small_widths):
    region, cols = gathered.shape[3:]
    any_spec = pl.BlockSpec(memory_space=pl.ANY)
    vmem_spec = pl.BlockSpec(memory_space=pltpu.VMEM)
    smalls = [jax.ShapeDtypeStruct((small.shape[0], width), jnp.float32) for width in small_widths]
    return pl.pallas_call(
        functools.partial(widen_kernel, (first, count, place, layer, kind, down_subs, small_widths, into is not None)),
        in_specs=[any_spec] + [vmem_spec] * bool(smalls) + [any_spec] * (into is not None),
        out_specs=[any_spec] + [vmem_spec] * len(smalls),
        out_shape=[jax.ShapeDtypeStruct(shape, jnp.float32)] + smalls,
        input_output_aliases={} if into is None else {1 + bool(smalls): 0},
        scratch_shapes=widen_scratch(region, cols),
        cost_estimate=widen_cost(count, region, cols),
        compiler_params=pltpu.CompilerParams(vmem_limit_bytes=67043328),
    )(gathered, *([small] if smalls else []), *([] if into is None else [into]))


def split_at_gradients(first, count, per_mat):
    sizes = []
    while count:
        sizes.append(min(count, per_mat - first % per_mat))
        first, count = first + sizes[-1], count - sizes[-1]
    return sizes


def join(parts, skip, count, place, layer, kind, into, down_subs, axis):
    _, part_rows, cols = parts[0].shape
    any_spec = pl.BlockSpec(memory_space=pl.ANY)
    return pl.pallas_call(
        functools.partial(join_kernel, (skip, count, place, layer, kind, down_subs, axis)),
        in_specs=[any_spec] * (len(parts) + 1),
        out_specs=any_spec,
        out_shape=jax.ShapeDtypeStruct(into.shape, jnp.float32),
        scratch_shapes=widen_scratch(2 * part_rows, cols),
        input_output_aliases={len(parts): 0},
        cost_estimate=widen_cost(count, 2 * part_rows, cols),
        compiler_params=pltpu.CompilerParams(vmem_limit_bytes=67043328),
    )(*parts, into)


def swap(array, axis, num_devices, bit):
    return lax.ppermute(array, axis, flip_pairs(num_devices, bit))


def full_gradients(gathered, parts, small, num_layers, row_dim, hidden, chunk_cols, axis, num_devices):
    per_mat = hidden // chunk_cols
    down_subs = row_dim // chunk_cols
    groups = range(len(PART_GROUPS))
    mine = [[parts[(group * COLORS + color) * 2] for color in range(COLORS)] for group in groups]
    theirs = [[parts[(group * COLORS + color) * 2 + 1] for color in range(COLORS)] for group in groups]
    far = [[swap(mine[group][color], axis, num_devices, COLOR_DIMS[color][0])
            for color in range(COLORS)] for group in groups]
    last = num_layers - 1
    full = [None, None]
    shapes = ((num_layers, hidden, row_dim), (num_layers, row_dim, hidden))
    for call, count in enumerate(WIDEN_CALLS):
        first = sum(WIDEN_CALLS[:call])
        kind, place = divmod(first, per_mat)
        small_widths = (row_dim, hidden, row_dim) if call == 0 else ()
        full[kind], *rest = widen(
            gathered, first, count, place, last, kind, shapes[kind], full[kind], down_subs, small, small_widths)
        smalls = rest or smalls
    chunk = 2 * num_layers * per_mat - sum(PART_GROUPS)
    for group in groups:
        pieces = []
        for color in range(COLORS):
            shared = swap(far[group][color], axis, num_devices, CORE)
            pieces += [mine[group][color], theirs[group][color], far[group][color], shared]
        skip = 0
        for count in split_at_gradients(chunk, PART_GROUPS[group], per_mat):
            mat, place = divmod(chunk, per_mat)
            kind, layer = mat % 2, last - mat // 2
            full[kind] = join(pieces, skip, count, place, layer, kind, full[kind], down_subs, axis)
            chunk, skip = chunk + count, skip + count
    return smalls[0], full[1], smalls[1], full[0], smalls[2]


def solution(mesh):
    axis = mesh.axis_names[0]

    def device_grads(tokens, upstream, norm_gain, w_up, bias_up, w_down, bias_down):
        num_layers, width = norm_gain.shape
        hidden_width = w_up.shape[2]
        chunk_cols = width // 2
        hid_1, normed, pre_act, activated, grad_top, grad_top_b, small = forward_pass(
            tokens, upstream, norm_gain, w_up, bias_up, w_down, bias_down, width)
        gathered, small, parts = backward_pass(
            (tokens, hid_1), (normed, pre_act, activated), grad_top, grad_top_b, norm_gain, w_up, w_down, small, axis, chunk_cols)
        return full_gradients(gathered, parts, small, num_layers, width, hidden_width, chunk_cols, axis, mesh.size)

    row_spec = P(axis, None)
    full_spec = P()
    return jax.shard_map(
        device_grads,
        mesh=mesh,
        in_specs=(row_spec, row_spec, full_spec, full_spec, full_spec, full_spec, full_spec),
        out_specs=(full_spec, full_spec, full_spec, full_spec, full_spec),
        check_vma=False,
    )
```

```python
import functools

import jax
import jax.numpy as jnp
from jax import lax
from jax.experimental import pallas as pl
from jax.experimental.pallas import tpu as pltpu
from jax.sharding import PartitionSpec as P


EPSILON = 1e-6
FEATURE_DIMS = (((1,), (1,)), ((), ()))
MESH = pl.DeviceIdType.MESH
COLORS = 3
CORE, DIM_X, DIM_Y, DIM_Z = range(4)
COLOR_DIMS = ((DIM_X, DIM_Y, DIM_Z), (DIM_Y, DIM_Z, DIM_X), (DIM_Z, DIM_X, DIM_Y))
PIPELINE = (
    ("load", 0), ("compute_sent", 0), ("share_core", 0), ("send_3", 2), ("send_back_2", 4), ("send_back_1", 5),
    ("compute_kept", 0), ("send_back_core", 6), ("load_weights", 0), ("backward_0", 0), ("send_2", 1), ("backward_1", 0),
    ("send_1", 0), ("backward_2", 0), ("send_back_3", 2), ("store", 6), ("input_grad", 0),
)
MAX_LAG = 6
PART_GROUPS = (7, 5, 3, 3)
WIDEN_CALLS = (8, 6)
RECV_SLOTS = 2
KEPT_SLOTS = 3
GATHER_SLOTS = 6
TILE = 256
UP_COLS = 512
ACT_ROWS = 16
ACT_COLS = 256
STREAM_SLOTS = 4
NORM_ROWS = 128
GELU_SCALE = 0.7978845608028654
GELU_CUBIC = 0.044715


def inverse_rms(hid_f):
    return lax.rsqrt(jnp.mean(hid_f * hid_f, axis=-1, keepdims=True) + EPSILON)


def gelu(values):
    return (0.5 * values) * (1.0 + jnp.tanh(values * (GELU_SCALE + GELU_SCALE * GELU_CUBIC * (values * values))))


def forward_phase(
    sizes, hbm, branch, grad_b, small_out, before_top, io_sem, up_sem, down_sem, pre_sem, act_sem, up_rows_sem,
    hid, normed, up_buf, down_buf, pre_buf, act_buf, up_rows, gain, bias_up, bias_down,
):
    (tokens, upstream, w_up, w_down, gain_in, bias_up_in, bias_down_in, hid_out, normed_out, pre_act_out, act_out,
     grad_top_out, grad_b_out) = hbm
    num_layers, num_tiles, tile_cols = sizes
    num_tokens, row_dim = hid.shape
    steps = num_tiles + 1
    parts = tile_cols // UP_COLS

    def up_load(layer, tile):
        cols = pl.ds(pl.multiple_of(tile * tile_cols, 128), tile_cols)
        return pltpu.make_async_copy(w_up.at[layer, :, cols], up_buf.at[tile % 2], up_sem.at[tile % 2])

    def down_load(layer, tile):
        rows = pl.ds(pl.multiple_of(tile * tile_cols, 128), tile_cols)
        return pltpu.make_async_copy(w_down.at[layer, rows, :], down_buf.at[tile % 2], down_sem.at[tile % 2])

    def pre_store(layer, tile):
        cols = pl.ds(pl.multiple_of(tile * tile_cols, 128), tile_cols)
        return pltpu.make_async_copy(pre_buf.at[tile % 2], pre_act_out.at[layer, :, cols], pre_sem.at[tile % 2])

    def act_store(layer, tile):
        cols = pl.ds(pl.multiple_of(tile * tile_cols, 128), tile_cols)
        return pltpu.make_async_copy(act_buf.at[tile % 2], act_out.at[layer, :, cols], act_sem.at[tile % 2])

    def normed_store(layer):
        return pltpu.make_async_copy(normed, normed_out.at[layer], io_sem.at[1])

    def hid_store():
        return pltpu.make_async_copy(hid, hid_out, io_sem.at[2])

    tokens_load = pltpu.make_async_copy(tokens, hid, io_sem.at[0])
    tokens_load.start()
    up_load(0, 0).start()
    small_out[...] = jnp.zeros_like(small_out)
    branch[...] = jnp.zeros_like(branch)
    pre_buf[0, :, :UP_COLS] = jnp.zeros((num_tokens, UP_COLS), jnp.bfloat16)
    gain[...] = gain_in[...].astype(jnp.float32)
    bias_up[...] = bias_up_in[...].astype(jnp.float32)
    bias_down[...] = bias_down_in[...].astype(jnp.float32)
    tokens_load.wait()

    def each_block(action):
        @pl.loop(0, num_tokens // NORM_ROWS)
        def _(block):
            action(pl.ds(pl.multiple_of(block * NORM_ROWS, NORM_ROWS), NORM_ROWS))

    def normalize(layer, rows, hid_f):
        normed[rows, :] = ((hid_f * inverse_rms(hid_f)) * gain[pl.ds(layer, 1), :]).astype(jnp.bfloat16)

    def next_rows(layer, rows):
        new = ((hid[rows, :].astype(jnp.float32) + branch[rows, :]) + bias_down[pl.ds(layer, 1), :]).astype(jnp.bfloat16)
        hid[rows, :] = new
        return new.astype(jnp.float32)

    def activate(slot, part):
        start = part * UP_COLS
        for row in range(0, num_tokens, ACT_ROWS):
            for col in range(0, UP_COLS, ACT_COLS):
                piece = (slot, pl.ds(row, ACT_ROWS), pl.ds(pl.multiple_of(start + col, 128), ACT_COLS))
                act_buf[piece] = gelu(pre_buf[piece].astype(jnp.float32)).astype(jnp.bfloat16)

    def up_product(layer, tile):
        @pl.loop(0, parts)
        def _(part):
            fresh = tile * parts + part == 0
            last_slot = jnp.where((part == 0) & (tile > 0), (tile + 1) % 2, tile % 2)
            activate(last_slot, jnp.where(fresh, 0, (part + parts - 1) % parts))
            cols = pl.ds(pl.multiple_of(part * UP_COLS, 128), UP_COLS)
            bias = bias_up[pl.ds(layer, 1), pl.ds(pl.multiple_of(tile * tile_cols + part * UP_COLS, 128), UP_COLS)]
            pre_buf[tile % 2, :, cols] = (
                jnp.dot(normed[...], up_buf[tile % 2, :, cols], preferred_element_type=jnp.float32) + bias
            ).astype(jnp.bfloat16)

    def down_product(tile):
        slot = tile % 2
        for part in range(row_dim // UP_COLS):
            cols = slice(part * UP_COLS, (part + 1) * UP_COLS)
            branch[:, cols] += jnp.dot(act_buf[slot], down_buf[slot, :, cols], preferred_element_type=jnp.float32)

    each_block(lambda rows: normalize(0, rows, hid[rows, :].astype(jnp.float32)))

    @pl.loop(0, num_layers * steps)
    def _(step):
        layer, tile = step // steps, step % steps

        @pl.when(tile < num_tiles)
        def _():
            up_load(layer, tile).wait()

            @pl.when(tile + 1 < num_tiles)
            def _():
                up_load(layer, tile + 1).start()

            @pl.when((tile == num_tiles - 1) & (layer + 1 < num_layers))
            def _():
                up_load(layer + 1, 0).start()

            @pl.when(step == 0)
            def _():
                normed_store(0).start()
                down_load(0, 0).start()

            @pl.when(tile > 1)
            def _():
                pre_store(layer, tile - 2).wait()
                act_store(layer, tile - 2).wait()

            up_product(layer, tile)
            pre_store(layer, tile).start()

        @pl.when(tile == num_tiles)
        def _():
            activate((num_tiles - 1) % 2, parts - 1)

        @pl.when(tile > 0)
        def _():
            act_store(layer, tile - 1).start()
            down_load(layer, tile - 1).wait()

            @pl.when(tile < num_tiles)
            def _():
                down_load(layer, tile).start()

            @pl.when((tile == num_tiles) & (layer + 1 < num_layers))
            def _():
                down_load(layer + 1, 0).start()

            down_product(tile - 1)

        @pl.when(tile == num_tiles)
        def _():
            for back in (2, 1):
                pre_store(layer, num_tiles - back).wait()
                act_store(layer, num_tiles - back).wait()
            normed_store(layer).wait()

            @pl.when(layer + 1 < num_layers)
            def _():
                def to_next(rows):
                    normalize(layer + 1, rows, next_rows(layer, rows))
                    branch[rows, :] = jnp.zeros((NORM_ROWS, row_dim), jnp.float32)

                each_block(to_next)
                hid_store().start()
                normed_store(layer + 1).start()

    hid_store().wait()
    before_top()
    bias_start = small_out.shape[1] - row_dim
    num_blocks = num_tokens // NORM_ROWS

    def block_rows(block):
        return pl.ds(pl.multiple_of(block * NORM_ROWS, NORM_ROWS), NORM_ROWS)

    def up_rows_load(block):
        return pltpu.make_async_copy(upstream.at[block_rows(block), :], up_rows.at[block % 2], up_rows_sem.at[block % 2])

    up_rows_load(0).start()

    @pl.loop(0, num_blocks)
    def _(block):
        rows = block_rows(block)
        up_rows_load(block).wait()

        @pl.when(block + 1 < num_blocks)
        def _():
            up_rows_load(block + 1).start()

        top_f = next_rows(num_layers - 1, rows)
        top_scale = inverse_rms(top_f)
        top_hat = top_f * top_scale
        up_f = up_rows[block % 2].astype(jnp.float32)
        grad = top_scale * (up_f - top_hat * jnp.mean(up_f * top_hat, axis=-1, keepdims=True))
        branch[rows, :] = grad
        grad_b[rows, :] = grad.astype(jnp.bfloat16)
        small_out[num_layers - 1:, bias_start:] += jnp.sum(grad, axis=0, keepdims=True)

    pltpu.make_async_copy(branch, grad_top_out, io_sem.at[0]).start()
    pltpu.make_async_copy(grad_b, grad_b_out, io_sem.at[1]).start()


def gelu_slope(values):
    square = values * values
    bend = jnp.tanh(values * (GELU_SCALE + GELU_SCALE * GELU_CUBIC * square))
    return 0.5 * (1.0 + bend) + (0.5 * values) * (1.0 - bend * bend) * (GELU_SCALE + 3.0 * GELU_SCALE * GELU_CUBIC * square)


def stack_kernel(sizes, *refs):
    num_layers, chunks_per_mat, row_dim, chunk_cols, region, _, tile_cols, axis = sizes
    inputs, refs = refs[:7], refs[7:]
    part_count = 2 * COLORS * len(PART_GROUPS)
    outputs, part_refs, refs = refs[:9], refs[9:9 + part_count], refs[9 + part_count:]
    tokens, upstream, w_up, w_down, gain_in, bias_up_in, bias_down_in = inputs
    gathered, small_out, grad_pre_hbm, grad_b_hbm, hid_out, normed, pre_act, activated, grad_top = outputs
    rows_buf, grad_b, grad_normed, *shared = refs[:9]
    io_sem, up_sem, down_sem, pre_sem, act_sem, up_rows_sem, *sems = refs[9:]
    load_sem = sems[0]
    num_tokens = grad_b.shape[0]
    hidden_dim = chunks_per_mat * chunk_cols
    f32, bf16 = jnp.float32, jnp.bfloat16
    me = lax.axis_index(axis)
    barrier = pltpu.get_barrier_semaphore()
    for dim in range(4):
        pl.semaphore_signal(barrier, inc=1, device_id=(flip(me, dim),), device_id_type=MESH)

    def first_rows_load():
        pltpu.make_async_copy(activated.at[num_layers - 1, :, :row_dim], rows_buf, load_sem.at[0, 0]).start()

    hbm = (tokens, upstream, w_up, w_down, gain_in, bias_up_in, bias_down_in, hid_out, normed, pre_act, activated, grad_top, grad_b_hbm)
    pl.run_scoped(
        functools.partial(
            forward_phase, (num_layers, hidden_dim // tile_cols, tile_cols), hbm, grad_normed, grad_b, small_out, first_rows_load,
            io_sem, up_sem, down_sem, pre_sem, act_sem, up_rows_sem),
        pltpu.VMEM((num_tokens, row_dim), bf16),
        pltpu.VMEM((num_tokens, row_dim), bf16),
        pltpu.VMEM((2, row_dim, tile_cols), bf16),
        pltpu.VMEM((2, tile_cols, row_dim), bf16),
        pltpu.VMEM((2, num_tokens, tile_cols), bf16),
        pltpu.VMEM((2, num_tokens, tile_cols), bf16),
        pltpu.VMEM((2, NORM_ROWS, row_dim), bf16),
        pltpu.VMEM((num_layers, row_dim), f32),
        pltpu.VMEM((num_layers, hidden_dim), f32),
        pltpu.VMEM((num_layers, row_dim), f32),
    )
    hbm = ((tokens, hid_out), normed, pre_act, activated, grad_top, w_up, w_down, gain_in, gathered, grad_pre_hbm, grad_b_hbm, part_refs)
    pl.run_scoped(
        functools.partial(
            backward_phase, sizes, hbm, small_out, rows_buf, grad_b, grad_normed, shared, barrier, io_sem, sems),
        pltpu.VMEM((row_dim, num_tokens), bf16),
        pltpu.VMEM((2, num_tokens, chunk_cols), bf16),
        pltpu.VMEM((COLORS, region, chunk_cols), bf16),
        pltpu.VMEM((KEPT_SLOTS, COLORS, region, chunk_cols), f32),
        pltpu.VMEM((COLORS, region // 2, chunk_cols), bf16),
        pltpu.VMEM((COLORS, region // 4, chunk_cols), bf16),
        pltpu.VMEM((COLORS, region // 8, chunk_cols), bf16),
        pltpu.VMEM((2, chunk_cols, row_dim), bf16),
        pltpu.VMEM((2, num_tokens, chunk_cols), bf16),
        pltpu.VMEM((num_tokens, chunk_cols), bf16),
        pltpu.VMEM((2, NORM_ROWS, row_dim), bf16),
        pltpu.VMEM((2, NORM_ROWS, row_dim), f32),
    )


def flip(device, dim):
    step = 1 << dim
    return device + step - 2 * step * ((device // step) % 2)


def backward_phase(
    sizes, hbm, small_out, rows_buf, grad_b, grad_normed, shared, barrier, io_sem, sems, turned, cols_buf, sent_core, kept,
    sent_1, sent_2, sent_3, weight_buf, pre_buf, grad_pre_buf, hid_buf, grad_buf,
):
    num_layers, chunks_per_mat, row_dim, chunk_cols, region, down_subs, _, axis = sizes
    num_mats = 2 * num_layers
    hidden_dim = chunks_per_mat * chunk_cols
    (hid_refs, normed, pre_act, activated, grad_top, w_up, w_down, gain_in, gathered, grad_pre_hbm, grad_b_hbm, part_refs) = hbm
    recv_core, recv_1, recv_2, recv_3, ring, small_recv = shared[:6]
    (load_sem, grad_pre_sem, norm_sem, grad_b_sem, core_send, core_recv, out_send, out_recv, back_send, back_recv,
     share_send, share_recv, store_sem, small_send_sem, small_recv_sem, part_sem) = sems
    num_chunks = num_mats * chunks_per_mat
    full_chunks = num_chunks - sum(PART_GROUPS)
    half = COLORS * region
    me = lax.axis_index(axis)
    bits = [me % 2, (me // 2) % 2, (me // 4) % 2, me // 8]
    partners = [flip(me, dim) for dim in range(4)]
    core = bits[CORE]
    sent_bufs, recv_bufs = (sent_1, sent_2, sent_3), (recv_1, recv_2, recv_3)
    spans = (region // 2, region // 4, region // 8)

    def base(color, level):
        total = 0
        for step in range(level):
            total = total + bits[COLOR_DIMS[color][step]] * spans[step]
        return total

    def other(color, level):
        return base(color, level) + (1 - bits[COLOR_DIMS[color][level]]) * spans[level]

    def rows_at(start, size):
        return pl.ds(pl.multiple_of(start, spans[2]), size)

    def rows_load(mat, chunk):
        layer = num_layers - 1 - mat // 2
        if mat % 2 == 0:
            start = ((chunk % chunks_per_mat) // down_subs) * row_dim
            source = activated.at[layer, :, pl.ds(pl.multiple_of(start, 128), row_dim)]
        else:
            source = normed.at[layer]
        return pltpu.make_async_copy(source, rows_buf, load_sem.at[0, 0])

    def weight_loads(mat, chunk):
        slot = chunk % 2
        layer = num_layers - 1 - mat // 2
        cols = pl.ds(pl.multiple_of((chunk % chunks_per_mat) * chunk_cols, 128), chunk_cols)
        if mat % 2 == 0:
            return [
                pltpu.make_async_copy(w_down.at[layer, cols, :], weight_buf.at[slot], load_sem.at[1, slot]),
                pltpu.make_async_copy(pre_act.at[layer, :, cols], pre_buf.at[slot], load_sem.at[2, slot]),
            ]
        return [
            pltpu.make_async_copy(
                w_up.at[layer, part * chunk_cols:(part + 1) * chunk_cols, cols],
                weight_buf.at[slot, :, part * chunk_cols:(part + 1) * chunk_cols], load_sem.at[1 + part, slot])
            for part in range(down_subs)
        ]

    def cols_load(mat, chunk):
        sub = chunk % chunks_per_mat
        if mat % 2 == 0:
            source = grad_b_hbm.at[:, pl.ds(pl.multiple_of((sub % down_subs) * chunk_cols, 128), chunk_cols)]
        else:
            source = grad_pre_hbm.at[sub]
        return pltpu.make_async_copy(source, cols_buf.at[chunk % 2], load_sem.at[3, chunk % 2])

    def for_mat(chunk, action):
        for mat in range(num_mats):
            @pl.when(chunk // chunks_per_mat == mat)
            def _(mat=mat):
                action(mat)

    def grad_pre_store(sub):
        return pltpu.make_async_copy(grad_pre_buf, grad_pre_hbm.at[sub], grad_pre_sem)

    def core_copy(chunk):
        slot = chunk % RECV_SLOTS
        return pltpu.make_async_remote_copy(
            src_ref=sent_core, dst_ref=recv_core.at[slot], send_sem=core_send, recv_sem=core_recv.at[slot],
            device_id=(partners[CORE],), device_id_type=MESH)

    def out_copy(level, color, chunk):
        slot = chunk % RECV_SLOTS
        return pltpu.make_async_remote_copy(
            src_ref=sent_bufs[level].at[color], dst_ref=recv_bufs[level].at[slot, color],
            send_sem=out_send.at[level, color], recv_sem=out_recv.at[level, color, slot],
            device_id=(partners[COLOR_DIMS[color][level]],), device_id_type=MESH)

    def back_copy(level, color, chunk, arriving):
        slot = chunk % GATHER_SLOTS
        mine = ring.at[slot, core, color, rows_at(base(color, level + 1), spans[level]), :]
        theirs = ring.at[slot, core, color, rows_at(other(color, level), spans[level]), :]
        return pltpu.make_async_remote_copy(
            src_ref=mine, dst_ref=theirs if arriving else mine,
            send_sem=back_send.at[level, color, slot], recv_sem=back_recv.at[level, color, slot],
            device_id=(partners[COLOR_DIMS[color][level]],), device_id_type=MESH)

    def part_rows(color):
        return rows_at(base(color, 1), spans[0])

    def part_share_copy(color, chunk, arriving):
        slot = chunk % GATHER_SLOTS
        mine = ring.at[slot, core, color, part_rows(color), :]
        theirs = ring.at[slot, 1 - core, color, part_rows(color), :]
        return pltpu.make_async_remote_copy(
            src_ref=mine, dst_ref=theirs if arriving else mine,
            send_sem=back_send.at[0, color, slot], recv_sem=back_recv.at[0, color, slot],
            device_id=(partners[CORE],), device_id_type=MESH)

    def part_stores(group, chunk):
        slot = chunk % GATHER_SLOTS
        place = chunk - full_chunks - sum(PART_GROUPS[:group])
        copies = []
        for color in range(COLORS):
            for which in range(2):
                out_ref = part_refs[(group * COLORS + color) * 2 + which]
                source = ring.at[slot, core if which == 0 else 1 - core, color, part_rows(color), :]
                copies.append(pltpu.make_async_copy(
                    source, out_ref.at[place], part_sem.at[color, which, slot]))
        return copies

    def share_copy(chunk, arriving):
        slot = chunk % GATHER_SLOTS
        return pltpu.make_async_remote_copy(
            src_ref=ring.at[slot, core], dst_ref=ring.at[slot, 1 - core if arriving else core],
            send_sem=share_send.at[slot], recv_sem=share_recv.at[slot],
            device_id=(partners[CORE],), device_id_type=MESH)

    def store_copy(chunk):
        slot = chunk % GATHER_SLOTS
        return pltpu.make_async_copy(ring.at[slot], gathered.at[chunk], store_sem.at[slot])

    def small_copy(step):
        return pltpu.make_async_remote_copy(
            src_ref=small_out, dst_ref=small_recv.at[step], send_sem=small_send_sem.at[step],
            recv_sem=small_recv_sem.at[step], device_id=(partners[step],), device_id_type=MESH)

    def product(chunk, which_core):
        rows = pl.ds(pl.multiple_of(which_core * half, 128), half)
        return jnp.dot(turned[rows, :], cols_buf[chunk % 2], preferred_element_type=jnp.float32)

    def opens_layer(chunk):
        return (chunk > 0) & (chunk % (2 * chunks_per_mat) == 0)

    def turn_rows(chunk):
        down = (chunk // chunks_per_mat) % 2 == 0

        @pl.when((chunk % chunks_per_mat == 0) | (down & (chunk % down_subs == 0)))
        def _():
            rows_load(1, chunk).wait()
            for start in range(0, row_dim, TILE):
                turned[start:start + TILE, :] = rows_buf[:, start:start + TILE].T
            for period, here in ((down_subs, down), (chunks_per_mat, jnp.logical_not(down))):
                following = chunk + period

                @pl.when(here & (following < num_chunks))
                def _(following=following):
                    for_mat(following, lambda mat: rows_load(mat, following).start())

    grad_top_store = pltpu.make_async_copy(grad_normed, grad_top, io_sem.at[0])
    grad_b_store = pltpu.make_async_copy(grad_b, grad_b_hbm, io_sem.at[1])

    def load(chunk):
        turn_rows(chunk)

        @pl.when(chunk > 0)
        def _():
            for_mat(chunk, lambda mat: cols_load(mat, chunk).wait())

        @pl.when(chunk == 0)
        def _():
            for copy in weight_loads(0, chunk):
                copy.start()
            grad_b_store.wait()

        @pl.when(chunk == 1)
        def _():
            grad_top_store.wait()
            grad_normed[...] = jnp.zeros_like(grad_normed)

        after = chunk + 1

        @pl.when((after < num_chunks) & jnp.logical_not(opens_layer(after)))
        def _():
            for_mat(after, lambda mat: cols_load(mat, after).start())

    def load_weights(chunk):
        def arrive(mat):
            for copy in weight_loads(mat, chunk):
                copy.wait()

        for_mat(chunk, arrive)
        after, before = chunk + 1, chunk - 1

        @pl.when(after < num_chunks)
        def _():
            def start(mat):
                for copy in weight_loads(mat, after):
                    copy.start()

            for_mat(after, start)

        @pl.when((before >= 0) & ((before // chunks_per_mat) % 2 == 0))
        def _():
            grad_pre_store(before % chunks_per_mat).wait()

    def compute_sent(chunk):
        value = product(chunk, 1 - core).astype(jnp.bfloat16)
        for color in range(COLORS):
            sent_core[color] = value[color * region:(color + 1) * region]

    def share_core(chunk):
        core_copy(chunk).start()

    def compute_kept(chunk):
        value = product(chunk, core)
        for color in range(COLORS):
            kept[chunk % KEPT_SLOTS, color] = value[color * region:(color + 1) * region]

    def halve(level, chunk, arrived):
        slot = chunk % KEPT_SLOTS
        recv_slot = chunk % RECV_SLOTS
        for color in range(COLORS):
            if level > 0:
                out_copy(level - 1, color, chunk).wait()
            held = base(color, level)

            def total(start, size, color=color, held=held):
                own = kept[slot, color, rows_at(start, size), :]
                return own + arrived[recv_slot, color, rows_at(start - held, size), :].astype(jnp.float32)

            if level < 3:
                mine = base(color, level + 1)
                sent_bufs[level][color] = total(other(color, level), spans[level]).astype(jnp.bfloat16)
                kept[slot, color, rows_at(mine, spans[level]), :] = total(mine, spans[level])
                out_copy(level, color, chunk).start()
            else:
                gather_slot = chunk % GATHER_SLOTS
                ring[gather_slot, core, color, rows_at(held, spans[2]), :] = total(held, spans[2]).astype(jnp.bfloat16)
                back_copy(2, color, chunk, False).start()

    def send_1(chunk):
        core_copy(chunk).wait()
        halve(0, chunk, recv_core)

    def send_2(chunk):
        halve(1, chunk, recv_1)

    def send_3(chunk):
        halve(2, chunk, recv_2)

    def send_back_3(chunk):
        halve(3, chunk, recv_3)

    def pass_back(level, chunk):
        for color in range(COLORS):
            back_copy(level + 1, color, chunk, True).wait()
            back_copy(level, color, chunk, False).start()

    def send_back_2(chunk):
        pass_back(1, chunk)

    def send_back_1(chunk):
        @pl.when(chunk < full_chunks)
        def _():
            pass_back(0, chunk)

        @pl.when(chunk >= full_chunks)
        def _():
            for color in range(COLORS):
                back_copy(1, color, chunk, True).wait()
                part_share_copy(color, chunk, False).start()

    def send_back_core(chunk):
        @pl.when(chunk < full_chunks)
        def _():
            for color in range(COLORS):
                back_copy(0, color, chunk, True).wait()
            share_copy(chunk, False).start()

        @pl.when(chunk >= full_chunks)
        def _():
            for color in range(COLORS):
                part_share_copy(color, chunk, True).wait()

        for group, size in enumerate(PART_GROUPS):
            first = full_chunks + sum(PART_GROUPS[:group])

            @pl.when((chunk >= first) & (chunk < first + size))
            def _(group=group):
                for copy in part_stores(group, chunk):
                    copy.start()

    def store(chunk):
        @pl.when(chunk < full_chunks)
        def _():
            share_copy(chunk, True).wait()
            store_copy(chunk).start()

        @pl.when((chunk > 0) & (chunk <= full_chunks))
        def _():
            store_copy(chunk - 1).wait()

        for group, size in enumerate(PART_GROUPS):
            first = full_chunks + sum(PART_GROUPS[:group])

            @pl.when((chunk >= first) & (chunk < first + size))
            def _(group=group):
                for copy in part_stores(group, chunk):
                    copy.wait()

    token_half = grad_b.shape[0] // 2

    def backward(part, chunk):
        slot = chunk % 2
        sub = chunk % chunks_per_mat
        mat = chunk // chunks_per_mat
        layer = num_layers - 1 - mat // 2

        @pl.when(mat % 2 == 0)
        def _():
            cols = slice(part * TILE, (part + 1) * TILE)

            @pl.loop(0, 2)
            def _(which):
                rows = pl.ds(pl.multiple_of(which * token_half, 128), token_half)
                grad_act = lax.dot_general(
                    grad_b[rows, :], weight_buf[slot, cols, :], FEATURE_DIMS, preferred_element_type=jnp.float32)
                grad_pre = grad_act * gelu_slope(pre_buf[slot, rows, cols].astype(jnp.float32))
                grad_pre_buf[rows, cols] = grad_pre.astype(jnp.bfloat16)
                start = row_dim + sub * chunk_cols + part * TILE
                small_out[pl.ds(layer, 1), pl.ds(pl.multiple_of(start, 128), TILE)] += jnp.sum(grad_pre, axis=0, keepdims=True)

            if part == chunk_cols // TILE - 1:
                grad_pre_store(sub).start()

        @pl.when(mat % 2 == 1)
        def _():
            pieces = row_dim // chunk_cols * (chunk_cols // TILE) // 3
            grad_rows = []
            for piece in range(part * pieces, (part + 1) * pieces):
                start, first = divmod(piece * TILE, chunk_cols)
                grad_rows.append((piece, lax.dot_general(
                    cols_buf[slot], weight_buf[slot, first:first + TILE, start * chunk_cols:(start + 1) * chunk_cols],
                    FEATURE_DIMS, preferred_element_type=jnp.float32)))
            for piece, value in grad_rows:
                grad_normed[:, piece * TILE:(piece + 1) * TILE] += value

    def norm_loads(layer, block):
        rows = pl.ds(pl.multiple_of(block * NORM_ROWS, NORM_ROWS), NORM_ROWS)
        slot = block % 2
        copies = [pltpu.make_async_copy(hid_refs[layer].at[rows, :], hid_buf.at[slot], norm_sem.at[0, slot])]
        if layer > 0:
            copies.append(pltpu.make_async_copy(grad_top.at[rows, :], grad_buf.at[slot], norm_sem.at[1, slot]))
        return copies

    def layer_input_grad(layer):
        num_blocks = grad_b.shape[0] // NORM_ROWS
        for copy in norm_loads(layer, 0):
            copy.start()

        @pl.loop(0, num_blocks)
        def _(block):
            @pl.when(block + 1 < num_blocks)
            def _():
                for copy in norm_loads(layer, block + 1):
                    copy.start()

            for copy in norm_loads(layer, block):
                copy.wait()
            rows = pl.ds(pl.multiple_of(block * NORM_ROWS, NORM_ROWS), NORM_ROWS)
            hid_f = hid_buf[block % 2].astype(jnp.float32)
            hid_scale = inverse_rms(hid_f)
            hid_hat = hid_f * hid_scale
            normed_grad = grad_normed[rows, :]
            small_out[layer:layer + 1, :row_dim] += jnp.sum(normed_grad * hid_hat, axis=0, keepdims=True)
            if layer > 0:
                grad_normed[rows, :] = jnp.zeros((NORM_ROWS, row_dim), jnp.float32)
                grad_hat = normed_grad * gain_in[layer:layer + 1, :].astype(jnp.float32)
                grad_new = grad_buf[block % 2] + hid_scale * (
                    grad_hat - hid_hat * jnp.mean(grad_hat * hid_hat, axis=-1, keepdims=True))
                grad_b[rows, :] = grad_new.astype(jnp.bfloat16)
                small_out[layer - 1:layer, row_dim + hidden_dim:] += jnp.sum(grad_new, axis=0, keepdims=True)

        if layer > 0:
            copy = pltpu.make_async_copy(grad_b, grad_b_hbm, grad_b_sem)
            copy.start()
            copy.wait()
            following = jnp.int32((num_layers - layer) * 2 * chunks_per_mat)
            cols_load((num_layers - layer) * 2, following).start()

    def input_grad(chunk):
        for layer in range(num_layers):
            last = (num_layers - 1 - layer) * 2 * chunks_per_mat + 2 * chunks_per_mat - 1

            @pl.when(chunk == last)
            def _(layer=layer):
                layer_input_grad(layer)

    events = dict(
        load=load, load_weights=load_weights, compute_sent=compute_sent, share_core=share_core, compute_kept=compute_kept, send_1=send_1, send_2=send_2, send_3=send_3,
        send_back_3=send_back_3, send_back_2=send_back_2, send_back_1=send_back_1, send_back_core=send_back_core, store=store,
        backward_0=functools.partial(backward, 0), backward_1=functools.partial(backward, 1),
        backward_2=functools.partial(backward, 2), input_grad=input_grad)

    cols_buf[0] = grad_b[:, :chunk_cols]
    pl.semaphore_wait(barrier, 4)

    @pl.loop(0, num_chunks + MAX_LAG)
    def _(it):
        for step in range(4):
            @pl.when(it == num_chunks + step)
            def _(step=step):
                small_copy(step).start()
        for name, lag in PIPELINE:
            chunk = it - lag

            @pl.when((chunk >= 0) & (chunk < num_chunks))
            def _(name=name, chunk=chunk):
                events[name](chunk)
        for step in range(4):
            @pl.when(it == num_chunks + step)
            def _(step=step):
                small_copy(step).wait()
                small_out[...] += small_recv[step]


def run_stack(tokens, upstream, norm_gain, w_up, bias_up, w_down, bias_down, axis, chunk_cols, tile_cols):
    num_layers, row_dim, hidden = w_up.shape
    num_tokens = tokens.shape[0]
    chunks_per_mat = hidden // chunk_cols
    region = row_dim // (2 * COLORS)
    half = (COLORS, region, chunk_cols)
    sizes = (num_layers, chunks_per_mat, row_dim, chunk_cols, region, row_dim // chunk_cols, tile_cols, axis)
    full_chunks = 2 * num_layers * chunks_per_mat - sum(PART_GROUPS)
    bf16, f32 = jnp.bfloat16, jnp.float32
    dma = pltpu.SemaphoreType.DMA
    any_spec = pl.BlockSpec(memory_space=pl.ANY)
    vmem_spec = pl.BlockSpec(memory_space=pltpu.VMEM)
    shape = jax.ShapeDtypeStruct
    rows, wide, small = (num_tokens, row_dim), (num_layers, num_tokens, hidden), (num_layers, 2 * row_dim + hidden)
    part_shapes = [shape((size, region // 2, chunk_cols), bf16) for size in PART_GROUPS for _ in range(2 * COLORS)]
    gathered, small_sum, *rest = pl.pallas_call(
        functools.partial(stack_kernel, sizes),
        out_shape=[
            shape((full_chunks, 2) + half, bf16), shape(small, f32), shape((chunks_per_mat, num_tokens, chunk_cols), bf16),
            shape(rows, bf16), shape(rows, bf16), shape((num_layers,) + rows, bf16), shape(wide, bf16), shape(wide, bf16),
            shape(rows, f32),
        ] + part_shapes,
        in_specs=[any_spec] * 4 + [vmem_spec] * 3,
        out_specs=[any_spec, vmem_spec] + [any_spec] * (7 + len(part_shapes)),
        scratch_shapes=[
            pltpu.VMEM(rows, bf16),
            pltpu.VMEM(rows, bf16),
            pltpu.VMEM(rows, f32),
            pltpu.VMEM((RECV_SLOTS,) + half, bf16),
            pltpu.VMEM((RECV_SLOTS, COLORS, region // 2, chunk_cols), bf16),
            pltpu.VMEM((RECV_SLOTS, COLORS, region // 4, chunk_cols), bf16),
            pltpu.VMEM((RECV_SLOTS, COLORS, region // 8, chunk_cols), bf16),
            pltpu.VMEM((GATHER_SLOTS, 2) + half, bf16),
            pltpu.VMEM((4,) + small, f32),
            dma((3,)), dma((2,)), dma((2,)), dma((2,)), dma((2,)), dma((2,)),
            dma((4, 2)), dma, dma((2, 2)), dma,
            dma, dma((RECV_SLOTS,)), dma((3, COLORS)), dma((3, COLORS, RECV_SLOTS)),
            dma((3, COLORS, GATHER_SLOTS)), dma((3, COLORS, GATHER_SLOTS)), dma((GATHER_SLOTS,)), dma((GATHER_SLOTS,)),
            dma((GATHER_SLOTS,)), dma((4,)), dma((4,)), dma((COLORS, 2, GATHER_SLOTS)),
        ],
        compiler_params=pltpu.CompilerParams(collective_id=0, has_side_effects=True, vmem_limit_bytes=67043328),
        name="stack",
    )(tokens, upstream, w_up, w_down, norm_gain, bias_up, bias_down)
    return gathered, small_sum, rest[7:]


def flip_pairs(num_devices, bit):
    return [(dev, dev ^ (1 << bit)) for dev in range(num_devices)]


def stream_blocks(num_blocks, start_loads, wait_loads, store_of, in_buf, out_buf, after_first=None):
    slots, region = in_buf.shape[0], in_buf.shape[2]
    for block in range(min(slots - 1, num_blocks)):
        start_loads(jnp.int32(block), block)

    @pl.loop(0, num_blocks)
    def _(block):
        slot = block % slots

        @pl.when(block + slots - 1 < num_blocks)
        def _():
            start_loads(block + slots - 1, (block + slots - 1) % slots)

        wait_loads(block, slot)

        @pl.when(block >= slots)
        def _():
            store_of(block - slots, slot).wait()

        for color in range(COLORS):
            out_buf[slot, color * region:(color + 1) * region, :] = in_buf[slot, color].astype(jnp.float32)
        store_of(block, slot).start()
        if after_first is not None:
            pl.when(block == 0)(after_first)

    for block in range(max(num_blocks - slots, 0), num_blocks):
        store_of(jnp.int32(block), block % slots).wait()


def block_target(out_ref, layer, kind, down_subs, chunk, which_core, rows, cols):
    half = pl.multiple_of(which_core * rows, rows)
    if kind == 0:
        first = pl.multiple_of((chunk // down_subs) * 2 * rows + half, rows)
        return out_ref.at[layer, pl.ds(first, rows), pl.ds(pl.multiple_of((chunk % down_subs) * cols, 128), cols)]
    return out_ref.at[layer, pl.ds(half, rows), pl.ds(pl.multiple_of(chunk * cols, 128), cols)]


def widen_kernel(spec, *refs):
    first, count, place, layer, kind, down_subs, small_widths, in_place = spec
    if in_place:
        refs = refs[:1 + bool(small_widths)] + refs[2 + bool(small_widths):]
    if small_widths:
        gathered, small, out_ref, *small_outs, in_buf, out_buf, in_sem, out_sem, small_buf, small_sem = refs
        small_load = pltpu.make_async_copy(small, small_buf, small_sem.at[0])
        small_load.start()
        starts = [sum(small_widths[:n]) for n in range(len(small_widths))]
        small_stores = [
            pltpu.make_async_copy(small_buf.at[:, start:start + width], small_out, small_sem.at[1 + n])
            for n, (start, width, small_out) in enumerate(zip(starts, small_widths, small_outs))]
    else:
        gathered, out_ref, in_buf, out_buf, in_sem, out_sem = refs
        small_stores = []

    def after_first():
        if small_stores:
            small_load.wait()
        for copy in small_stores:
            copy.start()

    rows, cols = out_buf.shape[1:]

    def load(block, slot):
        return pltpu.make_async_copy(gathered.at[first + block // 2, block % 2], in_buf.at[slot], in_sem.at[slot])

    def store(block, slot):
        target = block_target(out_ref, layer, kind, down_subs, place + block // 2, block % 2, rows, cols)
        return pltpu.make_async_copy(out_buf.at[slot], target, out_sem.at[slot])

    stream_blocks(
        2 * count, lambda block, slot: load(block, slot).start(), lambda block, slot: load(block, slot).wait(),
        store, in_buf, out_buf, after_first)
    for copy in small_stores:
        copy.wait()


def join_kernel(spec, *refs):
    skip, count, place, layer, kind, down_subs, axis = spec
    parts, (_, out_ref, in_buf, out_buf, in_sem, out_sem) = refs[:4 * COLORS], refs[4 * COLORS:]
    rows, cols = out_buf.shape[1:]
    part_rows = in_buf.shape[2] // 2
    me = lax.axis_index(axis)
    core = me % 2

    def copies(which, chunk, slot):
        found = []
        for color in range(COLORS):
            upper = (me >> COLOR_DIMS[color][0]) & 1
            for far in range(2):
                start = pl.multiple_of((upper if far == 0 else 1 - upper) * part_rows, part_rows)
                found.append(pltpu.make_async_copy(
                    parts[color * 4 + far * 2 + which].at[skip + chunk],
                    in_buf.at[slot, color, pl.ds(start, part_rows), :], in_sem.at[slot]))
        return found

    def start_loads(block, slot):
        for which in range(2):
            @pl.when(block % 2 == which)
            def _(which=which):
                for copy in copies(which, block // 2, slot):
                    copy.start()

    def wait_loads(block, slot):
        for copy in copies(0, block // 2, slot):
            copy.wait()

    def store(block, slot):
        which_core = jnp.where(block % 2 == 0, core, 1 - core)
        target = block_target(out_ref, layer, kind, down_subs, place + block // 2, which_core, rows, cols)
        return pltpu.make_async_copy(out_buf.at[slot], target, out_sem.at[slot])

    stream_blocks(2 * count, start_loads, wait_loads, store, in_buf, out_buf)


def widen_scratch(region, cols):
    return [
        pltpu.VMEM((STREAM_SLOTS, COLORS, region, cols), jnp.bfloat16),
        pltpu.VMEM((STREAM_SLOTS, COLORS * region, cols), jnp.float32),
        pltpu.SemaphoreType.DMA((STREAM_SLOTS,)),
        pltpu.SemaphoreType.DMA((STREAM_SLOTS,)),
    ]


def widen_cost(count, region, cols):
    size = count * 2 * COLORS * region * cols
    return pl.CostEstimate(flops=500 * size, bytes_accessed=6 * size, transcendentals=0)


def widen(gathered, first, count, place, layer, kind, shape, into, down_subs, small, small_widths):
    region, cols = gathered.shape[3:]
    any_spec = pl.BlockSpec(memory_space=pl.ANY)
    smalls = [jax.ShapeDtypeStruct((small.shape[0], width), jnp.float32) for width in small_widths]
    small_scratch = [pltpu.VMEM(small.shape, jnp.float32), pltpu.SemaphoreType.DMA((1 + len(smalls),))] if smalls else []
    return pl.pallas_call(
        functools.partial(widen_kernel, (first, count, place, layer, kind, down_subs, small_widths, into is not None)),
        in_specs=[any_spec] * (1 + bool(smalls) + (into is not None)),
        out_specs=[any_spec] * (1 + len(smalls)),
        out_shape=[jax.ShapeDtypeStruct(shape, jnp.float32)] + smalls,
        input_output_aliases={} if into is None else {1 + bool(smalls): 0},
        scratch_shapes=widen_scratch(region, cols) + small_scratch,
        cost_estimate=widen_cost(count, region, cols),
        compiler_params=pltpu.CompilerParams(vmem_limit_bytes=67043328),
    )(gathered, *([small] if smalls else []), *([] if into is None else [into]))


def split_at_gradients(first, count, per_mat):
    sizes = []
    while count:
        sizes.append(min(count, per_mat - first % per_mat))
        first, count = first + sizes[-1], count - sizes[-1]
    return sizes


def join(parts, skip, count, place, layer, kind, into, down_subs, axis):
    _, part_rows, cols = parts[0].shape
    any_spec = pl.BlockSpec(memory_space=pl.ANY)
    return pl.pallas_call(
        functools.partial(join_kernel, (skip, count, place, layer, kind, down_subs, axis)),
        in_specs=[any_spec] * (len(parts) + 1),
        out_specs=any_spec,
        out_shape=jax.ShapeDtypeStruct(into.shape, jnp.float32),
        scratch_shapes=widen_scratch(2 * part_rows, cols),
        input_output_aliases={len(parts): 0},
        cost_estimate=widen_cost(count, 2 * part_rows, cols),
        compiler_params=pltpu.CompilerParams(vmem_limit_bytes=67043328),
    )(*parts, into)


def swap(array, axis, num_devices, bit):
    return lax.ppermute(array, axis, flip_pairs(num_devices, bit))


def full_gradients(gathered, parts, small, num_layers, row_dim, hidden, chunk_cols, axis, num_devices):
    per_mat = hidden // chunk_cols
    down_subs = row_dim // chunk_cols
    groups = range(len(PART_GROUPS))
    mine = [[parts[(group * COLORS + color) * 2] for color in range(COLORS)] for group in groups]
    theirs = [[parts[(group * COLORS + color) * 2 + 1] for color in range(COLORS)] for group in groups]
    far = [[swap(mine[group][color], axis, num_devices, COLOR_DIMS[color][0])
            for color in range(COLORS)] for group in groups]
    last = num_layers - 1
    full = [None, None]
    shapes = ((num_layers, hidden, row_dim), (num_layers, row_dim, hidden))
    for call, count in enumerate(WIDEN_CALLS):
        first = sum(WIDEN_CALLS[:call])
        kind, place = divmod(first, per_mat)
        small_widths = (row_dim, hidden, row_dim) if call == 0 else ()
        full[kind], *rest = widen(
            gathered, first, count, place, last, kind, shapes[kind], full[kind], down_subs, small, small_widths)
        smalls = rest or smalls
    chunk = 2 * num_layers * per_mat - sum(PART_GROUPS)
    for group in groups:
        pieces = []
        for color in range(COLORS):
            shared = swap(far[group][color], axis, num_devices, CORE)
            pieces += [mine[group][color], theirs[group][color], far[group][color], shared]
        skip = 0
        for count in split_at_gradients(chunk, PART_GROUPS[group], per_mat):
            mat, place = divmod(chunk, per_mat)
            kind, layer = mat % 2, last - mat // 2
            full[kind] = join(pieces, skip, count, place, layer, kind, full[kind], down_subs, axis)
            chunk, skip = chunk + count, skip + count
    return smalls[0], full[1], smalls[1], full[0], smalls[2]


def solution(mesh):
    axis = mesh.axis_names[0]

    def device_grads(tokens, upstream, norm_gain, w_up, bias_up, w_down, bias_down):
        num_layers, width = norm_gain.shape
        hidden_width = w_up.shape[2]
        chunk_cols = width // 2
        gathered, small, parts = run_stack(
            tokens, upstream, norm_gain, w_up, bias_up, w_down, bias_down, axis, chunk_cols, 2 * UP_COLS)
        return full_gradients(gathered, parts, small, num_layers, width, hidden_width, chunk_cols, axis, mesh.size)

    row_spec = P(axis, None)
    full_spec = P()
    return jax.shard_map(
        device_grads,
        mesh=mesh,
        in_specs=(row_spec, row_spec, full_spec, full_spec, full_spec, full_spec, full_spec),
        out_specs=(full_spec, full_spec, full_spec, full_spec, full_spec),
        check_vma=False,
    )
```

```python
import functools

import jax
import jax.numpy as jnp
from jax import lax
from jax.experimental import pallas as pl
from jax.experimental.pallas import tpu as pltpu
from jax.sharding import PartitionSpec as P


EPSILON = 1e-6
FEATURE_DIMS = (((1,), (1,)), ((), ()))
MESH = pl.DeviceIdType.MESH
COLORS = 3
CORE, DIM_X, DIM_Y, DIM_Z = range(4)
COLOR_DIMS = ((DIM_X, DIM_Y, DIM_Z), (DIM_Y, DIM_Z, DIM_X), (DIM_Z, DIM_X, DIM_Y))
PIPELINE = (
    ("load", 0), ("compute_sent", 0), ("share_core", 0), ("send_3", 2), ("send_back_2", 4), ("send_back_1", 5),
    ("compute_kept", 0), ("send_back_core", 6), ("load_weights", 0), ("backward_0", 0), ("send_2", 1), ("backward_1", 0),
    ("send_1", 0), ("backward_2", 0), ("send_back_3", 2), ("store", 6), ("input_grad", 0),
)
MAX_LAG = 6
PART_GROUPS = (7, 5, 3, 3)
WIDEN_CALLS = (8, 6)
RECV_SLOTS = 2
KEPT_SLOTS = 3
GATHER_SLOTS = 6
TILE = 256
UP_COLS = 512
ACT_ROWS = 16
ACT_COLS = 256
STREAM_SLOTS = 4
NORM_ROWS = 128
GELU_SCALE = 0.7978845608028654
GELU_CUBIC = 0.044715


def inverse_rms(hid_f):
    return lax.rsqrt(jnp.mean(hid_f * hid_f, axis=-1, keepdims=True) + EPSILON)


def gelu(values):
    return (0.5 * values) * (1.0 + jnp.tanh(values * (GELU_SCALE + GELU_SCALE * GELU_CUBIC * (values * values))))


def forward_phase(
    sizes, hbm, branch, grad_b, small_out, before_top, io_sem, up_sem, down_sem, pre_sem, act_sem,
    hid, normed, up_buf, down_buf, pre_buf, act_buf, gain, bias_up, bias_down,
):
    (tokens, upstream, w_up, w_down, gain_in, bias_up_in, bias_down_in, hid_out, normed_out, pre_act_out, act_out,
     grad_top_out, grad_b_out) = hbm
    num_layers, num_tiles, tile_cols = sizes
    num_tokens, row_dim = hid.shape
    steps = num_tiles + 1
    parts = tile_cols // UP_COLS

    def up_load(layer, tile):
        cols = pl.ds(pl.multiple_of(tile * tile_cols, 128), tile_cols)
        return pltpu.make_async_copy(w_up.at[layer, :, cols], up_buf, up_sem)

    def down_load(layer, tile):
        rows = pl.ds(pl.multiple_of(tile * tile_cols, 128), tile_cols)
        return pltpu.make_async_copy(w_down.at[layer, rows, :], down_buf, down_sem)

    def pre_store(layer, tile):
        cols = pl.ds(pl.multiple_of(tile * tile_cols, 128), tile_cols)
        return pltpu.make_async_copy(pre_buf.at[tile % 2], pre_act_out.at[layer, :, cols], pre_sem.at[tile % 2])

    def act_store(layer, tile):
        cols = pl.ds(pl.multiple_of(tile * tile_cols, 128), tile_cols)
        return pltpu.make_async_copy(act_buf.at[tile % 2], act_out.at[layer, :, cols], act_sem.at[tile % 2])

    def normed_store(layer):
        return pltpu.make_async_copy(normed, normed_out.at[layer], io_sem.at[1])

    def hid_store():
        return pltpu.make_async_copy(hid, hid_out, io_sem.at[3])

    upstream_load = pltpu.make_async_copy(upstream, up_buf.at[:num_tokens, :], io_sem.at[2])
    tokens_load = pltpu.make_async_copy(tokens, hid, io_sem.at[0])
    tokens_load.start()
    up_load(0, 0).start()
    small_out[...] = jnp.zeros_like(small_out)
    branch[...] = jnp.zeros_like(branch)
    pre_buf[0, :, :UP_COLS] = jnp.zeros((num_tokens, UP_COLS), jnp.bfloat16)
    gain[...] = gain_in[...].astype(jnp.float32)
    bias_up[...] = bias_up_in[...].astype(jnp.float32)
    bias_down[...] = bias_down_in[...].astype(jnp.float32)
    tokens_load.wait()

    def each_block(action):
        @pl.loop(0, num_tokens // NORM_ROWS)
        def _(block):
            action(pl.ds(pl.multiple_of(block * NORM_ROWS, NORM_ROWS), NORM_ROWS))

    def normalize(layer, rows, hid_f):
        normed[rows, :] = ((hid_f * inverse_rms(hid_f)) * gain[pl.ds(layer, 1), :]).astype(jnp.bfloat16)

    def next_rows(layer, rows):
        new = ((hid[rows, :].astype(jnp.float32) + branch[rows, :]) + bias_down[pl.ds(layer, 1), :]).astype(jnp.bfloat16)
        hid[rows, :] = new
        return new.astype(jnp.float32)

    def activate(slot, part):
        start = part * UP_COLS
        for row in range(0, num_tokens, ACT_ROWS):
            for col in range(0, UP_COLS, ACT_COLS):
                piece = (slot, pl.ds(row, ACT_ROWS), pl.ds(pl.multiple_of(start + col, 128), ACT_COLS))
                act_buf[piece] = gelu(pre_buf[piece].astype(jnp.float32)).astype(jnp.bfloat16)

    def up_product(layer, tile):
        @pl.loop(0, parts)
        def _(part):
            fresh = tile * parts + part == 0
            last_slot = jnp.where((part == 0) & (tile > 0), (tile + 1) % 2, tile % 2)
            activate(last_slot, jnp.where(fresh, 0, (part + parts - 1) % parts))
            cols = pl.ds(pl.multiple_of(part * UP_COLS, 128), UP_COLS)
            bias = bias_up[pl.ds(layer, 1), pl.ds(pl.multiple_of(tile * tile_cols + part * UP_COLS, 128), UP_COLS)]
            pre_buf[tile % 2, :, cols] = (
                jnp.dot(normed[...], up_buf[:, cols], preferred_element_type=jnp.float32) + bias
            ).astype(jnp.bfloat16)

    def down_product(tile):
        slot = tile % 2
        for part in range(row_dim // UP_COLS):
            cols = slice(part * UP_COLS, (part + 1) * UP_COLS)
            branch[:, cols] += jnp.dot(act_buf[slot], down_buf[:, cols], preferred_element_type=jnp.float32)

    each_block(lambda rows: normalize(0, rows, hid[rows, :].astype(jnp.float32)))

    @pl.loop(0, num_layers * steps)
    def _(step):
        layer, tile = step // steps, step % steps

        @pl.when(tile < num_tiles)
        def _():
            up_load(layer, tile).wait()

            @pl.when(step == 0)
            def _():
                normed_store(0).start()
                down_load(0, 0).start()

            @pl.when(tile > 1)
            def _():
                pre_store(layer, tile - 2).wait()
                act_store(layer, tile - 2).wait()

            up_product(layer, tile)
            pre_store(layer, tile).start()

            @pl.when(tile + 1 < num_tiles)
            def _():
                up_load(layer, tile + 1).start()

            @pl.when((tile + 1 == num_tiles) & (layer + 1 < num_layers))
            def _():
                up_load(layer + 1, 0).start()

            @pl.when((tile + 1 == num_tiles) & (layer + 1 == num_layers))
            def _():
                upstream_load.start()

        @pl.when(tile == num_tiles)
        def _():
            activate((num_tiles - 1) % 2, parts - 1)

        @pl.when(tile > 0)
        def _():
            act_store(layer, tile - 1).start()
            down_load(layer, tile - 1).wait()
            down_product(tile - 1)

            @pl.when(tile < num_tiles)
            def _():
                down_load(layer, tile).start()

            @pl.when((tile == num_tiles) & (layer + 1 < num_layers))
            def _():
                down_load(layer + 1, 0).start()

        @pl.when(tile == num_tiles)
        def _():
            for back in (2, 1):
                pre_store(layer, num_tiles - back).wait()
                act_store(layer, num_tiles - back).wait()
            normed_store(layer).wait()

            @pl.when(layer + 1 < num_layers)
            def _():
                def to_next(rows):
                    normalize(layer + 1, rows, next_rows(layer, rows))
                    branch[rows, :] = jnp.zeros((NORM_ROWS, row_dim), jnp.float32)

                each_block(to_next)
                hid_store().start()
                normed_store(layer + 1).start()

    hid_store().wait()
    before_top()
    bias_start = small_out.shape[1] - row_dim
    upstream_load.wait()

    def top_rows(rows):
        top_f = next_rows(num_layers - 1, rows)
        top_scale = inverse_rms(top_f)
        top_hat = top_f * top_scale
        up_f = up_buf[rows, :].astype(jnp.float32)
        grad = top_scale * (up_f - top_hat * jnp.mean(up_f * top_hat, axis=-1, keepdims=True))
        branch[rows, :] = grad
        grad_b[rows, :] = grad.astype(jnp.bfloat16)
        small_out[num_layers - 1:, bias_start:] += jnp.sum(grad, axis=0, keepdims=True)

    def store_rows(block):
        rows = pl.ds(pl.multiple_of(block * NORM_ROWS, NORM_ROWS), NORM_ROWS)
        pltpu.make_async_copy(grad_b.at[rows, :], grad_b_out.at[rows, :], io_sem.at[1]).start()
        pltpu.make_async_copy(branch.at[rows, :], grad_top_out.at[rows, :], io_sem.at[0]).start()

    num_blocks = num_tokens // NORM_ROWS

    @pl.loop(0, num_blocks)
    def _(block):
        top_rows(pl.ds(pl.multiple_of(block * NORM_ROWS, NORM_ROWS), NORM_ROWS))
        pl.when(block > 0)(lambda: store_rows(block - 1))

    store_rows(num_blocks - 1)


def gelu_slope(values):
    square = values * values
    bend = jnp.tanh(values * (GELU_SCALE + GELU_SCALE * GELU_CUBIC * square))
    return 0.5 * (1.0 + bend) + (0.5 * values) * (1.0 - bend * bend) * (GELU_SCALE + 3.0 * GELU_SCALE * GELU_CUBIC * square)


def stack_kernel(sizes, *refs):
    num_layers, chunks_per_mat, row_dim, chunk_cols, region, _, tile_cols, axis = sizes
    inputs, refs = refs[:7], refs[7:]
    part_count = 2 * COLORS * len(PART_GROUPS)
    outputs, part_refs, refs = refs[:9], refs[9:9 + part_count], refs[9 + part_count:]
    tokens, upstream, w_up, w_down, gain_in, bias_up_in, bias_down_in = inputs
    gathered, small_out, grad_pre_hbm, grad_b_hbm, hid_out, normed, pre_act, activated, grad_top = outputs
    rows_buf, grad_b, grad_normed, *shared = refs[:9]
    io_sem, up_sem, down_sem, pre_sem, act_sem, *sems = refs[9:]
    load_sem = sems[0]
    num_tokens = grad_b.shape[0]
    hidden_dim = chunks_per_mat * chunk_cols
    f32, bf16 = jnp.float32, jnp.bfloat16
    me = lax.axis_index(axis)
    barrier = pltpu.get_barrier_semaphore()
    for dim in range(4):
        pl.semaphore_signal(barrier, inc=1, device_id=(flip(me, dim),), device_id_type=MESH)

    def first_rows_load():
        pltpu.make_async_copy(activated.at[num_layers - 1, :, :row_dim], rows_buf, load_sem.at[0, 0]).start()

    hbm = (tokens, upstream, w_up, w_down, gain_in, bias_up_in, bias_down_in, hid_out, normed, pre_act, activated, grad_top, grad_b_hbm)
    pl.run_scoped(
        functools.partial(
            forward_phase, (num_layers, hidden_dim // tile_cols, tile_cols), hbm, grad_normed, grad_b, small_out, first_rows_load,
            io_sem, up_sem, down_sem, pre_sem, act_sem),
        pltpu.VMEM((num_tokens, row_dim), bf16),
        pltpu.VMEM((num_tokens, row_dim), bf16),
        pltpu.VMEM((row_dim, tile_cols), bf16),
        pltpu.VMEM((tile_cols, row_dim), bf16),
        pltpu.VMEM((2, num_tokens, tile_cols), bf16),
        pltpu.VMEM((2, num_tokens, tile_cols), bf16),
        pltpu.VMEM((num_layers, row_dim), f32),
        pltpu.VMEM((num_layers, hidden_dim), f32),
        pltpu.VMEM((num_layers, row_dim), f32),
    )
    hbm = ((tokens, hid_out), normed, pre_act, activated, grad_top, w_up, w_down, gain_in, gathered, grad_pre_hbm, grad_b_hbm, part_refs)
    pl.run_scoped(
        functools.partial(
            backward_phase, sizes, hbm, small_out, rows_buf, grad_b, grad_normed, shared, barrier, io_sem, sems),
        pltpu.VMEM((row_dim, num_tokens), bf16),
        pltpu.VMEM((2, num_tokens, chunk_cols), bf16),
        pltpu.VMEM((COLORS, region, chunk_cols), bf16),
        pltpu.VMEM((KEPT_SLOTS, COLORS, region, chunk_cols), f32),
        pltpu.VMEM((COLORS, region // 2, chunk_cols), bf16),
        pltpu.VMEM((COLORS, region // 4, chunk_cols), bf16),
        pltpu.VMEM((COLORS, region // 8, chunk_cols), bf16),
        pltpu.VMEM((2, chunk_cols, row_dim), bf16),
        pltpu.VMEM((2, num_tokens, chunk_cols), bf16),
        pltpu.VMEM((num_tokens, chunk_cols), bf16),
        pltpu.VMEM((2, NORM_ROWS, row_dim), bf16),
        pltpu.VMEM((2, NORM_ROWS, row_dim), f32),
    )


def flip(device, dim):
    step = 1 << dim
    return device + step - 2 * step * ((device // step) % 2)


def backward_phase(
    sizes, hbm, small_out, rows_buf, grad_b, grad_normed, shared, barrier, io_sem, sems, turned, cols_buf, sent_core, kept,
    sent_1, sent_2, sent_3, weight_buf, pre_buf, grad_pre_buf, hid_buf, grad_buf,
):
    num_layers, chunks_per_mat, row_dim, chunk_cols, region, down_subs, _, axis = sizes
    num_mats = 2 * num_layers
    hidden_dim = chunks_per_mat * chunk_cols
    (hid_refs, normed, pre_act, activated, grad_top, w_up, w_down, gain_in, gathered, grad_pre_hbm, grad_b_hbm, part_refs) = hbm
    recv_core, recv_1, recv_2, recv_3, ring, small_recv = shared[:6]
    (load_sem, grad_pre_sem, norm_sem, grad_b_sem, core_send, core_recv, out_send, out_recv, back_send, back_recv,
     share_send, share_recv, store_sem, small_send_sem, small_recv_sem, part_sem) = sems
    num_chunks = num_mats * chunks_per_mat
    full_chunks = num_chunks - sum(PART_GROUPS)
    half = COLORS * region
    me = lax.axis_index(axis)
    bits = [me % 2, (me // 2) % 2, (me // 4) % 2, me // 8]
    partners = [flip(me, dim) for dim in range(4)]
    core = bits[CORE]
    sent_bufs, recv_bufs = (sent_1, sent_2, sent_3), (recv_1, recv_2, recv_3)
    spans = (region // 2, region // 4, region // 8)

    def base(color, level):
        total = 0
        for step in range(level):
            total = total + bits[COLOR_DIMS[color][step]] * spans[step]
        return total

    def other(color, level):
        return base(color, level) + (1 - bits[COLOR_DIMS[color][level]]) * spans[level]

    def rows_at(start, size):
        return pl.ds(pl.multiple_of(start, spans[2]), size)

    def rows_load(mat, chunk):
        layer = num_layers - 1 - mat // 2
        if mat % 2 == 0:
            start = ((chunk % chunks_per_mat) // down_subs) * row_dim
            source = activated.at[layer, :, pl.ds(pl.multiple_of(start, 128), row_dim)]
        else:
            source = normed.at[layer]
        return pltpu.make_async_copy(source, rows_buf, load_sem.at[0, 0])

    def weight_loads(mat, chunk):
        slot = chunk % 2
        layer = num_layers - 1 - mat // 2
        cols = pl.ds(pl.multiple_of((chunk % chunks_per_mat) * chunk_cols, 128), chunk_cols)
        if mat % 2 == 0:
            return [
                pltpu.make_async_copy(w_down.at[layer, cols, :], weight_buf.at[slot], load_sem.at[1, slot]),
                pltpu.make_async_copy(pre_act.at[layer, :, cols], pre_buf.at[slot], load_sem.at[2, slot]),
            ]
        return [
            pltpu.make_async_copy(
                w_up.at[layer, part * chunk_cols:(part + 1) * chunk_cols, cols],
                weight_buf.at[slot, :, part * chunk_cols:(part + 1) * chunk_cols], load_sem.at[1 + part, slot])
            for part in range(down_subs)
        ]

    def cols_load(mat, chunk):
        sub = chunk % chunks_per_mat
        if mat % 2 == 0:
            source = grad_b_hbm.at[:, pl.ds(pl.multiple_of((sub % down_subs) * chunk_cols, 128), chunk_cols)]
        else:
            source = grad_pre_hbm.at[sub]
        return pltpu.make_async_copy(source, cols_buf.at[chunk % 2], load_sem.at[3, chunk % 2])

    def for_mat(chunk, action):
        for mat in range(num_mats):
            @pl.when(chunk // chunks_per_mat == mat)
            def _(mat=mat):
                action(mat)

    def grad_pre_store(sub):
        return pltpu.make_async_copy(grad_pre_buf, grad_pre_hbm.at[sub], grad_pre_sem)

    def core_copy(chunk):
        slot = chunk % RECV_SLOTS
        return pltpu.make_async_remote_copy(
            src_ref=sent_core, dst_ref=recv_core.at[slot], send_sem=core_send, recv_sem=core_recv.at[slot],
            device_id=(partners[CORE],), device_id_type=MESH)

    def out_copy(level, color, chunk):
        slot = chunk % RECV_SLOTS
        return pltpu.make_async_remote_copy(
            src_ref=sent_bufs[level].at[color], dst_ref=recv_bufs[level].at[slot, color],
            send_sem=out_send.at[level, color], recv_sem=out_recv.at[level, color, slot],
            device_id=(partners[COLOR_DIMS[color][level]],), device_id_type=MESH)

    def back_copy(level, color, chunk, arriving):
        slot = chunk % GATHER_SLOTS
        mine = ring.at[slot, core, color, rows_at(base(color, level + 1), spans[level]), :]
        theirs = ring.at[slot, core, color, rows_at(other(color, level), spans[level]), :]
        return pltpu.make_async_remote_copy(
            src_ref=mine, dst_ref=theirs if arriving else mine,
            send_sem=back_send.at[level, color, slot], recv_sem=back_recv.at[level, color, slot],
            device_id=(partners[COLOR_DIMS[color][level]],), device_id_type=MESH)

    def part_rows(color):
        return rows_at(base(color, 1), spans[0])

    def part_share_copy(color, chunk, arriving):
        slot = chunk % GATHER_SLOTS
        mine = ring.at[slot, core, color, part_rows(color), :]
        theirs = ring.at[slot, 1 - core, color, part_rows(color), :]
        return pltpu.make_async_remote_copy(
            src_ref=mine, dst_ref=theirs if arriving else mine,
            send_sem=back_send.at[0, color, slot], recv_sem=back_recv.at[0, color, slot],
            device_id=(partners[CORE],), device_id_type=MESH)

    def part_stores(group, chunk):
        slot = chunk % GATHER_SLOTS
        place = chunk - full_chunks - sum(PART_GROUPS[:group])
        copies = []
        for color in range(COLORS):
            for which in range(2):
                out_ref = part_refs[(group * COLORS + color) * 2 + which]
                source = ring.at[slot, core if which == 0 else 1 - core, color, part_rows(color), :]
                copies.append(pltpu.make_async_copy(
                    source, out_ref.at[place], part_sem.at[color, which, slot]))
        return copies

    def share_copy(chunk, arriving):
        slot = chunk % GATHER_SLOTS
        return pltpu.make_async_remote_copy(
            src_ref=ring.at[slot, core], dst_ref=ring.at[slot, 1 - core if arriving else core],
            send_sem=share_send.at[slot], recv_sem=share_recv.at[slot],
            device_id=(partners[CORE],), device_id_type=MESH)

    def store_copy(chunk):
        slot = chunk % GATHER_SLOTS
        return pltpu.make_async_copy(ring.at[slot], gathered.at[chunk], store_sem.at[slot])

    def small_copy(step):
        return pltpu.make_async_remote_copy(
            src_ref=small_out, dst_ref=small_recv.at[step], send_sem=small_send_sem.at[step],
            recv_sem=small_recv_sem.at[step], device_id=(partners[step],), device_id_type=MESH)

    def product(chunk, which_core):
        rows = pl.ds(pl.multiple_of(which_core * half, 128), half)
        return jnp.dot(turned[rows, :], cols_buf[chunk % 2], preferred_element_type=jnp.float32)

    def opens_layer(chunk):
        return (chunk > 0) & (chunk % (2 * chunks_per_mat) == 0)

    def turn_rows(chunk):
        down = (chunk // chunks_per_mat) % 2 == 0

        @pl.when((chunk % chunks_per_mat == 0) | (down & (chunk % down_subs == 0)))
        def _():
            rows_load(1, chunk).wait()
            for start in range(0, row_dim, TILE):
                turned[start:start + TILE, :] = rows_buf[:, start:start + TILE].T
            for period, here in ((down_subs, down), (chunks_per_mat, jnp.logical_not(down))):
                following = chunk + period

                @pl.when(here & (following < num_chunks))
                def _(following=following):
                    for_mat(following, lambda mat: rows_load(mat, following).start())

    grad_top_store = pltpu.make_async_copy(grad_normed, grad_top, io_sem.at[0])
    grad_b_store = pltpu.make_async_copy(grad_b, grad_b_hbm, io_sem.at[1])

    def load(chunk):
        turn_rows(chunk)

        @pl.when(chunk > 0)
        def _():
            for_mat(chunk, lambda mat: cols_load(mat, chunk).wait())

        @pl.when(chunk == 0)
        def _():
            for copy in weight_loads(0, chunk):
                copy.start()

        @pl.when(chunk == 1)
        def _():
            grad_top_store.wait()
            grad_normed[...] = jnp.zeros_like(grad_normed)

        after = chunk + 1

        @pl.when((chunk > 0) & (after < num_chunks) & jnp.logical_not(opens_layer(after)))
        def _():
            for_mat(after, lambda mat: cols_load(mat, after).start())

    def load_weights(chunk):
        @pl.when(chunk == 0)
        def _():
            grad_b_store.wait()
            cols_load(0, chunk + 1).start()

        def arrive(mat):
            for copy in weight_loads(mat, chunk):
                copy.wait()

        for_mat(chunk, arrive)
        after, before = chunk + 1, chunk - 1

        @pl.when(after < num_chunks)
        def _():
            def start(mat):
                for copy in weight_loads(mat, after):
                    copy.start()

            for_mat(after, start)

        @pl.when((before >= 0) & ((before // chunks_per_mat) % 2 == 0))
        def _():
            grad_pre_store(before % chunks_per_mat).wait()

    def compute_sent(chunk):
        value = product(chunk, 1 - core).astype(jnp.bfloat16)
        for color in range(COLORS):
            sent_core[color] = value[color * region:(color + 1) * region]

    def share_core(chunk):
        core_copy(chunk).start()

    def compute_kept(chunk):
        value = product(chunk, core)
        for color in range(COLORS):
            kept[chunk % KEPT_SLOTS, color] = value[color * region:(color + 1) * region]

    def halve(level, chunk, arrived):
        slot = chunk % KEPT_SLOTS
        recv_slot = chunk % RECV_SLOTS
        for color in range(COLORS):
            if level > 0:
                out_copy(level - 1, color, chunk).wait()
            held = base(color, level)

            def total(start, size, color=color, held=held):
                own = kept[slot, color, rows_at(start, size), :]
                return own + arrived[recv_slot, color, rows_at(start - held, size), :].astype(jnp.float32)

            if level < 3:
                mine = base(color, level + 1)
                sent_bufs[level][color] = total(other(color, level), spans[level]).astype(jnp.bfloat16)
                kept[slot, color, rows_at(mine, spans[level]), :] = total(mine, spans[level])
                out_copy(level, color, chunk).start()
            else:
                gather_slot = chunk % GATHER_SLOTS
                ring[gather_slot, core, color, rows_at(held, spans[2]), :] = total(held, spans[2]).astype(jnp.bfloat16)
                back_copy(2, color, chunk, False).start()

    def send_1(chunk):
        core_copy(chunk).wait()
        halve(0, chunk, recv_core)

    def send_2(chunk):
        halve(1, chunk, recv_1)

    def send_3(chunk):
        halve(2, chunk, recv_2)

    def send_back_3(chunk):
        halve(3, chunk, recv_3)

    def pass_back(level, chunk):
        for color in range(COLORS):
            back_copy(level + 1, color, chunk, True).wait()
            back_copy(level, color, chunk, False).start()

    def send_back_2(chunk):
        pass_back(1, chunk)

    def send_back_1(chunk):
        @pl.when(chunk < full_chunks)
        def _():
            pass_back(0, chunk)

        @pl.when(chunk >= full_chunks)
        def _():
            for color in range(COLORS):
                back_copy(1, color, chunk, True).wait()
                part_share_copy(color, chunk, False).start()

    def send_back_core(chunk):
        @pl.when(chunk < full_chunks)
        def _():
            for color in range(COLORS):
                back_copy(0, color, chunk, True).wait()
            share_copy(chunk, False).start()

        @pl.when(chunk >= full_chunks)
        def _():
            for color in range(COLORS):
                part_share_copy(color, chunk, True).wait()

        for group, size in enumerate(PART_GROUPS):
            first = full_chunks + sum(PART_GROUPS[:group])

            @pl.when((chunk >= first) & (chunk < first + size))
            def _(group=group):
                for copy in part_stores(group, chunk):
                    copy.start()

    def store(chunk):
        @pl.when(chunk < full_chunks)
        def _():
            share_copy(chunk, True).wait()
            store_copy(chunk).start()

        @pl.when((chunk > 0) & (chunk <= full_chunks))
        def _():
            store_copy(chunk - 1).wait()

        for group, size in enumerate(PART_GROUPS):
            first = full_chunks + sum(PART_GROUPS[:group])

            @pl.when((chunk >= first) & (chunk < first + size))
            def _(group=group):
                for copy in part_stores(group, chunk):
                    copy.wait()

    token_half = grad_b.shape[0] // 2

    def backward(part, chunk):
        slot = chunk % 2
        sub = chunk % chunks_per_mat
        mat = chunk // chunks_per_mat
        layer = num_layers - 1 - mat // 2

        @pl.when(mat % 2 == 0)
        def _():
            cols = slice(part * TILE, (part + 1) * TILE)

            @pl.loop(0, 2)
            def _(which):
                rows = pl.ds(pl.multiple_of(which * token_half, 128), token_half)
                grad_act = lax.dot_general(
                    grad_b[rows, :], weight_buf[slot, cols, :], FEATURE_DIMS, preferred_element_type=jnp.float32)
                grad_pre = grad_act * gelu_slope(pre_buf[slot, rows, cols].astype(jnp.float32))
                grad_pre_buf[rows, cols] = grad_pre.astype(jnp.bfloat16)
                start = row_dim + sub * chunk_cols + part * TILE
                small_out[pl.ds(layer, 1), pl.ds(pl.multiple_of(start, 128), TILE)] += jnp.sum(grad_pre, axis=0, keepdims=True)

            if part == chunk_cols // TILE - 1:
                grad_pre_store(sub).start()

        @pl.when(mat % 2 == 1)
        def _():
            pieces = row_dim // chunk_cols * (chunk_cols // TILE) // 3
            grad_rows = []
            for piece in range(part * pieces, (part + 1) * pieces):
                start, first = divmod(piece * TILE, chunk_cols)
                grad_rows.append((piece, lax.dot_general(
                    cols_buf[slot], weight_buf[slot, first:first + TILE, start * chunk_cols:(start + 1) * chunk_cols],
                    FEATURE_DIMS, preferred_element_type=jnp.float32)))
            for piece, value in grad_rows:
                grad_normed[:, piece * TILE:(piece + 1) * TILE] += value

    def norm_loads(layer, block):
        rows = pl.ds(pl.multiple_of(block * NORM_ROWS, NORM_ROWS), NORM_ROWS)
        slot = block % 2
        copies = [pltpu.make_async_copy(hid_refs[layer].at[rows, :], hid_buf.at[slot], norm_sem.at[0, slot])]
        if layer > 0:
            copies.append(pltpu.make_async_copy(grad_top.at[rows, :], grad_buf.at[slot], norm_sem.at[1, slot]))
        return copies

    def layer_input_grad(layer):
        num_blocks = grad_b.shape[0] // NORM_ROWS
        for copy in norm_loads(layer, 0):
            copy.start()

        @pl.loop(0, num_blocks)
        def _(block):
            @pl.when(block + 1 < num_blocks)
            def _():
                for copy in norm_loads(layer, block + 1):
                    copy.start()

            for copy in norm_loads(layer, block):
                copy.wait()
            rows = pl.ds(pl.multiple_of(block * NORM_ROWS, NORM_ROWS), NORM_ROWS)
            hid_f = hid_buf[block % 2].astype(jnp.float32)
            hid_scale = inverse_rms(hid_f)
            hid_hat = hid_f * hid_scale
            normed_grad = grad_normed[rows, :]
            small_out[layer:layer + 1, :row_dim] += jnp.sum(normed_grad * hid_hat, axis=0, keepdims=True)
            if layer > 0:
                grad_normed[rows, :] = jnp.zeros((NORM_ROWS, row_dim), jnp.float32)
                grad_hat = normed_grad * gain_in[layer:layer + 1, :].astype(jnp.float32)
                grad_new = grad_buf[block % 2] + hid_scale * (
                    grad_hat - hid_hat * jnp.mean(grad_hat * hid_hat, axis=-1, keepdims=True))
                grad_b[rows, :] = grad_new.astype(jnp.bfloat16)
                small_out[layer - 1:layer, row_dim + hidden_dim:] += jnp.sum(grad_new, axis=0, keepdims=True)

        if layer > 0:
            copy = pltpu.make_async_copy(grad_b, grad_b_hbm, grad_b_sem)
            copy.start()
            copy.wait()
            following = jnp.int32((num_layers - layer) * 2 * chunks_per_mat)
            cols_load((num_layers - layer) * 2, following).start()

    def input_grad(chunk):
        for layer in range(num_layers):
            last = (num_layers - 1 - layer) * 2 * chunks_per_mat + 2 * chunks_per_mat - 1

            @pl.when(chunk == last)
            def _(layer=layer):
                layer_input_grad(layer)

    events = dict(
        load=load, load_weights=load_weights, compute_sent=compute_sent, share_core=share_core, compute_kept=compute_kept, send_1=send_1, send_2=send_2, send_3=send_3,
        send_back_3=send_back_3, send_back_2=send_back_2, send_back_1=send_back_1, send_back_core=send_back_core, store=store,
        backward_0=functools.partial(backward, 0), backward_1=functools.partial(backward, 1),
        backward_2=functools.partial(backward, 2), input_grad=input_grad)

    cols_buf[0] = grad_b[:, :chunk_cols]
    pl.semaphore_wait(barrier, 4)

    @pl.loop(0, num_chunks + MAX_LAG)
    def _(it):
        for step in range(4):
            @pl.when(it == num_chunks + step)
            def _(step=step):
                small_copy(step).start()
        for name, lag in PIPELINE:
            chunk = it - lag

            @pl.when((chunk >= 0) & (chunk < num_chunks))
            def _(name=name, chunk=chunk):
                events[name](chunk)
        for step in range(4):
            @pl.when(it == num_chunks + step)
            def _(step=step):
                small_copy(step).wait()
                small_out[...] += small_recv[step]


def run_stack(tokens, upstream, norm_gain, w_up, bias_up, w_down, bias_down, axis, chunk_cols, tile_cols):
    num_layers, row_dim, hidden = w_up.shape
    num_tokens = tokens.shape[0]
    chunks_per_mat = hidden // chunk_cols
    region = row_dim // (2 * COLORS)
    half = (COLORS, region, chunk_cols)
    sizes = (num_layers, chunks_per_mat, row_dim, chunk_cols, region, row_dim // chunk_cols, tile_cols, axis)
    full_chunks = 2 * num_layers * chunks_per_mat - sum(PART_GROUPS)
    bf16, f32 = jnp.bfloat16, jnp.float32
    dma = pltpu.SemaphoreType.DMA
    any_spec = pl.BlockSpec(memory_space=pl.ANY)
    vmem_spec = pl.BlockSpec(memory_space=pltpu.VMEM)
    shape = jax.ShapeDtypeStruct
    rows, wide, small = (num_tokens, row_dim), (num_layers, num_tokens, hidden), (num_layers, 2 * row_dim + hidden)
    part_shapes = [shape((size, region // 2, chunk_cols), bf16) for size in PART_GROUPS for _ in range(2 * COLORS)]
    gathered, small_sum, *rest = pl.pallas_call(
        functools.partial(stack_kernel, sizes),
        out_shape=[
            shape((full_chunks, 2) + half, bf16), shape(small, f32), shape((chunks_per_mat, num_tokens, chunk_cols), bf16),
            shape(rows, bf16), shape(rows, bf16), shape((num_layers,) + rows, bf16), shape(wide, bf16), shape(wide, bf16),
            shape(rows, f32),
        ] + part_shapes,
        in_specs=[any_spec] * 4 + [vmem_spec] * 3,
        out_specs=[any_spec, vmem_spec] + [any_spec] * (7 + len(part_shapes)),
        scratch_shapes=[
            pltpu.VMEM(rows, bf16),
            pltpu.VMEM(rows, bf16),
            pltpu.VMEM(rows, f32),
            pltpu.VMEM((RECV_SLOTS,) + half, bf16),
            pltpu.VMEM((RECV_SLOTS, COLORS, region // 2, chunk_cols), bf16),
            pltpu.VMEM((RECV_SLOTS, COLORS, region // 4, chunk_cols), bf16),
            pltpu.VMEM((RECV_SLOTS, COLORS, region // 8, chunk_cols), bf16),
            pltpu.VMEM((GATHER_SLOTS, 2) + half, bf16),
            pltpu.VMEM((4,) + small, f32),
            dma((4,)), dma, dma, dma((2,)), dma((2,)),
            dma((4, 2)), dma, dma((2, 2)), dma,
            dma, dma((RECV_SLOTS,)), dma((3, COLORS)), dma((3, COLORS, RECV_SLOTS)),
            dma((3, COLORS, GATHER_SLOTS)), dma((3, COLORS, GATHER_SLOTS)), dma((GATHER_SLOTS,)), dma((GATHER_SLOTS,)),
            dma((GATHER_SLOTS,)), dma((4,)), dma((4,)), dma((COLORS, 2, GATHER_SLOTS)),
        ],
        compiler_params=pltpu.CompilerParams(collective_id=0, has_side_effects=True, vmem_limit_bytes=67043328),
        name="stack",
    )(tokens, upstream, w_up, w_down, norm_gain, bias_up, bias_down)
    return gathered, small_sum, rest[7:]


def flip_pairs(num_devices, bit):
    return [(dev, dev ^ (1 << bit)) for dev in range(num_devices)]


def stream_blocks(num_blocks, start_loads, wait_loads, store_of, in_buf, out_buf, after_first=None):
    slots, region = in_buf.shape[0], in_buf.shape[2]
    for block in range(min(slots - 1, num_blocks)):
        start_loads(jnp.int32(block), block)

    @pl.loop(0, num_blocks)
    def _(block):
        slot = block % slots

        @pl.when(block + slots - 1 < num_blocks)
        def _():
            start_loads(block + slots - 1, (block + slots - 1) % slots)

        wait_loads(block, slot)

        @pl.when(block >= slots)
        def _():
            store_of(block - slots, slot).wait()

        for color in range(COLORS):
            out_buf[slot, color * region:(color + 1) * region, :] = in_buf[slot, color].astype(jnp.float32)
        store_of(block, slot).start()
        if after_first is not None:
            pl.when(block == 0)(after_first)

    for block in range(max(num_blocks - slots, 0), num_blocks):
        store_of(jnp.int32(block), block % slots).wait()


def block_target(out_ref, layer, kind, down_subs, chunk, which_core, rows, cols):
    half = pl.multiple_of(which_core * rows, rows)
    if kind == 0:
        first = pl.multiple_of((chunk // down_subs) * 2 * rows + half, rows)
        return out_ref.at[layer, pl.ds(first, rows), pl.ds(pl.multiple_of((chunk % down_subs) * cols, 128), cols)]
    return out_ref.at[layer, pl.ds(half, rows), pl.ds(pl.multiple_of(chunk * cols, 128), cols)]


def widen_kernel(spec, *refs):
    first, count, place, layer, kind, down_subs, small_widths, in_place = spec
    if in_place:
        refs = refs[:1 + bool(small_widths)] + refs[2 + bool(small_widths):]
    if small_widths:
        gathered, small, out_ref, *small_outs, in_buf, out_buf, in_sem, out_sem, small_buf, small_sem = refs
        small_load = pltpu.make_async_copy(small, small_buf, small_sem.at[0])
        small_load.start()
        starts = [sum(small_widths[:n]) for n in range(len(small_widths))]
        small_stores = [
            pltpu.make_async_copy(small_buf.at[:, start:start + width], small_out, small_sem.at[1 + n])
            for n, (start, width, small_out) in enumerate(zip(starts, small_widths, small_outs))]
    else:
        gathered, out_ref, in_buf, out_buf, in_sem, out_sem = refs
        small_stores = []

    def after_first():
        if small_stores:
            small_load.wait()
        for copy in small_stores:
            copy.start()

    rows, cols = out_buf.shape[1:]

    def load(block, slot):
        return pltpu.make_async_copy(gathered.at[first + block // 2, block % 2], in_buf.at[slot], in_sem.at[slot])

    def store(block, slot):
        target = block_target(out_ref, layer, kind, down_subs, place + block // 2, block % 2, rows, cols)
        return pltpu.make_async_copy(out_buf.at[slot], target, out_sem.at[slot])

    stream_blocks(
        2 * count, lambda block, slot: load(block, slot).start(), lambda block, slot: load(block, slot).wait(),
        store, in_buf, out_buf, after_first)
    for copy in small_stores:
        copy.wait()


def join_kernel(spec, *refs):
    skip, count, place, layer, kind, down_subs, axis = spec
    parts, (_, out_ref, in_buf, out_buf, in_sem, out_sem) = refs[:4 * COLORS], refs[4 * COLORS:]
    rows, cols = out_buf.shape[1:]
    part_rows = in_buf.shape[2] // 2
    me = lax.axis_index(axis)
    core = me % 2

    def copies(which, chunk, slot):
        found = []
        for color in range(COLORS):
            upper = (me >> COLOR_DIMS[color][0]) & 1
            for far in range(2):
                start = pl.multiple_of((upper if far == 0 else 1 - upper) * part_rows, part_rows)
                found.append(pltpu.make_async_copy(
                    parts[color * 4 + far * 2 + which].at[skip + chunk],
                    in_buf.at[slot, color, pl.ds(start, part_rows), :], in_sem.at[slot]))
        return found

    def start_loads(block, slot):
        for which in range(2):
            @pl.when(block % 2 == which)
            def _(which=which):
                for copy in copies(which, block // 2, slot):
                    copy.start()

    def wait_loads(block, slot):
        for copy in copies(0, block // 2, slot):
            copy.wait()

    def store(block, slot):
        which_core = jnp.where(block % 2 == 0, core, 1 - core)
        target = block_target(out_ref, layer, kind, down_subs, place + block // 2, which_core, rows, cols)
        return pltpu.make_async_copy(out_buf.at[slot], target, out_sem.at[slot])

    stream_blocks(2 * count, start_loads, wait_loads, store, in_buf, out_buf)


def widen_scratch(region, cols):
    return [
        pltpu.VMEM((STREAM_SLOTS, COLORS, region, cols), jnp.bfloat16),
        pltpu.VMEM((STREAM_SLOTS, COLORS * region, cols), jnp.float32),
        pltpu.SemaphoreType.DMA((STREAM_SLOTS,)),
        pltpu.SemaphoreType.DMA((STREAM_SLOTS,)),
    ]


def widen_cost(count, region, cols):
    size = count * 2 * COLORS * region * cols
    return pl.CostEstimate(flops=500 * size, bytes_accessed=6 * size, transcendentals=0)


def widen(gathered, first, count, place, layer, kind, shape, into, down_subs, small, small_widths):
    region, cols = gathered.shape[3:]
    any_spec = pl.BlockSpec(memory_space=pl.ANY)
    smalls = [jax.ShapeDtypeStruct((small.shape[0], width), jnp.float32) for width in small_widths]
    small_scratch = [pltpu.VMEM(small.shape, jnp.float32), pltpu.SemaphoreType.DMA((1 + len(smalls),))] if smalls else []
    return pl.pallas_call(
        functools.partial(widen_kernel, (first, count, place, layer, kind, down_subs, small_widths, into is not None)),
        in_specs=[any_spec] * (1 + bool(smalls) + (into is not None)),
        out_specs=[any_spec] * (1 + len(smalls)),
        out_shape=[jax.ShapeDtypeStruct(shape, jnp.float32)] + smalls,
        input_output_aliases={} if into is None else {1 + bool(smalls): 0},
        scratch_shapes=widen_scratch(region, cols) + small_scratch,
        cost_estimate=widen_cost(count, region, cols),
        compiler_params=pltpu.CompilerParams(vmem_limit_bytes=67043328),
    )(gathered, *([small] if smalls else []), *([] if into is None else [into]))


def split_at_gradients(first, count, per_mat):
    sizes = []
    while count:
        sizes.append(min(count, per_mat - first % per_mat))
        first, count = first + sizes[-1], count - sizes[-1]
    return sizes


def join(parts, skip, count, place, layer, kind, into, down_subs, axis):
    _, part_rows, cols = parts[0].shape
    any_spec = pl.BlockSpec(memory_space=pl.ANY)
    return pl.pallas_call(
        functools.partial(join_kernel, (skip, count, place, layer, kind, down_subs, axis)),
        in_specs=[any_spec] * (len(parts) + 1),
        out_specs=any_spec,
        out_shape=jax.ShapeDtypeStruct(into.shape, jnp.float32),
        scratch_shapes=widen_scratch(2 * part_rows, cols),
        input_output_aliases={len(parts): 0},
        cost_estimate=widen_cost(count, 2 * part_rows, cols),
        compiler_params=pltpu.CompilerParams(vmem_limit_bytes=67043328),
    )(*parts, into)


def swap(array, axis, num_devices, bit):
    return lax.ppermute(array, axis, flip_pairs(num_devices, bit))


def full_gradients(gathered, parts, small, num_layers, row_dim, hidden, chunk_cols, axis, num_devices):
    per_mat = hidden // chunk_cols
    down_subs = row_dim // chunk_cols
    groups = range(len(PART_GROUPS))
    mine = [[parts[(group * COLORS + color) * 2] for color in range(COLORS)] for group in groups]
    theirs = [[parts[(group * COLORS + color) * 2 + 1] for color in range(COLORS)] for group in groups]
    far = [[swap(mine[group][color], axis, num_devices, COLOR_DIMS[color][0])
            for color in range(COLORS)] for group in groups]
    last = num_layers - 1
    full = [None, None]
    shapes = ((num_layers, hidden, row_dim), (num_layers, row_dim, hidden))
    for call, count in enumerate(WIDEN_CALLS):
        first = sum(WIDEN_CALLS[:call])
        kind, place = divmod(first, per_mat)
        small_widths = (row_dim, hidden, row_dim) if call == 0 else ()
        full[kind], *rest = widen(
            gathered, first, count, place, last, kind, shapes[kind], full[kind], down_subs, small, small_widths)
        smalls = rest or smalls
    chunk = 2 * num_layers * per_mat - sum(PART_GROUPS)
    for group in groups:
        pieces = []
        for color in range(COLORS):
            shared = swap(far[group][color], axis, num_devices, CORE)
            pieces += [mine[group][color], theirs[group][color], far[group][color], shared]
        skip = 0
        for count in split_at_gradients(chunk, PART_GROUPS[group], per_mat):
            mat, place = divmod(chunk, per_mat)
            kind, layer = mat % 2, last - mat // 2
            full[kind] = join(pieces, skip, count, place, layer, kind, full[kind], down_subs, axis)
            chunk, skip = chunk + count, skip + count
    return smalls[0], full[1], smalls[1], full[0], smalls[2]


def solution(mesh):
    axis = mesh.axis_names[0]

    def device_grads(tokens, upstream, norm_gain, w_up, bias_up, w_down, bias_down):
        num_layers, width = norm_gain.shape
        hidden_width = w_up.shape[2]
        chunk_cols = width // 2
        gathered, small, parts = run_stack(
            tokens, upstream, norm_gain, w_up, bias_up, w_down, bias_down, axis, chunk_cols, width)
        return full_gradients(gathered, parts, small, num_layers, width, hidden_width, chunk_cols, axis, mesh.size)

    row_spec = P(axis, None)
    full_spec = P()
    return jax.shard_map(
        device_grads,
        mesh=mesh,
        in_specs=(row_spec, row_spec, full_spec, full_spec, full_spec, full_spec, full_spec),
        out_specs=(full_spec, full_spec, full_spec, full_spec, full_spec),
        check_vma=False,
    )
```

```python
import functools

import jax
import jax.numpy as jnp
from jax import lax
from jax.experimental import pallas as pl
from jax.experimental.pallas import tpu as pltpu
from jax.sharding import PartitionSpec as P


EPSILON = 1e-6
FEATURE_DIMS = (((1,), (1,)), ((), ()))
MESH = pl.DeviceIdType.MESH
COLORS = 3
CORE, DIM_X, DIM_Y, DIM_Z = range(4)
COLOR_DIMS = ((DIM_X, DIM_Y, DIM_Z), (DIM_Y, DIM_Z, DIM_X), (DIM_Z, DIM_X, DIM_Y))
PIPELINE = (
    ("load", 0), ("compute_sent", 0), ("share_core", 0), ("send_3", 2), ("send_back_2", 4), ("send_back_1", 5),
    ("compute_kept", 0), ("send_back_core", 6), ("load_weights", 0), ("backward_0", 0), ("send_2", 1), ("backward_1", 0),
    ("send_1", 0), ("backward_2", 0), ("send_back_3", 2), ("store", 6), ("input_grad", 0),
)
MAX_LAG = 6
PART_GROUPS = (7, 5, 2, 3, 3)
WIDEN_CALLS = (8, 4)
RECV_SLOTS = 2
KEPT_SLOTS = 3
GATHER_SLOTS = 6
TILE = 256
UP_COLS = 512
ACT_ROWS = 16
ACT_COLS = 256
STREAM_SLOTS = 4
NORM_ROWS = 128
GELU_SCALE = 0.7978845608028654
GELU_CUBIC = 0.044715


def inverse_rms(hid_f):
    return lax.rsqrt(jnp.mean(hid_f * hid_f, axis=-1, keepdims=True) + EPSILON)


def gelu(values):
    return (0.5 * values) * (1.0 + jnp.tanh(values * (GELU_SCALE + GELU_SCALE * GELU_CUBIC * (values * values))))


def forward_kernel(
    sizes, tokens, upstream, w_up, w_down, gain_in, bias_up_in, bias_down_in, hid_out, normed_out, pre_act_out, act_out,
    grad_top_out, grad_top_b_out, small_out, hid, normed, branch, up_buf, down_buf, pre_buf, act_buf, up_rows, grad_b_buf,
    gain, bias_up, bias_down, io_sem, up_sem, down_sem, pre_sem, act_sem,
):
    num_layers, num_tiles, tile_cols = sizes
    num_tokens, row_dim = hid.shape
    steps = num_tiles + 1
    parts = tile_cols // UP_COLS

    def up_load(layer, tile):
        cols = pl.ds(pl.multiple_of(tile * tile_cols, 128), tile_cols)
        return pltpu.make_async_copy(w_up.at[layer, :, cols], up_buf.at[tile % 2], up_sem.at[tile % 2])

    def down_load(layer, tile):
        rows = pl.ds(pl.multiple_of(tile * tile_cols, 128), tile_cols)
        return pltpu.make_async_copy(w_down.at[layer, rows, :], down_buf.at[tile % 2], down_sem.at[tile % 2])

    def pre_store(layer, tile):
        cols = pl.ds(pl.multiple_of(tile * tile_cols, 128), tile_cols)
        return pltpu.make_async_copy(pre_buf.at[tile % 2], pre_act_out.at[layer, :, cols], pre_sem.at[tile % 2])

    def act_store(layer, tile):
        cols = pl.ds(pl.multiple_of(tile * tile_cols, 128), tile_cols)
        return pltpu.make_async_copy(act_buf.at[tile % 2], act_out.at[layer, :, cols], act_sem.at[tile % 2])

    def normed_store(layer):
        return pltpu.make_async_copy(normed, normed_out.at[layer], io_sem.at[1])

    def hid_store():
        return pltpu.make_async_copy(hid, hid_out, io_sem.at[2])

    tokens_load = pltpu.make_async_copy(tokens, hid, io_sem.at[0])
    tokens_load.start()
    up_load(0, 0).start()
    upstream_load = pltpu.make_async_copy(upstream, up_rows, io_sem.at[3])
    small_out[...] = jnp.zeros_like(small_out)
    branch[...] = jnp.zeros_like(branch)
    pre_buf[0, :, :UP_COLS] = jnp.zeros((num_tokens, UP_COLS), jnp.bfloat16)
    gain[...] = gain_in[...].astype(jnp.float32)
    bias_up[...] = bias_up_in[...].astype(jnp.float32)
    bias_down[...] = bias_down_in[...].astype(jnp.float32)
    tokens_load.wait()

    def each_block(action):
        @pl.loop(0, num_tokens // NORM_ROWS)
        def _(block):
            action(pl.ds(pl.multiple_of(block * NORM_ROWS, NORM_ROWS), NORM_ROWS))

    def normalize(layer, rows, hid_f):
        normed[rows, :] = ((hid_f * inverse_rms(hid_f)) * gain[pl.ds(layer, 1), :]).astype(jnp.bfloat16)

    def next_rows(layer, rows):
        new = ((hid[rows, :].astype(jnp.float32) + branch[rows, :]) + bias_down[pl.ds(layer, 1), :]).astype(jnp.bfloat16)
        hid[rows, :] = new
        return new.astype(jnp.float32)

    def activate(slot, part):
        start = part * UP_COLS
        for row in range(0, num_tokens, ACT_ROWS):
            for col in range(0, UP_COLS, ACT_COLS):
                piece = (slot, pl.ds(row, ACT_ROWS), pl.ds(pl.multiple_of(start + col, 128), ACT_COLS))
                act_buf[piece] = gelu(pre_buf[piece].astype(jnp.float32)).astype(jnp.bfloat16)

    def up_product(layer, tile):
        @pl.loop(0, parts)
        def _(part):
            fresh = tile * parts + part == 0
            last_slot = jnp.where((part == 0) & (tile > 0), (tile + 1) % 2, tile % 2)
            activate(last_slot, jnp.where(fresh, 0, (part + parts - 1) % parts))
            cols = pl.ds(pl.multiple_of(part * UP_COLS, 128), UP_COLS)
            bias = bias_up[pl.ds(layer, 1), pl.ds(pl.multiple_of(tile * tile_cols + part * UP_COLS, 128), UP_COLS)]
            pre_buf[tile % 2, :, cols] = (
                jnp.dot(normed[...], up_buf[tile % 2, :, cols], preferred_element_type=jnp.float32) + bias
            ).astype(jnp.bfloat16)

    def down_product(tile):
        slot = tile % 2
        for part in range(row_dim // UP_COLS):
            cols = slice(part * UP_COLS, (part + 1) * UP_COLS)
            branch[:, cols] += jnp.dot(act_buf[slot], down_buf[slot, :, cols], preferred_element_type=jnp.float32)

    each_block(lambda rows: normalize(0, rows, hid[rows, :].astype(jnp.float32)))

    @pl.loop(0, num_layers * steps)
    def _(step):
        layer, tile = step // steps, step % steps

        @pl.when(tile < num_tiles)
        def _():
            up_load(layer, tile).wait()

            @pl.when(tile + 1 < num_tiles)
            def _():
                up_load(layer, tile + 1).start()

            @pl.when((tile == num_tiles - 1) & (layer + 1 < num_layers))
            def _():
                up_load(layer + 1, 0).start()

            @pl.when(step == 0)
            def _():
                normed_store(0).start()
                down_load(0, 0).start()
                upstream_load.start()

            @pl.when(tile > 1)
            def _():
                pre_store(layer, tile - 2).wait()
                act_store(layer, tile - 2).wait()

            up_product(layer, tile)
            pre_store(layer, tile).start()

        @pl.when(tile == num_tiles)
        def _():
            activate((num_tiles - 1) % 2, parts - 1)

        @pl.when(tile > 0)
        def _():
            act_store(layer, tile - 1).start()
            down_load(layer, tile - 1).wait()

            @pl.when(tile < num_tiles)
            def _():
                down_load(layer, tile).start()

            @pl.when((tile == num_tiles) & (layer + 1 < num_layers))
            def _():
                down_load(layer + 1, 0).start()

            down_product(tile - 1)

        @pl.when(tile == num_tiles)
        def _():
            for back in (2, 1):
                pre_store(layer, num_tiles - back).wait()
                act_store(layer, num_tiles - back).wait()
            normed_store(layer).wait()

            @pl.when(layer + 1 < num_layers)
            def _():
                def to_next(rows):
                    normalize(layer + 1, rows, next_rows(layer, rows))
                    branch[rows, :] = jnp.zeros((NORM_ROWS, row_dim), jnp.float32)

                each_block(to_next)
                hid_store().start()
                normed_store(layer + 1).start()

    hid_store().wait()
    upstream_load.wait()
    bias_start = small_out.shape[1] - row_dim

    def grad_stores(rows):
        return (
            pltpu.make_async_copy(branch.at[rows, :], grad_top_out.at[rows, :], io_sem.at[0]),
            pltpu.make_async_copy(grad_b_buf.at[rows, :], grad_top_b_out.at[rows, :], io_sem.at[1]),
        )

    def top_rows(rows):
        top_f = next_rows(num_layers - 1, rows)
        top_scale = inverse_rms(top_f)
        top_hat = top_f * top_scale
        up_f = up_rows[rows, :].astype(jnp.float32)
        grad = top_scale * (up_f - top_hat * jnp.mean(up_f * top_hat, axis=-1, keepdims=True))
        branch[rows, :] = grad
        grad_b_buf[rows, :] = grad.astype(jnp.bfloat16)
        small_out[num_layers - 1:, bias_start:] += jnp.sum(grad, axis=0, keepdims=True)

    num_blocks = num_tokens // NORM_ROWS

    def store_block(block):
        for copy in grad_stores(pl.ds(pl.multiple_of(block * NORM_ROWS, NORM_ROWS), NORM_ROWS)):
            copy.start()

    @pl.loop(0, num_blocks)
    def _(block):
        top_rows(pl.ds(pl.multiple_of(block * NORM_ROWS, NORM_ROWS), NORM_ROWS))
        pl.when(block > 0)(lambda: store_block(block - 1))

    store_block(num_blocks - 1)
    for copy in grad_stores(pl.ds(0, num_tokens)):
        copy.wait()


def forward_pass(tokens, upstream, norm_gain, w_up, bias_up, w_down, bias_down, tile_cols):
    num_tokens, row_dim = tokens.shape
    num_layers, _, hidden = w_up.shape
    bf16, f32 = jnp.bfloat16, jnp.float32
    dma = pltpu.SemaphoreType.DMA
    any_spec = pl.BlockSpec(memory_space=pl.ANY)
    vmem_spec = pl.BlockSpec(memory_space=pltpu.VMEM)
    rows = (num_tokens, row_dim)
    wide = (num_layers, num_tokens, hidden)
    return pl.pallas_call(
        functools.partial(forward_kernel, (num_layers, hidden // tile_cols, tile_cols)),
        out_shape=(
            jax.ShapeDtypeStruct(rows, bf16),
            jax.ShapeDtypeStruct((num_layers,) + rows, bf16),
            jax.ShapeDtypeStruct(wide, bf16),
            jax.ShapeDtypeStruct(wide, bf16),
            jax.ShapeDtypeStruct(rows, f32),
            jax.ShapeDtypeStruct(rows, bf16),
            jax.ShapeDtypeStruct((num_layers, 2 * row_dim + hidden), f32),
        ),
        in_specs=[any_spec] * 4 + [vmem_spec] * 3,
        out_specs=(any_spec,) * 6 + (vmem_spec,),
        scratch_shapes=[
            pltpu.VMEM(rows, bf16),
            pltpu.VMEM(rows, bf16),
            pltpu.VMEM(rows, f32),
            pltpu.VMEM((2, row_dim, tile_cols), bf16),
            pltpu.VMEM((2, tile_cols, row_dim), bf16),
            pltpu.VMEM((2, num_tokens, tile_cols), bf16),
            pltpu.VMEM((2, num_tokens, tile_cols), bf16),
            pltpu.VMEM(rows, bf16),
            pltpu.VMEM(rows, bf16),
            pltpu.VMEM((num_layers, row_dim), f32),
            pltpu.VMEM((num_layers, hidden), f32),
            pltpu.VMEM((num_layers, row_dim), f32),
            dma((4,)), dma((2,)), dma((2,)), dma((2,)), dma((2,)),
        ],
        compiler_params=pltpu.CompilerParams(vmem_limit_bytes=60 * 2**20),
        name="forward",
    )(tokens, upstream, w_up, w_down, norm_gain, bias_up, bias_down)


def gelu_slope(values):
    square = values * values
    bend = jnp.tanh(values * (GELU_SCALE + GELU_SCALE * GELU_CUBIC * square))
    return 0.5 * (1.0 + bend) + (0.5 * values) * (1.0 - bend * bend) * (GELU_SCALE + 3.0 * GELU_SCALE * GELU_CUBIC * square)


def backward_kernel(sizes, *refs):
    num_layers, chunks_per_mat, row_dim, chunk_cols, region, down_subs, axis = sizes
    num_mats = 2 * num_layers
    hidden_dim = chunks_per_mat * chunk_cols
    hid_refs, refs = refs[:num_layers], refs[num_layers:]
    (normed, pre_act, activated, grad_top, grad_top_b, w_up, w_down, gain_in, small_in,
     gathered, small_out, grad_pre_hbm, grad_b_hbm) = refs[:13]
    part_count = 2 * COLORS * len(PART_GROUPS)
    part_refs, refs = refs[13:13 + part_count], refs[13 + part_count:]
    (rows_buf, turned, cols_buf, sent_core, kept, recv_core, sent_1, sent_2, sent_3, recv_1, recv_2, recv_3, ring,
     weight_buf, pre_buf, grad_pre_buf, grad_b, grad_normed, hid_buf, grad_buf,
     small_recv, load_sem, grad_pre_sem, norm_sem, grad_b_sem, core_send, core_recv, out_send, out_recv, back_send, back_recv,
     share_send, share_recv, store_sem, small_send_sem, small_recv_sem, part_sem) = refs
    num_chunks = num_mats * chunks_per_mat
    full_chunks = num_chunks - sum(PART_GROUPS)
    half = COLORS * region
    me = lax.axis_index(axis)
    bits = [me % 2, (me // 2) % 2, (me // 4) % 2, me // 8]
    partners = [me + (1 << d) - 2 * (1 << d) * bits[d] for d in range(4)]
    core = bits[CORE]
    sent_bufs, recv_bufs = (sent_1, sent_2, sent_3), (recv_1, recv_2, recv_3)
    spans = (region // 2, region // 4, region // 8)

    def base(color, level):
        total = 0
        for step in range(level):
            total = total + bits[COLOR_DIMS[color][step]] * spans[step]
        return total

    def other(color, level):
        return base(color, level) + (1 - bits[COLOR_DIMS[color][level]]) * spans[level]

    def rows_at(start, size):
        return pl.ds(pl.multiple_of(start, spans[2]), size)

    def rows_load(mat, chunk):
        layer = num_layers - 1 - mat // 2
        if mat % 2 == 0:
            start = ((chunk % chunks_per_mat) // down_subs) * row_dim
            source = activated.at[layer, :, pl.ds(pl.multiple_of(start, 128), row_dim)]
        else:
            source = normed.at[layer]
        return pltpu.make_async_copy(source, rows_buf, load_sem.at[0, 0])

    def weight_loads(mat, chunk):
        slot = chunk % 2
        layer = num_layers - 1 - mat // 2
        cols = pl.ds(pl.multiple_of((chunk % chunks_per_mat) * chunk_cols, 128), chunk_cols)
        if mat % 2 == 0:
            return [
                pltpu.make_async_copy(w_down.at[layer, cols, :], weight_buf.at[slot], load_sem.at[1, slot]),
                pltpu.make_async_copy(pre_act.at[layer, :, cols], pre_buf.at[slot], load_sem.at[2, slot]),
            ]
        return [
            pltpu.make_async_copy(
                w_up.at[layer, part * chunk_cols:(part + 1) * chunk_cols, cols],
                weight_buf.at[slot, :, part * chunk_cols:(part + 1) * chunk_cols], load_sem.at[1 + part, slot])
            for part in range(down_subs)
        ]

    def cols_load(mat, chunk):
        sub = chunk % chunks_per_mat
        if mat % 2 == 0:
            source = grad_top_b if mat == 0 else grad_b_hbm
            source = source.at[:, pl.ds(pl.multiple_of((sub % down_subs) * chunk_cols, 128), chunk_cols)]
        else:
            source = grad_pre_hbm.at[sub]
        return pltpu.make_async_copy(source, cols_buf.at[chunk % 2], load_sem.at[3, chunk % 2])

    def for_mat(chunk, action):
        for mat in range(num_mats):
            @pl.when(chunk // chunks_per_mat == mat)
            def _(mat=mat):
                action(mat)

    def grad_pre_store(sub):
        return pltpu.make_async_copy(grad_pre_buf, grad_pre_hbm.at[sub], grad_pre_sem)

    def core_copy(chunk):
        slot = chunk % RECV_SLOTS
        return pltpu.make_async_remote_copy(
            src_ref=sent_core, dst_ref=recv_core.at[slot], send_sem=core_send, recv_sem=core_recv.at[slot],
            device_id=(partners[CORE],), device_id_type=MESH)

    def out_copy(level, color, chunk):
        slot = chunk % RECV_SLOTS
        return pltpu.make_async_remote_copy(
            src_ref=sent_bufs[level].at[color], dst_ref=recv_bufs[level].at[slot, color],
            send_sem=out_send.at[level, color], recv_sem=out_recv.at[level, color, slot],
            device_id=(partners[COLOR_DIMS[color][level]],), device_id_type=MESH)

    def back_copy(level, color, chunk, arriving):
        slot = chunk % GATHER_SLOTS
        mine = ring.at[slot, core, color, rows_at(base(color, level + 1), spans[level]), :]
        theirs = ring.at[slot, core, color, rows_at(other(color, level), spans[level]), :]
        return pltpu.make_async_remote_copy(
            src_ref=mine, dst_ref=theirs if arriving else mine,
            send_sem=back_send.at[level, color, slot], recv_sem=back_recv.at[level, color, slot],
            device_id=(partners[COLOR_DIMS[color][level]],), device_id_type=MESH)

    def part_rows(color):
        return rows_at(base(color, 1), spans[0])

    def part_share_copy(color, chunk, arriving):
        slot = chunk % GATHER_SLOTS
        mine = ring.at[slot, core, color, part_rows(color), :]
        theirs = ring.at[slot, 1 - core, color, part_rows(color), :]
        return pltpu.make_async_remote_copy(
            src_ref=mine, dst_ref=theirs if arriving else mine,
            send_sem=back_send.at[0, color, slot], recv_sem=back_recv.at[0, color, slot],
            device_id=(partners[CORE],), device_id_type=MESH)

    def part_stores(group, chunk):
        slot = chunk % GATHER_SLOTS
        place = chunk - full_chunks - sum(PART_GROUPS[:group])
        copies = []
        for color in range(COLORS):
            for which in range(2):
                out_ref = part_refs[(group * COLORS + color) * 2 + which]
                source = ring.at[slot, core if which == 0 else 1 - core, color, part_rows(color), :]
                copies.append(pltpu.make_async_copy(
                    source, out_ref.at[place], part_sem.at[color, which, slot]))
        return copies

    def share_copy(chunk, arriving):
        slot = chunk % GATHER_SLOTS
        return pltpu.make_async_remote_copy(
            src_ref=ring.at[slot, core], dst_ref=ring.at[slot, 1 - core if arriving else core],
            send_sem=share_send.at[slot], recv_sem=share_recv.at[slot],
            device_id=(partners[CORE],), device_id_type=MESH)

    def store_copy(chunk):
        slot = chunk % GATHER_SLOTS
        return pltpu.make_async_copy(ring.at[slot], gathered.at[chunk], store_sem.at[slot])

    def small_copy(step):
        return pltpu.make_async_remote_copy(
            src_ref=small_out, dst_ref=small_recv.at[step], send_sem=small_send_sem.at[step],
            recv_sem=small_recv_sem.at[step], device_id=(partners[step],), device_id_type=MESH)

    def product(chunk, which_core):
        rows = pl.ds(pl.multiple_of(which_core * half, 128), half)
        return jnp.dot(turned[rows, :], cols_buf[chunk % 2], preferred_element_type=jnp.float32)

    def opens_layer(chunk):
        return (chunk > 0) & (chunk % (2 * chunks_per_mat) == 0)

    def turn_rows(chunk):
        down = (chunk // chunks_per_mat) % 2 == 0

        @pl.when((chunk % chunks_per_mat == 0) | (down & (chunk % down_subs == 0)))
        def _():
            rows_load(1, chunk).wait()
            for start in range(0, row_dim, TILE):
                turned[start:start + TILE, :] = rows_buf[:, start:start + TILE].T
            for period, here in ((down_subs, down), (chunks_per_mat, jnp.logical_not(down))):
                following = chunk + period

                @pl.when(here & (following < num_chunks))
                def _(following=following):
                    for_mat(following, lambda mat: rows_load(mat, following).start())

    def load(chunk):
        turn_rows(chunk)
        for_mat(chunk, lambda mat: cols_load(mat, chunk).wait())
        after = chunk + 1

        @pl.when(chunk == 0)
        def _():
            grad_b_copy.start()
            for copy in weight_loads(0, chunk):
                copy.start()

        @pl.when((after < num_chunks) & jnp.logical_not(opens_layer(after)))
        def _():
            for_mat(after, lambda mat: cols_load(mat, after).start())

    def load_weights(chunk):
        def arrive(mat):
            for copy in weight_loads(mat, chunk):
                copy.wait()

        for_mat(chunk, arrive)
        after, before = chunk + 1, chunk - 1

        @pl.when(chunk == 0)
        def _():
            grad_b_copy.wait()

        @pl.when(after < num_chunks)
        def _():
            def start(mat):
                for copy in weight_loads(mat, after):
                    copy.start()

            for_mat(after, start)

        @pl.when((before >= 0) & ((before // chunks_per_mat) % 2 == 0))
        def _():
            grad_pre_store(before % chunks_per_mat).wait()

    def compute_sent(chunk):
        value = product(chunk, 1 - core).astype(jnp.bfloat16)
        for color in range(COLORS):
            sent_core[color] = value[color * region:(color + 1) * region]

    def share_core(chunk):
        core_copy(chunk).start()

    def compute_kept(chunk):
        value = product(chunk, core)
        for color in range(COLORS):
            kept[chunk % KEPT_SLOTS, color] = value[color * region:(color + 1) * region]

    def halve(level, chunk, arrived):
        slot = chunk % KEPT_SLOTS
        recv_slot = chunk % RECV_SLOTS
        for color in range(COLORS):
            if level > 0:
                out_copy(level - 1, color, chunk).wait()
            held = base(color, level)

            def total(start, size, color=color, held=held):
                own = kept[slot, color, rows_at(start, size), :]
                return own + arrived[recv_slot, color, rows_at(start - held, size), :].astype(jnp.float32)

            if level < 3:
                mine = base(color, level + 1)
                sent_bufs[level][color] = total(other(color, level), spans[level]).astype(jnp.bfloat16)
                kept[slot, color, rows_at(mine, spans[level]), :] = total(mine, spans[level])
                out_copy(level, color, chunk).start()
            else:
                gather_slot = chunk % GATHER_SLOTS
                ring[gather_slot, core, color, rows_at(held, spans[2]), :] = total(held, spans[2]).astype(jnp.bfloat16)
                back_copy(2, color, chunk, False).start()

    def send_1(chunk):
        core_copy(chunk).wait()
        halve(0, chunk, recv_core)

    def send_2(chunk):
        halve(1, chunk, recv_1)

    def send_3(chunk):
        halve(2, chunk, recv_2)

    def send_back_3(chunk):
        halve(3, chunk, recv_3)

    def pass_back(level, chunk):
        for color in range(COLORS):
            back_copy(level + 1, color, chunk, True).wait()
            back_copy(level, color, chunk, False).start()

    def send_back_2(chunk):
        pass_back(1, chunk)

    def send_back_1(chunk):
        @pl.when(chunk < full_chunks)
        def _():
            pass_back(0, chunk)

        @pl.when(chunk >= full_chunks)
        def _():
            for color in range(COLORS):
                back_copy(1, color, chunk, True).wait()
                part_share_copy(color, chunk, False).start()

    def send_back_core(chunk):
        @pl.when(chunk < full_chunks)
        def _():
            for color in range(COLORS):
                back_copy(0, color, chunk, True).wait()
            share_copy(chunk, False).start()

        @pl.when(chunk >= full_chunks)
        def _():
            for color in range(COLORS):
                part_share_copy(color, chunk, True).wait()

        for group, size in enumerate(PART_GROUPS):
            first = full_chunks + sum(PART_GROUPS[:group])

            @pl.when((chunk >= first) & (chunk < first + size))
            def _(group=group):
                for copy in part_stores(group, chunk):
                    copy.start()

    def store(chunk):
        @pl.when(chunk < full_chunks)
        def _():
            share_copy(chunk, True).wait()
            store_copy(chunk).start()

        @pl.when((chunk > 0) & (chunk <= full_chunks))
        def _():
            store_copy(chunk - 1).wait()

        for group, size in enumerate(PART_GROUPS):
            first = full_chunks + sum(PART_GROUPS[:group])

            @pl.when((chunk >= first) & (chunk < first + size))
            def _(group=group):
                for copy in part_stores(group, chunk):
                    copy.wait()

    token_half = grad_b.shape[0] // 2

    def backward(part, chunk):
        slot = chunk % 2
        sub = chunk % chunks_per_mat
        mat = chunk // chunks_per_mat
        layer = num_layers - 1 - mat // 2

        @pl.when(mat % 2 == 0)
        def _():
            cols = slice(part * TILE, (part + 1) * TILE)

            @pl.loop(0, 2)
            def _(which):
                rows = pl.ds(pl.multiple_of(which * token_half, 128), token_half)
                grad_act = lax.dot_general(
                    grad_b[rows, :], weight_buf[slot, cols, :], FEATURE_DIMS, preferred_element_type=jnp.float32)
                grad_pre = grad_act * gelu_slope(pre_buf[slot, rows, cols].astype(jnp.float32))
                grad_pre_buf[rows, cols] = grad_pre.astype(jnp.bfloat16)
                start = row_dim + sub * chunk_cols + part * TILE
                small_out[pl.ds(layer, 1), pl.ds(pl.multiple_of(start, 128), TILE)] += jnp.sum(grad_pre, axis=0, keepdims=True)

            if part == chunk_cols // TILE - 1:
                grad_pre_store(sub).start()

        @pl.when(mat % 2 == 1)
        def _():
            pieces = row_dim // chunk_cols * (chunk_cols // TILE) // 3
            grad_rows = []
            for piece in range(part * pieces, (part + 1) * pieces):
                start, first = divmod(piece * TILE, chunk_cols)
                grad_rows.append((piece, lax.dot_general(
                    cols_buf[slot], weight_buf[slot, first:first + TILE, start * chunk_cols:(start + 1) * chunk_cols],
                    FEATURE_DIMS, preferred_element_type=jnp.float32)))
            for piece, value in grad_rows:
                grad_normed[:, piece * TILE:(piece + 1) * TILE] += value

    def norm_loads(layer, block):
        rows = pl.ds(pl.multiple_of(block * NORM_ROWS, NORM_ROWS), NORM_ROWS)
        slot = block % 2
        copies = [pltpu.make_async_copy(hid_refs[layer].at[rows, :], hid_buf.at[slot], norm_sem.at[0, slot])]
        if layer > 0:
            copies.append(pltpu.make_async_copy(grad_top.at[rows, :], grad_buf.at[slot], norm_sem.at[1, slot]))
        return copies

    def layer_input_grad(layer):
        num_blocks = grad_b.shape[0] // NORM_ROWS
        for copy in norm_loads(layer, 0):
            copy.start()

        @pl.loop(0, num_blocks)
        def _(block):
            @pl.when(block + 1 < num_blocks)
            def _():
                for copy in norm_loads(layer, block + 1):
                    copy.start()

            for copy in norm_loads(layer, block):
                copy.wait()
            rows = pl.ds(pl.multiple_of(block * NORM_ROWS, NORM_ROWS), NORM_ROWS)
            hid_f = hid_buf[block % 2].astype(jnp.float32)
            hid_scale = inverse_rms(hid_f)
            hid_hat = hid_f * hid_scale
            normed_grad = grad_normed[rows, :]
            small_out[layer:layer + 1, :row_dim] += jnp.sum(normed_grad * hid_hat, axis=0, keepdims=True)
            if layer > 0:
                grad_normed[rows, :] = jnp.zeros((NORM_ROWS, row_dim), jnp.float32)
                grad_hat = normed_grad * gain_in[layer:layer + 1, :].astype(jnp.float32)
                grad_new = grad_buf[block % 2] + hid_scale * (
                    grad_hat - hid_hat * jnp.mean(grad_hat * hid_hat, axis=-1, keepdims=True))
                grad_b[rows, :] = grad_new.astype(jnp.bfloat16)
                small_out[layer - 1:layer, row_dim + hidden_dim:] += jnp.sum(grad_new, axis=0, keepdims=True)

        if layer > 0:
            copy = pltpu.make_async_copy(grad_b, grad_b_hbm, grad_b_sem)
            copy.start()
            copy.wait()
            following = jnp.int32((num_layers - layer) * 2 * chunks_per_mat)
            cols_load((num_layers - layer) * 2, following).start()

    def input_grad(chunk):
        for layer in range(num_layers):
            last = (num_layers - 1 - layer) * 2 * chunks_per_mat + 2 * chunks_per_mat - 1

            @pl.when(chunk == last)
            def _(layer=layer):
                layer_input_grad(layer)

    events = dict(
        load=load, load_weights=load_weights, compute_sent=compute_sent, share_core=share_core, compute_kept=compute_kept, send_1=send_1, send_2=send_2, send_3=send_3,
        send_back_3=send_back_3, send_back_2=send_back_2, send_back_1=send_back_1, send_back_core=send_back_core, store=store,
        backward_0=functools.partial(backward, 0), backward_1=functools.partial(backward, 1),
        backward_2=functools.partial(backward, 2), input_grad=input_grad)

    first = jnp.int32(0)
    rows_load(0, first).start()
    cols_load(0, first).start()
    grad_b_copy = pltpu.make_async_copy(grad_top_b, grad_b, grad_b_sem)
    barrier = pltpu.get_barrier_semaphore()
    for partner in partners:
        pl.semaphore_signal(barrier, inc=1, device_id=(partner,), device_id_type=MESH)
    small_out[...] = small_in[...]
    grad_normed[...] = jnp.zeros_like(grad_normed)
    pl.semaphore_wait(barrier, 4)

    @pl.loop(0, num_chunks + MAX_LAG)
    def _(it):
        for step in range(4):
            @pl.when(it == num_chunks + step)
            def _(step=step):
                small_copy(step).start()
        for name, lag in PIPELINE:
            chunk = it - lag

            @pl.when((chunk >= 0) & (chunk < num_chunks))
            def _(name=name, chunk=chunk):
                events[name](chunk)
        for step in range(4):
            @pl.when(it == num_chunks + step)
            def _(step=step):
                small_copy(step).wait()
                small_out[...] += small_recv[step]


def backward_pass(hid_rows, saved, grad_top, grad_top_b, norm_gain, w_up, w_down, small, axis, chunk_cols):
    num_layers, row_dim, hidden = w_up.shape
    tokens = grad_top.shape[0]
    chunks_per_mat = hidden // chunk_cols
    region = row_dim // (2 * COLORS)
    half = (COLORS, region, chunk_cols)
    sizes = (num_layers, chunks_per_mat, row_dim, chunk_cols, region, row_dim // chunk_cols, axis)
    num_chunks = 2 * num_layers * chunks_per_mat
    bf16, f32 = jnp.bfloat16, jnp.float32
    dma = pltpu.SemaphoreType.DMA
    any_spec = pl.BlockSpec(memory_space=pl.ANY)
    vmem_spec = pl.BlockSpec(memory_space=pltpu.VMEM)
    full_chunks = num_chunks - sum(PART_GROUPS)
    part_shapes = [jax.ShapeDtypeStruct((size, region // 2, chunk_cols), bf16) for size in PART_GROUPS for _ in range(2 * COLORS)]
    gathered, small_sum, _, _, *parts = pl.pallas_call(
        functools.partial(backward_kernel, sizes),
        out_shape=[
            jax.ShapeDtypeStruct((full_chunks, 2) + half, bf16),
            jax.ShapeDtypeStruct(small.shape, f32),
            jax.ShapeDtypeStruct((chunks_per_mat, tokens, chunk_cols), bf16),
            jax.ShapeDtypeStruct((tokens, row_dim), bf16),
        ] + part_shapes,
        in_specs=[any_spec] * (num_layers + 7) + [vmem_spec] * 2,
        out_specs=[any_spec, vmem_spec, any_spec, any_spec] + [any_spec] * len(part_shapes),
        scratch_shapes=[
            pltpu.VMEM((tokens, row_dim), bf16),
            pltpu.VMEM((row_dim, tokens), bf16),
            pltpu.VMEM((2, tokens, chunk_cols), bf16),
            pltpu.VMEM(half, bf16),
            pltpu.VMEM((KEPT_SLOTS,) + half, f32),
            pltpu.VMEM((RECV_SLOTS,) + half, bf16),
            pltpu.VMEM((COLORS, region // 2, chunk_cols), bf16),
            pltpu.VMEM((COLORS, region // 4, chunk_cols), bf16),
            pltpu.VMEM((COLORS, region // 8, chunk_cols), bf16),
            pltpu.VMEM((RECV_SLOTS, COLORS, region // 2, chunk_cols), bf16),
            pltpu.VMEM((RECV_SLOTS, COLORS, region // 4, chunk_cols), bf16),
            pltpu.VMEM((RECV_SLOTS, COLORS, region // 8, chunk_cols), bf16),
            pltpu.VMEM((GATHER_SLOTS, 2) + half, bf16),
            pltpu.VMEM((2, chunk_cols, row_dim), bf16),
            pltpu.VMEM((2, tokens, chunk_cols), bf16),
            pltpu.VMEM((tokens, chunk_cols), bf16),
            pltpu.VMEM((tokens, row_dim), bf16),
            pltpu.VMEM((tokens, row_dim), f32),
            pltpu.VMEM((2, NORM_ROWS, row_dim), bf16),
            pltpu.VMEM((2, NORM_ROWS, row_dim), f32),
            pltpu.VMEM((4,) + small.shape, f32),
            dma((4, 2)), dma, dma((2, 2)), dma,
            dma, dma((RECV_SLOTS,)), dma((3, COLORS)), dma((3, COLORS, RECV_SLOTS)),
            dma((3, COLORS, GATHER_SLOTS)), dma((3, COLORS, GATHER_SLOTS)), dma((GATHER_SLOTS,)), dma((GATHER_SLOTS,)),
            dma((GATHER_SLOTS,)), dma((4,)), dma((4,)), dma((COLORS, 2, GATHER_SLOTS)),
        ],
        compiler_params=pltpu.CompilerParams(collective_id=0, has_side_effects=True, vmem_limit_bytes=67043328),
        name="backward",
    )(*hid_rows, *saved, grad_top, grad_top_b, w_up, w_down, norm_gain, small)
    return gathered, small_sum, parts


def flip_pairs(num_devices, bit):
    return [(dev, dev ^ (1 << bit)) for dev in range(num_devices)]


def stream_blocks(num_blocks, start_loads, wait_loads, store_of, in_buf, out_buf, after_first=None):
    slots, region = in_buf.shape[0], in_buf.shape[2]
    for block in range(min(slots - 1, num_blocks)):
        start_loads(jnp.int32(block), block)

    @pl.loop(0, num_blocks)
    def _(block):
        slot = block % slots

        @pl.when(block + slots - 1 < num_blocks)
        def _():
            start_loads(block + slots - 1, (block + slots - 1) % slots)

        wait_loads(block, slot)

        @pl.when(block >= slots)
        def _():
            store_of(block - slots, slot).wait()

        for color in range(COLORS):
            out_buf[slot, color * region:(color + 1) * region, :] = in_buf[slot, color].astype(jnp.float32)
        store_of(block, slot).start()
        if after_first is not None:
            pl.when(block == 0)(after_first)

    for block in range(max(num_blocks - slots, 0), num_blocks):
        store_of(jnp.int32(block), block % slots).wait()


def block_target(out_ref, layer, kind, down_subs, chunk, which_core, rows, cols):
    half = pl.multiple_of(which_core * rows, rows)
    if kind == 0:
        first = pl.multiple_of((chunk // down_subs) * 2 * rows + half, rows)
        return out_ref.at[layer, pl.ds(first, rows), pl.ds(pl.multiple_of((chunk % down_subs) * cols, 128), cols)]
    return out_ref.at[layer, pl.ds(half, rows), pl.ds(pl.multiple_of(chunk * cols, 128), cols)]


def widen_kernel(spec, *refs):
    first, count, place, layer, kind, down_subs, small_widths, in_place = spec
    if in_place:
        refs = refs[:1 + bool(small_widths)] + refs[2 + bool(small_widths):]
    if small_widths:
        gathered, small, out_ref, *small_outs, in_buf, out_buf, in_sem, out_sem, small_buf, small_sem = refs
        small_load = pltpu.make_async_copy(small, small_buf, small_sem.at[0])
        small_load.start()
        starts = [sum(small_widths[:n]) for n in range(len(small_widths))]
        small_stores = [
            pltpu.make_async_copy(small_buf.at[:, start:start + width], small_out, small_sem.at[1 + n])
            for n, (start, width, small_out) in enumerate(zip(starts, small_widths, small_outs))]
    else:
        gathered, out_ref, in_buf, out_buf, in_sem, out_sem = refs
        small_stores = []

    def after_first():
        if small_stores:
            small_load.wait()
        for copy in small_stores:
            copy.start()

    rows, cols = out_buf.shape[1:]

    def load(block, slot):
        return pltpu.make_async_copy(gathered.at[first + block // 2, block % 2], in_buf.at[slot], in_sem.at[slot])

    def store(block, slot):
        target = block_target(out_ref, layer, kind, down_subs, place + block // 2, block % 2, rows, cols)
        return pltpu.make_async_copy(out_buf.at[slot], target, out_sem.at[slot])

    stream_blocks(
        2 * count, lambda block, slot: load(block, slot).start(), lambda block, slot: load(block, slot).wait(),
        store, in_buf, out_buf, after_first)
    for copy in small_stores:
        copy.wait()


def join_kernel(spec, *refs):
    skip, count, place, layer, kind, down_subs, axis = spec
    parts, (_, out_ref, in_buf, out_buf, in_sem, out_sem) = refs[:4 * COLORS], refs[4 * COLORS:]
    rows, cols = out_buf.shape[1:]
    part_rows = in_buf.shape[2] // 2
    me = lax.axis_index(axis)
    core = me % 2

    def copies(which, chunk, slot):
        found = []
        for color in range(COLORS):
            upper = (me >> COLOR_DIMS[color][0]) & 1
            for far in range(2):
                start = pl.multiple_of((upper if far == 0 else 1 - upper) * part_rows, part_rows)
                found.append(pltpu.make_async_copy(
                    parts[color * 4 + far * 2 + which].at[skip + chunk],
                    in_buf.at[slot, color, pl.ds(start, part_rows), :], in_sem.at[slot]))
        return found

    def start_loads(block, slot):
        for which in range(2):
            @pl.when(block % 2 == which)
            def _(which=which):
                for copy in copies(which, block // 2, slot):
                    copy.start()

    def wait_loads(block, slot):
        for copy in copies(0, block // 2, slot):
            copy.wait()

    def store(block, slot):
        which_core = jnp.where(block % 2 == 0, core, 1 - core)
        target = block_target(out_ref, layer, kind, down_subs, place + block // 2, which_core, rows, cols)
        return pltpu.make_async_copy(out_buf.at[slot], target, out_sem.at[slot])

    stream_blocks(2 * count, start_loads, wait_loads, store, in_buf, out_buf)


def widen_scratch(region, cols):
    return [
        pltpu.VMEM((STREAM_SLOTS, COLORS, region, cols), jnp.bfloat16),
        pltpu.VMEM((STREAM_SLOTS, COLORS * region, cols), jnp.float32),
        pltpu.SemaphoreType.DMA((STREAM_SLOTS,)),
        pltpu.SemaphoreType.DMA((STREAM_SLOTS,)),
    ]


def widen_cost(count, region, cols):
    size = count * 2 * COLORS * region * cols
    return pl.CostEstimate(flops=500 * size, bytes_accessed=6 * size, transcendentals=0)


def widen(gathered, first, count, place, layer, kind, shape, into, down_subs, small, small_widths):
    region, cols = gathered.shape[3:]
    any_spec = pl.BlockSpec(memory_space=pl.ANY)
    smalls = [jax.ShapeDtypeStruct((small.shape[0], width), jnp.float32) for width in small_widths]
    small_scratch = [pltpu.VMEM(small.shape, jnp.float32), pltpu.SemaphoreType.DMA((1 + len(smalls),))] if smalls else []
    return pl.pallas_call(
        functools.partial(widen_kernel, (first, count, place, layer, kind, down_subs, small_widths, into is not None)),
        in_specs=[any_spec] * (1 + bool(smalls) + (into is not None)),
        out_specs=[any_spec] * (1 + len(smalls)),
        out_shape=[jax.ShapeDtypeStruct(shape, jnp.float32)] + smalls,
        input_output_aliases={} if into is None else {1 + bool(smalls): 0},
        scratch_shapes=widen_scratch(region, cols) + small_scratch,
        cost_estimate=widen_cost(count, region, cols),
        compiler_params=pltpu.CompilerParams(vmem_limit_bytes=67043328),
    )(gathered, *([small] if smalls else []), *([] if into is None else [into]))


def split_at_gradients(first, count, per_mat):
    sizes = []
    while count:
        sizes.append(min(count, per_mat - first % per_mat))
        first, count = first + sizes[-1], count - sizes[-1]
    return sizes


def join(parts, skip, count, place, layer, kind, into, down_subs, axis):
    _, part_rows, cols = parts[0].shape
    any_spec = pl.BlockSpec(memory_space=pl.ANY)
    return pl.pallas_call(
        functools.partial(join_kernel, (skip, count, place, layer, kind, down_subs, axis)),
        in_specs=[any_spec] * (len(parts) + 1),
        out_specs=any_spec,
        out_shape=jax.ShapeDtypeStruct(into.shape, jnp.float32),
        scratch_shapes=widen_scratch(2 * part_rows, cols),
        input_output_aliases={len(parts): 0},
        cost_estimate=widen_cost(count, 2 * part_rows, cols),
        compiler_params=pltpu.CompilerParams(vmem_limit_bytes=67043328),
    )(*parts, into)


def swap(array, axis, num_devices, bit):
    return lax.ppermute(array, axis, flip_pairs(num_devices, bit))


def full_gradients(gathered, parts, small, num_layers, row_dim, hidden, chunk_cols, axis, num_devices):
    per_mat = hidden // chunk_cols
    down_subs = row_dim // chunk_cols
    groups = range(len(PART_GROUPS))
    mine = [[parts[(group * COLORS + color) * 2] for color in range(COLORS)] for group in groups]
    theirs = [[parts[(group * COLORS + color) * 2 + 1] for color in range(COLORS)] for group in groups]
    far = [[swap(mine[group][color], axis, num_devices, COLOR_DIMS[color][0])
            for color in range(COLORS)] for group in groups]
    last = num_layers - 1
    full = [None, None]
    shapes = ((num_layers, hidden, row_dim), (num_layers, row_dim, hidden))
    for call, count in enumerate(WIDEN_CALLS):
        first = sum(WIDEN_CALLS[:call])
        kind, place = divmod(first, per_mat)
        small_widths = (row_dim, hidden, row_dim) if call == 0 else ()
        full[kind], *rest = widen(
            gathered, first, count, place, last, kind, shapes[kind], full[kind], down_subs, small, small_widths)
        smalls = rest or smalls
    chunk = 2 * num_layers * per_mat - sum(PART_GROUPS)
    for group in groups:
        pieces = []
        for color in range(COLORS):
            shared = swap(far[group][color], axis, num_devices, CORE)
            pieces += [mine[group][color], theirs[group][color], far[group][color], shared]
        skip = 0
        for count in split_at_gradients(chunk, PART_GROUPS[group], per_mat):
            mat, place = divmod(chunk, per_mat)
            kind, layer = mat % 2, last - mat // 2
            full[kind] = join(pieces, skip, count, place, layer, kind, full[kind], down_subs, axis)
            chunk, skip = chunk + count, skip + count
    return smalls[0], full[1], smalls[1], full[0], smalls[2]


def solution(mesh):
    axis = mesh.axis_names[0]

    def device_grads(tokens, upstream, norm_gain, w_up, bias_up, w_down, bias_down):
        num_layers, width = norm_gain.shape
        hidden_width = w_up.shape[2]
        chunk_cols = width // 2
        hid_1, normed, pre_act, activated, grad_top, grad_top_b, small = forward_pass(
            tokens, upstream, norm_gain, w_up, bias_up, w_down, bias_down, width)
        gathered, small, parts = backward_pass(
            (tokens, hid_1), (normed, pre_act, activated), grad_top, grad_top_b, norm_gain, w_up, w_down, small, axis, chunk_cols)
        return full_gradients(gathered, parts, small, num_layers, width, hidden_width, chunk_cols, axis, mesh.size)

    row_spec = P(axis, None)
    full_spec = P()
    return jax.shard_map(
        device_grads,
        mesh=mesh,
        in_specs=(row_spec, row_spec, full_spec, full_spec, full_spec, full_spec, full_spec),
        out_specs=(full_spec, full_spec, full_spec, full_spec, full_spec),
        check_vma=False,
    )
```

```python
import functools

import jax
import jax.numpy as jnp
from jax import lax
from jax.experimental import pallas as pl
from jax.experimental.pallas import tpu as pltpu
from jax.sharding import PartitionSpec as P


EPSILON = 1e-6
FEATURE_DIMS = (((1,), (1,)), ((), ()))
MESH = pl.DeviceIdType.MESH
COLORS = 3
CORE, DIM_X, DIM_Y, DIM_Z = range(4)
COLOR_DIMS = ((DIM_X, DIM_Y, DIM_Z), (DIM_Y, DIM_Z, DIM_X), (DIM_Z, DIM_X, DIM_Y))
PIPELINE = (
    ("load", 0), ("compute_sent", 0), ("share_core", 0), ("send_3", 2), ("send_back_2", 4), ("send_back_1", 5),
    ("compute_kept", 0), ("send_back_core", 6), ("load_weights", 0), ("backward_0", 0), ("send_2", 1), ("backward_1", 0),
    ("send_1", 0), ("backward_2", 0), ("send_back_3", 2), ("store", 6), ("input_grad", 0),
)
MAX_LAG = 6
PART_GROUPS = (7, 5, 2, 3, 3)
WIDEN_CALLS = (8, 4)
RECV_SLOTS = 2
KEPT_SLOTS = 3
GATHER_SLOTS = 6
TILE = 256
UP_COLS = 512
ACT_ROWS = 16
ACT_COLS = 256
STREAM_SLOTS = 4
NORM_ROWS = 128
GELU_SCALE = 0.7978845608028654
GELU_CUBIC = 0.044715


def inverse_rms(hid_f):
    return lax.rsqrt(jnp.mean(hid_f * hid_f, axis=-1, keepdims=True) + EPSILON)


def gelu(values):
    return (0.5 * values) * (1.0 + jnp.tanh(values * (GELU_SCALE + GELU_SCALE * GELU_CUBIC * (values * values))))


def forward_kernel(
    sizes, tokens, upstream, w_up, w_down, gain_in, bias_up_in, bias_down_in, hid_out, normed_out, pre_act_out, act_out,
    grad_top_out, grad_top_b_out, small_out, hid, normed, branch, up_buf, down_buf, pre_buf, act_buf, up_rows, grad_b_buf,
    gain, bias_up, bias_down, io_sem, up_sem, down_sem, pre_sem, act_sem,
):
    num_layers, num_tiles, tile_cols = sizes
    num_tokens, row_dim = hid.shape
    steps = num_tiles + 1
    parts = tile_cols // UP_COLS

    def up_load(layer, tile):
        cols = pl.ds(pl.multiple_of(tile * tile_cols, 128), tile_cols)
        return pltpu.make_async_copy(w_up.at[layer, :, cols], up_buf.at[tile % 2], up_sem.at[tile % 2])

    def down_load(layer, tile):
        rows = pl.ds(pl.multiple_of(tile * tile_cols, 128), tile_cols)
        return pltpu.make_async_copy(w_down.at[layer, rows, :], down_buf.at[tile % 2], down_sem.at[tile % 2])

    def pre_store(layer, tile):
        cols = pl.ds(pl.multiple_of(tile * tile_cols, 128), tile_cols)
        return pltpu.make_async_copy(pre_buf.at[tile % 2], pre_act_out.at[layer, :, cols], pre_sem.at[tile % 2])

    def act_store(layer, tile):
        cols = pl.ds(pl.multiple_of(tile * tile_cols, 128), tile_cols)
        return pltpu.make_async_copy(act_buf.at[tile % 2], act_out.at[layer, :, cols], act_sem.at[tile % 2])

    def normed_store(layer):
        return pltpu.make_async_copy(normed, normed_out.at[layer], io_sem.at[1])

    def hid_store():
        return pltpu.make_async_copy(hid, hid_out, io_sem.at[2])

    tokens_load = pltpu.make_async_copy(tokens, hid, io_sem.at[0])
    tokens_load.start()
    up_load(0, 0).start()
    upstream_load = pltpu.make_async_copy(upstream, up_rows, io_sem.at[3])
    small_out[...] = jnp.zeros_like(small_out)
    pre_buf[0, :, :UP_COLS] = jnp.zeros((num_tokens, UP_COLS), jnp.bfloat16)
    gain[...] = gain_in[...].astype(jnp.float32)
    bias_up[...] = bias_up_in[...].astype(jnp.float32)
    bias_down[...] = bias_down_in[...].astype(jnp.float32)
    tokens_load.wait()

    def each_block(action):
        @pl.loop(0, num_tokens // NORM_ROWS)
        def _(block):
            action(pl.ds(pl.multiple_of(block * NORM_ROWS, NORM_ROWS), NORM_ROWS))

    def normalize(layer, rows, hid_f):
        normed[rows, :] = ((hid_f * inverse_rms(hid_f)) * gain[pl.ds(layer, 1), :]).astype(jnp.bfloat16)

    def next_rows(layer, rows):
        new = ((hid[rows, :].astype(jnp.float32) + branch[rows, :]) + bias_down[pl.ds(layer, 1), :]).astype(jnp.bfloat16)
        hid[rows, :] = new
        return new.astype(jnp.float32)

    def activate(slot, part):
        start = part * UP_COLS
        for row in range(0, num_tokens, ACT_ROWS):
            for col in range(0, UP_COLS, ACT_COLS):
                piece = (slot, pl.ds(row, ACT_ROWS), pl.ds(pl.multiple_of(start + col, 128), ACT_COLS))
                act_buf[piece] = gelu(pre_buf[piece].astype(jnp.float32)).astype(jnp.bfloat16)

    def up_product(layer, tile):
        @pl.loop(0, parts)
        def _(part):
            fresh = tile * parts + part == 0
            last_slot = jnp.where((part == 0) & (tile > 0), (tile + 1) % 2, tile % 2)
            activate(last_slot, jnp.where(fresh, 0, (part + parts - 1) % parts))
            cols = pl.ds(pl.multiple_of(part * UP_COLS, 128), UP_COLS)
            bias = bias_up[pl.ds(layer, 1), pl.ds(pl.multiple_of(tile * tile_cols + part * UP_COLS, 128), UP_COLS)]
            pre_buf[tile % 2, :, cols] = (
                jnp.dot(normed[...], up_buf[tile % 2, :, cols], preferred_element_type=jnp.float32) + bias
            ).astype(jnp.bfloat16)

    def down_product(tile):
        slot = tile % 2

        def product(cols):
            return jnp.dot(act_buf[slot], down_buf[slot, :, cols], preferred_element_type=jnp.float32)

        all_cols = [slice(start, start + UP_COLS) for start in range(0, row_dim, UP_COLS)]

        @pl.when(tile == 0)
        def _():
            for cols in all_cols:
                branch[:, cols] = product(cols)

        @pl.when(tile > 0)
        def _():
            for cols in all_cols:
                branch[:, cols] += product(cols)

    each_block(lambda rows: normalize(0, rows, hid[rows, :].astype(jnp.float32)))

    @pl.loop(0, num_layers * steps)
    def _(step):
        layer, tile = step // steps, step % steps

        @pl.when(tile < num_tiles)
        def _():
            up_load(layer, tile).wait()

            @pl.when(tile + 1 < num_tiles)
            def _():
                up_load(layer, tile + 1).start()

            @pl.when((tile == num_tiles - 1) & (layer + 1 < num_layers))
            def _():
                up_load(layer + 1, 0).start()

            @pl.when(step == 0)
            def _():
                normed_store(0).start()
                down_load(0, 0).start()
                upstream_load.start()

            @pl.when(tile > 1)
            def _():
                pre_store(layer, tile - 2).wait()
                act_store(layer, tile - 2).wait()

            up_product(layer, tile)
            pre_store(layer, tile).start()

        @pl.when(tile == num_tiles)
        def _():
            activate((num_tiles - 1) % 2, parts - 1)

        @pl.when(tile > 0)
        def _():
            act_store(layer, tile - 1).start()
            down_load(layer, tile - 1).wait()

            @pl.when(tile < num_tiles)
            def _():
                down_load(layer, tile).start()

            @pl.when((tile == num_tiles) & (layer + 1 < num_layers))
            def _():
                down_load(layer + 1, 0).start()

            down_product(tile - 1)

        @pl.when(tile == num_tiles)
        def _():
            for back in (2, 1):
                pre_store(layer, num_tiles - back).wait()
                act_store(layer, num_tiles - back).wait()
            normed_store(layer).wait()

            @pl.when(layer + 1 < num_layers)
            def _():
                def to_next(rows):
                    normalize(layer + 1, rows, next_rows(layer, rows))

                each_block(to_next)
                hid_store().start()
                normed_store(layer + 1).start()

    hid_store().wait()
    upstream_load.wait()
    bias_start = small_out.shape[1] - row_dim

    def grad_stores(rows):
        return (
            pltpu.make_async_copy(branch.at[rows, :], grad_top_out.at[rows, :], io_sem.at[0]),
            pltpu.make_async_copy(grad_b_buf.at[rows, :], grad_top_b_out.at[rows, :], io_sem.at[1]),
        )

    def top_rows(rows):
        top_f = next_rows(num_layers - 1, rows)
        top_scale = inverse_rms(top_f)
        top_hat = top_f * top_scale
        up_f = up_rows[rows, :].astype(jnp.float32)
        grad = top_scale * (up_f - top_hat * jnp.mean(up_f * top_hat, axis=-1, keepdims=True))
        branch[rows, :] = grad
        grad_b_buf[rows, :] = grad.astype(jnp.bfloat16)
        small_out[num_layers - 1:, bias_start:] += jnp.sum(grad, axis=0, keepdims=True)

    num_blocks = num_tokens // NORM_ROWS

    def store_block(block):
        for copy in grad_stores(pl.ds(pl.multiple_of(block * NORM_ROWS, NORM_ROWS), NORM_ROWS)):
            copy.start()

    @pl.loop(0, num_blocks)
    def _(block):
        top_rows(pl.ds(pl.multiple_of(block * NORM_ROWS, NORM_ROWS), NORM_ROWS))
        pl.when(block > 0)(lambda: store_block(block - 1))

    store_block(num_blocks - 1)
    for copy in grad_stores(pl.ds(0, num_tokens)):
        copy.wait()


def forward_pass(tokens, upstream, norm_gain, w_up, bias_up, w_down, bias_down, tile_cols):
    num_tokens, row_dim = tokens.shape
    num_layers, _, hidden = w_up.shape
    bf16, f32 = jnp.bfloat16, jnp.float32
    dma = pltpu.SemaphoreType.DMA
    any_spec = pl.BlockSpec(memory_space=pl.ANY)
    vmem_spec = pl.BlockSpec(memory_space=pltpu.VMEM)
    rows = (num_tokens, row_dim)
    wide = (num_layers, num_tokens, hidden)
    return pl.pallas_call(
        functools.partial(forward_kernel, (num_layers, hidden // tile_cols, tile_cols)),
        out_shape=(
            jax.ShapeDtypeStruct(rows, bf16),
            jax.ShapeDtypeStruct((num_layers,) + rows, bf16),
            jax.ShapeDtypeStruct(wide, bf16),
            jax.ShapeDtypeStruct(wide, bf16),
            jax.ShapeDtypeStruct(rows, f32),
            jax.ShapeDtypeStruct(rows, bf16),
            jax.ShapeDtypeStruct((num_layers, 2 * row_dim + hidden), f32),
        ),
        in_specs=[any_spec] * 4 + [vmem_spec] * 3,
        out_specs=(any_spec,) * 6 + (vmem_spec,),
        scratch_shapes=[
            pltpu.VMEM(rows, bf16),
            pltpu.VMEM(rows, bf16),
            pltpu.VMEM(rows, f32),
            pltpu.VMEM((2, row_dim, tile_cols), bf16),
            pltpu.VMEM((2, tile_cols, row_dim), bf16),
            pltpu.VMEM((2, num_tokens, tile_cols), bf16),
            pltpu.VMEM((2, num_tokens, tile_cols), bf16),
            pltpu.VMEM(rows, bf16),
            pltpu.VMEM(rows, bf16),
            pltpu.VMEM((num_layers, row_dim), f32),
            pltpu.VMEM((num_layers, hidden), f32),
            pltpu.VMEM((num_layers, row_dim), f32),
            dma((4,)), dma((2,)), dma((2,)), dma((2,)), dma((2,)),
        ],
        compiler_params=pltpu.CompilerParams(vmem_limit_bytes=60 * 2**20),
        name="forward",
    )(tokens, upstream, w_up, w_down, norm_gain, bias_up, bias_down)


def gelu_slope(values):
    square = values * values
    bend = jnp.tanh(values * (GELU_SCALE + GELU_SCALE * GELU_CUBIC * square))
    return 0.5 * (1.0 + bend) + (0.5 * values) * (1.0 - bend * bend) * (GELU_SCALE + 3.0 * GELU_SCALE * GELU_CUBIC * square)


def backward_kernel(sizes, *refs):
    num_layers, chunks_per_mat, row_dim, chunk_cols, region, down_subs, axis = sizes
    num_mats = 2 * num_layers
    hidden_dim = chunks_per_mat * chunk_cols
    hid_refs, refs = refs[:num_layers], refs[num_layers:]
    (normed, pre_act, activated, grad_top, grad_top_b, w_up, w_down, gain_in, small_in,
     gathered, small_out, grad_pre_hbm, grad_b_hbm) = refs[:13]
    part_count = 2 * COLORS * len(PART_GROUPS)
    part_refs, refs = refs[13:13 + part_count], refs[13 + part_count:]
    (rows_buf, turned, cols_buf, sent_core, kept, recv_core, sent_1, sent_2, sent_3, recv_1, recv_2, recv_3, ring,
     weight_buf, pre_buf, grad_pre_buf, grad_b, grad_normed, hid_buf, grad_buf,
     small_recv, load_sem, grad_pre_sem, norm_sem, grad_b_sem, core_send, core_recv, out_send, out_recv, back_send, back_recv,
     share_send, share_recv, store_sem, small_send_sem, small_recv_sem, part_sem) = refs
    num_chunks = num_mats * chunks_per_mat
    full_chunks = num_chunks - sum(PART_GROUPS)
    half = COLORS * region
    me = lax.axis_index(axis)
    bits = [me % 2, (me // 2) % 2, (me // 4) % 2, me // 8]
    partners = [me + (1 << d) - 2 * (1 << d) * bits[d] for d in range(4)]
    core = bits[CORE]
    sent_bufs, recv_bufs = (sent_1, sent_2, sent_3), (recv_1, recv_2, recv_3)
    spans = (region // 2, region // 4, region // 8)

    def base(color, level):
        total = 0
        for step in range(level):
            total = total + bits[COLOR_DIMS[color][step]] * spans[step]
        return total

    def other(color, level):
        return base(color, level) + (1 - bits[COLOR_DIMS[color][level]]) * spans[level]

    def rows_at(start, size):
        return pl.ds(pl.multiple_of(start, spans[2]), size)

    def rows_loads(mat, chunk):
        layer = num_layers - 1 - mat // 2
        copies = []
        for order, which_core in enumerate((1 - core, core)):
            cols = pl.ds(pl.multiple_of(which_core * half, 128), half)
            if mat % 2 == 0:
                start = ((chunk % chunks_per_mat) // down_subs) * row_dim + which_core * half
                source = activated.at[layer, :, pl.ds(pl.multiple_of(start, 128), half)]
            else:
                source = normed.at[layer, :, cols]
            copies.append(pltpu.make_async_copy(source, rows_buf.at[:, cols], load_sem.at[0, order]))
        return copies

    def weight_loads(mat, chunk):
        slot = chunk % 2
        layer = num_layers - 1 - mat // 2
        cols = pl.ds(pl.multiple_of((chunk % chunks_per_mat) * chunk_cols, 128), chunk_cols)
        if mat % 2 == 0:
            return [
                pltpu.make_async_copy(w_down.at[layer, cols, :], weight_buf.at[slot], load_sem.at[1, slot]),
                pltpu.make_async_copy(pre_act.at[layer, :, cols], pre_buf.at[slot], load_sem.at[2, slot]),
            ]
        return [
            pltpu.make_async_copy(
                w_up.at[layer, part * chunk_cols:(part + 1) * chunk_cols, cols],
                weight_buf.at[slot, :, part * chunk_cols:(part + 1) * chunk_cols], load_sem.at[1 + part, slot])
            for part in range(down_subs)
        ]

    def cols_load(mat, chunk):
        sub = chunk % chunks_per_mat
        if mat % 2 == 0:
            source = grad_top_b if mat == 0 else grad_b_hbm
            source = source.at[:, pl.ds(pl.multiple_of((sub % down_subs) * chunk_cols, 128), chunk_cols)]
        else:
            source = grad_pre_hbm.at[sub]
        return pltpu.make_async_copy(source, cols_buf.at[chunk % 2], load_sem.at[3, chunk % 2])

    def for_mat(chunk, action):
        for mat in range(num_mats):
            @pl.when(chunk // chunks_per_mat == mat)
            def _(mat=mat):
                action(mat)

    def grad_pre_store(sub):
        return pltpu.make_async_copy(grad_pre_buf, grad_pre_hbm.at[sub], grad_pre_sem)

    def core_copy(chunk):
        slot = chunk % RECV_SLOTS
        return pltpu.make_async_remote_copy(
            src_ref=sent_core, dst_ref=recv_core.at[slot], send_sem=core_send, recv_sem=core_recv.at[slot],
            device_id=(partners[CORE],), device_id_type=MESH)

    def out_copy(level, color, chunk):
        slot = chunk % RECV_SLOTS
        return pltpu.make_async_remote_copy(
            src_ref=sent_bufs[level].at[color], dst_ref=recv_bufs[level].at[slot, color],
            send_sem=out_send.at[level, color], recv_sem=out_recv.at[level, color, slot],
            device_id=(partners[COLOR_DIMS[color][level]],), device_id_type=MESH)

    def back_copy(level, color, chunk, arriving):
        slot = chunk % GATHER_SLOTS
        mine = ring.at[slot, core, color, rows_at(base(color, level + 1), spans[level]), :]
        theirs = ring.at[slot, core, color, rows_at(other(color, level), spans[level]), :]
        return pltpu.make_async_remote_copy(
            src_ref=mine, dst_ref=theirs if arriving else mine,
            send_sem=back_send.at[level, color, slot], recv_sem=back_recv.at[level, color, slot],
            device_id=(partners[COLOR_DIMS[color][level]],), device_id_type=MESH)

    def part_rows(color):
        return rows_at(base(color, 1), spans[0])

    def part_share_copy(color, chunk, arriving):
        slot = chunk % GATHER_SLOTS
        mine = ring.at[slot, core, color, part_rows(color), :]
        theirs = ring.at[slot, 1 - core, color, part_rows(color), :]
        return pltpu.make_async_remote_copy(
            src_ref=mine, dst_ref=theirs if arriving else mine,
            send_sem=back_send.at[0, color, slot], recv_sem=back_recv.at[0, color, slot],
            device_id=(partners[CORE],), device_id_type=MESH)

    def part_stores(group, chunk, which_parts=(0, 1)):
        slot = chunk % GATHER_SLOTS
        place = chunk - full_chunks - sum(PART_GROUPS[:group])
        copies = []
        for color in range(COLORS):
            for which in which_parts:
                out_ref = part_refs[(group * COLORS + color) * 2 + which]
                source = ring.at[slot, core if which == 0 else 1 - core, color, part_rows(color), :]
                copies.append(pltpu.make_async_copy(
                    source, out_ref.at[place], part_sem.at[color, which, slot]))
        return copies

    def share_copy(chunk, arriving):
        slot = chunk % GATHER_SLOTS
        return pltpu.make_async_remote_copy(
            src_ref=ring.at[slot, core], dst_ref=ring.at[slot, 1 - core if arriving else core],
            send_sem=share_send.at[slot], recv_sem=share_recv.at[slot],
            device_id=(partners[CORE],), device_id_type=MESH)

    def store_copy(chunk):
        slot = chunk % GATHER_SLOTS
        return pltpu.make_async_copy(ring.at[slot], gathered.at[chunk], store_sem.at[slot])

    def small_copy(step):
        return pltpu.make_async_remote_copy(
            src_ref=small_out, dst_ref=small_recv.at[step], send_sem=small_send_sem.at[step],
            recv_sem=small_recv_sem.at[step], device_id=(partners[step],), device_id_type=MESH)

    def product(chunk, which_core):
        rows = pl.ds(pl.multiple_of(which_core * half, 128), half)
        return jnp.dot(turned[rows, :], cols_buf[chunk % 2], preferred_element_type=jnp.float32)

    def opens_layer(chunk):
        return (chunk > 0) & (chunk % (2 * chunks_per_mat) == 0)

    def opens_rows(chunk):
        down = (chunk // chunks_per_mat) % 2 == 0
        return (chunk % chunks_per_mat == 0) | (down & (chunk % down_subs == 0))

    def turn_rows(chunk, order):
        @pl.when(opens_rows(chunk))
        def _():
            rows_loads(1, chunk)[order].wait()
            first = (1 - core if order == 0 else core) * half
            for start in range(0, half, TILE):
                cols = pl.ds(pl.multiple_of(first + start, 128), TILE)
                turned[cols, :] = rows_buf[:, cols].T

    def next_rows_loads(chunk):
        down = (chunk // chunks_per_mat) % 2 == 0
        for period, here in ((down_subs, down), (chunks_per_mat, jnp.logical_not(down))):
            following = chunk + period

            @pl.when(opens_rows(chunk) & here & (following < num_chunks))
            def _(following=following):
                def start(mat):
                    for copy in rows_loads(mat, following):
                        copy.start()

                for_mat(following, start)

    def load(chunk):
        for_mat(chunk, lambda mat: cols_load(mat, chunk).wait())
        turn_rows(chunk, 0)
        after = chunk + 1

        @pl.when(chunk == 0)
        def _():
            grad_b_copy.start()
            for copy in weight_loads(0, chunk):
                copy.start()

        @pl.when((after < num_chunks) & jnp.logical_not(opens_layer(after)))
        def _():
            for_mat(after, lambda mat: cols_load(mat, after).start())

    def load_weights(chunk):
        def arrive(mat):
            for copy in weight_loads(mat, chunk):
                copy.wait()

        for_mat(chunk, arrive)
        after, before = chunk + 1, chunk - 1

        @pl.when(chunk == 0)
        def _():
            grad_b_copy.wait()

        @pl.when(after < num_chunks)
        def _():
            def start(mat):
                for copy in weight_loads(mat, after):
                    copy.start()

            for_mat(after, start)

        @pl.when((before >= 0) & ((before // chunks_per_mat) % 2 == 0))
        def _():
            grad_pre_store(before % chunks_per_mat).wait()

    def compute_sent(chunk):
        value = product(chunk, 1 - core).astype(jnp.bfloat16)
        for color in range(COLORS):
            sent_core[color] = value[color * region:(color + 1) * region]

    def share_core(chunk):
        core_copy(chunk).start()

    def compute_kept(chunk):
        turn_rows(chunk, 1)
        next_rows_loads(chunk)
        value = product(chunk, core)
        for color in range(COLORS):
            kept[chunk % KEPT_SLOTS, color] = value[color * region:(color + 1) * region]

    def halve(level, chunk, arrived):
        slot = chunk % KEPT_SLOTS
        recv_slot = chunk % RECV_SLOTS
        for color in range(COLORS):
            if level > 0:
                out_copy(level - 1, color, chunk).wait()
            held = base(color, level)

            def total(start, size, color=color, held=held):
                own = kept[slot, color, rows_at(start, size), :]
                return own + arrived[recv_slot, color, rows_at(start - held, size), :].astype(jnp.float32)

            if level < 3:
                mine = base(color, level + 1)
                sent_bufs[level][color] = total(other(color, level), spans[level]).astype(jnp.bfloat16)
                kept[slot, color, rows_at(mine, spans[level]), :] = total(mine, spans[level])
                out_copy(level, color, chunk).start()
            else:
                gather_slot = chunk % GATHER_SLOTS
                ring[gather_slot, core, color, rows_at(held, spans[2]), :] = total(held, spans[2]).astype(jnp.bfloat16)
                back_copy(2, color, chunk, False).start()

    def send_1(chunk):
        core_copy(chunk).wait()
        halve(0, chunk, recv_core)

    def send_2(chunk):
        halve(1, chunk, recv_1)

    def send_3(chunk):
        halve(2, chunk, recv_2)

    def send_back_3(chunk):
        halve(3, chunk, recv_3)

    def pass_back(level, chunk):
        for color in range(COLORS):
            back_copy(level + 1, color, chunk, True).wait()
            back_copy(level, color, chunk, False).start()

    def send_back_2(chunk):
        pass_back(1, chunk)

    def send_back_1(chunk):
        @pl.when(chunk < full_chunks)
        def _():
            pass_back(0, chunk)

        @pl.when(chunk >= full_chunks)
        def _():
            for color in range(COLORS):
                back_copy(1, color, chunk, True).wait()
                part_share_copy(color, chunk, False).start()

        start_part_stores(chunk, (0,))

    def start_part_stores(chunk, which_parts):
        for group, size in enumerate(PART_GROUPS):
            first = full_chunks + sum(PART_GROUPS[:group])

            @pl.when((chunk >= first) & (chunk < first + size))
            def _(group=group):
                for copy in part_stores(group, chunk, which_parts):
                    copy.start()

    def send_back_core(chunk):
        @pl.when(chunk < full_chunks)
        def _():
            for color in range(COLORS):
                back_copy(0, color, chunk, True).wait()
            share_copy(chunk, False).start()

        @pl.when(chunk >= full_chunks)
        def _():
            for color in range(COLORS):
                part_share_copy(color, chunk, True).wait()

        start_part_stores(chunk, (1,))

    def store(chunk):
        @pl.when(chunk < full_chunks)
        def _():
            share_copy(chunk, True).wait()
            store_copy(chunk).start()

        @pl.when((chunk > 0) & (chunk <= full_chunks))
        def _():
            store_copy(chunk - 1).wait()

        for group, size in enumerate(PART_GROUPS):
            first = full_chunks + sum(PART_GROUPS[:group])

            @pl.when((chunk >= first) & (chunk < first + size))
            def _(group=group):
                for copy in part_stores(group, chunk):
                    copy.wait()

    def backward(part, chunk):
        slot = chunk % 2
        sub = chunk % chunks_per_mat
        mat = chunk // chunks_per_mat
        layer = num_layers - 1 - mat // 2

        @pl.when(mat % 2 == 0)
        def _():
            cols = slice(part * TILE, (part + 1) * TILE)

            grad_act = lax.dot_general(
                grad_b[...], weight_buf[slot, cols, :], FEATURE_DIMS, preferred_element_type=jnp.float32)
            grad_pre = grad_act * gelu_slope(pre_buf[slot, :, cols].astype(jnp.float32))
            grad_pre_buf[:, cols] = grad_pre.astype(jnp.bfloat16)
            start = row_dim + sub * chunk_cols + part * TILE
            small_out[pl.ds(layer, 1), pl.ds(pl.multiple_of(start, 128), TILE)] += jnp.sum(grad_pre, axis=0, keepdims=True)

            if part == chunk_cols // TILE - 1:
                grad_pre_store(sub).start()

        @pl.when(mat % 2 == 1)
        def _():
            pieces = row_dim // chunk_cols * (chunk_cols // TILE) // 3
            grad_rows = []
            for piece in range(part * pieces, (part + 1) * pieces):
                start, first = divmod(piece * TILE, chunk_cols)
                grad_rows.append((piece, lax.dot_general(
                    cols_buf[slot], weight_buf[slot, first:first + TILE, start * chunk_cols:(start + 1) * chunk_cols],
                    FEATURE_DIMS, preferred_element_type=jnp.float32)))
            for piece, value in grad_rows:
                grad_normed[:, piece * TILE:(piece + 1) * TILE] += value

    def norm_loads(layer, block):
        rows = pl.ds(pl.multiple_of(block * NORM_ROWS, NORM_ROWS), NORM_ROWS)
        slot = block % 2
        copies = [pltpu.make_async_copy(hid_refs[layer].at[rows, :], hid_buf.at[slot], norm_sem.at[0, slot])]
        if layer > 0:
            copies.append(pltpu.make_async_copy(grad_top.at[rows, :], grad_buf.at[slot], norm_sem.at[1, slot]))
        return copies

    def layer_input_grad(layer):
        num_blocks = grad_b.shape[0] // NORM_ROWS
        for copy in norm_loads(layer, 0):
            copy.start()

        @pl.loop(0, num_blocks)
        def _(block):
            @pl.when(block + 1 < num_blocks)
            def _():
                for copy in norm_loads(layer, block + 1):
                    copy.start()

            for copy in norm_loads(layer, block):
                copy.wait()
            rows = pl.ds(pl.multiple_of(block * NORM_ROWS, NORM_ROWS), NORM_ROWS)
            hid_f = hid_buf[block % 2].astype(jnp.float32)
            hid_scale = inverse_rms(hid_f)
            hid_hat = hid_f * hid_scale
            normed_grad = grad_normed[rows, :]
            small_out[layer:layer + 1, :row_dim] += jnp.sum(normed_grad * hid_hat, axis=0, keepdims=True)
            if layer > 0:
                grad_normed[rows, :] = jnp.zeros((NORM_ROWS, row_dim), jnp.float32)
                grad_hat = normed_grad * gain_in[layer:layer + 1, :].astype(jnp.float32)
                grad_new = grad_buf[block % 2] + hid_scale * (
                    grad_hat - hid_hat * jnp.mean(grad_hat * hid_hat, axis=-1, keepdims=True))
                grad_b[rows, :] = grad_new.astype(jnp.bfloat16)
                small_out[layer - 1:layer, row_dim + hidden_dim:] += jnp.sum(grad_new, axis=0, keepdims=True)

        if layer > 0:
            copy = pltpu.make_async_copy(grad_b, grad_b_hbm, grad_b_sem)
            copy.start()
            copy.wait()
            following = jnp.int32((num_layers - layer) * 2 * chunks_per_mat)
            cols_load((num_layers - layer) * 2, following).start()

    def input_grad(chunk):
        for layer in range(num_layers):
            last = (num_layers - 1 - layer) * 2 * chunks_per_mat + 2 * chunks_per_mat - 1

            @pl.when(chunk == last)
            def _(layer=layer):
                layer_input_grad(layer)

    events = dict(
        load=load, load_weights=load_weights, compute_sent=compute_sent, share_core=share_core, compute_kept=compute_kept, send_1=send_1, send_2=send_2, send_3=send_3,
        send_back_3=send_back_3, send_back_2=send_back_2, send_back_1=send_back_1, send_back_core=send_back_core, store=store,
        backward_0=functools.partial(backward, 0), backward_1=functools.partial(backward, 1),
        backward_2=functools.partial(backward, 2), input_grad=input_grad)

    first = jnp.int32(0)
    other_rows, own_rows = rows_loads(0, first)
    other_rows.start()
    cols_load(0, first).start()
    own_rows.start()
    grad_b_copy = pltpu.make_async_copy(grad_top_b, grad_b, grad_b_sem)
    barrier = pltpu.get_barrier_semaphore()
    for partner in partners:
        pl.semaphore_signal(barrier, inc=1, device_id=(partner,), device_id_type=MESH)
    small_out[...] = small_in[...]
    grad_normed[...] = jnp.zeros_like(grad_normed)
    pl.semaphore_wait(barrier, 4)

    @pl.loop(0, num_chunks + MAX_LAG)
    def _(it):
        for step in range(4):
            @pl.when(it == num_chunks + step)
            def _(step=step):
                small_copy(step).start()
        for name, lag in PIPELINE:
            chunk = it - lag

            @pl.when((chunk >= 0) & (chunk < num_chunks))
            def _(name=name, chunk=chunk):
                events[name](chunk)
        for step in range(4):
            @pl.when(it == num_chunks + step)
            def _(step=step):
                small_copy(step).wait()
                small_out[...] += small_recv[step]


def backward_pass(hid_rows, saved, grad_top, grad_top_b, norm_gain, w_up, w_down, small, axis, chunk_cols):
    num_layers, row_dim, hidden = w_up.shape
    tokens = grad_top.shape[0]
    chunks_per_mat = hidden // chunk_cols
    region = row_dim // (2 * COLORS)
    half = (COLORS, region, chunk_cols)
    sizes = (num_layers, chunks_per_mat, row_dim, chunk_cols, region, row_dim // chunk_cols, axis)
    num_chunks = 2 * num_layers * chunks_per_mat
    bf16, f32 = jnp.bfloat16, jnp.float32
    dma = pltpu.SemaphoreType.DMA
    any_spec = pl.BlockSpec(memory_space=pl.ANY)
    vmem_spec = pl.BlockSpec(memory_space=pltpu.VMEM)
    full_chunks = num_chunks - sum(PART_GROUPS)
    part_shapes = [jax.ShapeDtypeStruct((size, region // 2, chunk_cols), bf16) for size in PART_GROUPS for _ in range(2 * COLORS)]
    gathered, small_sum, _, _, *parts = pl.pallas_call(
        functools.partial(backward_kernel, sizes),
        out_shape=[
            jax.ShapeDtypeStruct((full_chunks, 2) + half, bf16),
            jax.ShapeDtypeStruct(small.shape, f32),
            jax.ShapeDtypeStruct((chunks_per_mat, tokens, chunk_cols), bf16),
            jax.ShapeDtypeStruct((tokens, row_dim), bf16),
        ] + part_shapes,
        in_specs=[any_spec] * (num_layers + 7) + [vmem_spec] * 2,
        out_specs=[any_spec, vmem_spec, any_spec, any_spec] + [any_spec] * len(part_shapes),
        scratch_shapes=[
            pltpu.VMEM((tokens, row_dim), bf16),
            pltpu.VMEM((row_dim, tokens), bf16),
            pltpu.VMEM((2, tokens, chunk_cols), bf16),
            pltpu.VMEM(half, bf16),
            pltpu.VMEM((KEPT_SLOTS,) + half, f32),
            pltpu.VMEM((RECV_SLOTS,) + half, bf16),
            pltpu.VMEM((COLORS, region // 2, chunk_cols), bf16),
            pltpu.VMEM((COLORS, region // 4, chunk_cols), bf16),
            pltpu.VMEM((COLORS, region // 8, chunk_cols), bf16),
            pltpu.VMEM((RECV_SLOTS, COLORS, region // 2, chunk_cols), bf16),
            pltpu.VMEM((RECV_SLOTS, COLORS, region // 4, chunk_cols), bf16),
            pltpu.VMEM((RECV_SLOTS, COLORS, region // 8, chunk_cols), bf16),
            pltpu.VMEM((GATHER_SLOTS, 2) + half, bf16),
            pltpu.VMEM((2, chunk_cols, row_dim), bf16),
            pltpu.VMEM((2, tokens, chunk_cols), bf16),
            pltpu.VMEM((tokens, chunk_cols), bf16),
            pltpu.VMEM((tokens, row_dim), bf16),
            pltpu.VMEM((tokens, row_dim), f32),
            pltpu.VMEM((2, NORM_ROWS, row_dim), bf16),
            pltpu.VMEM((2, NORM_ROWS, row_dim), f32),
            pltpu.VMEM((4,) + small.shape, f32),
            dma((4, 2)), dma, dma((2, 2)), dma,
            dma, dma((RECV_SLOTS,)), dma((3, COLORS)), dma((3, COLORS, RECV_SLOTS)),
            dma((3, COLORS, GATHER_SLOTS)), dma((3, COLORS, GATHER_SLOTS)), dma((GATHER_SLOTS,)), dma((GATHER_SLOTS,)),
            dma((GATHER_SLOTS,)), dma((4,)), dma((4,)), dma((COLORS, 2, GATHER_SLOTS)),
        ],
        compiler_params=pltpu.CompilerParams(collective_id=0, has_side_effects=True, vmem_limit_bytes=67043328),
        name="backward",
    )(*hid_rows, *saved, grad_top, grad_top_b, w_up, w_down, norm_gain, small)
    return gathered, small_sum, parts


def flip_pairs(num_devices, bit):
    return [(dev, dev ^ (1 << bit)) for dev in range(num_devices)]


def stream_blocks(num_blocks, start_loads, wait_loads, store_of, in_buf, out_buf, after_first=None):
    slots, region = in_buf.shape[0], in_buf.shape[2]
    for block in range(min(slots - 1, num_blocks)):
        start_loads(jnp.int32(block), block)

    @pl.loop(0, num_blocks)
    def _(block):
        slot = block % slots

        @pl.when(block + slots - 1 < num_blocks)
        def _():
            start_loads(block + slots - 1, (block + slots - 1) % slots)

        wait_loads(block, slot)

        @pl.when(block >= slots)
        def _():
            store_of(block - slots, slot).wait()

        for color in range(COLORS):
            out_buf[slot, color * region:(color + 1) * region, :] = in_buf[slot, color].astype(jnp.float32)
        store_of(block, slot).start()
        if after_first is not None:
            pl.when(block == 0)(after_first)

    for block in range(max(num_blocks - slots, 0), num_blocks):
        store_of(jnp.int32(block), block % slots).wait()


def block_target(out_ref, layer, kind, down_subs, chunk, which_core, rows, cols):
    half = pl.multiple_of(which_core * rows, rows)
    if kind == 0:
        first = pl.multiple_of((chunk // down_subs) * 2 * rows + half, rows)
        return out_ref.at[layer, pl.ds(first, rows), pl.ds(pl.multiple_of((chunk % down_subs) * cols, 128), cols)]
    return out_ref.at[layer, pl.ds(half, rows), pl.ds(pl.multiple_of(chunk * cols, 128), cols)]


def widen_kernel(spec, *refs):
    first, count, place, layer, kind, down_subs, small_widths, in_place = spec
    if in_place:
        refs = refs[:1 + bool(small_widths)] + refs[2 + bool(small_widths):]
    if small_widths:
        gathered, small, out_ref, *small_outs, in_buf, out_buf, in_sem, out_sem, small_buf, small_sem = refs
        small_load = pltpu.make_async_copy(small, small_buf, small_sem.at[0])
        small_load.start()
        starts = [sum(small_widths[:n]) for n in range(len(small_widths))]
        small_stores = [
            pltpu.make_async_copy(small_buf.at[:, start:start + width], small_out, small_sem.at[1 + n])
            for n, (start, width, small_out) in enumerate(zip(starts, small_widths, small_outs))]
    else:
        gathered, out_ref, in_buf, out_buf, in_sem, out_sem = refs
        small_stores = []

    def after_first():
        if small_stores:
            small_load.wait()
        for copy in small_stores:
            copy.start()

    rows, cols = out_buf.shape[1:]

    def load(block, slot):
        return pltpu.make_async_copy(gathered.at[first + block // 2, block % 2], in_buf.at[slot], in_sem.at[slot])

    def store(block, slot):
        target = block_target(out_ref, layer, kind, down_subs, place + block // 2, block % 2, rows, cols)
        return pltpu.make_async_copy(out_buf.at[slot], target, out_sem.at[slot])

    stream_blocks(
        2 * count, lambda block, slot: load(block, slot).start(), lambda block, slot: load(block, slot).wait(),
        store, in_buf, out_buf, after_first)
    for copy in small_stores:
        copy.wait()


def join_kernel(spec, *refs):
    skip, count, place, layer, kind, down_subs, axis = spec
    parts, (_, out_ref, in_buf, out_buf, in_sem, out_sem) = refs[:4 * COLORS], refs[4 * COLORS:]
    rows, cols = out_buf.shape[1:]
    part_rows = in_buf.shape[2] // 2
    me = lax.axis_index(axis)
    core = me % 2

    def copies(which, chunk, slot):
        found = []
        for color in range(COLORS):
            upper = (me >> COLOR_DIMS[color][0]) & 1
            for far in range(2):
                start = pl.multiple_of((upper if far == 0 else 1 - upper) * part_rows, part_rows)
                found.append(pltpu.make_async_copy(
                    parts[color * 4 + far * 2 + which].at[skip + chunk],
                    in_buf.at[slot, color, pl.ds(start, part_rows), :], in_sem.at[slot]))
        return found

    def start_loads(block, slot):
        for which in range(2):
            @pl.when(block % 2 == which)
            def _(which=which):
                for copy in copies(which, block // 2, slot):
                    copy.start()

    def wait_loads(block, slot):
        for copy in copies(0, block // 2, slot):
            copy.wait()

    def store(block, slot):
        which_core = jnp.where(block % 2 == 0, core, 1 - core)
        target = block_target(out_ref, layer, kind, down_subs, place + block // 2, which_core, rows, cols)
        return pltpu.make_async_copy(out_buf.at[slot], target, out_sem.at[slot])

    stream_blocks(2 * count, start_loads, wait_loads, store, in_buf, out_buf)


def widen_scratch(region, cols):
    return [
        pltpu.VMEM((STREAM_SLOTS, COLORS, region, cols), jnp.bfloat16),
        pltpu.VMEM((STREAM_SLOTS, COLORS * region, cols), jnp.float32),
        pltpu.SemaphoreType.DMA((STREAM_SLOTS,)),
        pltpu.SemaphoreType.DMA((STREAM_SLOTS,)),
    ]


def widen_cost(count, region, cols):
    size = count * 2 * COLORS * region * cols
    return pl.CostEstimate(flops=500 * size, bytes_accessed=6 * size, transcendentals=0)


def widen(gathered, first, count, place, layer, kind, shape, into, down_subs, small, small_widths):
    region, cols = gathered.shape[3:]
    any_spec = pl.BlockSpec(memory_space=pl.ANY)
    smalls = [jax.ShapeDtypeStruct((small.shape[0], width), jnp.float32) for width in small_widths]
    small_scratch = [pltpu.VMEM(small.shape, jnp.float32), pltpu.SemaphoreType.DMA((1 + len(smalls),))] if smalls else []
    return pl.pallas_call(
        functools.partial(widen_kernel, (first, count, place, layer, kind, down_subs, small_widths, into is not None)),
        in_specs=[any_spec] * (1 + bool(smalls) + (into is not None)),
        out_specs=[any_spec] * (1 + len(smalls)),
        out_shape=[jax.ShapeDtypeStruct(shape, jnp.float32)] + smalls,
        input_output_aliases={} if into is None else {1 + bool(smalls): 0},
        scratch_shapes=widen_scratch(region, cols) + small_scratch,
        cost_estimate=widen_cost(count, region, cols),
        compiler_params=pltpu.CompilerParams(vmem_limit_bytes=67043328),
    )(gathered, *([small] if smalls else []), *([] if into is None else [into]))


def split_at_gradients(first, count, per_mat):
    sizes = []
    while count:
        sizes.append(min(count, per_mat - first % per_mat))
        first, count = first + sizes[-1], count - sizes[-1]
    return sizes


def join(parts, skip, count, place, layer, kind, into, down_subs, axis):
    _, part_rows, cols = parts[0].shape
    any_spec = pl.BlockSpec(memory_space=pl.ANY)
    return pl.pallas_call(
        functools.partial(join_kernel, (skip, count, place, layer, kind, down_subs, axis)),
        in_specs=[any_spec] * (len(parts) + 1),
        out_specs=any_spec,
        out_shape=jax.ShapeDtypeStruct(into.shape, jnp.float32),
        scratch_shapes=widen_scratch(2 * part_rows, cols),
        input_output_aliases={len(parts): 0},
        cost_estimate=widen_cost(count, 2 * part_rows, cols),
        compiler_params=pltpu.CompilerParams(vmem_limit_bytes=67043328),
    )(*parts, into)


def swap(array, axis, num_devices, bit):
    return lax.ppermute(array, axis, flip_pairs(num_devices, bit))


def full_gradients(gathered, parts, small, num_layers, row_dim, hidden, chunk_cols, axis, num_devices):
    per_mat = hidden // chunk_cols
    down_subs = row_dim // chunk_cols
    groups = range(len(PART_GROUPS))
    mine = [[parts[(group * COLORS + color) * 2] for color in range(COLORS)] for group in groups]
    theirs = [[parts[(group * COLORS + color) * 2 + 1] for color in range(COLORS)] for group in groups]
    far = [[swap(mine[group][color], axis, num_devices, COLOR_DIMS[color][0])
            for color in range(COLORS)] for group in groups]
    last = num_layers - 1
    full = [None, None]
    shapes = ((num_layers, hidden, row_dim), (num_layers, row_dim, hidden))
    for call, count in enumerate(WIDEN_CALLS):
        first = sum(WIDEN_CALLS[:call])
        kind, place = divmod(first, per_mat)
        small_widths = (row_dim, hidden, row_dim) if call == 0 else ()
        full[kind], *rest = widen(
            gathered, first, count, place, last, kind, shapes[kind], full[kind], down_subs, small, small_widths)
        smalls = rest or smalls
    chunk = 2 * num_layers * per_mat - sum(PART_GROUPS)
    for group in groups:
        pieces = []
        for color in range(COLORS):
            shared = swap(far[group][color], axis, num_devices, CORE)
            pieces += [mine[group][color], theirs[group][color], far[group][color], shared]
        skip = 0
        for count in split_at_gradients(chunk, PART_GROUPS[group], per_mat):
            mat, place = divmod(chunk, per_mat)
            kind, layer = mat % 2, last - mat // 2
            full[kind] = join(pieces, skip, count, place, layer, kind, full[kind], down_subs, axis)
            chunk, skip = chunk + count, skip + count
    return smalls[0], full[1], smalls[1], full[0], smalls[2]


def solution(mesh):
    axis = mesh.axis_names[0]

    def device_grads(tokens, upstream, norm_gain, w_up, bias_up, w_down, bias_down):
        num_layers, width = norm_gain.shape
        hidden_width = w_up.shape[2]
        chunk_cols = width // 2
        hid_1, normed, pre_act, activated, grad_top, grad_top_b, small = forward_pass(
            tokens, upstream, norm_gain, w_up, bias_up, w_down, bias_down, width)
        gathered, small, parts = backward_pass(
            (tokens, hid_1), (normed, pre_act, activated), grad_top, grad_top_b, norm_gain, w_up, w_down, small, axis, chunk_cols)
        return full_gradients(gathered, parts, small, num_layers, width, hidden_width, chunk_cols, axis, mesh.size)

    row_spec = P(axis, None)
    full_spec = P()
    return jax.shard_map(
        device_grads,
        mesh=mesh,
        in_specs=(row_spec, row_spec, full_spec, full_spec, full_spec, full_spec, full_spec),
        out_specs=(full_spec, full_spec, full_spec, full_spec, full_spec),
        check_vma=False,
    )
```
